32 devices in a mesh: ctx: 8 (over z, x), fsdp: 4 (over y, core).
Axes of the slice: x: 2, y: 2, z: 4, core: 2. Of those that a mesh axis runs over, the one named last changes fastest.
Arguments:
- tokens: bfloat16 [4, 1024, 1600], P('fsdp', 'ctx'), may hold values from -40 to 40, as said below
- ln1_gain: bfloat16 [1600], P('fsdp'), may hold values from 0.099609375 to 1.8984375
- ln1_shift: bfloat16 [1600], P('fsdp'), may hold values from -3 to 3
- qkv_weight: bfloat16 [1600, 4800], P('fsdp'), may hold values from -0.15625 to 0.15625
- qv_bias: bfloat16 [3200], P('fsdp'), may hold values from -3 to 3
- out_weight: bfloat16 [1600, 1600], P('fsdp'), may hold values from -1.25 to 1.25
- out_bias: bfloat16 [1600], P('fsdp'), may hold values from -3 to 3
- ln2_gain: bfloat16 [1600], P('fsdp'), may hold values from 0.099609375 to 1.8984375
- ln2_shift: bfloat16 [1600], P('fsdp'), may hold values from -3 to 3
- up_weight: bfloat16 [1600, 6400], P('fsdp'), may hold values from -0.15625 to 0.15625
- up_bias: bfloat16 [6400], P('fsdp'), may hold values from -3 to 3
- down_weight: bfloat16 [6400, 1600], P('fsdp'), may hold values from -0.078125 to 0.078125
- down_bias: bfloat16 [1600], P('fsdp'), may hold values from -3 to 3
- block_table: int32 [8], replicated, may hold values from 0 to 7, each once
- cotangent: bfloat16 [4, 1024, 1600], P('fsdp', 'ctx'), may hold values from -6 to 6
Outputs:
- block_out: float32 [4, 1024, 1600], P('fsdp', 'ctx')
- input_grad: float32 [4, 1024, 1600], P('fsdp', 'ctx')
- ln1_gain_grad: float32 [1600], P('fsdp')
- ln1_shift_grad: float32 [1600], P('fsdp')
- qkv_weight_grad: float32 [1600, 4800], P('fsdp')
- qv_bias_grad: float32 [3200], P('fsdp')
- out_weight_grad: float32 [1600, 1600], P('fsdp')
- out_bias_grad: float32 [1600], P('fsdp')
- ln2_gain_grad: float32 [1600], P('fsdp')
- ln2_shift_grad: float32 [1600], P('fsdp')
- up_weight_grad: float32 [1600, 6400], P('fsdp')
- up_bias_grad: float32 [6400], P('fsdp')
- down_weight_grad: float32 [6400, 1600], P('fsdp')
- down_bias_grad: float32 [1600], P('fsdp')
The draws below stay inside these ranges and needn't reach their ends.
Inputs may be any that keep to these rules, and one draw needn't show every extreme that they name: Device c of ctx holds blocks block_table[c] and 15 - block_table[c] of each of its sequence, in that order; every value appears once. `tokens`: activations of order one.
All inputs are finite; a program needn't handle non-finite values.
Results may differ from the reference program's by a relative error of at most 0.017.
Values may be sent and summed in bfloat16 or wider, within the bound.
A program may use at most 384 MiB of HBM per device.

```python
import math
import jax
import jax.numpy as jnp
from jax import lax

D = 1600
HEADS = 25
HEAD_DIM = 64
FF = 6400
BLK = 64
SEQ = 1024
SEQS = 4
N_CTX = 8


def draw_tokens(key, part):
    key_base, key_rows, key_cols = jax.random.split(key, 3)
    span = math.log(10.0)
    row_scale = jnp.exp(jax.random.uniform(key_rows, (SEQS, SEQ, 1), jnp.float32, -0.5 * span, 0.5 * span))
    col_scale = jnp.exp(jax.random.uniform(key_cols, (1, 1, D), jnp.float32, -0.5 * span, 0.5 * span))
    base = jax.random.normal(key_base, (SEQS, SEQ, D), jnp.float32)
    base = jnp.clip(base, -4.0, 4.0)
    return (base * row_scale * col_scale).astype(jnp.bfloat16)


def levels(stream_key, dims, cuts, smallest, largest):
    loudness, own = 1.0, jax.random.fold_in(stream_key, 6)
    for dim, shards_of in cuts:
        heights = jnp.exp(jax.random.uniform(jax.random.fold_in(own, dim), (shards_of,), jnp.float32, smallest / len(cuts), largest / len(cuts)))
        loudness = loudness * jnp.repeat(heights, dims[dim] // shards_of).reshape([-1 if axis == dim else 1 for axis in range(len(dims))])
    return loudness


def noise(stream_key, extent, scale, limit, cuts=(), held_as=jnp.bfloat16):
    array = scale * jax.random.normal(stream_key, extent, jnp.float32)
    if cuts:
        array = array * levels(stream_key, extent, cuts, -0.22, 0.18)
    return jnp.clip(array, -limit, limit).astype(held_as)


def setup_inputs(seed: int = 0) -> dict:
    streams_of = jax.random.split(jax.random.key(seed), 16)
    tokens = draw_tokens(jax.random.fold_in(streams_of[15], 71), 0)
    ln1_gain = jnp.clip(1.0 + 0.18 * jax.random.normal(streams_of[1], (D,), jnp.float32), 0.099609375, 1.8984375).astype(jnp.bfloat16)
    ln1_shift = noise(streams_of[2], (D,), 0.5, 3.0, ((0, 4),))
    qkv_weight = noise(streams_of[3], (D, 3 * D), D ** -0.5, 0.15625, ((0, 4),))
    qv_bias = noise(streams_of[4], (2 * D,), 0.5, 3.0, ((0, 4),))
    out_weight = noise(streams_of[5], (D, D), (max(16, 16 * D // SEQ)) ** -0.5, 1.25, ((0, 4),))
    out_bias = noise(streams_of[6], (D,), 0.5, 3.0, ((0, 4),))
    ln2_gain = jnp.clip(1.0 + 0.18 * jax.random.normal(streams_of[7], (D,), jnp.float32), 0.099609375, 1.8984375).astype(jnp.bfloat16)
    ln2_shift = noise(streams_of[8], (D,), 0.5, 3.0, ((0, 4),))
    up_weight = noise(streams_of[9], (D, FF), D ** -0.5, 0.15625, ((0, 4),))
    up_bias = noise(streams_of[10], (FF,), 0.5, 3.0, ((0, 4),))
    down_weight = noise(streams_of[11], (FF, D), FF ** -0.5, 0.078125, ((0, 4),))
    down_bias = noise(streams_of[12], (D,), 0.5, 3.0, ((0, 4),))
    block_table = jax.random.permutation(streams_of[13], N_CTX).astype(jnp.int32)
    cotangent = noise(streams_of[14], (SEQS, SEQ, D), 1.0, 6.0, ((0, 4), (1, 8)))
    return {"tokens": tokens, "ln1_gain": ln1_gain, "ln1_shift": ln1_shift, "qkv_weight": qkv_weight, "qv_bias": qv_bias, "out_weight": out_weight, "out_bias": out_bias, "ln2_gain": ln2_gain, "ln2_shift": ln2_shift, "up_weight": up_weight, "up_bias": up_bias, "down_weight": down_weight, "down_bias": down_bias, "block_table": block_table, "cotangent": cotangent}


EPS = 1e-05
SCALE = 0.125
HIGH = lax.Precision.HIGHEST

@jax.custom_vjp
def low(v):
    return lax.optimization_barrier(v.astype(jnp.bfloat16)).astype(jnp.float32)

@jax.custom_vjp
def low_back(v):
    return v

def low_keep(v):
    return (low(v), None)

def low_pass(kept, grad):
    return (grad,)

def back_keep(v):
    return (v, None)

def back_low(kept, grad):
    return (low(grad),)
low.defvjp(low_keep, low_pass)
low_back.defvjp(back_keep, back_low)

def layer_norm(value, gain, shift):
    centre = value - lax.optimization_barrier(jnp.mean(value, axis=-1, keepdims=True))
    spread = lax.optimization_barrier(jnp.mean(centre * centre, axis=-1, keepdims=True))
    return centre * lax.rsqrt(spread + EPS) * gain + shift

def forward(inputs, params, key_place):
    gain1, shift1, w_qkv, b_qv, w_out, b_out, gain2, shift2, w_up, b_up, w_down, b_down = params
    act1 = low(layer_norm(inputs, gain1, shift1))
    projected = jnp.dot(act1, w_qkv, precision=HIGH, preferred_element_type=jnp.float32)
    query = low_back(low(projected[:, :D] + b_qv[:D]))
    keys = low_back(low(projected[:, D:2 * D]))
    values = low_back(low(projected[:, 2 * D:] + b_qv[D:]))
    query3 = query.reshape(SEQ, HEADS, HEAD_DIM)
    keys3 = keys.reshape(SEQ, HEADS, HEAD_DIM)
    values3 = values.reshape(SEQ, HEADS, HEAD_DIM)
    qblock = 8 * BLK
    nblock = SEQ // qblock

    @jax.checkpoint
    def attend(query_part, query_place):
        raw = jnp.einsum('qhd,khd->hqk', query_part, keys3, precision=HIGH)
        scores = low_back(raw * SCALE)
        allowed = key_place[None, None, :] <= query_place[None, :, None]
        expo = jnp.where(allowed, jnp.exp(scores), 0.0)
        total = lax.optimization_barrier(jnp.sum(expo, axis=2))
        numerator = low_back(jnp.einsum('hqk,khd->qhd', low(expo), values3, precision=HIGH))
        return numerator / total.T[:, :, None]

    def attend_pair(parts):
        return attend(parts[0], parts[1])
    attended = lax.map(attend_pair, (query3.reshape(nblock, qblock, HEADS, HEAD_DIM), key_place.reshape(nblock, qblock)))
    attn = low(attended.reshape(SEQ, D))
    mid = inputs + low_back(jnp.dot(attn, w_out, precision=HIGH, preferred_element_type=jnp.float32) + b_out)
    act2 = low(layer_norm(mid, gain2, shift2))
    hidden_in = low_back(jnp.dot(act2, w_up, precision=HIGH, preferred_element_type=jnp.float32) + b_up)
    hidden = low(jax.nn.gelu(hidden_in, approximate=True))
    return mid + low_back(jnp.dot(hidden, w_down, precision=HIGH, preferred_element_type=jnp.float32) + b_down)

def reference(tokens, ln1_gain, ln1_shift, qkv_weight, qv_bias, out_weight, out_bias, ln2_gain, ln2_shift, up_weight, up_bias, down_weight, down_bias, block_table, cotangent):
    within = jnp.arange(2 * BLK).astype(jnp.int32)
    table = block_table.astype(jnp.int32)
    block_of = jnp.where(within[None, :] < BLK, table[:, None], 2 * N_CTX - 1 - table[:, None])
    key_place = (block_of * BLK + within[None, :] % BLK).reshape(-1).astype(jnp.int32)
    params = tuple((p.astype(jnp.float32) for p in (ln1_gain, ln1_shift, qkv_weight, qv_bias, out_weight, out_bias, ln2_gain, ln2_shift, up_weight, up_bias, down_weight, down_bias)))

    def one_sequence(grads, parts):
        seq_in, seq_cot = parts

        def run(value, weights):
            return forward(value, weights, key_place)
        result, backward = jax.vjp(run, seq_in.astype(jnp.float32), params)
        d_input, d_params = backward(seq_cot.astype(jnp.float32))
        summed = tuple((g + d for g, d in zip(grads, d_params)))
        return (summed, (result, d_input))
    zeros = tuple((jnp.zeros_like(p) for p in params))
    grads, (block_out, input_grad) = lax.scan(one_sequence, zeros, (tokens, cotangent))
    return (block_out, input_grad, grads[0], grads[1], grads[2], grads[3], grads[4], grads[5], grads[6], grads[7], grads[8], grads[9], grads[10], grads[11])
```

```python
import functools

import jax
import jax.numpy as jnp
from jax import lax
from jax.experimental import pallas as pl
from jax.experimental.pallas import tpu as pltpu
from jax.sharding import PartitionSpec as P

HEAD_DIM = 64
EPS = 1e-05
SCALE = 0.125
F32 = jnp.float32
BF16 = jnp.bfloat16


def dot(left, right):
    return jnp.dot(left, right, preferred_element_type=F32)


def dot_t(left, right):
    return lax.dot_general(left, right, (((1,), (1,)), ((), ())), preferred_element_type=F32)


def t_dot(left, right):
    return lax.dot_general(left, right, (((0,), (0,)), ((), ())), preferred_element_type=F32)


def ln_stats(value):
    centre = value - jnp.mean(value, axis=-1, keepdims=True)
    spread = jnp.mean(centre * centre, axis=-1, keepdims=True)
    rstd = lax.rsqrt(spread + EPS)
    return centre * rstd, rstd


def ln_back(grad, normed, rstd, gain):
    dn = grad * gain
    first = jnp.mean(dn, axis=-1, keepdims=True)
    second = jnp.mean(dn * normed, axis=-1, keepdims=True)
    return (dn - first - normed * second) * rstd


def attn_fwd_body(slots, qp_ref, kp_ref, q_ref, k_ref, v_ref, attn_ref, o_ref, l_ref):
    allowed = kp_ref[...] <= qp_ref[...]
    for h in range(slots):
        cols = slice(h * HEAD_DIM, (h + 1) * HEAD_DIM)
        raw = dot_t(q_ref[:, cols], k_ref[:, cols])
        e = jnp.where(allowed, jnp.exp(raw * SCALE), 0.0)
        total = jnp.sum(e, axis=1, keepdims=True)
        numer = dot(e.astype(BF16), v_ref[:, cols])
        o = numer / total
        o_ref[:, cols] = o
        attn_ref[:, cols] = o.astype(BF16)
        l_ref[:, h : h + 1] = total


def attn_bwd_body(
    slots, qp_ref, kp_ref, q_ref, k_ref, v_ref, do_ref, o_ref, l_ref, dq_ref, dk_ref, dv_ref, dk_acc, dv_acc
):
    step = pl.program_id(0)

    @pl.when(step == 0)
    def _():
        dk_acc[...] = jnp.zeros_like(dk_acc)
        dv_acc[...] = jnp.zeros_like(dv_acc)

    allowed = kp_ref[...] <= qp_ref[...]
    for h in range(slots):
        cols = slice(h * HEAD_DIM, (h + 1) * HEAD_DIM)
        q = q_ref[:, cols]
        k = k_ref[:, cols]
        v = v_ref[:, cols]
        do = do_ref[:, cols]
        total = l_ref[:, h : h + 1]
        w = (do / total).astype(BF16)
        corr = jnp.sum(do * o_ref[:, cols], axis=1, keepdims=True) / total
        e = jnp.where(allowed, jnp.exp(dot_t(q, k) * SCALE), 0.0)
        de = dot_t(w, v)
        ds = (e * (de - corr)).astype(BF16)
        dq_ref[:, cols] = (dot(ds, k) * SCALE).astype(BF16)
        dk_acc[:, cols] += t_dot(ds, q)
        dv_acc[:, cols] += t_dot(e.astype(BF16), w)

    @pl.when(step == pl.num_programs(0) - 1)
    def _():
        dk_ref[...] = (dk_acc[...] * SCALE).astype(BF16)
        dv_ref[...] = dv_acc[...].astype(BF16)


def attn_specs(rows, wide, slots):
    qb = 256 if rows <= 1024 else 128
    q_spec = pl.BlockSpec((qb, wide), lambda i: (i, 0))
    l_spec = pl.BlockSpec((qb, slots), lambda i: (i, 0))
    all_spec = pl.BlockSpec((rows, wide), lambda i: (0, 0))
    qp_spec = pl.BlockSpec((qb, 1), lambda i: (i, 0))
    kp_spec = pl.BlockSpec((1, rows), lambda i: (0, 0))
    return rows // qb, q_spec, l_spec, all_spec, qp_spec, kp_spec


def attention_fwd(place, q, k, v, slots):
    rows, wide = q.shape
    steps, q_spec, l_spec, all_spec, qp_spec, kp_spec = attn_specs(rows, wide, slots)
    return pl.pallas_call(
        functools.partial(attn_fwd_body, slots),
        grid=(steps,),
        in_specs=[qp_spec, kp_spec, q_spec, all_spec, all_spec],
        out_specs=[q_spec, q_spec, l_spec],
        out_shape=[
            jax.ShapeDtypeStruct((rows, wide), BF16),
            jax.ShapeDtypeStruct((rows, wide), F32),
            jax.ShapeDtypeStruct((rows, slots), F32),
        ],
        name="attn_fwd",
        cost_estimate=pl.CostEstimate(
            flops=4 * rows * rows * wide, bytes_accessed=16 * rows * wide, transcendentals=rows * rows * slots
        ),
        compiler_params=pltpu.CompilerParams(vmem_limit_bytes=60 * 2**20),
    )(place.reshape(rows, 1), place.reshape(1, rows), q, k, v)


def attention_bwd(place, q, k, v, do, o, total, slots):
    rows, wide = q.shape
    steps, q_spec, l_spec, all_spec, qp_spec, kp_spec = attn_specs(rows, wide, slots)
    shape = jax.ShapeDtypeStruct((rows, wide), BF16)
    return pl.pallas_call(
        functools.partial(attn_bwd_body, slots),
        grid=(steps,),
        in_specs=[qp_spec, kp_spec, q_spec, all_spec, all_spec, q_spec, q_spec, l_spec],
        out_specs=[q_spec, all_spec, all_spec],
        out_shape=[shape, shape, shape],
        scratch_shapes=[pltpu.VMEM((rows, wide), F32), pltpu.VMEM((rows, wide), F32)],
        name="attn_bwd",
        cost_estimate=pl.CostEstimate(
            flops=10 * rows * rows * wide, bytes_accessed=24 * rows * wide, transcendentals=rows * rows * slots
        ),
        compiler_params=pltpu.CompilerParams(vmem_limit_bytes=60 * 2**20),
    )(place.reshape(rows, 1), place.reshape(1, rows), q, k, v, do, o, total)


def ag_ctx(value):
    return lax.all_gather(value, "ctx", axis=0, tiled=True)


def rs_ctx(value):
    return lax.psum_scatter(value.astype(BF16), "ctx", scatter_dimension=0, tiled=True)


def ag_fsdp(value):
    return lax.all_gather(value, "fsdp", axis=0, tiled=True)


def rs_fsdp(value):
    return lax.psum_scatter(value.astype(BF16), "fsdp", scatter_dimension=0, tiled=True)


def head_columns(value, width, c, n):
    heads = width // HEAD_DIM
    base, rest = divmod(heads, n)
    parts = []
    if base:
        parts.append(lax.dynamic_slice_in_dim(value, c * base * HEAD_DIM, base * HEAD_DIM, axis=-1))
    if rest:
        start = jnp.minimum(base * n + c, heads - 1) * HEAD_DIM
        extra = lax.dynamic_slice_in_dim(value, start, HEAD_DIM, axis=-1)
        parts.append(jnp.where(c < rest, extra, jnp.zeros_like(extra)))
    return jnp.concatenate(parts, axis=-1)


def spread_heads(value, heads, n):
    base, rest = divmod(heads, n)
    rows = value.shape[1]
    parts = []
    if base:
        body = value[:, :, : base * HEAD_DIM]
        parts.append(jnp.transpose(body, (1, 0, 2)).reshape(rows, n * base * HEAD_DIM))
    if rest:
        tail = value[:rest, :, base * HEAD_DIM :]
        parts.append(jnp.transpose(tail, (1, 0, 2)).reshape(rows, rest * HEAD_DIM))
    return jnp.concatenate(parts, axis=1)


def place_heads(value, heads, c, n):
    base, rest = divmod(heads, n)
    out = jnp.zeros((heads * HEAD_DIM,), value.dtype)
    if rest:
        start = jnp.minimum(base * n + c, heads - 1) * HEAD_DIM
        extra = jnp.where(c < rest, value[base * HEAD_DIM :], 0.0)
        out = lax.dynamic_update_slice(out, extra, (start,))
    if base:
        out = lax.dynamic_update_slice(out, value[: base * HEAD_DIM], (c * base * HEAD_DIM,))
    return out


def head_rows(value, heads, c, f, n):
    base, rest = divmod(heads, n)
    local, width = value.shape
    pad = max(base, 1) * HEAD_DIM
    padded = jnp.pad(value, ((pad, pad), (0, 0)))
    parts = []
    if base:
        start = jnp.clip(c * base * HEAD_DIM - f * local + pad, 0, local + 2 * pad - base * HEAD_DIM)
        parts.append(lax.dynamic_slice_in_dim(padded, start, base * HEAD_DIM, axis=0))
    if rest:
        start = jnp.clip((base * n + c) * HEAD_DIM - f * local + pad, 0, local + 2 * pad - HEAD_DIM)
        extra = lax.dynamic_slice_in_dim(padded, start, HEAD_DIM, axis=0)
        parts.append(jnp.where(c < rest, extra, jnp.zeros_like(extra)))
    return jnp.concatenate(parts, axis=0)


def on_device(
    tokens,
    ln1_gain,
    ln1_shift,
    qkv_weight,
    qv_bias,
    out_weight,
    out_bias,
    ln2_gain,
    ln2_shift,
    up_weight,
    up_bias,
    down_weight,
    down_bias,
    block_table,
    cotangent,
):
    rows, width = tokens.shape[1:]
    heads = width // HEAD_DIM
    n = lax.axis_size("ctx")
    nf = lax.axis_size("fsdp")
    c = lax.axis_index("ctx")
    f = lax.axis_index("fsdp")
    slots = -(-heads // n)
    wide = slots * HEAD_DIM
    half = rows // 2
    local = width // nf
    ff = up_weight.shape[1]
    ff_local = ff // nf
    ff_part = ff_local // n

    within = jnp.arange(rows, dtype=jnp.int32)
    block_of = jnp.where(within[None, :] < half, block_table[:, None], 2 * n - 1 - block_table[:, None])
    place = (block_of * half + within[None, :] % half).reshape(-1)

    vectors = (ln1_gain, ln1_shift, qv_bias, out_bias, ln2_gain, ln2_shift, up_bias, down_bias)
    packed = lax.all_gather(jnp.concatenate(vectors), "fsdp", axis=0, tiled=False)
    full, at = [], 0
    for vector in vectors:
        size = vector.shape[0]
        full.append(packed[:, at : at + size].reshape(-1).astype(F32))
        at += size
    gain1, shift1, b_qv, b_out, gain2, shift2, b_up, b_down = full

    x_all = ag_ctx(tokens[0])
    q_w = head_columns(qkv_weight[:, :width], width, c, n)
    k_w = head_columns(qkv_weight[:, width : 2 * width], width, c, n)
    v_w = head_columns(qkv_weight[:, 2 * width :], width, c, n)
    w_qkv = ag_fsdp(jnp.concatenate([q_w, k_w, v_w], axis=1))
    w_out = lax.psum(head_rows(out_weight, heads, c, f, n), "fsdp")
    g2_all = ag_ctx(cotangent[0])
    up_mine = lax.dynamic_slice_in_dim(up_weight.reshape(local, nf, n, ff_part), c, 1, axis=2)
    w_up = ag_fsdp(up_mine.reshape(local, nf * ff_part))
    w_down = ag_fsdp(lax.dynamic_slice_in_dim(down_weight, c * ff_part, ff_part, axis=0))
    b_up_mine = lax.dynamic_slice_in_dim(b_up.reshape(nf, n, ff_part), c, 1, axis=1).reshape(-1)
    bq = head_columns(b_qv[:width], width, c, n)
    bv = head_columns(b_qv[width:], width, c, n)

    n1_all, _ = ln_stats(x_all.astype(F32))
    act1 = (n1_all * gain1 + shift1).astype(BF16)
    proj = dot(act1, w_qkv)
    q = (proj[:, :wide] + bq).astype(BF16)
    k = proj[:, wide : 2 * wide].astype(BF16)
    v = (proj[:, 2 * wide :] + bv).astype(BF16)
    attn, o, total = attention_fwd(place, q, k, v, slots)
    x = tokens[0].astype(F32)
    mid = x + rs_ctx(dot(attn, w_out)).astype(F32) + b_out
    attn_all = spread_heads(lax.all_gather(attn, "ctx", axis=0, tiled=False), heads, n)

    n2, rstd2 = ln_stats(mid)
    act2 = ag_ctx((n2 * gain2 + shift2).astype(BF16))
    u = dot(act2, w_up) + b_up_mine
    activated, gelu_back = jax.vjp(lambda t: jax.nn.gelu(t, approximate=True), u)
    hidden = activated.astype(BF16)
    dh = dot_t(g2_all, w_down)
    du = gelu_back(dh)[0].astype(BF16)
    da2 = rs_ctx(dot_t(du, w_up)).astype(F32)
    result = mid + rs_ctx(dot(hidden, w_down)).astype(F32) + b_down
    d_down = rs_fsdp(t_dot(hidden, g2_all))
    d_up = rs_fsdp(t_dot(act2, du))
    d_up_bias = jnp.sum(du.astype(F32), axis=0)
    grad_out = cotangent[0].astype(F32)
    d_down_bias = jnp.sum(grad_out, axis=0)
    d_down = lax.all_gather(d_down, "ctx", axis=0, tiled=True)
    d_up = lax.all_gather(d_up, "ctx", axis=0, tiled=False)

    d_gain2 = jnp.sum(da2 * n2, axis=0)
    d_shift2 = jnp.sum(da2, axis=0)
    d_mid = grad_out + ln_back(da2, n2, rstd2, gain2)
    g1 = d_mid.astype(BF16)
    d_out_bias = jnp.sum(g1.astype(F32), axis=0)
    g1_all = ag_ctx(g1)
    d_attn = dot_t(g1_all, w_out)
    gq, gk, gv = attention_bwd(place, q, k, v, d_attn, o, total, slots)
    g_qkv = jnp.concatenate([gq, gk, gv], axis=1)
    da1 = rs_ctx(dot_t(g_qkv, w_qkv)).astype(F32)
    d_qkv = rs_fsdp(t_dot(act1, g_qkv))
    out_part = width // n
    g1_mine = lax.dynamic_slice_in_dim(g1_all, c * out_part, out_part, axis=1)
    d_out = rs_fsdp(t_dot(attn_all, g1_mine))
    gathered = lax.all_gather(jnp.concatenate([d_qkv, d_out], axis=1), "ctx", axis=0, tiled=False)
    d_qkv_full = jnp.concatenate(
        [spread_heads(gathered[:, :, i * wide : (i + 1) * wide], heads, n) for i in range(3)], axis=1
    ).astype(F32)
    d_out_full = jnp.transpose(gathered[:, :, 3 * wide :], (1, 0, 2)).reshape(local, width).astype(F32)
    d_up_full = jnp.transpose(d_up.reshape(n, local, nf, ff_part), (1, 2, 0, 3)).reshape(local, ff).astype(F32)
    d_down_full = d_down.astype(F32)

    n1, rstd1 = ln_stats(x)
    d_gain1 = jnp.sum(da1 * n1, axis=0)
    d_shift1 = jnp.sum(da1, axis=0)
    input_grad = d_mid + ln_back(da1, n1, rstd1, gain1)

    dq_bias = place_heads(jnp.sum(gq.astype(F32), axis=0), heads, c, n)
    dv_bias = place_heads(jnp.sum(gv.astype(F32), axis=0), heads, c, n)
    up_placed = lax.dynamic_update_slice(
        jnp.zeros((nf, n, ff_part), F32), d_up_bias.reshape(nf, 1, ff_part), (0, c, 0)
    )
    smalls = (
        d_gain1,
        d_shift1,
        jnp.concatenate([dq_bias, dv_bias]),
        d_out_bias,
        d_gain2,
        d_shift2,
        up_placed.reshape(-1),
        d_down_bias,
    )
    packed = jnp.concatenate([s.reshape(nf, -1) for s in smalls], axis=1)
    summed = lax.psum(packed, ("ctx", "fsdp"))
    mine = lax.dynamic_slice_in_dim(summed, f, 1, axis=0)[0]
    out, at = [], 0
    for s in smalls:
        size = s.size // nf
        out.append(mine[at : at + size])
        at += size
    return (
        result[None],
        input_grad[None],
        out[0],
        out[1],
        d_qkv_full,
        out[2],
        d_out_full,
        out[3],
        out[4],
        out[5],
        d_up_full,
        out[6],
        d_down_full,
        out[7],
    )


def solution(mesh):
    rows, one, two = P("fsdp", "ctx", None), P("fsdp"), P("fsdp", None)
    return jax.shard_map(
        on_device,
        mesh=mesh,
        in_specs=(rows, one, one, two, one, two, one, one, one, two, one, two, one, P(), rows),
        out_specs=(rows, rows, one, one, two, one, two, one, one, one, two, one, two, one),
        check_vma=False,
    )
```

```python
import functools

import jax
import jax.numpy as jnp
from jax import lax
from jax.experimental import pallas as pl
from jax.experimental.pallas import tpu as pltpu
from jax.sharding import PartitionSpec as P

HEAD_DIM = 64
EPS = 1e-05
SCALE = 0.125
F32 = jnp.float32
BF16 = jnp.bfloat16
MESH = pl.DeviceIdType.MESH


def dot(left, right):
    return jnp.dot(left, right, preferred_element_type=F32)


def dot_t(left, right):
    return lax.dot_general(left, right, (((1,), (1,)), ((), ())), preferred_element_type=F32)


def t_dot(left, right):
    return lax.dot_general(left, right, (((0,), (0,)), ((), ())), preferred_element_type=F32)


def ln_stats(value):
    centre = value - jnp.mean(value, axis=-1, keepdims=True)
    spread = jnp.mean(centre * centre, axis=-1, keepdims=True)
    rstd = lax.rsqrt(spread + EPS)
    return centre * rstd, rstd


def ln_back(grad, normed, rstd, gain):
    dn = grad * gain
    first = jnp.mean(dn, axis=-1, keepdims=True)
    second = jnp.mean(dn * normed, axis=-1, keepdims=True)
    return (dn - first - normed * second) * rstd


def attn_fwd_body(slots, qp_ref, kp_ref, q_ref, k_ref, v_ref, attn_ref, o_ref, l_ref):
    allowed = kp_ref[...] <= qp_ref[...]
    for h in range(slots):
        cols = slice(h * HEAD_DIM, (h + 1) * HEAD_DIM)
        raw = dot_t(q_ref[:, cols], k_ref[:, cols])
        e = jnp.where(allowed, jnp.exp(raw * SCALE), 0.0)
        total = jnp.sum(e, axis=1, keepdims=True)
        numer = dot(e.astype(BF16), v_ref[:, cols])
        o = numer / total
        o_ref[:, cols] = o
        attn_ref[:, cols] = o.astype(BF16)
        l_ref[:, h : h + 1] = total


def attn_bwd_body(
    slots, qp_ref, kp_ref, q_ref, k_ref, v_ref, do_ref, o_ref, l_ref, dq_ref, dk_ref, dv_ref, dk_acc, dv_acc
):
    step = pl.program_id(0)

    @pl.when(step == 0)
    def _():
        dk_acc[...] = jnp.zeros_like(dk_acc)
        dv_acc[...] = jnp.zeros_like(dv_acc)

    allowed = kp_ref[...] <= qp_ref[...]
    for h in range(slots):
        cols = slice(h * HEAD_DIM, (h + 1) * HEAD_DIM)
        q = q_ref[:, cols]
        k = k_ref[:, cols]
        v = v_ref[:, cols]
        do = do_ref[:, cols]
        total = l_ref[:, h : h + 1]
        w = (do / total).astype(BF16)
        corr = jnp.sum(do * o_ref[:, cols], axis=1, keepdims=True) / total
        e = jnp.where(allowed, jnp.exp(dot_t(q, k) * SCALE), 0.0)
        de = dot_t(w, v)
        ds = (e * (de - corr)).astype(BF16)
        dq_ref[:, cols] = (dot(ds, k) * SCALE).astype(BF16)
        dk_acc[:, cols] += t_dot(ds, q)
        dv_acc[:, cols] += t_dot(e.astype(BF16), w)

    @pl.when(step == pl.num_programs(0) - 1)
    def _():
        dk_ref[...] = (dk_acc[...] * SCALE).astype(BF16)
        dv_ref[...] = dv_acc[...].astype(BF16)


def attn_specs(rows, wide, slots):
    qb = 256 if rows <= 1024 else 128
    q_spec = pl.BlockSpec((qb, wide), lambda i: (i, 0))
    l_spec = pl.BlockSpec((qb, slots), lambda i: (i, 0))
    all_spec = pl.BlockSpec((rows, wide), lambda i: (0, 0))
    qp_spec = pl.BlockSpec((qb, 1), lambda i: (i, 0))
    kp_spec = pl.BlockSpec((1, rows), lambda i: (0, 0))
    return rows // qb, q_spec, l_spec, all_spec, qp_spec, kp_spec


def attention_fwd(place, q, k, v, slots):
    rows, wide = q.shape
    steps, q_spec, l_spec, all_spec, qp_spec, kp_spec = attn_specs(rows, wide, slots)
    return pl.pallas_call(
        functools.partial(attn_fwd_body, slots),
        grid=(steps,),
        in_specs=[qp_spec, kp_spec, q_spec, all_spec, all_spec],
        out_specs=[q_spec, q_spec, l_spec],
        out_shape=[
            jax.ShapeDtypeStruct((rows, wide), BF16),
            jax.ShapeDtypeStruct((rows, wide), F32),
            jax.ShapeDtypeStruct((rows, slots), F32),
        ],
        name="attn_fwd",
        cost_estimate=pl.CostEstimate(
            flops=4 * rows * rows * wide, bytes_accessed=16 * rows * wide, transcendentals=rows * rows * slots
        ),
        compiler_params=pltpu.CompilerParams(vmem_limit_bytes=60 * 2**20),
    )(place.reshape(rows, 1), place.reshape(1, rows), q, k, v)


def attention_bwd(place, q, k, v, do, o, total, slots):
    rows, wide = q.shape
    steps, q_spec, l_spec, all_spec, qp_spec, kp_spec = attn_specs(rows, wide, slots)
    shape = jax.ShapeDtypeStruct((rows, wide), BF16)
    return pl.pallas_call(
        functools.partial(attn_bwd_body, slots),
        grid=(steps,),
        in_specs=[qp_spec, kp_spec, q_spec, all_spec, all_spec, q_spec, q_spec, l_spec],
        out_specs=[q_spec, all_spec, all_spec],
        out_shape=[shape, shape, shape],
        scratch_shapes=[pltpu.VMEM((rows, wide), F32), pltpu.VMEM((rows, wide), F32)],
        name="attn_bwd",
        cost_estimate=pl.CostEstimate(
            flops=10 * rows * rows * wide, bytes_accessed=24 * rows * wide, transcendentals=rows * rows * slots
        ),
        compiler_params=pltpu.CompilerParams(vmem_limit_bytes=60 * 2**20),
    )(place.reshape(rows, 1), place.reshape(1, rows), q, k, v, do, o, total)


def split_axis(n):
    across = 2 if n <= 8 else 4
    return n // across, across


def line_neighbours(me, lines, across):
    a, b = lax.div(me, across), lax.rem(me, across)
    return a, b, [
        (a < lines - 1, me + across),
        (a > 0, me - across),
        (b < across - 1, me + 1),
        (b > 0, me - 1),
    ]


def exchange_body(n, nf, counts, *refs):
    n_ctx, n_fsdp, n_red = counts
    total = n_ctx + n_fsdp + n_red
    ctx_in = refs[:n_ctx]
    fsdp_in = refs[n_ctx : n_ctx + n_fsdp]
    red_in = refs[n_ctx + n_fsdp : total]
    ctx_out = refs[total : total + n_ctx]
    fsdp_out = refs[total + n_ctx : total + n_ctx + n_fsdp]
    red_out = refs[total + n_ctx + n_fsdp : 2 * total]
    scratch = refs[2 * total :]
    land = scratch[:n_red]
    sums = scratch[n_red : 2 * n_red]
    copy_sem, send_sem, recv_sem, fs_send, fs_recv = scratch[2 * n_red :]

    lines, across = split_axis(n)
    me = lax.axis_index("ctx")
    f = lax.axis_index("fsdp")
    a, b, near = line_neighbours(me, lines, across)
    peers = [lax.rem(f + k, nf) for k in range(1, nf)] if n_fsdp + n_red else []
    barrier = pltpu.get_barrier_semaphore()
    if n_ctx + n_red:
        for exists, target in near:

            @pl.when(exists)
            def _(target=target):
                pl.semaphore_signal(barrier, inc=1, device_id={"ctx": target}, device_id_type=MESH)

    for peer in peers:
        pl.semaphore_signal(barrier, inc=1, device_id={"fsdp": peer}, device_id_type=MESH)
    waits = len(peers)
    if n_ctx + n_red:
        waits = waits + sum(exists.astype(jnp.int32) for exists, _ in near)
    pl.semaphore_wait(barrier, waits)

    gathered = list(zip(ctx_in, ctx_out)) + list(zip(sums, red_out))

    def hop(i, block, way, own=False):
        source, out = gathered[i]
        return pltpu.make_async_remote_copy(
            src_ref=source if own else out.at[block],
            dst_ref=out.at[block],
            send_sem=send_sem.at[i, way, block],
            recv_sem=recv_sem.at[i, way, block],
            device_id={"ctx": me + (across, -across, 1, -1)[way]},
            device_id_type=MESH,
        )

    def fs_hop(i, peer, source):
        if i < n_fsdp:
            src, dst = fsdp_in[i], fsdp_out[i].at[source]
        else:
            src, dst = red_in[i - n_fsdp].at[peer], land[i - n_fsdp].at[source]
        return pltpu.make_async_remote_copy(
            src_ref=src,
            dst_ref=dst,
            send_sem=fs_send.at[i, peer],
            recv_sem=fs_recv.at[i, source],
            device_id={"fsdp": peer},
            device_id_type=MESH,
        )

    keeps = []
    for i in range(n_fsdp + n_red):
        for peer in peers:
            fs_hop(i, peer, f).start()

    def begin(i):
        for way in range(4):
            pl.when(near[way][0])(lambda way=way: hop(i, me, way, True).start())
        keep = pltpu.make_async_copy(gathered[i][0], gathered[i][1].at[me], copy_sem.at[i])
        keep.start()
        keeps.append(keep)

    for i in range(n_ctx):
        begin(i)
    for i in range(n_fsdp):
        keep = pltpu.make_async_copy(fsdp_in[i], fsdp_out[i].at[f], copy_sem.at[n_ctx + n_red + i])
        keep.start()
        keeps.append(keep)
    for i in range(n_red):
        value = red_in[i][f].astype(F32)
        for peer in peers:
            fs_hop(n_fsdp + i, peer, peer).wait_recv()
            value = value + land[i][peer].astype(F32)
        sums[i][...] = value.astype(sums[i].dtype)
        begin(n_ctx + i)

    for i in range(len(gathered)):
        for d in range(1, lines):
            for way, there, source in ((0, a >= d, me - d * across), (1, a + d < lines, me + d * across)):

                @pl.when(there)
                def _(i=i, source=source, way=way):
                    hop(i, source, way).wait_recv()
                    for on in (way, 2, 3):
                        pl.when(near[on][0])(lambda on=on: hop(i, source, on).start())

    for i in range(len(gathered)):
        for d in range(1, across):
            for step in range(lines):
                for sign in (1, -1) if step else (1,):
                    for way, there, shift in ((2, b >= d, -d), (3, b + d < across, d)):
                        other = a + sign * step

                        @pl.when(there & (other >= 0) & (other < lines))
                        def _(i=i, source=other * across + b + shift, way=way):
                            hop(i, source, way).wait_recv()
                            if d < across - 1:
                                pl.when(near[way][0])(lambda: hop(i, source, way).start())

    for i in range(n_fsdp):
        for peer in peers:
            fs_hop(i, peer, peer).wait_recv()

    for keep in keeps:
        keep.wait()
    for i in range(n_fsdp + n_red):
        for peer in peers:
            fs_hop(i, peer, f).wait_send()
    for i in range(len(gathered)):
        for way in range(4):
            pl.when(near[way][0])(lambda i=i, way=way: hop(i, me, way, True).wait_send())
        for d in range(1, lines):
            for way, there, source in ((0, a >= d, me - d * across), (1, a + d < lines, me + d * across)):

                @pl.when(there)
                def _(i=i, source=source, way=way):
                    for on in (way, 2, 3):
                        pl.when(near[on][0])(lambda on=on: hop(i, source, on).wait_send())

        for d in range(1, across - 1):
            for line in range(lines):
                for way, there, shift in ((2, b >= d, -d), (3, b + d < across, d)):

                    @pl.when(there & near[way][0])
                    def _(i=i, source=line * across + b + shift, way=way):
                        hop(i, source, way).wait_send()


def exchange(call, n, nf, ctx=(), fsdp=(), red=()):
    shape = jax.ShapeDtypeStruct
    gathered = len(ctx) + len(red)
    outs = [shape((n, *x.shape), x.dtype) for x in ctx]
    outs += [shape((nf, *x.shape), x.dtype) for x in fsdp]
    outs += [shape((n, *x.shape[1:]), x.dtype) for x in red]
    sent = max(len(fsdp) + len(red), 1)
    return pl.pallas_call(
        functools.partial(exchange_body, n, nf, (len(ctx), len(fsdp), len(red))),
        in_specs=[pl.BlockSpec(memory_space=pltpu.VMEM)] * len(outs),
        out_specs=[pl.BlockSpec(memory_space=pl.ANY)] * len(outs),
        out_shape=outs,
        scratch_shapes=[pltpu.VMEM(x.shape, x.dtype) for x in red]
        + [pltpu.VMEM(x.shape[1:], x.dtype) for x in red]
        + [
            pltpu.SemaphoreType.DMA((len(outs),)),
            pltpu.SemaphoreType.DMA((max(gathered, 1), 4, n)),
            pltpu.SemaphoreType.DMA((max(gathered, 1), 4, n)),
            pltpu.SemaphoreType.DMA((sent, nf)),
            pltpu.SemaphoreType.DMA((sent, nf)),
        ],
        name=f"exchange_{call}",
        compiler_params=pltpu.CompilerParams(collective_id=call, has_side_effects=True, vmem_limit_bytes=60 * 2**20),
    )(*ctx, *fsdp, *red)


def scatter_body(n, p_ref, out_ref, across_in, sums, line_in, a_send, a_recv, l_send, l_recv):
    lines, across = split_axis(n)
    me = lax.axis_index("ctx")
    a, b, near = line_neighbours(me, lines, across)
    peers = [me - b + lax.rem(b + k, across) for k in range(1, across)]
    barrier = pltpu.get_barrier_semaphore()
    for peer in peers:
        pl.semaphore_signal(barrier, inc=1, device_id={"ctx": peer}, device_id_type=MESH)
    for exists, target in near[:2]:

        @pl.when(exists)
        def _(target=target):
            pl.semaphore_signal(barrier, inc=1, device_id={"ctx": target}, device_id_type=MESH)

    pl.semaphore_wait(barrier, len(peers) + sum(exists.astype(jnp.int32) for exists, _ in near[:2]))

    def over(line, k):
        return pltpu.make_async_remote_copy(
            src_ref=p_ref.at[line * across + lax.rem(b + k, across)],
            dst_ref=across_in.at[k - 1, line],
            send_sem=a_send.at[k - 1, line],
            recv_sem=a_recv.at[k - 1, line],
            device_id={"ctx": peers[k - 1]},
            device_id_type=MESH,
        )

    def along(line, way):
        return pltpu.make_async_remote_copy(
            src_ref=sums.at[line],
            dst_ref=line_in.at[way, line],
            send_sem=l_send.at[way, line],
            recv_sem=l_recv.at[way, line],
            device_id={"ctx": me + (across, -across)[way]},
            device_id_type=MESH,
        )

    for av in range(lines):

        @pl.when(a == av)
        def _(av=av):
            order = sorted(range(lines), key=lambda j: (-abs(j - av), j))
            for line in order:
                for k in range(1, across):
                    over(line, k).start()
            for line in order:
                value = p_ref[line * across + b].astype(F32)
                for k in range(1, across):
                    over(line, k).wait_recv()
                    value = value + across_in[k - 1, line].astype(F32)
                if line != av:
                    way = 0 if line > av else 1
                    if av > 0 if way == 0 else av < lines - 1:
                        along(line, way).wait_recv()
                        value = value + line_in[way, line].astype(F32)
                    sums[line] = value.astype(BF16)
                    along(line, way).start()
                else:
                    for way, there in ((0, av > 0), (1, av < lines - 1)):
                        if there:
                            along(line, way).wait_recv()
                            value = value + line_in[way, line].astype(F32)
                    out_ref[...] = value
            for line in order:
                for k in range(1, across):
                    over(line, k).wait_send()
                if line != av:
                    along(line, 0 if line > av else 1).wait_send()


def scatter(p, n, call):
    rows, width = p.shape[0] // n, p.shape[1]
    lines, across = split_axis(n)
    return pl.pallas_call(
        functools.partial(scatter_body, n),
        in_specs=[pl.BlockSpec(memory_space=pltpu.VMEM)],
        out_specs=pl.BlockSpec(memory_space=pltpu.VMEM),
        out_shape=jax.ShapeDtypeStruct((rows, width), F32),
        scratch_shapes=[
            pltpu.VMEM((across - 1, lines, rows, width), BF16),
            pltpu.VMEM((lines, rows, width), BF16),
            pltpu.VMEM((2, lines, rows, width), BF16),
            pltpu.SemaphoreType.DMA((across - 1, lines)),
            pltpu.SemaphoreType.DMA((across - 1, lines)),
            pltpu.SemaphoreType.DMA((2, lines)),
            pltpu.SemaphoreType.DMA((2, lines)),
        ],
        name=f"scatter_{call}",
        compiler_params=pltpu.CompilerParams(collective_id=call, has_side_effects=True, vmem_limit_bytes=60 * 2**20),
    )(p.astype(BF16).reshape(n, rows, width))


def columns_body(moves, in_ref, out_ref):
    for block, start, goal, size in moves:
        out_ref[:, goal : goal + size] = in_ref[block, :, start : start + size].astype(F32)


def place_columns(value, moves, width):
    n, rows, part = value.shape
    step = next(s for s in (80, 16, rows) if rows % s == 0)
    return pl.pallas_call(
        functools.partial(columns_body, tuple(moves)),
        grid=(rows // step,),
        in_specs=[pl.BlockSpec((n, step, part), lambda i: (0, i, 0))],
        out_specs=pl.BlockSpec((step, width), lambda i: (i, 0)),
        out_shape=jax.ShapeDtypeStruct((rows, width), F32),
        name="place_columns",
        cost_estimate=pl.CostEstimate(flops=0, bytes_accessed=6 * rows * width, transcendentals=0),
        compiler_params=pltpu.CompilerParams(vmem_limit_bytes=48 * 2**20),
    )(value)


def head_moves(n, heads, offset, goal):
    base, rest = divmod(heads, n)
    moves = [(c, offset, goal + c * base * HEAD_DIM, base * HEAD_DIM) for c in range(n) if base]
    moves += [
        (c, offset + base * HEAD_DIM, goal + (base * n + c) * HEAD_DIM, HEAD_DIM) for c in range(rest)
    ]
    return moves


def ag_ctx(value):
    return lax.all_gather(value, "ctx", axis=0, tiled=True)


def rs_ctx(value):
    return lax.psum_scatter(value.astype(BF16), "ctx", scatter_dimension=0, tiled=True)


def ag_fsdp(value):
    return lax.all_gather(value, "fsdp", axis=0, tiled=True)


def head_columns(value, width, c, n):
    heads = width // HEAD_DIM
    base, rest = divmod(heads, n)
    parts = []
    if base:
        parts.append(lax.dynamic_slice_in_dim(value, c * base * HEAD_DIM, base * HEAD_DIM, axis=-1))
    if rest:
        start = jnp.minimum(base * n + c, heads - 1) * HEAD_DIM
        extra = lax.dynamic_slice_in_dim(value, start, HEAD_DIM, axis=-1)
        parts.append(jnp.where(c < rest, extra, jnp.zeros_like(extra)))
    return jnp.concatenate(parts, axis=-1)


def spread_heads(value, heads, n):
    base, rest = divmod(heads, n)
    rows = value.shape[1]
    parts = []
    if base:
        body = value[:, :, : base * HEAD_DIM]
        parts.append(jnp.transpose(body, (1, 0, 2)).reshape(rows, n * base * HEAD_DIM))
    if rest:
        tail = value[:rest, :, base * HEAD_DIM :]
        parts.append(jnp.transpose(tail, (1, 0, 2)).reshape(rows, rest * HEAD_DIM))
    return jnp.concatenate(parts, axis=1)


def place_heads(value, heads, c, n):
    base, rest = divmod(heads, n)
    out = jnp.zeros((heads * HEAD_DIM,), value.dtype)
    if rest:
        start = jnp.minimum(base * n + c, heads - 1) * HEAD_DIM
        extra = jnp.where(c < rest, value[base * HEAD_DIM :], 0.0)
        out = lax.dynamic_update_slice(out, extra, (start,))
    if base:
        out = lax.dynamic_update_slice(out, value[: base * HEAD_DIM], (c * base * HEAD_DIM,))
    return out


def head_rows(value, heads, c, f, n):
    base, rest = divmod(heads, n)
    local, width = value.shape
    pad = max(base, 1) * HEAD_DIM
    padded = jnp.pad(value, ((pad, pad), (0, 0)))
    parts = []
    if base:
        start = jnp.clip(c * base * HEAD_DIM - f * local + pad, 0, local + 2 * pad - base * HEAD_DIM)
        parts.append(lax.dynamic_slice_in_dim(padded, start, base * HEAD_DIM, axis=0))
    if rest:
        start = jnp.clip((base * n + c) * HEAD_DIM - f * local + pad, 0, local + 2 * pad - HEAD_DIM)
        extra = lax.dynamic_slice_in_dim(padded, start, HEAD_DIM, axis=0)
        parts.append(jnp.where(c < rest, extra, jnp.zeros_like(extra)))
    return jnp.concatenate(parts, axis=0)


def on_device(
    tokens,
    ln1_gain,
    ln1_shift,
    qkv_weight,
    qv_bias,
    out_weight,
    out_bias,
    ln2_gain,
    ln2_shift,
    up_weight,
    up_bias,
    down_weight,
    down_bias,
    block_table,
    cotangent,
):
    rows, width = tokens.shape[1:]
    heads = width // HEAD_DIM
    n = lax.axis_size("ctx")
    nf = lax.axis_size("fsdp")
    c = lax.axis_index("ctx")
    f = lax.axis_index("fsdp")
    slots = -(-heads // n)
    wide = slots * HEAD_DIM
    half = rows // 2
    local = width // nf
    ff = up_weight.shape[1]
    ff_local = ff // nf
    ff_part = ff_local // n

    within = jnp.arange(rows, dtype=jnp.int32)
    block_of = jnp.where(within[None, :] < half, block_table[:, None], 2 * n - 1 - block_table[:, None])
    place = (block_of * half + within[None, :] % half).reshape(-1)

    vectors = (ln1_gain, ln1_shift, qv_bias, out_bias, ln2_gain, ln2_shift, up_bias, down_bias)
    flat = jnp.concatenate(vectors)
    flat = jnp.pad(flat, (0, -flat.shape[0] % 2048)).reshape(-1, 128)
    q_w = head_columns(qkv_weight[:, :width], width, c, n)
    k_w = head_columns(qkv_weight[:, width : 2 * width], width, c, n)
    v_w = head_columns(qkv_weight[:, 2 * width :], width, c, n)
    x_all, packed, w_qkv = exchange(0, n, nf, ctx=[tokens[0]], fsdp=[flat, jnp.concatenate([q_w, k_w, v_w], axis=1)])
    x_all = x_all.reshape(n * rows, width)
    w_qkv = w_qkv.reshape(width, 3 * wide)
    packed = packed.reshape(nf, -1)
    full, at = [], 0
    for vector in vectors:
        size = vector.shape[0]
        full.append(packed[:, at : at + size].reshape(-1).astype(F32))
        at += size
    gain1, shift1, b_qv, b_out, gain2, shift2, b_up, b_down = full

    w_out = lax.psum(head_rows(out_weight, heads, c, f, n), "fsdp")
    g2_all = ag_ctx(cotangent[0])
    up_mine = [lax.dynamic_slice_in_dim(up_weight, i * ff_local + c * ff_part, ff_part, axis=1) for i in range(nf)]
    w_up = ag_fsdp(jnp.concatenate(up_mine, axis=1))
    w_down = ag_fsdp(lax.dynamic_slice_in_dim(down_weight, c * ff_part, ff_part, axis=0))
    b_up_mine = lax.dynamic_slice_in_dim(b_up.reshape(nf, n, ff_part), c, 1, axis=1).reshape(-1)
    bq = head_columns(b_qv[:width], width, c, n)
    bv = head_columns(b_qv[width:], width, c, n)

    n1_all, _ = ln_stats(x_all.astype(F32))
    act1 = (n1_all * gain1 + shift1).astype(BF16)
    proj = dot(act1, w_qkv)
    q = (proj[:, :wide] + bq).astype(BF16)
    k = proj[:, wide : 2 * wide].astype(BF16)
    v = (proj[:, 2 * wide :] + bv).astype(BF16)
    attn, o, total = attention_fwd(place, q, k, v, slots)
    x = tokens[0].astype(F32)
    mid = x + scatter(dot(attn, w_out), n, 1) + b_out
    attn_all = spread_heads(lax.all_gather(attn, "ctx", axis=0, tiled=False), heads, n)

    n2, rstd2 = ln_stats(mid)
    (act2,) = exchange(2, n, nf, ctx=[(n2 * gain2 + shift2).astype(BF16)])
    act2 = act2.reshape(n * rows, width)
    u = dot(act2, w_up) + b_up_mine
    activated, gelu_back = jax.vjp(lambda t: jax.nn.gelu(t, approximate=True), u)
    hidden = activated.astype(BF16)
    dh = dot_t(g2_all, w_down)
    du = gelu_back(dh)[0].astype(BF16)
    da2 = scatter(dot_t(du, w_up), n, 3)
    result = mid + rs_ctx(dot(hidden, w_down)).astype(F32) + b_down
    d_down = t_dot(hidden, g2_all).astype(BF16).reshape(nf, ff_part, width)
    d_up = t_dot(act2, du).astype(BF16).reshape(nf, local, nf * ff_part)
    d_up_bias = jnp.sum(du.astype(F32), axis=0)
    grad_out = cotangent[0].astype(F32)
    d_down_bias = jnp.sum(grad_out, axis=0)

    d_gain2 = jnp.sum(da2 * n2, axis=0)
    d_shift2 = jnp.sum(da2, axis=0)
    d_mid = grad_out + ln_back(da2, n2, rstd2, gain2)
    g1 = d_mid.astype(BF16)
    d_out_bias = jnp.sum(g1.astype(F32), axis=0)
    (g1_all,) = exchange(4, n, nf, ctx=[g1])
    g1_all = g1_all.reshape(n * rows, width)
    d_attn = dot_t(g1_all, w_out)
    gq, gk, gv = attention_bwd(place, q, k, v, d_attn, o, total, slots)
    g_qkv = jnp.concatenate([gq, gk, gv], axis=1)
    da1 = scatter(dot_t(g_qkv, w_qkv), n, 5)
    d_qkv = t_dot(act1, g_qkv).astype(BF16).reshape(nf, local, 3 * wide)
    out_part = width // n
    g1_mine = lax.dynamic_slice_in_dim(g1_all, c * out_part, out_part, axis=1)
    d_out = t_dot(attn_all, g1_mine).astype(BF16).reshape(nf, local, out_part)

    n1, rstd1 = ln_stats(x)
    d_gain1 = jnp.sum(da1 * n1, axis=0)
    d_shift1 = jnp.sum(da1, axis=0)
    input_grad = d_mid + ln_back(da1, n1, rstd1, gain1)

    dq_bias = place_heads(jnp.sum(gq.astype(F32), axis=0), heads, c, n)
    dv_bias = place_heads(jnp.sum(gv.astype(F32), axis=0), heads, c, n)
    up_placed = lax.dynamic_update_slice(
        jnp.zeros((nf, n, ff_part), F32), d_up_bias.reshape(nf, 1, ff_part), (0, c, 0)
    )
    smalls = (
        d_gain1,
        d_shift1,
        jnp.concatenate([dq_bias, dv_bias]),
        d_out_bias,
        d_gain2,
        d_shift2,
        up_placed.reshape(-1),
        d_down_bias,
    )
    packed = jnp.concatenate([s.reshape(nf, -1) for s in smalls], axis=1)
    packed = jnp.pad(packed, ((0, 0), (0, -packed.shape[1] % 1024))).reshape(nf, -1, 128)
    d_up, d_down, d_out, d_qkv, packed = exchange(6, n, nf, red=[d_up, d_down, d_out, d_qkv, packed])
    mine = jnp.sum(packed, axis=0).reshape(-1)
    d_up_full = place_columns(
        d_up,
        [(i, j * ff_part, j * ff_local + i * ff_part, ff_part) for i in range(n) for j in range(nf)],
        ff,
    )
    d_down_full = d_down.reshape(ff_local, width).astype(F32)
    d_out_full = place_columns(d_out, [(i, 0, i * out_part, out_part) for i in range(n)], width)
    moves = [m for i in range(3) for m in head_moves(n, heads, i * wide, i * width)]
    d_qkv_full = place_columns(d_qkv, moves, 3 * width)
    out, at = [], 0
    for s in smalls:
        size = s.size // nf
        out.append(mine[at : at + size])
        at += size
    return (
        result[None],
        input_grad[None],
        out[0],
        out[1],
        d_qkv_full,
        out[2],
        d_out_full,
        out[3],
        out[4],
        out[5],
        d_up_full,
        out[6],
        d_down_full,
        out[7],
    )


def solution(mesh):
    rows, one, two = P("fsdp", "ctx", None), P("fsdp"), P("fsdp", None)
    return jax.shard_map(
        on_device,
        mesh=mesh,
        in_specs=(rows, one, one, two, one, two, one, one, one, two, one, two, one, P(), rows),
        out_specs=(rows, rows, one, one, two, one, two, one, one, one, two, one, two, one),
        check_vma=False,
    )
```

```python
import functools

import jax
import jax.numpy as jnp
from jax import lax
from jax.experimental import pallas as pl
from jax.experimental.pallas import tpu as pltpu
from jax.sharding import PartitionSpec as P

HEAD_DIM = 64
EPS = 1e-05
SCALE = 0.125
F32 = jnp.float32
BF16 = jnp.bfloat16
MESH = pl.DeviceIdType.MESH


def dot(left, right):
    return jnp.dot(left, right, preferred_element_type=F32)


def dot_t(left, right):
    return lax.dot_general(left, right, (((1,), (1,)), ((), ())), preferred_element_type=F32)


def t_dot(left, right):
    return lax.dot_general(left, right, (((0,), (0,)), ((), ())), preferred_element_type=F32)


def ln_stats(value):
    centre = value - jnp.mean(value, axis=-1, keepdims=True)
    spread = jnp.mean(centre * centre, axis=-1, keepdims=True)
    rstd = lax.rsqrt(spread + EPS)
    return centre * rstd, rstd


def ln_back(grad, normed, rstd, gain):
    dn = grad * gain
    first = jnp.mean(dn, axis=-1, keepdims=True)
    second = jnp.mean(dn * normed, axis=-1, keepdims=True)
    return (dn - first - normed * second) * rstd


def attn_fwd_body(slots, qp_ref, kp_ref, q_ref, k_ref, v_ref, attn_ref, o_ref, l_ref):
    allowed = kp_ref[...] <= qp_ref[...]
    for h in range(slots):
        cols = slice(h * HEAD_DIM, (h + 1) * HEAD_DIM)
        raw = dot_t(q_ref[:, cols], k_ref[:, cols])
        e = jnp.where(allowed, jnp.exp(raw * SCALE), 0.0)
        total = jnp.sum(e, axis=1, keepdims=True)
        numer = dot(e.astype(BF16), v_ref[:, cols])
        o = numer / total
        o_ref[:, cols] = o
        attn_ref[:, cols] = o.astype(BF16)
        l_ref[:, h : h + 1] = total


def attn_bwd_body(
    slots, qp_ref, kp_ref, q_ref, k_ref, v_ref, do_ref, o_ref, l_ref, dq_ref, dk_ref, dv_ref, dk_acc, dv_acc
):
    step = pl.program_id(0)

    @pl.when(step == 0)
    def _():
        dk_acc[...] = jnp.zeros_like(dk_acc)
        dv_acc[...] = jnp.zeros_like(dv_acc)

    allowed = kp_ref[...] <= qp_ref[...]
    for h in range(slots):
        cols = slice(h * HEAD_DIM, (h + 1) * HEAD_DIM)
        q = q_ref[:, cols]
        k = k_ref[:, cols]
        v = v_ref[:, cols]
        do = do_ref[:, cols]
        total = l_ref[:, h : h + 1]
        w = (do / total).astype(BF16)
        corr = jnp.sum(do * o_ref[:, cols], axis=1, keepdims=True) / total
        e = jnp.where(allowed, jnp.exp(dot_t(q, k) * SCALE), 0.0)
        de = dot_t(w, v)
        ds = (e * (de - corr)).astype(BF16)
        dq_ref[:, cols] = (dot(ds, k) * SCALE).astype(BF16)
        dk_acc[:, cols] += t_dot(ds, q)
        dv_acc[:, cols] += t_dot(e.astype(BF16), w)

    @pl.when(step == pl.num_programs(0) - 1)
    def _():
        dk_ref[...] = (dk_acc[...] * SCALE).astype(BF16)
        dv_ref[...] = dv_acc[...].astype(BF16)


def attn_specs(rows, wide, slots):
    qb = 256 if rows <= 1024 else 128
    q_spec = pl.BlockSpec((qb, wide), lambda i: (i, 0))
    l_spec = pl.BlockSpec((qb, slots), lambda i: (i, 0))
    all_spec = pl.BlockSpec((rows, wide), lambda i: (0, 0))
    qp_spec = pl.BlockSpec((qb, 1), lambda i: (i, 0))
    kp_spec = pl.BlockSpec((1, rows), lambda i: (0, 0))
    return rows // qb, q_spec, l_spec, all_spec, qp_spec, kp_spec


def attention_fwd(place, q, k, v, slots):
    rows, wide = q.shape
    steps, q_spec, l_spec, all_spec, qp_spec, kp_spec = attn_specs(rows, wide, slots)
    return pl.pallas_call(
        functools.partial(attn_fwd_body, slots),
        grid=(steps,),
        in_specs=[qp_spec, kp_spec, q_spec, all_spec, all_spec],
        out_specs=[q_spec, q_spec, l_spec],
        out_shape=[
            jax.ShapeDtypeStruct((rows, wide), BF16),
            jax.ShapeDtypeStruct((rows, wide), F32),
            jax.ShapeDtypeStruct((rows, slots), F32),
        ],
        name="attn_fwd",
        cost_estimate=pl.CostEstimate(
            flops=4 * rows * rows * wide, bytes_accessed=16 * rows * wide, transcendentals=rows * rows * slots
        ),
        compiler_params=pltpu.CompilerParams(vmem_limit_bytes=60 * 2**20),
    )(place.reshape(rows, 1), place.reshape(1, rows), q, k, v)


def attention_bwd(place, q, k, v, do, o, total, slots):
    rows, wide = q.shape
    steps, q_spec, l_spec, all_spec, qp_spec, kp_spec = attn_specs(rows, wide, slots)
    shape = jax.ShapeDtypeStruct((rows, wide), BF16)
    return pl.pallas_call(
        functools.partial(attn_bwd_body, slots),
        grid=(steps,),
        in_specs=[qp_spec, kp_spec, q_spec, all_spec, all_spec, q_spec, q_spec, l_spec],
        out_specs=[q_spec, all_spec, all_spec],
        out_shape=[shape, shape, shape],
        scratch_shapes=[pltpu.VMEM((rows, wide), F32), pltpu.VMEM((rows, wide), F32)],
        name="attn_bwd",
        cost_estimate=pl.CostEstimate(
            flops=10 * rows * rows * wide, bytes_accessed=24 * rows * wide, transcendentals=rows * rows * slots
        ),
        compiler_params=pltpu.CompilerParams(vmem_limit_bytes=60 * 2**20),
    )(place.reshape(rows, 1), place.reshape(1, rows), q, k, v, do, o, total)


def split_axis(n):
    across = 2 if n <= 8 else 4
    return n // across, across


def place_of(me, lines, across):
    a, b = lax.div(me, across), lax.rem(me, across)
    near = [(a < lines - 1, me + across), (a > 0, me - across), (b < across - 1, me + 1), (b > 0, me - 1)]
    return a, b, near


def turned_rows(rows, dtype, across):
    tile = 16 if dtype == BF16 else 8
    return rows // 6 // tile * tile if across == 2 else 0


def meet(near, peers):
    barrier = pltpu.get_barrier_semaphore()
    for exists, target in near:

        @pl.when(exists)
        def _(target=target):
            pl.semaphore_signal(barrier, inc=1, device_id={"ctx": target}, device_id_type=MESH)

    for axis, peer in peers:
        pl.semaphore_signal(barrier, inc=1, device_id={axis: peer}, device_id_type=MESH)
    pl.semaphore_wait(barrier, len(peers) + sum(exists.astype(jnp.int32) for exists, _ in near))


class Fsdp:
    def __init__(self, nf, gather_in, gather_out, red_in, red_out, scratch):
        self.gather_in, self.gather_out, self.red_in, self.red_out = gather_in, gather_out, red_in, red_out
        n_gather, n_red = len(gather_in), len(red_in)
        self.near_in, self.stage, self.far_in = scratch[:n_red], scratch[n_red : 2 * n_red], scratch[2 * n_red : 3 * n_red]
        self.keep_sem, self.g_send, self.g_recv, self.r_send, self.r_recv = scratch[3 * n_red : 3 * n_red + 5]
        self.f = lax.axis_index("fsdp")
        self.core = lax.rem(self.f, 2)
        self.mate = self.f + 1 - 2 * self.core
        self.pairs = nf // 2
        self.pair = lax.div(self.f, 2)
        self.other = [lax.rem(self.pair + k, self.pairs) for k in range(1, self.pairs)]
        self.peers = [self.mate] + [2 * y + self.core for y in self.other] if n_gather + n_red else []

    @staticmethod
    def scratch(nf, gather, red):
        pairs = nf // 2
        dma = pltpu.SemaphoreType.DMA
        out = []
        for _ in range(3):
            out += [pltpu.VMEM((pairs, *x.shape[1:]), x.dtype) for x in red]
        g, r = max(len(gather), 1), max(len(red), 1)
        return out + [dma((g,)), dma((g, 2, nf)), dma((g, nf)), dma((r, 2, pairs)), dma((r, 2, pairs))]

    def copy(self, src, dst, send, recv, target):
        return pltpu.make_async_remote_copy(
            src_ref=src, dst_ref=dst, send_sem=send, recv_sem=recv, device_id={"fsdp": target}, device_id_type=MESH
        )

    def spread(self, i, source, target, own):
        out = self.gather_out[i].at[source]
        send = self.g_send.at[i, 0, target] if own else self.g_send.at[i, 1, source]
        return self.copy(self.gather_in[i] if own else out, out, send, self.g_recv.at[i, source], target)

    def keep(self, i):
        return pltpu.make_async_copy(self.gather_in[i], self.gather_out[i].at[self.f], self.keep_sem.at[i])

    def to_mate(self, j, y):
        src = self.red_in[j].at[2 * y + 1 - self.core]
        return self.copy(src, self.near_in[j].at[y], self.r_send.at[j, 0, y], self.r_recv.at[j, 0, y], self.mate)

    def to_far(self, j, y, source):
        send, recv = self.r_send.at[j, 1, y], self.r_recv.at[j, 1, source]
        return self.copy(self.stage[j].at[y], self.far_in[j].at[source], send, recv, 2 * y + self.core)

    def start(self):
        for j in range(len(self.red_in)):
            for y in range(self.pairs):
                self.to_mate(j, y).start()
        for i in range(len(self.gather_in)):
            for target in self.peers[1:] + self.peers[:1]:
                self.spread(i, self.f, target, True).start()
            self.keep(i).start()

    def middle(self):
        for j in range(len(self.red_in)):
            for y in range(self.pairs):
                self.to_mate(j, y).wait_recv()
            for y in self.other:
                value = self.red_in[j][2 * y + self.core].astype(F32) + self.near_in[j][y].astype(F32)
                self.stage[j][y] = value.astype(self.stage[j].dtype)
                self.to_far(j, y, self.pair).start()

    def end(self):
        for j in range(len(self.red_in)):
            value = self.red_in[j][self.f].astype(F32) + self.near_in[j][self.pair].astype(F32)
            for y in self.other:
                self.to_far(j, y, y).wait_recv()
                value = value + self.far_in[j][y].astype(F32)
            self.red_out[j][...] = value.astype(self.red_out[j].dtype)
        for i in range(len(self.gather_in)):
            for y in self.other:
                source = 2 * y + self.core
                self.spread(i, source, self.mate, False).wait_recv()
                self.spread(i, source, self.mate, False).start()

    def finish(self):
        for i in range(len(self.gather_in)):
            self.spread(i, self.mate, self.mate, False).wait_recv()
            for y in self.other:
                self.spread(i, 2 * y + 1 - self.core, self.mate, False).wait_recv()
            self.keep(i).wait()
            for target in self.peers:
                self.spread(i, self.f, target, True).wait_send()
            for y in self.other:
                self.spread(i, 2 * y + self.core, self.mate, False).wait_send()
        for j in range(len(self.red_in)):
            for y in range(self.pairs):
                self.to_mate(j, y).wait_send()
            for y in self.other:
                self.to_far(j, y, self.pair).wait_send()


def exchange_body(n, nf, counts, *refs):
    n_ctx, n_fsdp, n_red = counts
    total = n_ctx + n_fsdp + n_red
    ctx_in, fsdp_in, red_in = refs[:n_ctx], refs[n_ctx : n_ctx + n_fsdp], refs[n_ctx + n_fsdp : total]
    outs = refs[total : 2 * total]
    ctx_out, fsdp_out, red_out = outs[:n_ctx], outs[n_ctx : n_ctx + n_fsdp], outs[n_ctx + n_fsdp :]
    scratch = refs[2 * total :]
    sums = scratch[:n_red]
    copy_sem, send_sem, recv_sem = scratch[n_red : n_red + 3]
    fs = Fsdp(nf, fsdp_in, fsdp_out, red_in, sums, scratch[n_red + 3 :])

    lines, across = split_axis(n)
    me = lax.axis_index("ctx")
    a, b, near = place_of(me, lines, across)
    gathered = list(zip(ctx_in, ctx_out)) + list(zip(sums, red_out))
    meet(near if gathered else [], [("fsdp", peer) for peer in fs.peers])
    fs.start()

    def part(i, turned):
        rows = gathered[i][1].shape[1]
        last = turned_rows(rows, gathered[i][1].dtype, across)
        return pl.ds(rows - last, last) if turned else pl.ds(0, rows - last)

    def turns(i):
        return bool(turned_rows(gathered[i][1].shape[1], gathered[i][1].dtype, across))

    def hop(i, block, way, turned=False, own=False):
        source, out = gathered[i]
        rows = part(i, turned)
        return pltpu.make_async_remote_copy(
            src_ref=source.at[rows] if own else out.at[block, rows],
            dst_ref=out.at[block, rows],
            send_sem=send_sem.at[i, way, block, int(turned)],
            recv_sem=recv_sem.at[i, way, block, int(turned)],
            device_id={"ctx": me + (across, -across, 1, -1)[way]},
            device_id_type=MESH,
        )

    def keep(i):
        return pltpu.make_async_copy(gathered[i][0], gathered[i][1].at[me], copy_sem.at[i])

    def each_own(i, act):
        for turned in (True, False) if turns(i) else (False,):
            for way in (2, 3, 0, 1):
                pl.when(near[way][0])(lambda way=way: act(hop(i, me, way, turned, True)))

    def each_twin(i, wait, act):
        if turns(i):
            twin = me + 1 - 2 * b
            for way in (2, 3):

                @pl.when(near[5 - way][0])
                def _(way=way):
                    if wait:
                        hop(i, twin, way, True).wait_recv()
                    for on in (0, 1):
                        pl.when(near[on][0])(lambda on=on: act(hop(i, twin, on, True)))

    def each_relay(i, d, wait, act):
        for way, there, shift in ((0, a >= d, -d * across), (1, a + d < lines, d * across)):

            @pl.when(there)
            def _(way=way, shift=shift):
                for turned, block in [(False, me + shift)] + (
                    [(True, me + shift), (True, me + 1 - 2 * b + shift)] if turns(i) else []
                ):
                    if wait:
                        hop(i, block, way, turned).wait_recv()
                    for on in (way,) if turned else (2, 3, way):
                        pl.when(near[on][0])(lambda on=on: act(hop(i, block, on, turned)))

    def start(copy):
        copy.start()

    def wait_send(copy):
        copy.wait_send()

    for i in range(n_ctx):
        each_own(i, start)
        keep(i).start()
    fs.middle()
    for i in range(len(gathered)):
        if i == n_ctx:
            fs.end()
            for j in range(n_ctx, len(gathered)):
                each_own(j, start)
                keep(j).start()
        each_twin(i, True, start)
        for d in range(1, lines):
            each_relay(i, d, True, start)

    for i in range(len(gathered)):
        for d in range(1, across):
            for step in range(lines):
                for sign in (1, -1) if step else (1,):
                    for way, there, shift in ((2, b >= d, -d), (3, b + d < across, d)):
                        other = a + sign * step

                        @pl.when(there & (other >= 0) & (other < lines))
                        def _(i=i, source=other * across + b + shift, way=way):
                            hop(i, source, way).wait_recv()
                            if d < across - 1:
                                pl.when(near[way][0])(lambda: hop(i, source, way).start())

    if not n_red:
        fs.end()

    for i in range(len(gathered)):
        keep(i).wait()
        each_own(i, wait_send)
        each_twin(i, False, wait_send)
        for d in range(1, lines):
            each_relay(i, d, False, wait_send)
        for d in range(1, across - 1):
            for line in range(lines):
                for way, there, shift in ((2, b >= d, -d), (3, b + d < across, d)):

                    @pl.when(there & near[way][0])
                    def _(i=i, source=line * across + b + shift, way=way):
                        hop(i, source, way).wait_send()

    fs.finish()


def exchange(call, n, nf, ctx=(), fsdp=(), red=()):
    shape = jax.ShapeDtypeStruct
    gathered = max(len(ctx) + len(red), 1)
    outs = [shape((n, *x.shape), x.dtype) for x in ctx]
    outs += [shape((nf, *x.shape), x.dtype) for x in fsdp]
    outs += [shape((n, *x.shape[1:]), x.dtype) for x in red]
    return pl.pallas_call(
        functools.partial(exchange_body, n, nf, (len(ctx), len(fsdp), len(red))),
        in_specs=[pl.BlockSpec(memory_space=pltpu.VMEM)] * len(outs),
        out_specs=[pl.BlockSpec(memory_space=pl.ANY)] * len(outs),
        out_shape=outs,
        scratch_shapes=[pltpu.VMEM(x.shape[1:], x.dtype) for x in red]
        + [
            pltpu.SemaphoreType.DMA((gathered,)),
            pltpu.SemaphoreType.DMA((gathered, 4, n, 2)),
            pltpu.SemaphoreType.DMA((gathered, 4, n, 2)),
        ]
        + Fsdp.scratch(nf, fsdp, red),
        name=f"exchange_{call}",
        compiler_params=pltpu.CompilerParams(collective_id=call, has_side_effects=True, vmem_limit_bytes=60 * 2**20),
    )(*ctx, *fsdp, *red)


def product_body(n, nf, counts, transposed, *refs):
    n_fsdp, n_red = counts
    left, right = refs[:2]
    more = n_fsdp + n_red
    fsdp_in, red_in = refs[2 : 2 + n_fsdp], refs[2 + n_fsdp : 2 + more]
    out = refs[2 + more]
    fsdp_out, red_out = refs[3 + more : 3 + more + n_fsdp], refs[3 + more + n_fsdp : 3 + 2 * more]
    part, acc, acc_t, over_in, sums, sums_t, line_in, line_in_t, twin_in = refs[3 + 2 * more : 12 + 2 * more]
    o_send, o_recv, l_send, l_recv, t_send, t_recv, w_send, w_recv = refs[12 + 2 * more : 20 + 2 * more]
    fs = Fsdp(nf, fsdp_in, fsdp_out, red_in, red_out, refs[20 + 2 * more :])

    lines, across = split_axis(n)
    me = lax.axis_index("ctx")
    a, b, near = place_of(me, lines, across)
    rows = out.shape[0]
    last = turned_rows(rows, BF16, across)
    head, tail = pl.ds(0, rows - last), pl.ds(rows - last, last)
    peers = [me - b + lax.rem(b + k, across) for k in range(1, across)]
    meet(near[:2], [("ctx", peer) for peer in peers] + [("fsdp", peer) for peer in fs.peers])
    fs.start()

    def copy(src, dst, send, recv, target):
        return pltpu.make_async_remote_copy(
            src_ref=src, dst_ref=dst, send_sem=send, recv_sem=recv, device_id={"ctx": target}, device_id_type=MESH
        )

    def over(line, k):
        src = part.at[line, lax.rem(b + k, across), head]
        return copy(src, over_in.at[k - 1, line], o_send.at[k - 1, line], o_recv.at[k - 1, line], peers[k - 1])

    def along(line, way):
        target = me + (across, -across)[way]
        return copy(sums.at[line], line_in.at[way, line], l_send.at[way, line], l_recv.at[way, line], target)

    def along_t(line, way):
        target = me + (across, -across)[way]
        return copy(sums_t.at[line], line_in_t.at[way, line], t_send.at[way, line], t_recv.at[way, line], target)

    def twin():
        return copy(sums_t.at[a, 1 - b], twin_in, w_send, w_recv, peers[0])

    order = []
    for k in range(lines):
        line = jnp.int32(0)
        for av in range(lines):
            line = jnp.where(a == av, sorted(range(lines), key=lambda j: (-abs(j - av), j))[k], line)
        order.append(line)

    for line in order:
        lhs = left[pl.ds(pl.multiple_of(line * across * rows, across * rows), across * rows), :]
        value = dot_t(lhs, right[...]) if transposed else dot(lhs, right[...])
        part[line] = value.astype(BF16).reshape(across, rows, value.shape[1])
        for k in range(1, across):
            over(line, k).start()
    fs.middle()
    for line in order[:-1]:
        up, down = line > a, line < a
        if last:
            acc_t[...] = part[line, :, tail].astype(F32)
            for way, there in ((0, up & (a > 0)), (1, down & (a < lines - 1))):

                @pl.when(there)
                def _(way=way, line=line):
                    along_t(line, way).wait_recv()
                    acc_t[...] += line_in_t[way, line].astype(F32)

            sums_t[line] = acc_t[...].astype(BF16)
            pl.when(up)(lambda line=line: along_t(line, 0).start())
            pl.when(down)(lambda line=line: along_t(line, 1).start())
        value = part[line, b, head].astype(F32)
        for k in range(1, across):
            over(line, k).wait_recv()
            value = value + over_in[k - 1, line].astype(F32)
        acc[...] = value
        for way, there in ((0, up & (a > 0)), (1, down & (a < lines - 1))):

            @pl.when(there)
            def _(way=way, line=line):
                along(line, way).wait_recv()
                acc[...] += line_in[way, line].astype(F32)

        sums[line] = acc[...].astype(BF16)
        pl.when(up)(lambda line=line: along(line, 0).start())
        pl.when(down)(lambda line=line: along(line, 1).start())

    if last:
        acc_t[...] = part[a, :, tail].astype(F32)
        for way in range(2):

            @pl.when(near[1 - way][0])
            def _(way=way):
                along_t(a, way).wait_recv()
                acc_t[...] += line_in_t[way, a].astype(F32)

        sums_t[a] = acc_t[...].astype(BF16)
        twin().start()
    value = part[a, b, head].astype(F32)
    for k in range(1, across):
        over(a, k).wait_recv()
        value = value + over_in[k - 1, a].astype(F32)
    acc[...] = value
    for way in range(2):

        @pl.when(near[1 - way][0])
        def _(way=way):
            along(a, way).wait_recv()
            acc[...] += line_in[way, a].astype(F32)

    out[head, :] = acc[...]
    fs.end()
    if last:
        twin().wait_recv()
        out[tail, :] = acc_t[b] + twin_in[...].astype(F32)

    for line in order:
        for k in range(1, across):
            over(line, k).wait_send()
    for line in order[:-1]:
        for way, there in ((0, line > a), (1, line < a)):

            @pl.when(there)
            def _(way=way, line=line):
                along(line, way).wait_send()
                if last:
                    along_t(line, way).wait_send()

    if last:
        twin().wait_send()
    fs.finish()


def product(call, n, nf, left, right, transposed=False, fsdp=(), red=()):
    rows, width = left.shape[0] // n, right.shape[0 if transposed else 1]
    lines, across = split_axis(n)
    last = turned_rows(rows, BF16, across)
    some = max(last, 16)
    shape = jax.ShapeDtypeStruct
    vmem, dma = pltpu.VMEM, pltpu.SemaphoreType.DMA
    outs = [shape((rows, width), F32)]
    outs += [shape((nf, *x.shape), x.dtype) for x in fsdp]
    outs += [shape(x.shape[1:], x.dtype) for x in red]
    return pl.pallas_call(
        functools.partial(product_body, n, nf, (len(fsdp), len(red)), transposed),
        in_specs=[pl.BlockSpec(memory_space=vmem)] * (2 + len(fsdp) + len(red)),
        out_specs=[pl.BlockSpec(memory_space=vmem)]
        + [pl.BlockSpec(memory_space=pl.ANY)] * len(fsdp)
        + [pl.BlockSpec(memory_space=vmem)] * len(red),
        out_shape=outs,
        scratch_shapes=[
            vmem((lines, across, rows, width), BF16),
            vmem((rows - last, width), F32),
            vmem((across, some, width), F32),
            vmem((across - 1, lines, rows - last, width), BF16),
            vmem((lines, rows - last, width), BF16),
            vmem((lines, across, some, width), BF16),
            vmem((2, lines, rows - last, width), BF16),
            vmem((2, lines, across, some, width), BF16),
            vmem((some, width), BF16),
            dma((across - 1, lines)),
            dma((across - 1, lines)),
            dma((2, lines)),
            dma((2, lines)),
            dma((2, lines)),
            dma((2, lines)),
            dma,
            dma,
        ]
        + Fsdp.scratch(nf, fsdp, red),
        name=f"product_{call}",
        compiler_params=pltpu.CompilerParams(collective_id=call, has_side_effects=True, vmem_limit_bytes=63 * 2**20),
    )(left, right, *fsdp, *red)


def columns_body(moves, in_ref, out_ref):
    for block, start, goal, size in moves:
        out_ref[:, goal : goal + size] = in_ref[block, :, start : start + size].astype(F32)


def place_columns(value, moves, width):
    n, rows, part = value.shape
    step = next(s for s in (80, 16, rows) if rows % s == 0)
    return pl.pallas_call(
        functools.partial(columns_body, tuple(moves)),
        grid=(rows // step,),
        in_specs=[pl.BlockSpec((n, step, part), lambda i: (0, i, 0))],
        out_specs=pl.BlockSpec((step, width), lambda i: (i, 0)),
        out_shape=jax.ShapeDtypeStruct((rows, width), F32),
        name="place_columns",
        cost_estimate=pl.CostEstimate(flops=0, bytes_accessed=6 * rows * width, transcendentals=0),
        compiler_params=pltpu.CompilerParams(vmem_limit_bytes=48 * 2**20),
    )(value)


def head_moves(n, heads, offset, goal):
    base, rest = divmod(heads, n)
    moves = [(c, offset, goal + c * base * HEAD_DIM, base * HEAD_DIM) for c in range(n) if base]
    moves += [
        (c, offset + base * HEAD_DIM, goal + (base * n + c) * HEAD_DIM, HEAD_DIM) for c in range(rest)
    ]
    return moves


def ag_ctx(value):
    return lax.all_gather(value, "ctx", axis=0, tiled=True)


def rs_ctx(value):
    return lax.psum_scatter(value.astype(BF16), "ctx", scatter_dimension=0, tiled=True)


def ag_fsdp(value):
    return lax.all_gather(value, "fsdp", axis=0, tiled=True)


def head_columns(value, width, c, n):
    heads = width // HEAD_DIM
    base, rest = divmod(heads, n)
    parts = []
    if base:
        parts.append(lax.dynamic_slice_in_dim(value, c * base * HEAD_DIM, base * HEAD_DIM, axis=-1))
    if rest:
        start = jnp.minimum(base * n + c, heads - 1) * HEAD_DIM
        extra = lax.dynamic_slice_in_dim(value, start, HEAD_DIM, axis=-1)
        parts.append(jnp.where(c < rest, extra, jnp.zeros_like(extra)))
    return jnp.concatenate(parts, axis=-1)


def spread_heads(value, heads, n):
    base, rest = divmod(heads, n)
    rows = value.shape[1]
    parts = []
    if base:
        body = value[:, :, : base * HEAD_DIM]
        parts.append(jnp.transpose(body, (1, 0, 2)).reshape(rows, n * base * HEAD_DIM))
    if rest:
        tail = value[:rest, :, base * HEAD_DIM :]
        parts.append(jnp.transpose(tail, (1, 0, 2)).reshape(rows, rest * HEAD_DIM))
    return jnp.concatenate(parts, axis=1)


def place_heads(value, heads, c, n):
    base, rest = divmod(heads, n)
    out = jnp.zeros((heads * HEAD_DIM,), value.dtype)
    if rest:
        start = jnp.minimum(base * n + c, heads - 1) * HEAD_DIM
        extra = jnp.where(c < rest, value[base * HEAD_DIM :], 0.0)
        out = lax.dynamic_update_slice(out, extra, (start,))
    if base:
        out = lax.dynamic_update_slice(out, value[: base * HEAD_DIM], (c * base * HEAD_DIM,))
    return out


def head_rows(value, heads, c, f, n):
    base, rest = divmod(heads, n)
    local, width = value.shape
    pad = max(base, 1) * HEAD_DIM
    padded = jnp.pad(value, ((pad, pad), (0, 0)))
    parts = []
    if base:
        start = jnp.clip(c * base * HEAD_DIM - f * local + pad, 0, local + 2 * pad - base * HEAD_DIM)
        parts.append(lax.dynamic_slice_in_dim(padded, start, base * HEAD_DIM, axis=0))
    if rest:
        start = jnp.clip((base * n + c) * HEAD_DIM - f * local + pad, 0, local + 2 * pad - HEAD_DIM)
        extra = lax.dynamic_slice_in_dim(padded, start, HEAD_DIM, axis=0)
        parts.append(jnp.where(c < rest, extra, jnp.zeros_like(extra)))
    return jnp.concatenate(parts, axis=0)


def on_device(
    tokens,
    ln1_gain,
    ln1_shift,
    qkv_weight,
    qv_bias,
    out_weight,
    out_bias,
    ln2_gain,
    ln2_shift,
    up_weight,
    up_bias,
    down_weight,
    down_bias,
    block_table,
    cotangent,
):
    rows, width = tokens.shape[1:]
    heads = width // HEAD_DIM
    n = lax.axis_size("ctx")
    nf = lax.axis_size("fsdp")
    c = lax.axis_index("ctx")
    f = lax.axis_index("fsdp")
    slots = -(-heads // n)
    wide = slots * HEAD_DIM
    half = rows // 2
    local = width // nf
    ff = up_weight.shape[1]
    ff_local = ff // nf
    ff_part = ff_local // n

    within = jnp.arange(rows, dtype=jnp.int32)
    block_of = jnp.where(within[None, :] < half, block_table[:, None], 2 * n - 1 - block_table[:, None])
    place = (block_of * half + within[None, :] % half).reshape(-1)

    vectors = (ln1_gain, ln1_shift, qv_bias, out_bias, ln2_gain, ln2_shift, up_bias, down_bias)
    flat = jnp.concatenate(vectors)
    flat = jnp.pad(flat, (0, -flat.shape[0] % 2048)).reshape(-1, 128)
    q_w = head_columns(qkv_weight[:, :width], width, c, n)
    k_w = head_columns(qkv_weight[:, width : 2 * width], width, c, n)
    v_w = head_columns(qkv_weight[:, 2 * width :], width, c, n)
    x_all, packed, w_qkv = exchange(0, n, nf, ctx=[tokens[0]], fsdp=[flat, jnp.concatenate([q_w, k_w, v_w], axis=1)])
    x_all = x_all.reshape(n * rows, width)
    w_qkv = w_qkv.reshape(width, 3 * wide)
    up_weight, down_weight, cotangent, packed = lax.optimization_barrier((up_weight, down_weight, cotangent, packed))
    packed = packed.reshape(nf, -1)
    full, at = [], 0
    for vector in vectors:
        size = vector.shape[0]
        full.append(packed[:, at : at + size].reshape(-1).astype(F32))
        at += size
    gain1, shift1, b_qv, b_out, gain2, shift2, b_up, b_down = full

    w_out = lax.psum(head_rows(out_weight, heads, c, f, n), "fsdp")
    g2_all = ag_ctx(cotangent[0])
    up_mine = [lax.dynamic_slice_in_dim(up_weight, i * ff_local + c * ff_part, ff_part, axis=1) for i in range(nf)]
    w_up = ag_fsdp(jnp.concatenate(up_mine, axis=1))
    w_down = ag_fsdp(lax.dynamic_slice_in_dim(down_weight, c * ff_part, ff_part, axis=0))
    b_up_mine = lax.dynamic_slice_in_dim(b_up.reshape(nf, n, ff_part), c, 1, axis=1).reshape(-1)
    bq = head_columns(b_qv[:width], width, c, n)
    bv = head_columns(b_qv[width:], width, c, n)

    n1_all, _ = ln_stats(x_all.astype(F32))
    act1 = (n1_all * gain1 + shift1).astype(BF16)
    proj = dot(act1, w_qkv)
    q = (proj[:, :wide] + bq).astype(BF16)
    k = proj[:, wide : 2 * wide].astype(BF16)
    v = (proj[:, 2 * wide :] + bv).astype(BF16)
    attn, o, total = attention_fwd(place, q, k, v, slots)
    x = tokens[0].astype(F32)
    (mixed,) = product(1, n, nf, attn, w_out)
    mid = x + mixed + b_out
    attn_all = spread_heads(lax.all_gather(attn, "ctx", axis=0, tiled=False), heads, n)

    n2, rstd2 = ln_stats(mid)
    (act2,) = exchange(2, n, nf, ctx=[(n2 * gain2 + shift2).astype(BF16)])
    act2 = act2.reshape(n * rows, width)
    u = dot(act2, w_up) + b_up_mine
    activated, gelu_back = jax.vjp(lambda t: jax.nn.gelu(t, approximate=True), u)
    hidden = activated.astype(BF16)
    dh = dot_t(g2_all, w_down)
    du = gelu_back(dh)[0].astype(BF16)
    result = mid + rs_ctx(dot(hidden, w_down)).astype(F32) + b_down
    d_down = t_dot(hidden, g2_all).astype(BF16).reshape(nf, ff_part, width)
    d_up = t_dot(act2, du).astype(BF16).reshape(nf, local, nf * ff_part)
    da2, d_up, d_down = product(3, n, nf, du, w_up, True, red=[d_up, d_down])
    d_up_bias = jnp.sum(du.astype(F32), axis=0)
    grad_out = cotangent[0].astype(F32)
    d_down_bias = jnp.sum(grad_out, axis=0)

    d_gain2 = jnp.sum(da2 * n2, axis=0)
    d_shift2 = jnp.sum(da2, axis=0)
    d_mid = grad_out + ln_back(da2, n2, rstd2, gain2)
    g1 = d_mid.astype(BF16)
    d_out_bias = jnp.sum(g1.astype(F32), axis=0)
    (g1_all,) = exchange(4, n, nf, ctx=[g1])
    g1_all = g1_all.reshape(n * rows, width)
    d_attn = dot_t(g1_all, w_out)
    gq, gk, gv = attention_bwd(place, q, k, v, d_attn, o, total, slots)
    g_qkv = jnp.concatenate([gq, gk, gv], axis=1)
    d_qkv = t_dot(act1, g_qkv).astype(BF16).reshape(nf, local, 3 * wide)
    out_part = width // n
    g1_mine = lax.dynamic_slice_in_dim(g1_all, c * out_part, out_part, axis=1)
    d_out = t_dot(attn_all, g1_mine).astype(BF16).reshape(nf, local, out_part)
    da1, d_qkv, d_out = product(5, n, nf, g_qkv, w_qkv, True, red=[d_qkv, d_out])

    n1, rstd1 = ln_stats(x)
    d_gain1 = jnp.sum(da1 * n1, axis=0)
    d_shift1 = jnp.sum(da1, axis=0)
    input_grad = d_mid + ln_back(da1, n1, rstd1, gain1)

    dq_bias = place_heads(jnp.sum(gq.astype(F32), axis=0), heads, c, n)
    dv_bias = place_heads(jnp.sum(gv.astype(F32), axis=0), heads, c, n)
    up_placed = lax.dynamic_update_slice(
        jnp.zeros((nf, n, ff_part), F32), d_up_bias.reshape(nf, 1, ff_part), (0, c, 0)
    )
    smalls = (
        d_gain1,
        d_shift1,
        jnp.concatenate([dq_bias, dv_bias]),
        d_out_bias,
        d_gain2,
        d_shift2,
        up_placed.reshape(-1),
        d_down_bias,
    )
    packed = jnp.concatenate([s.reshape(nf, -1) for s in smalls], axis=1)
    packed = jnp.pad(packed, ((0, 0), (0, -packed.shape[1] % 1024))).reshape(nf, -1, 128)
    d_up, d_down, d_out, d_qkv, packed = exchange(
        6, n, nf, ctx=[d_up, d_down, d_out, d_qkv], red=[packed]
    )
    mine = jnp.sum(packed, axis=0).reshape(-1)
    d_up_full = place_columns(
        d_up,
        [(i, j * ff_part, j * ff_local + i * ff_part, ff_part) for i in range(n) for j in range(nf)],
        ff,
    )
    d_down_full = d_down.reshape(ff_local, width).astype(F32)
    d_out_full = place_columns(d_out, [(i, 0, i * out_part, out_part) for i in range(n)], width)
    moves = [m for i in range(3) for m in head_moves(n, heads, i * wide, i * width)]
    d_qkv_full = place_columns(d_qkv, moves, 3 * width)
    out, at = [], 0
    for s in smalls:
        size = s.size // nf
        out.append(mine[at : at + size])
        at += size
    return (
        result[None],
        input_grad[None],
        out[0],
        out[1],
        d_qkv_full,
        out[2],
        d_out_full,
        out[3],
        out[4],
        out[5],
        d_up_full,
        out[6],
        d_down_full,
        out[7],
    )


def solution(mesh):
    rows, one, two = P("fsdp", "ctx", None), P("fsdp"), P("fsdp", None)
    return jax.shard_map(
        on_device,
        mesh=mesh,
        in_specs=(rows, one, one, two, one, two, one, one, one, two, one, two, one, P(), rows),
        out_specs=(rows, rows, one, one, two, one, two, one, one, one, two, one, two, one),
        check_vma=False,
    )
```

```python
import functools

import jax
import jax.numpy as jnp
from jax import lax
from jax.experimental import pallas as pl
from jax.experimental.pallas import tpu as pltpu
from jax.sharding import PartitionSpec as P

HEAD_DIM = 64
EPS = 1e-05
SCALE = 0.125
F32 = jnp.float32
BF16 = jnp.bfloat16
MESH = pl.DeviceIdType.MESH


def dot(left, right):
    return jnp.dot(left, right, preferred_element_type=F32)


def dot_t(left, right):
    return lax.dot_general(left, right, (((1,), (1,)), ((), ())), preferred_element_type=F32)


def t_dot(left, right):
    return lax.dot_general(left, right, (((0,), (0,)), ((), ())), preferred_element_type=F32)


def ln_stats(value):
    centre = value - jnp.mean(value, axis=-1, keepdims=True)
    spread = jnp.mean(centre * centre, axis=-1, keepdims=True)
    rstd = lax.rsqrt(spread + EPS)
    return centre * rstd, rstd


def ln_back(grad, normed, rstd, gain):
    dn = grad * gain
    first = jnp.mean(dn, axis=-1, keepdims=True)
    second = jnp.mean(dn * normed, axis=-1, keepdims=True)
    return (dn - first - normed * second) * rstd


def attn_fwd_body(slots, qp_ref, kp_ref, q_ref, k_ref, v_ref, attn_ref, o_ref, l_ref):
    allowed = kp_ref[...] <= qp_ref[...]
    for h in range(slots):
        cols = slice(h * HEAD_DIM, (h + 1) * HEAD_DIM)
        raw = dot_t(q_ref[:, cols], k_ref[:, cols])
        e = jnp.where(allowed, jnp.exp(raw * SCALE), 0.0)
        total = jnp.sum(e, axis=1, keepdims=True)
        numer = dot(e.astype(BF16), v_ref[:, cols])
        o = numer / total
        o_ref[:, cols] = o
        attn_ref[:, cols] = o.astype(BF16)
        l_ref[:, h : h + 1] = total


def attn_bwd_body(
    slots, qp_ref, kp_ref, q_ref, k_ref, v_ref, do_ref, o_ref, l_ref, dq_ref, dk_ref, dv_ref, dk_acc, dv_acc
):
    step = pl.program_id(0)

    @pl.when(step == 0)
    def _():
        dk_acc[...] = jnp.zeros_like(dk_acc)
        dv_acc[...] = jnp.zeros_like(dv_acc)

    allowed = kp_ref[...] <= qp_ref[...]
    for h in range(slots):
        cols = slice(h * HEAD_DIM, (h + 1) * HEAD_DIM)
        q = q_ref[:, cols]
        k = k_ref[:, cols]
        v = v_ref[:, cols]
        do = do_ref[:, cols]
        total = l_ref[:, h : h + 1]
        w = (do / total).astype(BF16)
        corr = jnp.sum(do * o_ref[:, cols], axis=1, keepdims=True) / total
        e = jnp.where(allowed, jnp.exp(dot_t(q, k) * SCALE), 0.0)
        de = dot_t(w, v)
        ds = (e * (de - corr)).astype(BF16)
        dq_ref[:, cols] = (dot(ds, k) * SCALE).astype(BF16)
        dk_acc[:, cols] += t_dot(ds, q)
        dv_acc[:, cols] += t_dot(e.astype(BF16), w)

    @pl.when(step == pl.num_programs(0) - 1)
    def _():
        dk_ref[...] = (dk_acc[...] * SCALE).astype(BF16)
        dv_ref[...] = dv_acc[...].astype(BF16)


def attn_specs(rows, wide, slots):
    qb = 256 if rows <= 1024 else 128
    q_spec = pl.BlockSpec((qb, wide), lambda i: (i, 0))
    l_spec = pl.BlockSpec((qb, slots), lambda i: (i, 0))
    all_spec = pl.BlockSpec((rows, wide), lambda i: (0, 0))
    qp_spec = pl.BlockSpec((qb, 1), lambda i: (i, 0))
    kp_spec = pl.BlockSpec((1, rows), lambda i: (0, 0))
    return rows // qb, q_spec, l_spec, all_spec, qp_spec, kp_spec


def attention_fwd(place, q, k, v, slots):
    rows, wide = q.shape
    steps, q_spec, l_spec, all_spec, qp_spec, kp_spec = attn_specs(rows, wide, slots)
    return pl.pallas_call(
        functools.partial(attn_fwd_body, slots),
        grid=(steps,),
        in_specs=[qp_spec, kp_spec, q_spec, all_spec, all_spec],
        out_specs=[q_spec, q_spec, l_spec],
        out_shape=[
            jax.ShapeDtypeStruct((rows, wide), BF16),
            jax.ShapeDtypeStruct((rows, wide), F32),
            jax.ShapeDtypeStruct((rows, slots), F32),
        ],
        name="attn_fwd",
        cost_estimate=pl.CostEstimate(
            flops=4 * rows * rows * wide, bytes_accessed=16 * rows * wide, transcendentals=rows * rows * slots
        ),
        compiler_params=pltpu.CompilerParams(vmem_limit_bytes=60 * 2**20),
    )(place.reshape(rows, 1), place.reshape(1, rows), q, k, v)


def attention_bwd(place, q, k, v, do, o, total, slots):
    rows, wide = q.shape
    steps, q_spec, l_spec, all_spec, qp_spec, kp_spec = attn_specs(rows, wide, slots)
    shape = jax.ShapeDtypeStruct((rows, wide), BF16)
    return pl.pallas_call(
        functools.partial(attn_bwd_body, slots),
        grid=(steps,),
        in_specs=[qp_spec, kp_spec, q_spec, all_spec, all_spec, q_spec, q_spec, l_spec],
        out_specs=[q_spec, all_spec, all_spec],
        out_shape=[shape, shape, shape],
        scratch_shapes=[pltpu.VMEM((rows, wide), F32), pltpu.VMEM((rows, wide), F32)],
        name="attn_bwd",
        cost_estimate=pl.CostEstimate(
            flops=10 * rows * rows * wide, bytes_accessed=24 * rows * wide, transcendentals=rows * rows * slots
        ),
        compiler_params=pltpu.CompilerParams(vmem_limit_bytes=60 * 2**20),
    )(place.reshape(rows, 1), place.reshape(1, rows), q, k, v, do, o, total)


def split_axis(n):
    across = 2 if n <= 8 else 4
    return n // across, across


def place_of(me, lines, across):
    a, b = lax.div(me, across), lax.rem(me, across)
    near = [(a < lines - 1, me + across), (a > 0, me - across), (b < across - 1, me + 1), (b > 0, me - 1)]
    return a, b, near


def turned_rows(rows, dtype, across):
    tile = 16 if dtype == BF16 else 8
    share = 4 if rows <= 128 else 5
    return rows // share // tile * tile if across == 2 else 0


def meet(near, peers):
    barrier = pltpu.get_barrier_semaphore()
    for exists, target in near:

        @pl.when(exists)
        def _(target=target):
            pl.semaphore_signal(barrier, inc=1, device_id={"ctx": target}, device_id_type=MESH)

    for axis, peer in peers:
        pl.semaphore_signal(barrier, inc=1, device_id={axis: peer}, device_id_type=MESH)
    pl.semaphore_wait(barrier, len(peers) + sum(exists.astype(jnp.int32) for exists, _ in near))


class Fsdp:
    def __init__(self, nf, gather_in, gather_out, red_in, red_out, scratch):
        self.gather_in, self.gather_out, self.red_in, self.red_out = gather_in, gather_out, red_in, red_out
        n_gather, n_red = len(gather_in), len(red_in)
        self.near_in, self.stage, self.far_in = scratch[:n_red], scratch[n_red : 2 * n_red], scratch[2 * n_red : 3 * n_red]
        self.keep_sem, self.g_send, self.g_recv, self.r_send, self.r_recv = scratch[3 * n_red : 3 * n_red + 5]
        self.f = lax.axis_index("fsdp")
        self.core = lax.rem(self.f, 2)
        self.mate = self.f + 1 - 2 * self.core
        self.pairs = nf // 2
        self.pair = lax.div(self.f, 2)
        self.other = [lax.rem(self.pair + k, self.pairs) for k in range(1, self.pairs)]
        self.peers = [self.mate] + [2 * y + self.core for y in self.other] if n_gather + n_red else []

    @staticmethod
    def scratch(nf, gather, red):
        pairs = nf // 2
        dma = pltpu.SemaphoreType.DMA
        out = []
        for _ in range(3):
            out += [pltpu.VMEM((pairs, *x.shape[1:]), x.dtype) for x in red]
        g, r = max(len(gather), 1), max(len(red), 1)
        return out + [dma((g,)), dma((g, 2, nf)), dma((g, nf)), dma((r, 2, pairs)), dma((r, 2, pairs))]

    def copy(self, src, dst, send, recv, target):
        return pltpu.make_async_remote_copy(
            src_ref=src, dst_ref=dst, send_sem=send, recv_sem=recv, device_id={"fsdp": target}, device_id_type=MESH
        )

    def spread(self, i, source, target, own):
        out = self.gather_out[i].at[source]
        send = self.g_send.at[i, 0, target] if own else self.g_send.at[i, 1, source]
        return self.copy(self.gather_in[i] if own else out, out, send, self.g_recv.at[i, source], target)

    def keep(self, i):
        return pltpu.make_async_copy(self.gather_in[i], self.gather_out[i].at[self.f], self.keep_sem.at[i])

    def to_mate(self, j, y):
        src = self.red_in[j].at[2 * y + 1 - self.core]
        return self.copy(src, self.near_in[j].at[y], self.r_send.at[j, 0, y], self.r_recv.at[j, 0, y], self.mate)

    def to_far(self, j, y, source):
        send, recv = self.r_send.at[j, 1, y], self.r_recv.at[j, 1, source]
        return self.copy(self.stage[j].at[y], self.far_in[j].at[source], send, recv, 2 * y + self.core)

    def write(self, j, value):
        out, first = self.red_out[j]
        out[:, first : first + value.shape[1]] = value.astype(out.dtype)

    def start(self):
        for j in range(len(self.red_in)):
            for y in range(self.pairs):
                self.to_mate(j, y).start()
        for i in range(len(self.gather_in)):
            for target in self.peers[1:] + self.peers[:1]:
                self.spread(i, self.f, target, True).start()
            self.keep(i).start()

    def middle(self):
        for j in range(len(self.red_in)):
            for y in range(self.pairs):
                self.to_mate(j, y).wait_recv()
            for y in self.other:
                value = self.red_in[j][2 * y + self.core].astype(F32) + self.near_in[j][y].astype(F32)
                self.stage[j][y] = value.astype(self.stage[j].dtype)
                self.to_far(j, y, self.pair).start()

    def end(self):
        for j in range(len(self.red_in)):
            value = self.red_in[j][self.f].astype(F32) + self.near_in[j][self.pair].astype(F32)
            for y in self.other:
                self.to_far(j, y, y).wait_recv()
                value = value + self.far_in[j][y].astype(F32)
            self.write(j, value)
        for i in range(len(self.gather_in)):
            for y in self.other:
                source = 2 * y + self.core
                self.spread(i, source, self.mate, False).wait_recv()
                self.spread(i, source, self.mate, False).start()

    def finish(self):
        for i in range(len(self.gather_in)):
            self.spread(i, self.mate, self.mate, False).wait_recv()
            for y in self.other:
                self.spread(i, 2 * y + 1 - self.core, self.mate, False).wait_recv()
            self.keep(i).wait()
            for target in self.peers:
                self.spread(i, self.f, target, True).wait_send()
            for y in self.other:
                self.spread(i, 2 * y + self.core, self.mate, False).wait_send()
        for j in range(len(self.red_in)):
            for y in range(self.pairs):
                self.to_mate(j, y).wait_send()
            for y in self.other:
                self.to_far(j, y, self.pair).wait_send()


def exchange_body(n, nf, counts, firsts, *refs):
    n_ctx, n_fsdp, n_own, n_red, n_pack = counts
    bounds = [0]
    for size in counts:
        bounds.append(bounds[-1] + size)
    ctx_in, fsdp_in, own_in, red_in, pack_in = (refs[i:j] for i, j in zip(bounds, bounds[1:]))
    refs = refs[bounds[-1] :]
    n_joint = len(firsts) - n_pack
    n_sums = n_red - n_joint + (1 if n_pack else 0)
    ctx_out, fsdp_out, own_out = refs[:n_ctx], refs[n_ctx : n_ctx + n_fsdp], refs[n_ctx + n_fsdp : n_ctx + n_fsdp + n_own]
    refs = refs[n_ctx + n_fsdp + n_own :]
    red_out, sums, scratch = refs[:n_sums], refs[n_sums : 2 * n_sums], refs[2 * n_sums :]
    copy_sem, send_sem, recv_sem = scratch[:3]
    goals = [(out, 0) for out in own_out]
    goals += [(sums[0], firsts[j]) for j in range(n_joint)]
    goals += [(out, 0) for out in sums[1 if n_pack else 0 :]]
    fs = Fsdp(nf, fsdp_in, fsdp_out, own_in + red_in, goals, scratch[3:])

    lines, across = split_axis(n)
    me = lax.axis_index("ctx")
    a, b, near = place_of(me, lines, across)
    gathered = list(zip(ctx_in, ctx_out)) + list(zip(sums, red_out))
    meet(near if gathered else [], [("fsdp", peer) for peer in fs.peers])
    fs.start()

    def part(i, turned):
        rows = gathered[i][1].shape[1]
        last = turned_rows(rows, gathered[i][1].dtype, across)
        return pl.ds(rows - last, last) if turned else pl.ds(0, rows - last)

    def turns(i):
        return bool(turned_rows(gathered[i][1].shape[1], gathered[i][1].dtype, across))

    def hop(i, block, way, turned=False, own=False):
        source, out = gathered[i]
        rows = part(i, turned)
        return pltpu.make_async_remote_copy(
            src_ref=source.at[rows] if own else out.at[block, rows],
            dst_ref=out.at[block, rows],
            send_sem=send_sem.at[i, way, block, int(turned)],
            recv_sem=recv_sem.at[i, way, block, int(turned)],
            device_id={"ctx": me + (across, -across, 1, -1)[way]},
            device_id_type=MESH,
        )

    def keep(i):
        return pltpu.make_async_copy(gathered[i][0], gathered[i][1].at[me], copy_sem.at[i])

    def each_own(i, act):
        for turned in (True, False) if turns(i) else (False,):
            for way in (2, 3, 0, 1):
                pl.when(near[way][0])(lambda way=way: act(hop(i, me, way, turned, True)))

    def each_twin(i, wait, act):
        if turns(i):
            twin = me + 1 - 2 * b
            for way in (2, 3):

                @pl.when(near[5 - way][0])
                def _(way=way):
                    if wait:
                        hop(i, twin, way, True).wait_recv()
                    for on in (0, 1):
                        pl.when(near[on][0])(lambda on=on: act(hop(i, twin, on, True)))

    def each_relay(i, d, wait, act):
        for way, there, shift in ((0, a >= d, -d * across), (1, a + d < lines, d * across)):

            @pl.when(there)
            def _(way=way, shift=shift):
                for turned, block in [(False, me + shift)] + (
                    [(True, me + shift), (True, me + 1 - 2 * b + shift)] if turns(i) else []
                ):
                    if wait:
                        hop(i, block, way, turned).wait_recv()
                    for on in (way,) if turned else (2, 3, way):
                        pl.when(near[on][0])(lambda on=on: act(hop(i, block, on, turned)))

    def start(copy):
        copy.start()

    def wait_send(copy):
        copy.wait_send()

    for i in range(n_ctx):
        each_own(i, start)
        keep(i).start()
    fs.middle()
    for j in range(n_pack):
        first = firsts[n_joint + j]
        sums[0][:, first : first + pack_in[j].shape[1]] = pack_in[j][...]
    for i in range(len(gathered)):
        if i == n_ctx:
            fs.end()
            for j in range(n_ctx, len(gathered)):
                each_own(j, start)
                keep(j).start()
        each_twin(i, True, start)
        for d in range(1, lines):
            each_relay(i, d, True, start)

    for i in range(len(gathered)):
        for d in range(1, across):
            for step in range(lines):
                for sign in (1, -1) if step else (1,):
                    for way, there, shift in ((2, b >= d, -d), (3, b + d < across, d)):
                        other = a + sign * step

                        @pl.when(there & (other >= 0) & (other < lines))
                        def _(i=i, source=other * across + b + shift, way=way):
                            hop(i, source, way).wait_recv()
                            if d < across - 1:
                                pl.when(near[way][0])(lambda: hop(i, source, way).start())

    if len(gathered) == n_ctx:
        fs.end()

    for i in range(len(gathered)):
        keep(i).wait()
        each_own(i, wait_send)
        each_twin(i, False, wait_send)
        for d in range(1, lines):
            each_relay(i, d, False, wait_send)
        for d in range(1, across - 1):
            for line in range(lines):
                for way, there, shift in ((2, b >= d, -d), (3, b + d < across, d)):

                    @pl.when(there & near[way][0])
                    def _(i=i, source=line * across + b + shift, way=way):
                        hop(i, source, way).wait_send()

    fs.finish()


def exchange(call, n, nf, ctx=(), fsdp=(), own=(), red=(), pack=(), firsts=()):
    shape = jax.ShapeDtypeStruct
    sums = [shape(x.shape[1:], x.dtype) for x in red]
    if pack:
        joint = len(firsts) - len(pack)
        width = sum(x.shape[1] for x in [*sums[:joint], *pack])
        sums = [shape((pack[0].shape[0], width), pack[0].dtype)] + sums[joint:]
    outs = [shape((n, *x.shape), x.dtype) for x in ctx]
    outs += [shape((nf, *x.shape), x.dtype) for x in fsdp]
    outs += [shape(x.shape[1:], x.dtype) for x in own]
    outs += [shape((n, *x.shape), x.dtype) for x in sums]
    gathered = max(len(ctx) + len(sums), 1)
    any_spec, vmem_spec = pl.BlockSpec(memory_space=pl.ANY), pl.BlockSpec(memory_space=pltpu.VMEM)
    inputs = (*ctx, *fsdp, *own, *red, *pack)
    return pl.pallas_call(
        functools.partial(exchange_body, n, nf, (len(ctx), len(fsdp), len(own), len(red), len(pack)), firsts),
        in_specs=[vmem_spec] * len(inputs),
        out_specs=[any_spec] * (len(ctx) + len(fsdp)) + [vmem_spec] * len(own) + [any_spec] * len(sums),
        out_shape=outs,
        scratch_shapes=[pltpu.VMEM(x.shape, x.dtype) for x in sums]
        + [
            pltpu.SemaphoreType.DMA((gathered,)),
            pltpu.SemaphoreType.DMA((gathered, 4, n, 2)),
            pltpu.SemaphoreType.DMA((gathered, 4, n, 2)),
        ]
        + Fsdp.scratch(nf, fsdp, [*own, *red]),
        name=f"exchange_{call}",
        compiler_params=pltpu.CompilerParams(collective_id=call, has_side_effects=True, vmem_limit_bytes=60 * 2**20),
    )(*inputs)


def product_body(n, n_sides, transposed, *refs):
    left, right = refs[:2]
    side_in, refs = refs[2 : 2 + 2 * n_sides], refs[2 + 2 * n_sides :]
    out, side_out, refs = refs[0], refs[1 : 1 + n_sides], refs[1 + n_sides :]
    part, acc, acc_t, over_in, sums, sums_t, line_in, line_in_t, twin_in = refs[:9]
    o_send, o_recv, l_send, l_recv, t_send, t_recv, w_send, w_recv = refs[9:]

    lines, across = split_axis(n)
    me = lax.axis_index("ctx")
    a, b, near = place_of(me, lines, across)
    rows = out.shape[0]
    last = turned_rows(rows, BF16, across)
    head, tail = pl.ds(0, rows - last), pl.ds(rows - last, last)
    peers = [me - b + lax.rem(b + k, across) for k in range(1, across)]
    meet(near[:2], [("ctx", peer) for peer in peers])

    def copy(src, dst, send, recv, target):
        return pltpu.make_async_remote_copy(
            src_ref=src, dst_ref=dst, send_sem=send, recv_sem=recv, device_id={"ctx": target}, device_id_type=MESH
        )

    def over(line, k):
        src = part.at[line, lax.rem(b + k, across), head]
        return copy(src, over_in.at[k - 1, line], o_send.at[k - 1, line], o_recv.at[k - 1, line], peers[k - 1])

    def along(line, way):
        target = me + (across, -across)[way]
        return copy(sums.at[line], line_in.at[way, line], l_send.at[way, line], l_recv.at[way, line], target)

    def along_t(line, way):
        target = me + (across, -across)[way]
        return copy(sums_t.at[line], line_in_t.at[way, line], t_send.at[way, line], t_recv.at[way, line], target)

    def twin():
        return copy(sums_t.at[a, 1 - b], twin_in, w_send, w_recv, peers[0])

    order = []
    for k in range(lines):
        line = jnp.int32(0)
        for av in range(lines):
            line = jnp.where(a == av, sorted(range(lines), key=lambda j: (-abs(j - av), j))[k], line)
        order.append(line)

    for line in order:
        lhs = left[pl.ds(pl.multiple_of(line * across * rows, across * rows), across * rows), :]
        value = dot_t(lhs, right[...]) if transposed else dot(lhs, right[...])
        part[line] = value.astype(BF16).reshape(across, rows, value.shape[1])
        for k in range(1, across):
            over(line, k).start()
    for step, line in enumerate(order[:-1]):
        for j in range(step * n_sides // (lines - 1), (step + 1) * n_sides // (lines - 1)):
            side_out[j][...] = t_dot(side_in[2 * j][...], side_in[2 * j + 1][...]).astype(BF16)
        up, down = line > a, line < a
        if last:
            acc_t[...] = part[line, :, tail].astype(F32)
            for way, there in ((0, up & (a > 0)), (1, down & (a < lines - 1))):

                @pl.when(there)
                def _(way=way, line=line):
                    along_t(line, way).wait_recv()
                    acc_t[...] += line_in_t[way, line].astype(F32)

            sums_t[line] = acc_t[...].astype(BF16)
            pl.when(up)(lambda line=line: along_t(line, 0).start())
            pl.when(down)(lambda line=line: along_t(line, 1).start())
        value = part[line, b, head].astype(F32)
        for k in range(1, across):
            over(line, k).wait_recv()
            value = value + over_in[k - 1, line].astype(F32)
        acc[...] = value
        for way, there in ((0, up & (a > 0)), (1, down & (a < lines - 1))):

            @pl.when(there)
            def _(way=way, line=line):
                along(line, way).wait_recv()
                acc[...] += line_in[way, line].astype(F32)

        sums[line] = acc[...].astype(BF16)
        pl.when(up)(lambda line=line: along(line, 0).start())
        pl.when(down)(lambda line=line: along(line, 1).start())

    if last:
        acc_t[...] = part[a, :, tail].astype(F32)
        for way in range(2):

            @pl.when(near[1 - way][0])
            def _(way=way):
                along_t(a, way).wait_recv()
                acc_t[...] += line_in_t[way, a].astype(F32)

        sums_t[a] = acc_t[...].astype(BF16)
        twin().start()
    value = part[a, b, head].astype(F32)
    for k in range(1, across):
        over(a, k).wait_recv()
        value = value + over_in[k - 1, a].astype(F32)
    acc[...] = value
    for way in range(2):

        @pl.when(near[1 - way][0])
        def _(way=way):
            along(a, way).wait_recv()
            acc[...] += line_in[way, a].astype(F32)

    out[head, :] = acc[...]
    if last:
        twin().wait_recv()
        out[tail, :] = acc_t[b] + twin_in[...].astype(F32)

    for line in order:
        for k in range(1, across):
            over(line, k).wait_send()
    for line in order[:-1]:
        for way, there in ((0, line > a), (1, line < a)):

            @pl.when(there)
            def _(way=way, line=line):
                along(line, way).wait_send()
                if last:
                    along_t(line, way).wait_send()

    if last:
        twin().wait_send()


def product(call, n, left, right, transposed=False, sides=()):
    if sides and left.shape[0] > 1024:
        (total,) = product(call, n, left, right, transposed)
        return [total] + [t_dot(x, y).astype(BF16) for x, y in sides]
    rows, width = left.shape[0] // n, right.shape[0 if transposed else 1]
    lines, across = split_axis(n)
    last = turned_rows(rows, BF16, across)
    some = max(last, 16)
    shape = jax.ShapeDtypeStruct
    vmem, dma = pltpu.VMEM, pltpu.SemaphoreType.DMA
    outs = [shape((rows, width), F32)]
    outs += [shape((x.shape[1], y.shape[1]), BF16) for x, y in sides]
    return pl.pallas_call(
        functools.partial(product_body, n, len(sides), transposed),
        in_specs=[pl.BlockSpec(memory_space=vmem)] * (2 + 2 * len(sides)),
        out_specs=[pl.BlockSpec(memory_space=vmem)] * len(outs),
        out_shape=outs,
        scratch_shapes=[
            vmem((lines, across, rows, width), BF16),
            vmem((rows - last, width), F32),
            vmem((across, some, width), F32),
            vmem((across - 1, lines, rows - last, width), BF16),
            vmem((lines, rows - last, width), BF16),
            vmem((lines, across, some, width), BF16),
            vmem((2, lines, rows - last, width), BF16),
            vmem((2, lines, across, some, width), BF16),
            vmem((some, width), BF16),
            dma((across - 1, lines)),
            dma((across - 1, lines)),
            dma((2, lines)),
            dma((2, lines)),
            dma((2, lines)),
            dma((2, lines)),
            dma,
            dma,
        ],
        name=f"product_{call}",
        compiler_params=pltpu.CompilerParams(collective_id=call, has_side_effects=True, vmem_limit_bytes=63 * 2**20),
    )(left, right, *[z for pair in sides for z in pair])


def columns_body(moves, in_ref, out_ref):
    for block, start, goal, size in moves:
        out_ref[:, goal : goal + size] = in_ref[block, :, start : start + size].astype(F32)


def place_columns(value, moves, width):
    n, rows, part = value.shape
    step = next(s for s in (80, 16, rows) if rows % s == 0)
    return pl.pallas_call(
        functools.partial(columns_body, tuple(moves)),
        grid=(rows // step,),
        in_specs=[pl.BlockSpec((n, step, part), lambda i: (0, i, 0))],
        out_specs=pl.BlockSpec((step, width), lambda i: (i, 0)),
        out_shape=jax.ShapeDtypeStruct((rows, width), F32),
        name="place_columns",
        cost_estimate=pl.CostEstimate(flops=0, bytes_accessed=6 * rows * width, transcendentals=0),
        compiler_params=pltpu.CompilerParams(vmem_limit_bytes=48 * 2**20),
    )(value)


def head_moves(n, heads, offset, goal):
    base, rest = divmod(heads, n)
    moves = [(c, offset, goal + c * base * HEAD_DIM, base * HEAD_DIM) for c in range(n) if base]
    moves += [
        (c, offset + base * HEAD_DIM, goal + (base * n + c) * HEAD_DIM, HEAD_DIM) for c in range(rest)
    ]
    return moves


def ag_ctx(value):
    return lax.all_gather(value, "ctx", axis=0, tiled=True)


def rs_ctx(value):
    return lax.psum_scatter(value.astype(BF16), "ctx", scatter_dimension=0, tiled=True)


def ag_fsdp(value):
    return lax.all_gather(value, "fsdp", axis=0, tiled=True)


def head_columns(value, width, c, n):
    heads = width // HEAD_DIM
    base, rest = divmod(heads, n)
    parts = []
    if base:
        parts.append(lax.dynamic_slice_in_dim(value, c * base * HEAD_DIM, base * HEAD_DIM, axis=-1))
    if rest:
        start = jnp.minimum(base * n + c, heads - 1) * HEAD_DIM
        extra = lax.dynamic_slice_in_dim(value, start, HEAD_DIM, axis=-1)
        parts.append(jnp.where(c < rest, extra, jnp.zeros_like(extra)))
    return jnp.concatenate(parts, axis=-1)


def spread_heads(value, heads, n):
    base, rest = divmod(heads, n)
    rows = value.shape[1]
    parts = []
    if base:
        body = value[:, :, : base * HEAD_DIM]
        parts.append(jnp.transpose(body, (1, 0, 2)).reshape(rows, n * base * HEAD_DIM))
    if rest:
        tail = value[:rest, :, base * HEAD_DIM :]
        parts.append(jnp.transpose(tail, (1, 0, 2)).reshape(rows, rest * HEAD_DIM))
    return jnp.concatenate(parts, axis=1)


def place_heads(value, heads, c, n):
    base, rest = divmod(heads, n)
    out = jnp.zeros((heads * HEAD_DIM,), value.dtype)
    if rest:
        start = jnp.minimum(base * n + c, heads - 1) * HEAD_DIM
        extra = jnp.where(c < rest, value[base * HEAD_DIM :], 0.0)
        out = lax.dynamic_update_slice(out, extra, (start,))
    if base:
        out = lax.dynamic_update_slice(out, value[: base * HEAD_DIM], (c * base * HEAD_DIM,))
    return out


def head_rows(value, heads, c, f, n):
    base, rest = divmod(heads, n)
    local, width = value.shape
    pad = max(base, 1) * HEAD_DIM
    padded = jnp.pad(value, ((pad, pad), (0, 0)))
    parts = []
    if base:
        start = jnp.clip(c * base * HEAD_DIM - f * local + pad, 0, local + 2 * pad - base * HEAD_DIM)
        parts.append(lax.dynamic_slice_in_dim(padded, start, base * HEAD_DIM, axis=0))
    if rest:
        start = jnp.clip((base * n + c) * HEAD_DIM - f * local + pad, 0, local + 2 * pad - HEAD_DIM)
        extra = lax.dynamic_slice_in_dim(padded, start, HEAD_DIM, axis=0)
        parts.append(jnp.where(c < rest, extra, jnp.zeros_like(extra)))
    return jnp.concatenate(parts, axis=0)


def on_device(
    tokens,
    ln1_gain,
    ln1_shift,
    qkv_weight,
    qv_bias,
    out_weight,
    out_bias,
    ln2_gain,
    ln2_shift,
    up_weight,
    up_bias,
    down_weight,
    down_bias,
    block_table,
    cotangent,
):
    rows, width = tokens.shape[1:]
    heads = width // HEAD_DIM
    n = lax.axis_size("ctx")
    nf = lax.axis_size("fsdp")
    c = lax.axis_index("ctx")
    f = lax.axis_index("fsdp")
    slots = -(-heads // n)
    wide = slots * HEAD_DIM
    half = rows // 2
    local = width // nf
    ff = up_weight.shape[1]
    ff_local = ff // nf
    ff_part = ff_local // n

    within = jnp.arange(rows, dtype=jnp.int32)
    block_of = jnp.where(within[None, :] < half, block_table[:, None], 2 * n - 1 - block_table[:, None])
    place = (block_of * half + within[None, :] % half).reshape(-1)

    vectors = (ln1_gain, ln1_shift, qv_bias, out_bias, ln2_gain, ln2_shift, up_bias, down_bias)
    flat = jnp.concatenate(vectors)
    flat = jnp.pad(flat, (0, -flat.shape[0] % 2048)).reshape(-1, 128)
    q_w = head_columns(qkv_weight[:, :width], width, c, n)
    k_w = head_columns(qkv_weight[:, width : 2 * width], width, c, n)
    v_w = head_columns(qkv_weight[:, 2 * width :], width, c, n)
    x_all, packed, w_qkv = exchange(0, n, nf, ctx=[tokens[0]], fsdp=[flat, jnp.concatenate([q_w, k_w, v_w], axis=1)])
    x_all = x_all.reshape(n * rows, width)
    w_qkv = w_qkv.reshape(width, 3 * wide)
    cotangent, packed = lax.optimization_barrier((cotangent, packed))
    packed = packed.reshape(nf, -1)
    full, at = [], 0
    for vector in vectors:
        size = vector.shape[0]
        full.append(packed[:, at : at + size].reshape(-1).astype(F32))
        at += size
    gain1, shift1, b_qv, b_out, gain2, shift2, b_up, b_down = full

    w_out = lax.psum(head_rows(out_weight, heads, c, f, n), "fsdp")
    g2_all = ag_ctx(cotangent[0])
    b_up_mine = lax.dynamic_slice_in_dim(b_up.reshape(nf, n, ff_part), c, 1, axis=1).reshape(-1)
    bq = head_columns(b_qv[:width], width, c, n)
    bv = head_columns(b_qv[width:], width, c, n)

    n1_all, _ = ln_stats(x_all.astype(F32))
    act1 = (n1_all * gain1 + shift1).astype(BF16)
    proj = dot(act1, w_qkv)
    q = (proj[:, :wide] + bq).astype(BF16)
    k = proj[:, wide : 2 * wide].astype(BF16)
    v = (proj[:, 2 * wide :] + bv).astype(BF16)
    attn, o, total = attention_fwd(place, q, k, v, slots)
    up_weight, down_weight, attn = lax.optimization_barrier((up_weight, down_weight, attn))
    up_mine = [lax.dynamic_slice_in_dim(up_weight, i * ff_local + c * ff_part, ff_part, axis=1) for i in range(nf)]
    w_up = ag_fsdp(jnp.concatenate(up_mine, axis=1))
    w_down = ag_fsdp(lax.dynamic_slice_in_dim(down_weight, c * ff_part, ff_part, axis=0))
    x = tokens[0].astype(F32)
    (mixed,) = product(1, n, attn, w_out)
    mid = x + mixed + b_out
    attn_all = spread_heads(lax.all_gather(attn, "ctx", axis=0, tiled=False), heads, n)

    n2, rstd2 = ln_stats(mid)
    (act2,) = exchange(2, n, nf, ctx=[(n2 * gain2 + shift2).astype(BF16)])
    act2 = act2.reshape(n * rows, width)
    u = dot(act2, w_up) + b_up_mine
    activated, gelu_back = jax.vjp(lambda t: jax.nn.gelu(t, approximate=True), u)
    hidden = activated.astype(BF16)
    dh = dot_t(g2_all, w_down)
    du = gelu_back(dh)[0].astype(BF16)
    da2, d_up, d_down = product(3, n, du, w_up, True, sides=[(act2, du), (hidden, g2_all)])
    d_up = d_up.reshape(nf, local, nf * ff_part)
    d_down = d_down.reshape(nf, ff_part, width)
    d_up_bias = jnp.sum(du.astype(F32), axis=0)
    grad_out = cotangent[0].astype(F32)
    d_down_bias = jnp.sum(grad_out, axis=0)

    d_gain2 = jnp.sum(da2 * n2, axis=0)
    d_shift2 = jnp.sum(da2, axis=0)
    d_mid = grad_out + ln_back(da2, n2, rstd2, gain2)
    g1 = d_mid.astype(BF16)
    d_out_bias = jnp.sum(g1.astype(F32), axis=0)
    g1_all, d_up, d_down = exchange(4, n, nf, ctx=[g1], own=[d_up, d_down])
    g1_all = g1_all.reshape(n * rows, width)
    hidden, g1_all = lax.optimization_barrier((hidden, g1_all))
    result = mid + rs_ctx(dot(hidden, w_down)).astype(F32) + b_down
    d_attn = dot_t(g1_all, w_out)
    gq, gk, gv = attention_bwd(place, q, k, v, d_attn, o, total, slots)
    g_qkv = jnp.concatenate([gq, gk, gv], axis=1)
    out_part = width // n
    g1_mine = lax.dynamic_slice_in_dim(g1_all, c * out_part, out_part, axis=1)
    da1, d_qkv, d_out = product(5, n, g_qkv, w_qkv, True, sides=[(act1, g_qkv), (attn_all, g1_mine)])
    d_qkv = d_qkv.reshape(nf, local, 3 * wide)
    d_out = d_out.reshape(nf, local, out_part)

    n1, rstd1 = ln_stats(x)
    d_gain1 = jnp.sum(da1 * n1, axis=0)
    d_shift1 = jnp.sum(da1, axis=0)
    input_grad = d_mid + ln_back(da1, n1, rstd1, gain1)

    dq_bias = place_heads(jnp.sum(gq.astype(F32), axis=0), heads, c, n)
    dv_bias = place_heads(jnp.sum(gv.astype(F32), axis=0), heads, c, n)
    up_placed = lax.dynamic_update_slice(
        jnp.zeros((nf, n, ff_part), F32), d_up_bias.reshape(nf, 1, ff_part), (0, c, 0)
    )
    smalls = (
        d_gain1,
        d_shift1,
        jnp.concatenate([dq_bias, dv_bias]),
        d_out_bias,
        d_gain2,
        d_shift2,
        up_placed.reshape(-1),
        d_down_bias,
    )
    packed = jnp.concatenate([s.reshape(nf, -1) for s in smalls], axis=1)
    packed = jnp.pad(packed, ((0, 0), (0, -packed.shape[1] % 1024))).reshape(nf, -1, 128)
    at_up, at_out = 3 * wide, 3 * wide + nf * ff_part
    d_down, joint, packed = exchange(
        6, n, nf, ctx=[d_down], red=[d_qkv, d_out, packed], pack=[d_up], firsts=(0, at_out, at_up)
    )
    mine = jnp.sum(packed, axis=0).reshape(-1)
    d_up_full = place_columns(
        joint,
        [(i, at_up + j * ff_part, j * ff_local + i * ff_part, ff_part) for i in range(n) for j in range(nf)],
        ff,
    )
    d_down_full = d_down.reshape(ff_local, width).astype(F32)
    d_out_full = place_columns(joint, [(i, at_out, i * out_part, out_part) for i in range(n)], width)
    moves = [m for i in range(3) for m in head_moves(n, heads, i * wide, i * width)]
    d_qkv_full = place_columns(joint, moves, 3 * width)
    out, at = [], 0
    for s in smalls:
        size = s.size // nf
        out.append(mine[at : at + size])
        at += size
    return (
        result[None],
        input_grad[None],
        out[0],
        out[1],
        d_qkv_full,
        out[2],
        d_out_full,
        out[3],
        out[4],
        out[5],
        d_up_full,
        out[6],
        d_down_full,
        out[7],
    )


def solution(mesh):
    rows, one, two = P("fsdp", "ctx", None), P("fsdp"), P("fsdp", None)
    return jax.shard_map(
        on_device,
        mesh=mesh,
        in_specs=(rows, one, one, two, one, two, one, one, one, two, one, two, one, P(), rows),
        out_specs=(rows, rows, one, one, two, one, two, one, one, one, two, one, two, one),
        check_vma=False,
    )
```

```python
import functools

import jax
import jax.numpy as jnp
from jax import lax
from jax.experimental import pallas as pl
from jax.experimental.pallas import tpu as pltpu
from jax.sharding import PartitionSpec as P

HEAD_DIM = 64
EPS = 1e-05
SCALE = 0.125
F32 = jnp.float32
BF16 = jnp.bfloat16
MESH = pl.DeviceIdType.MESH


def dot(left, right):
    return jnp.dot(left, right, preferred_element_type=F32)


def dot_t(left, right):
    return lax.dot_general(left, right, (((1,), (1,)), ((), ())), preferred_element_type=F32)


def t_dot(left, right):
    return lax.dot_general(left, right, (((0,), (0,)), ((), ())), preferred_element_type=F32)


def ln_stats(value):
    centre = value - jnp.mean(value, axis=-1, keepdims=True)
    spread = jnp.mean(centre * centre, axis=-1, keepdims=True)
    rstd = lax.rsqrt(spread + EPS)
    return centre * rstd, rstd


def ln_back(grad, normed, rstd, gain):
    dn = grad * gain
    first = jnp.mean(dn, axis=-1, keepdims=True)
    second = jnp.mean(dn * normed, axis=-1, keepdims=True)
    return (dn - first - normed * second) * rstd


def attn_fwd_body(slots, qp_ref, kp_ref, q_ref, k_ref, v_ref, attn_ref, o_ref, l_ref):
    allowed = kp_ref[...] <= qp_ref[...]
    for h in range(slots):
        cols = slice(h * HEAD_DIM, (h + 1) * HEAD_DIM)
        raw = dot_t(q_ref[:, cols], k_ref[:, cols])
        e = jnp.where(allowed, jnp.exp(raw * SCALE), 0.0)
        total = jnp.sum(e, axis=1, keepdims=True)
        numer = dot(e.astype(BF16), v_ref[:, cols])
        o = numer / total
        o_ref[:, cols] = o
        attn_ref[:, cols] = o.astype(BF16)
        l_ref[:, h : h + 1] = total


def attn_bwd_body(
    slots, qp_ref, kp_ref, q_ref, k_ref, v_ref, do_ref, o_ref, l_ref, dq_ref, dk_ref, dv_ref, dk_acc, dv_acc
):
    step = pl.program_id(0)

    @pl.when(step == 0)
    def _():
        dk_acc[...] = jnp.zeros_like(dk_acc)
        dv_acc[...] = jnp.zeros_like(dv_acc)

    allowed = kp_ref[...] <= qp_ref[...]
    for h in range(slots):
        cols = slice(h * HEAD_DIM, (h + 1) * HEAD_DIM)
        q = q_ref[:, cols]
        k = k_ref[:, cols]
        v = v_ref[:, cols]
        do = do_ref[:, cols]
        total = l_ref[:, h : h + 1]
        w = (do / total).astype(BF16)
        corr = jnp.sum(do * o_ref[:, cols], axis=1, keepdims=True) / total
        e = jnp.where(allowed, jnp.exp(dot_t(q, k) * SCALE), 0.0)
        de = dot_t(w, v)
        ds = (e * (de - corr)).astype(BF16)
        dq_ref[:, cols] = (dot(ds, k) * SCALE).astype(BF16)
        dk_acc[:, cols] += t_dot(ds, q)
        dv_acc[:, cols] += t_dot(e.astype(BF16), w)

    @pl.when(step == pl.num_programs(0) - 1)
    def _():
        dk_ref[...] = (dk_acc[...] * SCALE).astype(BF16)
        dv_ref[...] = dv_acc[...].astype(BF16)


def attn_specs(rows, wide, slots):
    qb = 256 if rows <= 1024 else 128
    q_spec = pl.BlockSpec((qb, wide), lambda i: (i, 0))
    l_spec = pl.BlockSpec((qb, slots), lambda i: (i, 0))
    all_spec = pl.BlockSpec((rows, wide), lambda i: (0, 0))
    qp_spec = pl.BlockSpec((qb, 1), lambda i: (i, 0))
    kp_spec = pl.BlockSpec((1, rows), lambda i: (0, 0))
    return rows // qb, q_spec, l_spec, all_spec, qp_spec, kp_spec


def attention_fwd(place, q, k, v, slots):
    rows, wide = q.shape
    steps, q_spec, l_spec, all_spec, qp_spec, kp_spec = attn_specs(rows, wide, slots)
    return pl.pallas_call(
        functools.partial(attn_fwd_body, slots),
        grid=(steps,),
        in_specs=[qp_spec, kp_spec, q_spec, all_spec, all_spec],
        out_specs=[q_spec, q_spec, l_spec],
        out_shape=[
            jax.ShapeDtypeStruct((rows, wide), BF16),
            jax.ShapeDtypeStruct((rows, wide), F32),
            jax.ShapeDtypeStruct((rows, slots), F32),
        ],
        name="attn_fwd",
        cost_estimate=pl.CostEstimate(
            flops=4 * rows * rows * wide, bytes_accessed=16 * rows * wide, transcendentals=rows * rows * slots
        ),
        compiler_params=pltpu.CompilerParams(vmem_limit_bytes=60 * 2**20),
    )(place.reshape(rows, 1), place.reshape(1, rows), q, k, v)


def attention_bwd(place, q, k, v, do, o, total, slots):
    rows, wide = q.shape
    steps, q_spec, l_spec, all_spec, qp_spec, kp_spec = attn_specs(rows, wide, slots)
    shape = jax.ShapeDtypeStruct((rows, wide), BF16)
    return pl.pallas_call(
        functools.partial(attn_bwd_body, slots),
        grid=(steps,),
        in_specs=[qp_spec, kp_spec, q_spec, all_spec, all_spec, q_spec, q_spec, l_spec],
        out_specs=[q_spec, all_spec, all_spec],
        out_shape=[shape, shape, shape],
        scratch_shapes=[pltpu.VMEM((rows, wide), F32), pltpu.VMEM((rows, wide), F32)],
        name="attn_bwd",
        cost_estimate=pl.CostEstimate(
            flops=10 * rows * rows * wide, bytes_accessed=24 * rows * wide, transcendentals=rows * rows * slots
        ),
        compiler_params=pltpu.CompilerParams(vmem_limit_bytes=60 * 2**20),
    )(place.reshape(rows, 1), place.reshape(1, rows), q, k, v, do, o, total)


def split_axis(n):
    across = 2 if n <= 8 else 4
    return n // across, across


def place_of(me, lines, across):
    a, b = lax.div(me, across), lax.rem(me, across)
    near = [(a < lines - 1, me + across), (a > 0, me - across), (b < across - 1, me + 1), (b > 0, me - 1)]
    return a, b, near


def turned_rows(rows, dtype, across):
    tile = 16 if dtype == BF16 else 8
    share = 4 if rows <= 128 else 5
    return rows // share // tile * tile if across == 2 else 0


def meet(near, peers):
    barrier = pltpu.get_barrier_semaphore()
    for exists, target in near:

        @pl.when(exists)
        def _(target=target):
            pl.semaphore_signal(barrier, inc=1, device_id={"ctx": target}, device_id_type=MESH)

    for axis, peer in peers:
        pl.semaphore_signal(barrier, inc=1, device_id={axis: peer}, device_id_type=MESH)
    pl.semaphore_wait(barrier, len(peers) + sum(exists.astype(jnp.int32) for exists, _ in near))


class Fsdp:
    def __init__(self, nf, gather_in, gather_out, red_in, red_out, scratch):
        self.gather_in, self.gather_out, self.red_in, self.red_out = gather_in, gather_out, red_in, red_out
        n_gather, n_red = len(gather_in), len(red_in)
        self.near_in, self.stage, self.far_in = scratch[:n_red], scratch[n_red : 2 * n_red], scratch[2 * n_red : 3 * n_red]
        self.keep_sem, self.g_send, self.g_recv, self.r_send, self.r_recv = scratch[3 * n_red : 3 * n_red + 5]
        self.f = lax.axis_index("fsdp")
        self.core = lax.rem(self.f, 2)
        self.mate = self.f + 1 - 2 * self.core
        self.pairs = nf // 2
        self.pair = lax.div(self.f, 2)
        self.other = [lax.rem(self.pair + k, self.pairs) for k in range(1, self.pairs)]
        self.peers = [self.mate] + [2 * y + self.core for y in self.other] if n_gather + n_red else []

    @staticmethod
    def scratch(nf, gather, red):
        pairs = nf // 2
        dma = pltpu.SemaphoreType.DMA
        out = []
        for _ in range(3):
            out += [pltpu.VMEM((pairs, *x.shape[1:]), x.dtype) for x in red]
        g, r = max(len(gather), 1), max(len(red), 1)
        return out + [dma((g,)), dma((g, 2, nf)), dma((g, nf)), dma((r, 2, pairs)), dma((r, 2, pairs))]

    def copy(self, src, dst, send, recv, target):
        return pltpu.make_async_remote_copy(
            src_ref=src, dst_ref=dst, send_sem=send, recv_sem=recv, device_id={"fsdp": target}, device_id_type=MESH
        )

    def spread(self, i, source, target, own):
        out = self.gather_out[i].at[source]
        send = self.g_send.at[i, 0, target] if own else self.g_send.at[i, 1, source]
        return self.copy(self.gather_in[i] if own else out, out, send, self.g_recv.at[i, source], target)

    def keep(self, i):
        return pltpu.make_async_copy(self.gather_in[i], self.gather_out[i].at[self.f], self.keep_sem.at[i])

    def to_mate(self, j, y):
        src = self.red_in[j].at[2 * y + 1 - self.core]
        return self.copy(src, self.near_in[j].at[y], self.r_send.at[j, 0, y], self.r_recv.at[j, 0, y], self.mate)

    def to_far(self, j, y, source):
        send, recv = self.r_send.at[j, 1, y], self.r_recv.at[j, 1, source]
        return self.copy(self.stage[j].at[y], self.far_in[j].at[source], send, recv, 2 * y + self.core)

    def write(self, j, value):
        out, first = self.red_out[j]
        out[:, first : first + value.shape[1]] = value.astype(out.dtype)

    def start(self):
        for j in range(len(self.red_in)):
            for y in range(self.pairs):
                self.to_mate(j, y).start()
        for i in range(len(self.gather_in)):
            for target in self.peers[1:] + self.peers[:1]:
                self.spread(i, self.f, target, True).start()
            self.keep(i).start()

    def middle(self):
        for j in range(len(self.red_in)):
            for y in range(self.pairs):
                self.to_mate(j, y).wait_recv()
            for y in self.other:
                value = self.red_in[j][2 * y + self.core].astype(F32) + self.near_in[j][y].astype(F32)
                self.stage[j][y] = value.astype(self.stage[j].dtype)
                self.to_far(j, y, self.pair).start()

    def end(self):
        for j in range(len(self.red_in)):
            value = self.red_in[j][self.f].astype(F32) + self.near_in[j][self.pair].astype(F32)
            for y in self.other:
                self.to_far(j, y, y).wait_recv()
                value = value + self.far_in[j][y].astype(F32)
            self.write(j, value)
        for i in range(len(self.gather_in)):
            for y in self.other:
                source = 2 * y + self.core
                self.spread(i, source, self.mate, False).wait_recv()
                self.spread(i, source, self.mate, False).start()

    def finish(self):
        for i in range(len(self.gather_in)):
            self.spread(i, self.mate, self.mate, False).wait_recv()
            for y in self.other:
                self.spread(i, 2 * y + 1 - self.core, self.mate, False).wait_recv()
            self.keep(i).wait()
            for target in self.peers:
                self.spread(i, self.f, target, True).wait_send()
            for y in self.other:
                self.spread(i, 2 * y + self.core, self.mate, False).wait_send()
        for j in range(len(self.red_in)):
            for y in range(self.pairs):
                self.to_mate(j, y).wait_send()
            for y in self.other:
                self.to_far(j, y, self.pair).wait_send()


def exchange_body(n, nf, counts, firsts, *refs):
    n_ctx, n_fsdp, n_own, n_red, n_pack = counts
    bounds = [0]
    for size in counts:
        bounds.append(bounds[-1] + size)
    ctx_in, fsdp_in, own_in, red_in, pack_in = (refs[i:j] for i, j in zip(bounds, bounds[1:]))
    refs = refs[bounds[-1] :]
    n_joint = len(firsts) - n_pack
    n_sums = n_red - n_joint + (1 if n_pack else 0)
    ctx_out, fsdp_out, own_out = refs[:n_ctx], refs[n_ctx : n_ctx + n_fsdp], refs[n_ctx + n_fsdp : n_ctx + n_fsdp + n_own]
    refs = refs[n_ctx + n_fsdp + n_own :]
    red_out, sums, scratch = refs[:n_sums], refs[n_sums : 2 * n_sums], refs[2 * n_sums :]
    copy_sem, send_sem, recv_sem = scratch[:3]
    goals = [(out, 0) for out in own_out]
    goals += [(sums[0], firsts[j]) for j in range(n_joint)]
    goals += [(out, 0) for out in sums[1 if n_pack else 0 :]]
    fs = Fsdp(nf, fsdp_in, fsdp_out, own_in + red_in, goals, scratch[3:])

    lines, across = split_axis(n)
    me = lax.axis_index("ctx")
    a, b, near = place_of(me, lines, across)
    gathered = list(zip(ctx_in, ctx_out)) + list(zip(sums, red_out))
    meet(near if gathered else [], [("fsdp", peer) for peer in fs.peers])
    fs.start()

    def part(i, turned):
        rows = gathered[i][1].shape[1]
        last = turned_rows(rows, gathered[i][1].dtype, across)
        return pl.ds(rows - last, last) if turned else pl.ds(0, rows - last)

    def turns(i):
        return bool(turned_rows(gathered[i][1].shape[1], gathered[i][1].dtype, across))

    def hop(i, block, way, turned=False, own=False):
        source, out = gathered[i]
        rows = part(i, turned)
        return pltpu.make_async_remote_copy(
            src_ref=source.at[rows] if own else out.at[block, rows],
            dst_ref=out.at[block, rows],
            send_sem=send_sem.at[i, way, block, int(turned)],
            recv_sem=recv_sem.at[i, way, block, int(turned)],
            device_id={"ctx": me + (across, -across, 1, -1)[way]},
            device_id_type=MESH,
        )

    def keep(i):
        return pltpu.make_async_copy(gathered[i][0], gathered[i][1].at[me], copy_sem.at[i])

    def each_own(i, act):
        for turned in (True, False) if turns(i) else (False,):
            for way in (2, 3, 0, 1):
                pl.when(near[way][0])(lambda way=way: act(hop(i, me, way, turned, True)))

    def each_twin(i, wait, act):
        if turns(i):
            twin = me + 1 - 2 * b
            for way in (2, 3):

                @pl.when(near[5 - way][0])
                def _(way=way):
                    if wait:
                        hop(i, twin, way, True).wait_recv()
                    for on in (0, 1):
                        pl.when(near[on][0])(lambda on=on: act(hop(i, twin, on, True)))

    def each_relay(i, d, wait, act):
        for way, there, shift in ((0, a >= d, -d * across), (1, a + d < lines, d * across)):

            @pl.when(there)
            def _(way=way, shift=shift):
                for turned, block in [(False, me + shift)] + (
                    [(True, me + shift), (True, me + 1 - 2 * b + shift)] if turns(i) else []
                ):
                    if wait:
                        hop(i, block, way, turned).wait_recv()
                    for on in (way,) if turned else (2, 3, way):
                        pl.when(near[on][0])(lambda on=on: act(hop(i, block, on, turned)))

    def start(copy):
        copy.start()

    def wait_send(copy):
        copy.wait_send()

    for i in range(n_ctx):
        each_own(i, start)
        keep(i).start()
    fs.middle()
    for j in range(n_pack):
        first = firsts[n_joint + j]
        sums[0][:, first : first + pack_in[j].shape[1]] = pack_in[j][...]
    begun = n_ctx
    for i in range(len(gathered)):
        if i == begun:
            fs.end()
            for j in range(begun, len(gathered)):
                each_own(j, start)
                keep(j).start()
            begun = len(gathered)
        each_twin(i, True, start)
        for d in range(1, lines):
            each_relay(i, d, True, start)
            if i == 0 and d == 1 and n_sums:
                fs.end()
                for j in range(begun, len(gathered)):
                    each_own(j, start)
                    keep(j).start()
                begun = len(gathered)

    for i in range(len(gathered)):
        for d in range(1, across):
            for step in range(lines):
                for sign in (1, -1) if step else (1,):
                    for way, there, shift in ((2, b >= d, -d), (3, b + d < across, d)):
                        other = a + sign * step

                        @pl.when(there & (other >= 0) & (other < lines))
                        def _(i=i, source=other * across + b + shift, way=way):
                            hop(i, source, way).wait_recv()
                            if d < across - 1:
                                pl.when(near[way][0])(lambda: hop(i, source, way).start())

    if len(gathered) == n_ctx:
        fs.end()

    for i in range(len(gathered)):
        keep(i).wait()
        each_own(i, wait_send)
        each_twin(i, False, wait_send)
        for d in range(1, lines):
            each_relay(i, d, False, wait_send)
        for d in range(1, across - 1):
            for line in range(lines):
                for way, there, shift in ((2, b >= d, -d), (3, b + d < across, d)):

                    @pl.when(there & near[way][0])
                    def _(i=i, source=line * across + b + shift, way=way):
                        hop(i, source, way).wait_send()

    fs.finish()


def exchange(call, n, nf, ctx=(), fsdp=(), own=(), red=(), pack=(), firsts=()):
    shape = jax.ShapeDtypeStruct
    sums = [shape(x.shape[1:], x.dtype) for x in red]
    if pack:
        joint = len(firsts) - len(pack)
        width = sum(x.shape[1] for x in [*sums[:joint], *pack])
        sums = [shape((pack[0].shape[0], width), pack[0].dtype)] + sums[joint:]
    outs = [shape((n, *x.shape), x.dtype) for x in ctx]
    outs += [shape((nf, *x.shape), x.dtype) for x in fsdp]
    outs += [shape(x.shape[1:], x.dtype) for x in own]
    outs += [shape((n, *x.shape), x.dtype) for x in sums]
    gathered = max(len(ctx) + len(sums), 1)
    any_spec, vmem_spec = pl.BlockSpec(memory_space=pl.ANY), pl.BlockSpec(memory_space=pltpu.VMEM)
    inputs = (*ctx, *fsdp, *own, *red, *pack)
    return pl.pallas_call(
        functools.partial(exchange_body, n, nf, (len(ctx), len(fsdp), len(own), len(red), len(pack)), firsts),
        in_specs=[vmem_spec] * len(inputs),
        out_specs=[any_spec] * (len(ctx) + len(fsdp)) + [vmem_spec] * len(own) + [any_spec] * len(sums),
        out_shape=outs,
        scratch_shapes=[pltpu.VMEM(x.shape, x.dtype) for x in sums]
        + [
            pltpu.SemaphoreType.DMA((gathered,)),
            pltpu.SemaphoreType.DMA((gathered, 4, n, 2)),
            pltpu.SemaphoreType.DMA((gathered, 4, n, 2)),
        ]
        + Fsdp.scratch(nf, fsdp, [*own, *red]),
        name=f"exchange_{call}",
        compiler_params=pltpu.CompilerParams(collective_id=call, has_side_effects=True, vmem_limit_bytes=60 * 2**20),
    )(*inputs)


def side_product(x, y, out, moves):
    if moves is None:
        out[...] = t_dot(x[...], y[...]).astype(BF16)
        return
    for block in sorted({move[0] for move in moves}):
        value = t_dot(x[block], y[...]).astype(BF16)
        for _, start, goal, size in [move for move in moves if move[0] == block]:
            out[goal : goal + size, :] = value[start : start + size]


class Scatter:
    def __init__(self, n, transposed, left, right, out, scratch):
        self.left, self.right, self.out, self.transposed = left, right, out, transposed
        self.part, self.acc, self.acc_t, self.over_in, self.sums, self.sums_t = scratch[:6]
        self.line_in, self.line_in_t, self.twin_in = scratch[6:9]
        self.o_send, self.o_recv, self.l_send, self.l_recv, self.t_send, self.t_recv = scratch[9:15]
        self.w_send, self.w_recv = scratch[15:17]
        self.lines, self.across = split_axis(n)
        self.me = lax.axis_index("ctx")
        self.a, self.b, self.near = place_of(self.me, self.lines, self.across)
        self.rows = out.shape[0]
        self.last = turned_rows(self.rows, BF16, self.across)
        self.head, self.tail = pl.ds(0, self.rows - self.last), pl.ds(self.rows - self.last, self.last)
        self.peers = [self.me - self.b + lax.rem(self.b + k, self.across) for k in range(1, self.across)]

    @staticmethod
    def scratch(n, rows, width):
        lines, across = split_axis(n)
        last = turned_rows(rows, BF16, across)
        some = max(last, 16)
        vmem, dma = pltpu.VMEM, pltpu.SemaphoreType.DMA
        return [
            vmem((lines, across, rows, width), BF16),
            vmem((rows - last, width), F32),
            vmem((across, some, width), F32),
            vmem((across - 1, lines, rows - last, width), BF16),
            vmem((lines, rows - last, width), BF16),
            vmem((lines, across, some, width), BF16),
            vmem((2, lines, rows - last, width), BF16),
            vmem((2, lines, across, some, width), BF16),
            vmem((some, width), BF16),
            dma((across - 1, lines)),
            dma((across - 1, lines)),
            dma((2, lines)),
            dma((2, lines)),
            dma((2, lines)),
            dma((2, lines)),
            dma,
            dma,
        ]

    def copy(self, src, dst, send, recv, target):
        return pltpu.make_async_remote_copy(
            src_ref=src, dst_ref=dst, send_sem=send, recv_sem=recv, device_id={"ctx": target}, device_id_type=MESH
        )

    def over(self, line, k):
        src = self.part.at[line, lax.rem(self.b + k, self.across), self.head]
        send, recv = self.o_send.at[k - 1, line], self.o_recv.at[k - 1, line]
        return self.copy(src, self.over_in.at[k - 1, line], send, recv, self.peers[k - 1])

    def along(self, line, way):
        target = self.me + (self.across, -self.across)[way]
        send, recv = self.l_send.at[way, line], self.l_recv.at[way, line]
        return self.copy(self.sums.at[line], self.line_in.at[way, line], send, recv, target)

    def along_t(self, line, way):
        target = self.me + (self.across, -self.across)[way]
        send, recv = self.t_send.at[way, line], self.t_recv.at[way, line]
        return self.copy(self.sums_t.at[line], self.line_in_t.at[way, line], send, recv, target)

    def twin(self):
        return self.copy(self.sums_t.at[self.a, 1 - self.b], self.twin_in, self.w_send, self.w_recv, self.peers[0])

    def compute(self, line):
        size = self.across * self.rows
        lhs = self.left[pl.ds(pl.multiple_of(line * size, size), size), :]
        value = dot_t(lhs, self.right[...]) if self.transposed else dot(lhs, self.right[...])
        self.part[line] = value.astype(BF16).reshape(self.across, self.rows, value.shape[1])
        for k in range(1, self.across):
            self.over(line, k).start()

    def collect(self, line, acc, landed, hop, ways):
        for way, there in ways:

            @pl.when(there)
            def _(way=way):
                hop(line, way).wait_recv()
                acc[...] += landed[way, line].astype(F32)

    def across_sum(self, line):
        value = self.part[line, self.b, self.head].astype(F32)
        for k in range(1, self.across):
            self.over(line, k).wait_recv()
            value = value + self.over_in[k - 1, line].astype(F32)
        self.acc[...] = value

    def pass_on(self, line):
        up, down = line > self.a, line < self.a
        ways = ((0, up & (self.a > 0)), (1, down & (self.a < self.lines - 1)))
        if self.last:
            self.acc_t[...] = self.part[line, :, self.tail].astype(F32)
            self.collect(line, self.acc_t, self.line_in_t, self.along_t, ways)
            self.sums_t[line] = self.acc_t[...].astype(BF16)
            pl.when(up)(lambda: self.along_t(line, 0).start())
            pl.when(down)(lambda: self.along_t(line, 1).start())
        self.across_sum(line)
        self.collect(line, self.acc, self.line_in, self.along, ways)
        self.sums[line] = self.acc[...].astype(BF16)
        pl.when(up)(lambda: self.along(line, 0).start())
        pl.when(down)(lambda: self.along(line, 1).start())

    def own(self):
        ways = ((0, self.near[1][0]), (1, self.near[0][0]))
        if self.last:
            self.acc_t[...] = self.part[self.a, :, self.tail].astype(F32)
            self.collect(self.a, self.acc_t, self.line_in_t, self.along_t, ways)
            self.sums_t[self.a] = self.acc_t[...].astype(BF16)
            self.twin().start()
        self.across_sum(self.a)
        self.collect(self.a, self.acc, self.line_in, self.along, ways)
        self.out[self.head, :] = self.acc[...]
        if self.last:
            self.twin().wait_recv()
            self.out[self.tail, :] = self.acc_t[self.b] + self.twin_in[...].astype(F32)

    def sent(self, order):
        for line in order:
            for k in range(1, self.across):
                self.over(line, k).wait_send()
        for line in order[:-1]:
            for way, there in ((0, line > self.a), (1, line < self.a)):

                @pl.when(there)
                def _(way=way, line=line):
                    self.along(line, way).wait_send()
                    if self.last:
                        self.along_t(line, way).wait_send()

        if self.last:
            self.twin().wait_send()


def product_body(n, nf, counts, transposed, moves, *refs):
    n_prod, n_sides, n_fsdp = counts
    pairs, refs = refs[: 2 * n_prod], refs[2 * n_prod :]
    side_in, refs = refs[: 2 * n_sides], refs[2 * n_sides :]
    fsdp_in, refs = refs[:n_fsdp], refs[n_fsdp:]
    outs, side_out, fsdp_out = refs[:n_prod], refs[n_prod : n_prod + n_sides], refs[n_prod + n_sides : n_prod + n_sides + n_fsdp]
    scratch = refs[n_prod + n_sides + n_fsdp :]
    each = 17
    jobs = [
        Scatter(n, transposed[p], pairs[2 * p], pairs[2 * p + 1], outs[p], scratch[each * p : each * (p + 1)])
        for p in range(n_prod)
    ]
    fs = Fsdp(nf, fsdp_in, fsdp_out, [], [], scratch[each * n_prod :])
    a, lines = jobs[0].a, jobs[0].lines
    meet(jobs[0].near[:2], [("ctx", peer) for peer in jobs[0].peers] + [("fsdp", peer) for peer in fs.peers])

    order = []
    for k in range(lines):
        line = jnp.int32(0)
        for av in range(lines):
            line = jnp.where(a == av, sorted(range(lines), key=lambda j: (-abs(j - av), j))[k], line)
        order.append(line)

    for job in jobs:
        for line in order:
            job.compute(line)
    fs.start()
    steps = [(job, line) for job in jobs for line in order[:-1]]
    for step, (job, line) in enumerate(steps):
        job.pass_on(line)
        for j in range(step * n_sides // len(steps), (step + 1) * n_sides // len(steps)):
            side_product(side_in[2 * j], side_in[2 * j + 1], side_out[j], moves[j])
        if step == len(order) - 2:
            fs.end()
    for job in jobs:
        job.own()
    for job in jobs:
        job.sent(order)
    fs.finish()


def product(call, n, nf, products, sides=(), fsdp=()):
    length = products[0][0].shape[0]
    if length > 1024 and (sides or len(products) > 1):
        sums = []
        for i, one in enumerate(products):
            total, *gathered = product(call if i == 0 else call + 10, n, nf, [one], fsdp=fsdp if i == 0 else ())
            sums.append(total)
            fsdp_out = gathered if i == 0 else fsdp_out
        others = []
        for x, y, moves in sides:
            if moves is None:
                others.append(t_dot(x, y).astype(BF16))
            else:
                ordered = sorted(moves, key=lambda move: move[2])
                x = jnp.concatenate([x[block, :, start : start + size] for block, start, _, size in ordered], axis=1)
                others.append(t_dot(x, y).astype(BF16))
        return [*sums, *others, *fsdp_out]
    rows = length // n
    shape = jax.ShapeDtypeStruct
    widths = [right.shape[0 if turned else 1] for _, right, turned in products]
    outs = [shape((rows, width), F32) for width in widths]
    for x, y, moves in sides:
        outs.append(shape((x.shape[1] if moves is None else sum(m[3] for m in moves), y.shape[1]), BF16))
    outs += [shape((nf, *x.shape), x.dtype) for x in fsdp]
    inputs = [z for left, right, _ in products for z in (left, right)] + [z for x, y, _ in sides for z in (x, y)]
    vmem_spec, any_spec = pl.BlockSpec(memory_space=pltpu.VMEM), pl.BlockSpec(memory_space=pl.ANY)
    return pl.pallas_call(
        functools.partial(
            product_body,
            n,
            nf,
            (len(products), len(sides), len(fsdp)),
            tuple(turned for _, _, turned in products),
            tuple(moves for _, _, moves in sides),
        ),
        in_specs=[vmem_spec] * (len(inputs) + len(fsdp)),
        out_specs=[vmem_spec] * (len(outs) - len(fsdp)) + [any_spec] * len(fsdp),
        out_shape=outs,
        scratch_shapes=[s for width in widths for s in Scatter.scratch(n, rows, width)] + Fsdp.scratch(nf, fsdp, ()),
        name=f"product_{call}",
        compiler_params=pltpu.CompilerParams(collective_id=call, has_side_effects=True, vmem_limit_bytes=63 * 2**20),
    )(*inputs, *fsdp)


def layout_body(moves, joint_ref, down_ref, down_out, *outs):
    for out_ref, per_out in zip(outs, moves):
        for block, start, goal, size in per_out:
            out_ref[:, goal : goal + size] = joint_ref[block, :, start : start + size].astype(F32)
    down_out[...] = down_ref[...].astype(F32)


def lay_out(joint, down, widths, moves):
    n, rows, part = joint.shape
    step = next(s for s in (80, 16, rows) if rows % s == 0)
    grid = rows // step
    tall, wide = down.shape
    return pl.pallas_call(
        functools.partial(layout_body, tuple(tuple(m) for m in moves)),
        grid=(grid,),
        in_specs=[
            pl.BlockSpec((n, step, part), lambda i: (0, i, 0)),
            pl.BlockSpec((tall // grid, wide), lambda i: (i, 0)),
        ],
        out_specs=[pl.BlockSpec((tall // grid, wide), lambda i: (i, 0))]
        + [pl.BlockSpec((step, width), lambda i: (i, 0)) for width in widths],
        out_shape=[jax.ShapeDtypeStruct(down.shape, F32)]
        + [jax.ShapeDtypeStruct((rows, width), F32) for width in widths],
        name="lay_out",
        cost_estimate=pl.CostEstimate(
            flops=0, bytes_accessed=6 * (rows * sum(widths) + tall * wide), transcendentals=0
        ),
        compiler_params=pltpu.CompilerParams(vmem_limit_bytes=60 * 2**20),
    )(joint, down)


def head_moves(n, heads, offset, goal):
    base, rest = divmod(heads, n)
    moves = [(c, offset, goal + c * base * HEAD_DIM, base * HEAD_DIM) for c in range(n) if base]
    moves += [
        (c, offset + base * HEAD_DIM, goal + (base * n + c) * HEAD_DIM, HEAD_DIM) for c in range(rest)
    ]
    return moves


def head_columns(value, width, c, n):
    heads = width // HEAD_DIM
    base, rest = divmod(heads, n)
    parts = []
    if base:
        parts.append(lax.dynamic_slice_in_dim(value, c * base * HEAD_DIM, base * HEAD_DIM, axis=-1))
    if rest:
        start = jnp.minimum(base * n + c, heads - 1) * HEAD_DIM
        extra = lax.dynamic_slice_in_dim(value, start, HEAD_DIM, axis=-1)
        parts.append(jnp.where(c < rest, extra, jnp.zeros_like(extra)))
    return jnp.concatenate(parts, axis=-1)


def place_heads(value, heads, c, n):
    base, rest = divmod(heads, n)
    out = jnp.zeros((heads * HEAD_DIM,), value.dtype)
    if rest:
        start = jnp.minimum(base * n + c, heads - 1) * HEAD_DIM
        extra = jnp.where(c < rest, value[base * HEAD_DIM :], 0.0)
        out = lax.dynamic_update_slice(out, extra, (start,))
    if base:
        out = lax.dynamic_update_slice(out, value[: base * HEAD_DIM], (c * base * HEAD_DIM,))
    return out


def head_rows(value, heads, c, f, n):
    base, rest = divmod(heads, n)
    local, width = value.shape
    pad = max(base, 1) * HEAD_DIM
    padded = jnp.pad(value, ((pad, pad), (0, 0)))
    parts = []
    if base:
        start = jnp.clip(c * base * HEAD_DIM - f * local + pad, 0, local + 2 * pad - base * HEAD_DIM)
        parts.append(lax.dynamic_slice_in_dim(padded, start, base * HEAD_DIM, axis=0))
    if rest:
        start = jnp.clip((base * n + c) * HEAD_DIM - f * local + pad, 0, local + 2 * pad - HEAD_DIM)
        extra = lax.dynamic_slice_in_dim(padded, start, HEAD_DIM, axis=0)
        parts.append(jnp.where(c < rest, extra, jnp.zeros_like(extra)))
    return jnp.concatenate(parts, axis=0)


def on_device(
    tokens,
    ln1_gain,
    ln1_shift,
    qkv_weight,
    qv_bias,
    out_weight,
    out_bias,
    ln2_gain,
    ln2_shift,
    up_weight,
    up_bias,
    down_weight,
    down_bias,
    block_table,
    cotangent,
):
    rows, width = tokens.shape[1:]
    heads = width // HEAD_DIM
    n = lax.axis_size("ctx")
    nf = lax.axis_size("fsdp")
    c = lax.axis_index("ctx")
    f = lax.axis_index("fsdp")
    slots = -(-heads // n)
    wide = slots * HEAD_DIM
    half = rows // 2
    local = width // nf
    ff = up_weight.shape[1]
    ff_local = ff // nf
    ff_part = ff_local // n

    within = jnp.arange(rows, dtype=jnp.int32)
    block_of = jnp.where(within[None, :] < half, block_table[:, None], 2 * n - 1 - block_table[:, None])
    place = (block_of * half + within[None, :] % half).reshape(-1)

    vectors = (ln1_gain, ln1_shift, qv_bias, out_bias, ln2_gain, ln2_shift, up_bias, down_bias)
    flat = jnp.concatenate(vectors)
    flat = jnp.pad(flat, (0, -flat.shape[0] % 2048)).reshape(-1, 128)
    q_w = head_columns(qkv_weight[:, :width], width, c, n)
    k_w = head_columns(qkv_weight[:, width : 2 * width], width, c, n)
    v_w = head_columns(qkv_weight[:, 2 * width :], width, c, n)
    w_mine = jnp.concatenate([q_w, k_w, v_w], axis=1)
    out_mine = head_rows(out_weight, heads, c, f, n)
    x_all, packed, w_qkv, w_out = exchange(0, n, nf, ctx=[tokens[0]], fsdp=[flat, w_mine, out_mine])
    up_weight, down_weight, packed = lax.optimization_barrier((up_weight, down_weight, packed))
    w_out = jnp.sum(w_out.astype(F32), axis=0).astype(BF16)
    x_all = x_all.reshape(n * rows, width)
    w_qkv = w_qkv.reshape(width, 3 * wide)
    packed = packed.reshape(nf, -1)
    full, at = [], 0
    for vector in vectors:
        size = vector.shape[0]
        full.append(packed[:, at : at + size].reshape(-1).astype(F32))
        at += size
    gain1, shift1, b_qv, b_out, gain2, shift2, b_up, b_down = full

    b_up_mine = lax.dynamic_slice_in_dim(b_up.reshape(nf, n, ff_part), c, 1, axis=1).reshape(-1)
    bq = head_columns(b_qv[:width], width, c, n)
    bv = head_columns(b_qv[width:], width, c, n)

    n1_all, _ = ln_stats(x_all.astype(F32))
    act1 = (n1_all * gain1 + shift1).astype(BF16)
    proj = dot(act1, w_qkv)
    q = (proj[:, :wide] + bq).astype(BF16)
    k = proj[:, wide : 2 * wide].astype(BF16)
    v = (proj[:, 2 * wide :] + bv).astype(BF16)
    attn, o, total = attention_fwd(place, q, k, v, slots)
    up_mine = [lax.dynamic_slice_in_dim(up_weight, i * ff_local + c * ff_part, ff_part, axis=1) for i in range(nf)]
    mixed, w_up = product(1, n, nf, [(attn, w_out, False)], fsdp=[jnp.concatenate(up_mine, axis=1)])
    w_up = w_up.reshape(width, nf * ff_part)
    x = tokens[0].astype(F32)
    mid = x + mixed + b_out

    n2, rstd2 = ln_stats(mid)
    act2, g2_all, attn_all, w_down = exchange(
        2,
        n,
        nf,
        ctx=[(n2 * gain2 + shift2).astype(BF16), cotangent[0], attn],
        fsdp=[lax.dynamic_slice_in_dim(down_weight, c * ff_part, ff_part, axis=0)],
    )
    act2 = act2.reshape(n * rows, width)
    g2_all = g2_all.reshape(n * rows, width)
    w_down = w_down.reshape(nf * ff_part, width)
    u = dot(act2, w_up) + b_up_mine
    activated, gelu_back = jax.vjp(lambda t: jax.nn.gelu(t, approximate=True), u)
    hidden = activated.astype(BF16)
    dh = dot_t(g2_all, w_down)
    du = gelu_back(dh)[0].astype(BF16)
    da2, fed, d_up, d_down = product(
        3, n, nf, [(du, w_up, True), (hidden, w_down, False)], sides=[(act2, du, None), (hidden, g2_all, None)]
    )
    result = mid + fed + b_down
    d_up = d_up.reshape(nf, local, nf * ff_part)
    d_down = d_down.reshape(nf, ff_part, width)
    d_up_bias = jnp.sum(du.astype(F32), axis=0)
    grad_out = cotangent[0].astype(F32)
    d_down_bias = jnp.sum(grad_out, axis=0)

    d_gain2 = jnp.sum(da2 * n2, axis=0)
    d_shift2 = jnp.sum(da2, axis=0)
    d_mid = grad_out + ln_back(da2, n2, rstd2, gain2)
    g1 = d_mid.astype(BF16)
    d_out_bias = jnp.sum(g1.astype(F32), axis=0)
    g1_all, d_up, d_down = exchange(4, n, nf, ctx=[g1], own=[d_up, d_down])
    g1_all = g1_all.reshape(n * rows, width)
    d_attn = dot_t(g1_all, w_out)
    gq, gk, gv = attention_bwd(place, q, k, v, d_attn, o, total, slots)
    g_qkv = jnp.concatenate([gq, gk, gv], axis=1)
    out_part = width // n
    g1_mine = lax.dynamic_slice_in_dim(g1_all, c * out_part, out_part, axis=1)
    da1, d_qkv, d_out = product(
        5,
        n,
        nf,
        [(g_qkv, w_qkv, True)],
        sides=[(act1, g_qkv, None), (attn_all, g1_mine, head_moves(n, heads, 0, 0))],
    )
    d_qkv = d_qkv.reshape(nf, local, 3 * wide)
    d_out = d_out.reshape(nf, local, out_part)

    n1, rstd1 = ln_stats(x)
    d_gain1 = jnp.sum(da1 * n1, axis=0)
    d_shift1 = jnp.sum(da1, axis=0)
    input_grad = d_mid + ln_back(da1, n1, rstd1, gain1)

    dq_bias = place_heads(jnp.sum(gq.astype(F32), axis=0), heads, c, n)
    dv_bias = place_heads(jnp.sum(gv.astype(F32), axis=0), heads, c, n)
    up_placed = lax.dynamic_update_slice(
        jnp.zeros((nf, n, ff_part), F32), d_up_bias.reshape(nf, 1, ff_part), (0, c, 0)
    )
    smalls = (
        d_gain1,
        d_shift1,
        jnp.concatenate([dq_bias, dv_bias]),
        d_out_bias,
        d_gain2,
        d_shift2,
        up_placed.reshape(-1),
        d_down_bias,
    )
    packed = jnp.concatenate([s.reshape(nf, -1) for s in smalls], axis=1)
    packed = jnp.pad(packed, ((0, 0), (0, -packed.shape[1] % 1024))).reshape(nf, -1, 128)
    at_up, at_out = 3 * wide, 3 * wide + nf * ff_part
    d_down, joint, packed = exchange(
        6, n, nf, ctx=[d_down], red=[d_qkv, d_out, packed], pack=[d_up], firsts=(0, at_out, at_up)
    )
    mine = jnp.sum(packed, axis=0).reshape(-1)
    up_moves = [(i, at_up + j * ff_part, j * ff_local + i * ff_part, ff_part) for i in range(n) for j in range(nf)]
    out_moves = [(i, at_out, i * out_part, out_part) for i in range(n)]
    qkv_moves = [m for i in range(3) for m in head_moves(n, heads, i * wide, i * width)]
    d_down_full, d_up_full, d_out_full, d_qkv_full = lay_out(
        joint, d_down.reshape(ff_local, width), (ff, width, 3 * width), (up_moves, out_moves, qkv_moves)
    )
    out, at = [], 0
    for s in smalls:
        size = s.size // nf
        out.append(mine[at : at + size])
        at += size
    return (
        result[None],
        input_grad[None],
        out[0],
        out[1],
        d_qkv_full,
        out[2],
        d_out_full,
        out[3],
        out[4],
        out[5],
        d_up_full,
        out[6],
        d_down_full,
        out[7],
    )


def solution(mesh):
    rows, one, two = P("fsdp", "ctx", None), P("fsdp"), P("fsdp", None)
    return jax.shard_map(
        on_device,
        mesh=mesh,
        in_specs=(rows, one, one, two, one, two, one, one, one, two, one, two, one, P(), rows),
        out_specs=(rows, rows, one, one, two, one, two, one, one, one, two, one, two, one),
        check_vma=False,
    )
```

```python
import functools

import jax
import jax.numpy as jnp
from jax import lax
from jax.experimental import pallas as pl
from jax.experimental.pallas import tpu as pltpu
from jax.sharding import PartitionSpec as P

HEAD_DIM = 64
EPS = 1e-05
SCALE = 0.125
F32 = jnp.float32
BF16 = jnp.bfloat16
MESH = pl.DeviceIdType.MESH


def dot(left, right):
    return jnp.dot(left, right, preferred_element_type=F32)


def dot_t(left, right):
    return lax.dot_general(left, right, (((1,), (1,)), ((), ())), preferred_element_type=F32)


def t_dot(left, right):
    return lax.dot_general(left, right, (((0,), (0,)), ((), ())), preferred_element_type=F32)


def ln_stats(value):
    centre = value - jnp.mean(value, axis=-1, keepdims=True)
    spread = jnp.mean(centre * centre, axis=-1, keepdims=True)
    rstd = lax.rsqrt(spread + EPS)
    return centre * rstd, rstd


def ln_back(grad, normed, rstd, gain):
    dn = grad * gain
    first = jnp.mean(dn, axis=-1, keepdims=True)
    second = jnp.mean(dn * normed, axis=-1, keepdims=True)
    return (dn - first - normed * second) * rstd


def attn_fwd_body(slots, qp_ref, kp_ref, q_ref, k_ref, v_ref, attn_ref, o_ref, l_ref):
    allowed = kp_ref[...] <= qp_ref[...]
    for h in range(slots):
        cols = slice(h * HEAD_DIM, (h + 1) * HEAD_DIM)
        raw = dot_t(q_ref[:, cols], k_ref[:, cols])
        e = jnp.where(allowed, jnp.exp(raw * SCALE), 0.0)
        total = jnp.sum(e, axis=1, keepdims=True)
        numer = dot(e.astype(BF16), v_ref[:, cols])
        o = numer / total
        o_ref[:, cols] = o
        attn_ref[:, cols] = o.astype(BF16)
        l_ref[:, h : h + 1] = total


def attn_bwd_body(
    slots, qp_ref, kp_ref, q_ref, k_ref, v_ref, do_ref, o_ref, l_ref, dq_ref, dk_ref, dv_ref, dk_acc, dv_acc
):
    step = pl.program_id(0)

    @pl.when(step == 0)
    def _():
        dk_acc[...] = jnp.zeros_like(dk_acc)
        dv_acc[...] = jnp.zeros_like(dv_acc)

    allowed = kp_ref[...] <= qp_ref[...]
    for h in range(slots):
        cols = slice(h * HEAD_DIM, (h + 1) * HEAD_DIM)
        q = q_ref[:, cols]
        k = k_ref[:, cols]
        v = v_ref[:, cols]
        do = do_ref[:, cols]
        total = l_ref[:, h : h + 1]
        w = (do / total).astype(BF16)
        corr = jnp.sum(do * o_ref[:, cols], axis=1, keepdims=True) / total
        e = jnp.where(allowed, jnp.exp(dot_t(q, k) * SCALE), 0.0)
        de = dot_t(w, v)
        ds = (e * (de - corr)).astype(BF16)
        dq_ref[:, cols] = (dot(ds, k) * SCALE).astype(BF16)
        dk_acc[:, cols] += t_dot(ds, q)
        dv_acc[:, cols] += t_dot(e.astype(BF16), w)

    @pl.when(step == pl.num_programs(0) - 1)
    def _():
        dk_ref[...] = (dk_acc[...] * SCALE).astype(BF16)
        dv_ref[...] = dv_acc[...].astype(BF16)


def attn_specs(rows, wide, slots):
    qb = 256 if rows <= 1024 else 128
    q_spec = pl.BlockSpec((qb, wide), lambda i: (i, 0))
    l_spec = pl.BlockSpec((qb, slots), lambda i: (i, 0))
    all_spec = pl.BlockSpec((rows, wide), lambda i: (0, 0))
    qp_spec = pl.BlockSpec((qb, 1), lambda i: (i, 0))
    kp_spec = pl.BlockSpec((1, rows), lambda i: (0, 0))
    return rows // qb, q_spec, l_spec, all_spec, qp_spec, kp_spec


def attention_fwd(place, q, k, v, slots):
    rows, wide = q.shape
    steps, q_spec, l_spec, all_spec, qp_spec, kp_spec = attn_specs(rows, wide, slots)
    return pl.pallas_call(
        functools.partial(attn_fwd_body, slots),
        grid=(steps,),
        in_specs=[qp_spec, kp_spec, q_spec, all_spec, all_spec],
        out_specs=[q_spec, q_spec, l_spec],
        out_shape=[
            jax.ShapeDtypeStruct((rows, wide), BF16),
            jax.ShapeDtypeStruct((rows, wide), F32),
            jax.ShapeDtypeStruct((rows, slots), F32),
        ],
        name="attn_fwd",
        cost_estimate=pl.CostEstimate(
            flops=4 * rows * rows * wide, bytes_accessed=16 * rows * wide, transcendentals=rows * rows * slots
        ),
        compiler_params=pltpu.CompilerParams(vmem_limit_bytes=60 * 2**20),
    )(place.reshape(rows, 1), place.reshape(1, rows), q, k, v)


def attention_bwd(place, q, k, v, do, o, total, slots):
    rows, wide = q.shape
    steps, q_spec, l_spec, all_spec, qp_spec, kp_spec = attn_specs(rows, wide, slots)
    shape = jax.ShapeDtypeStruct((rows, wide), BF16)
    return pl.pallas_call(
        functools.partial(attn_bwd_body, slots),
        grid=(steps,),
        in_specs=[qp_spec, kp_spec, q_spec, all_spec, all_spec, q_spec, q_spec, l_spec],
        out_specs=[q_spec, all_spec, all_spec],
        out_shape=[shape, shape, shape],
        scratch_shapes=[pltpu.VMEM((rows, wide), F32), pltpu.VMEM((rows, wide), F32)],
        name="attn_bwd",
        cost_estimate=pl.CostEstimate(
            flops=10 * rows * rows * wide, bytes_accessed=24 * rows * wide, transcendentals=rows * rows * slots
        ),
        compiler_params=pltpu.CompilerParams(vmem_limit_bytes=60 * 2**20),
    )(place.reshape(rows, 1), place.reshape(1, rows), q, k, v, do, o, total)


def split_axis(n):
    across = 2 if n <= 8 else 4
    return n // across, across


def place_of(me, lines, across):
    a, b = lax.div(me, across), lax.rem(me, across)
    near = [(a < lines - 1, me + across), (a > 0, me - across), (b < across - 1, me + 1), (b > 0, me - 1)]
    return a, b, near


def turned_rows(rows, dtype, across):
    tile = 16 if dtype == BF16 else 8
    share = 4 if rows <= 128 else 5
    return rows // share // tile * tile if across == 2 else 0


def meet(near, peers):
    barrier = pltpu.get_barrier_semaphore()
    for exists, target in near:

        @pl.when(exists)
        def _(target=target):
            pl.semaphore_signal(barrier, inc=1, device_id={"ctx": target}, device_id_type=MESH)

    for axis, peer in peers:
        pl.semaphore_signal(barrier, inc=1, device_id={axis: peer}, device_id_type=MESH)
    pl.semaphore_wait(barrier, len(peers) + sum(exists.astype(jnp.int32) for exists, _ in near))


class Fsdp:
    def __init__(self, nf, gather_in, gather_out, red_in, red_out, scratch):
        self.gather_in, self.gather_out, self.red_in, self.red_out = gather_in, gather_out, red_in, red_out
        n_gather, n_red = len(gather_in), len(red_in)
        self.near_in, self.stage, self.far_in = scratch[:n_red], scratch[n_red : 2 * n_red], scratch[2 * n_red : 3 * n_red]
        self.keep_sem, self.g_send, self.g_recv, self.r_send, self.r_recv = scratch[3 * n_red : 3 * n_red + 5]
        self.f = lax.axis_index("fsdp")
        self.core = lax.rem(self.f, 2)
        self.mate = self.f + 1 - 2 * self.core
        self.pairs = nf // 2
        self.pair = lax.div(self.f, 2)
        self.other = [lax.rem(self.pair + k, self.pairs) for k in range(1, self.pairs)]
        self.peers = [self.mate] + [2 * y + self.core for y in self.other] if n_gather + n_red else []

    @staticmethod
    def scratch(nf, gather, red):
        pairs = nf // 2
        dma = pltpu.SemaphoreType.DMA
        out = []
        for _ in range(3):
            out += [pltpu.VMEM((pairs, *x.shape[1:]), x.dtype) for x in red]
        g, r = max(len(gather), 1), max(len(red), 1)
        return out + [dma((g,)), dma((g, 2, nf)), dma((g, nf)), dma((r, 2, pairs)), dma((r, 2, pairs))]

    def copy(self, src, dst, send, recv, target):
        return pltpu.make_async_remote_copy(
            src_ref=src, dst_ref=dst, send_sem=send, recv_sem=recv, device_id={"fsdp": target}, device_id_type=MESH
        )

    def spread(self, i, source, target, own):
        out = self.gather_out[i].at[source]
        send = self.g_send.at[i, 0, target] if own else self.g_send.at[i, 1, source]
        return self.copy(self.gather_in[i] if own else out, out, send, self.g_recv.at[i, source], target)

    def keep(self, i):
        return pltpu.make_async_copy(self.gather_in[i], self.gather_out[i].at[self.f], self.keep_sem.at[i])

    def to_mate(self, j, y):
        src = self.red_in[j].at[2 * y + 1 - self.core]
        return self.copy(src, self.near_in[j].at[y], self.r_send.at[j, 0, y], self.r_recv.at[j, 0, y], self.mate)

    def to_far(self, j, y, source):
        send, recv = self.r_send.at[j, 1, y], self.r_recv.at[j, 1, source]
        return self.copy(self.stage[j].at[y], self.far_in[j].at[source], send, recv, 2 * y + self.core)

    def write(self, j, value):
        out, first = self.red_out[j]
        out[:, first : first + value.shape[1]] = value.astype(out.dtype)

    def start(self):
        for j in range(len(self.red_in)):
            for y in range(self.pairs):
                self.to_mate(j, y).start()
        for i in range(len(self.gather_in)):
            for target in self.peers[1:] + self.peers[:1]:
                self.spread(i, self.f, target, True).start()
            self.keep(i).start()

    def middle(self):
        for j in range(len(self.red_in)):
            for y in range(self.pairs):
                self.to_mate(j, y).wait_recv()
            for y in self.other:
                value = self.red_in[j][2 * y + self.core].astype(F32) + self.near_in[j][y].astype(F32)
                self.stage[j][y] = value.astype(self.stage[j].dtype)
                self.to_far(j, y, self.pair).start()

    def end(self):
        for j in range(len(self.red_in)):
            value = self.red_in[j][self.f].astype(F32) + self.near_in[j][self.pair].astype(F32)
            for y in self.other:
                self.to_far(j, y, y).wait_recv()
                value = value + self.far_in[j][y].astype(F32)
            self.write(j, value)
        for i in range(len(self.gather_in)):
            for y in self.other:
                source = 2 * y + self.core
                self.spread(i, source, self.mate, False).wait_recv()
                self.spread(i, source, self.mate, False).start()

    def finish(self):
        for i in range(len(self.gather_in)):
            self.spread(i, self.mate, self.mate, False).wait_recv()
            for y in self.other:
                self.spread(i, 2 * y + 1 - self.core, self.mate, False).wait_recv()
            self.keep(i).wait()
            for target in self.peers:
                self.spread(i, self.f, target, True).wait_send()
            for y in self.other:
                self.spread(i, 2 * y + self.core, self.mate, False).wait_send()
        for j in range(len(self.red_in)):
            for y in range(self.pairs):
                self.to_mate(j, y).wait_send()
            for y in self.other:
                self.to_far(j, y, self.pair).wait_send()


def exchange_body(n, nf, counts, firsts, moves, *refs):
    n_ctx, n_fsdp, n_own, n_red, n_pack = counts
    bounds = [0]
    for size in counts:
        bounds.append(bounds[-1] + size)
    ctx_in, fsdp_in, own_in, red_in, pack_in = (refs[i:j] for i, j in zip(bounds, bounds[1:]))
    refs = refs[bounds[-1] :]
    n_joint = len(firsts) - n_pack
    n_sums = n_red - n_joint + (1 if n_pack else 0)
    ctx_out, fsdp_out, own_out = refs[:n_ctx], refs[n_ctx : n_ctx + n_fsdp], refs[n_ctx + n_fsdp : n_ctx + n_fsdp + n_own]
    refs = refs[n_ctx + n_fsdp + n_own :]
    red_out, refs = refs[:n_sums], refs[n_sums:]
    if moves:
        placed, refs = refs[0], refs[1:]
    sums, scratch = refs[:n_sums], refs[n_sums:]
    copy_sem, send_sem, recv_sem, place_send, place_recv = scratch[:5]
    goals = [(out, 0) for out in own_out]
    goals += [(sums[0], firsts[j]) for j in range(n_joint)]
    goals += [(out, 0) for out in sums[1 if n_pack else 0 :]]
    fs = Fsdp(nf, fsdp_in, fsdp_out, own_in + red_in, goals, scratch[5:])

    lines, across = split_axis(n)
    me = lax.axis_index("ctx")
    a, b, near = place_of(me, lines, across)
    pieces = [(src, out, 0, out.shape[1]) for src, out in zip(ctx_in, ctx_out)]
    late = len(pieces)
    for src, out in reversed(list(zip(sums, red_out))):
        pieces += [(src, out, first, rows) for first, rows in cut(out.shape[1])]
    peers = [lax.rem(fs.f + k, nf) for k in range(1, nf)] if moves else fs.peers
    meet(near if pieces else [], [("fsdp", peer) for peer in peers])
    fs.start()

    def turned_part(i):
        return turned_rows(pieces[i][3], pieces[i][1].dtype, across)

    def hop(i, block, way, turned=False, own=False):
        source, out, first, size = pieces[i]
        last = turned_part(i)
        rows = pl.ds(first + size - last, last) if turned else pl.ds(first, size - last)
        return pltpu.make_async_remote_copy(
            src_ref=source.at[rows] if own else out.at[block, rows],
            dst_ref=out.at[block, rows],
            send_sem=send_sem.at[i, way, block, int(turned)],
            recv_sem=recv_sem.at[i, way, block, int(turned)],
            device_id={"ctx": me + (across, -across, 1, -1)[way]},
            device_id_type=MESH,
        )

    def keep(i):
        source, out, first, size = pieces[i]
        rows = pl.ds(first, size)
        return pltpu.make_async_copy(source.at[rows], out.at[me, rows], copy_sem.at[i])

    def each_own(i, act):
        for turned in (True, False) if turned_part(i) else (False,):
            for way in (2, 3, 0, 1):
                pl.when(near[way][0])(lambda way=way: act(hop(i, me, way, turned, True)))

    def each_twin(i, wait, act):
        if turned_part(i):
            twin = me + 1 - 2 * b
            for way in (2, 3):

                @pl.when(near[5 - way][0])
                def _(way=way):
                    if wait:
                        hop(i, twin, way, True).wait_recv()
                    for on in (0, 1):
                        pl.when(near[on][0])(lambda on=on: act(hop(i, twin, on, True)))

    def each_relay(i, d, wait, act):
        for way, there, shift in ((0, a >= d, -d * across), (1, a + d < lines, d * across)):

            @pl.when(there)
            def _(way=way, shift=shift):
                for turned, block in [(False, me + shift)] + (
                    [(True, me + shift), (True, me + 1 - 2 * b + shift)] if turned_part(i) else []
                ):
                    if wait:
                        hop(i, block, way, turned).wait_recv()
                    for on in (way,) if turned else (2, 3, way):
                        pl.when(near[on][0])(lambda on=on: act(hop(i, block, on, turned)))

    def start(copy):
        copy.start()

    def wait_send(copy):
        copy.wait_send()

    def begin(these):
        for i in these:
            each_own(i, start)
            keep(i).start()

    begin(range(late))
    fs.middle()
    for j in range(n_pack):
        first = firsts[n_joint + j]
        sums[0][:, first : first + pack_in[j].shape[1]] = pack_in[j][...]
    if n_sums:
        if late:
            each_twin(0, True, start)
            each_relay(0, 1, True, start)
        fs.end()
        begin(range(late, len(pieces)))
    for d in range(1, lines):
        for i in range(len(pieces)):
            if d == 1:
                if i == 0 and late and n_sums:
                    continue
                each_twin(i, True, start)
            each_relay(i, d, True, start)

    def crossed(i):
        for d in range(1, across):
            for step in range(lines):
                for sign in (1, -1) if step else (1,):
                    for way, there, shift in ((2, b >= d, -d), (3, b + d < across, d)):
                        other = a + sign * step

                        @pl.when(there & (other >= 0) & (other < lines))
                        def _(source=other * across + b + shift, way=way):
                            hop(i, source, way).wait_recv()
                            if d < across - 1:
                                pl.when(near[way][0])(lambda: hop(i, source, way).start())

    def place(k, act_local, act_send):
        block, row, src, dst, goal, size = moves[k]
        source, goal = red_out[1].at[block, pl.ds(row, size)], placed.at[pl.ds(goal, size)]
        if src == dst:
            pl.when(fs.f == src)(lambda: act_local(pltpu.make_async_copy(source, goal, place_send.at[k])))
            return
        remote = pltpu.make_async_remote_copy(
            src_ref=source,
            dst_ref=goal,
            send_sem=place_send.at[k],
            recv_sem=place_recv.at[k],
            device_id={"fsdp": jnp.int32(dst)},
            device_id_type=MESH,
        )
        pl.when(fs.f == src)(lambda: act_send(remote))
        if act_local is wait_copy:
            pl.when(fs.f == dst)(remote.wait_recv)

    def wait_copy(copy):
        copy.wait()

    if moves:
        ready = [i for i in range(len(pieces)) if pieces[i][1] is red_out[1]]
        for i in ready:
            crossed(i)
            keep(i).wait()
        for k in range(len(moves)):
            place(k, start, start)
    else:
        ready = []
    for i in range(len(pieces)):
        if i not in ready:
            crossed(i)
            keep(i).wait()
    for k in range(len(moves)):
        place(k, wait_copy, wait_send)
    if not n_sums:
        fs.end()

    for i in range(len(pieces)):
        each_own(i, wait_send)
        each_twin(i, False, wait_send)
        for d in range(1, lines):
            each_relay(i, d, False, wait_send)
        for d in range(1, across - 1):
            for line in range(lines):
                for way, there, shift in ((2, b >= d, -d), (3, b + d < across, d)):

                    @pl.when(there & near[way][0])
                    def _(i=i, source=line * across + b + shift, way=way):
                        hop(i, source, way).wait_send()

    fs.finish()


def cut(rows):
    if rows < 400:
        return [(0, rows)]
    half = rows // 32 * 16
    return [(0, rows - half), (rows - half, half)]


def exchange(call, n, nf, ctx=(), fsdp=(), own=(), red=(), pack=(), firsts=(), moves=(), kept=0):
    shape = jax.ShapeDtypeStruct
    sums = [shape(x.shape[1:], x.dtype) for x in red]
    if pack:
        joint = len(firsts) - len(pack)
        width = sum(x.shape[1] for x in [*sums[:joint], *pack])
        sums = [shape((pack[0].shape[0], width), pack[0].dtype)] + sums[joint:]
    outs = [shape((n, *x.shape), x.dtype) for x in ctx]
    outs += [shape((nf, *x.shape), x.dtype) for x in fsdp]
    outs += [shape(x.shape[1:], x.dtype) for x in own]
    outs += [shape((n, *x.shape), x.dtype) for x in sums]
    outs += [shape((kept, sums[1].shape[1]), sums[1].dtype)] if moves else []
    gathered = max(len(ctx) + sum(len(cut(x.shape[0])) for x in sums), 1)
    any_spec, vmem_spec = pl.BlockSpec(memory_space=pl.ANY), pl.BlockSpec(memory_space=pltpu.VMEM)
    inputs = (*ctx, *fsdp, *own, *red, *pack)
    dma = pltpu.SemaphoreType.DMA
    return pl.pallas_call(
        functools.partial(
            exchange_body, n, nf, (len(ctx), len(fsdp), len(own), len(red), len(pack)), tuple(firsts), tuple(moves)
        ),
        in_specs=[vmem_spec] * len(inputs),
        out_specs=[any_spec] * (len(ctx) + len(fsdp))
        + [vmem_spec] * len(own)
        + [any_spec] * (len(sums) + (1 if moves else 0)),
        out_shape=outs,
        scratch_shapes=[pltpu.VMEM(x.shape, x.dtype) for x in sums]
        + [dma((gathered,)), dma((gathered, 4, n, 2)), dma((gathered, 4, n, 2))]
        + [dma((max(len(moves), 1),))] * 2
        + Fsdp.scratch(nf, fsdp, [*own, *red]),
        name=f"exchange_{call}",
        compiler_params=pltpu.CompilerParams(collective_id=call, has_side_effects=True, vmem_limit_bytes=60 * 2**20),
    )(*inputs)


class Scatter:
    def __init__(self, n, transposed, left, right, out, scratch):
        self.left, self.right, self.out, self.transposed = left, right, out, transposed
        self.part, self.acc, self.acc_t, self.over_in, self.sums, self.sums_t = scratch[:6]
        self.line_in, self.line_in_t, self.twin_in = scratch[6:9]
        self.o_send, self.o_recv, self.l_send, self.l_recv, self.t_send, self.t_recv = scratch[9:15]
        self.w_send, self.w_recv = scratch[15:17]
        self.lines, self.across = split_axis(n)
        self.me = lax.axis_index("ctx")
        self.a, self.b, self.near = place_of(self.me, self.lines, self.across)
        self.rows = out.shape[0]
        self.last = turned_rows(self.rows, BF16, self.across)
        self.head, self.tail = pl.ds(0, self.rows - self.last), pl.ds(self.rows - self.last, self.last)
        self.peers = [self.me - self.b + lax.rem(self.b + k, self.across) for k in range(1, self.across)]

    @staticmethod
    def scratch(n, rows, width):
        lines, across = split_axis(n)
        last = turned_rows(rows, BF16, across)
        some = max(last, 16)
        vmem, dma = pltpu.VMEM, pltpu.SemaphoreType.DMA
        return [
            vmem((lines, across, rows, width), BF16),
            vmem((rows - last, width), F32),
            vmem((across, some, width), F32),
            vmem((across - 1, lines, rows - last, width), BF16),
            vmem((lines, rows - last, width), BF16),
            vmem((lines, across, some, width), BF16),
            vmem((2, lines, rows - last, width), BF16),
            vmem((2, lines, across, some, width), BF16),
            vmem((some, width), BF16),
            dma((across - 1, lines)),
            dma((across - 1, lines)),
            dma((2, lines)),
            dma((2, lines)),
            dma((2, lines)),
            dma((2, lines)),
            dma,
            dma,
        ]

    def copy(self, src, dst, send, recv, target):
        return pltpu.make_async_remote_copy(
            src_ref=src, dst_ref=dst, send_sem=send, recv_sem=recv, device_id={"ctx": target}, device_id_type=MESH
        )

    def over(self, line, k):
        src = self.part.at[line, lax.rem(self.b + k, self.across), self.head]
        send, recv = self.o_send.at[k - 1, line], self.o_recv.at[k - 1, line]
        return self.copy(src, self.over_in.at[k - 1, line], send, recv, self.peers[k - 1])

    def along(self, line, way):
        target = self.me + (self.across, -self.across)[way]
        send, recv = self.l_send.at[way, line], self.l_recv.at[way, line]
        return self.copy(self.sums.at[line], self.line_in.at[way, line], send, recv, target)

    def along_t(self, line, way):
        target = self.me + (self.across, -self.across)[way]
        send, recv = self.t_send.at[way, line], self.t_recv.at[way, line]
        return self.copy(self.sums_t.at[line], self.line_in_t.at[way, line], send, recv, target)

    def twin(self):
        return self.copy(self.sums_t.at[self.a, 1 - self.b], self.twin_in, self.w_send, self.w_recv, self.peers[0])

    def compute(self, line):
        size = self.across * self.rows
        lhs = self.left[pl.ds(pl.multiple_of(line * size, size), size), :]
        value = dot_t(lhs, self.right[...]) if self.transposed else dot(lhs, self.right[...])
        self.part[line] = value.astype(BF16).reshape(self.across, self.rows, value.shape[1])
        for k in range(1, self.across):
            self.over(line, k).start()

    def collect(self, line, acc, landed, hop, ways):
        for way, there in ways:

            @pl.when(there)
            def _(way=way):
                hop(line, way).wait_recv()
                acc[...] += landed[way, line].astype(F32)

    def across_sum(self, line):
        value = self.part[line, self.b, self.head].astype(F32)
        for k in range(1, self.across):
            self.over(line, k).wait_recv()
            value = value + self.over_in[k - 1, line].astype(F32)
        self.acc[...] = value

    def pass_on(self, line):
        up, down = line > self.a, line < self.a
        ways = ((0, up & (self.a > 0)), (1, down & (self.a < self.lines - 1)))
        if self.last:
            self.acc_t[...] = self.part[line, :, self.tail].astype(F32)
            self.collect(line, self.acc_t, self.line_in_t, self.along_t, ways)
            self.sums_t[line] = self.acc_t[...].astype(BF16)
            pl.when(up)(lambda: self.along_t(line, 0).start())
            pl.when(down)(lambda: self.along_t(line, 1).start())
        self.across_sum(line)
        self.collect(line, self.acc, self.line_in, self.along, ways)
        self.sums[line] = self.acc[...].astype(BF16)
        pl.when(up)(lambda: self.along(line, 0).start())
        pl.when(down)(lambda: self.along(line, 1).start())

    def own(self):
        ways = ((0, self.near[1][0]), (1, self.near[0][0]))
        if self.last:
            self.acc_t[...] = self.part[self.a, :, self.tail].astype(F32)
            self.collect(self.a, self.acc_t, self.line_in_t, self.along_t, ways)
            self.sums_t[self.a] = self.acc_t[...].astype(BF16)
            self.twin().start()
        self.across_sum(self.a)
        self.collect(self.a, self.acc, self.line_in, self.along, ways)
        self.out[self.head, :] = self.acc[...]
        if self.last:
            self.twin().wait_recv()
            self.out[self.tail, :] = self.acc_t[self.b] + self.twin_in[...].astype(F32)

    def sent(self, order):
        for line in order:
            for k in range(1, self.across):
                self.over(line, k).wait_send()
        for line in order[:-1]:
            for way, there in ((0, line > self.a), (1, line < self.a)):

                @pl.when(there)
                def _(way=way, line=line):
                    self.along(line, way).wait_send()
                    if self.last:
                        self.along_t(line, way).wait_send()

        if self.last:
            self.twin().wait_send()


def product_body(n, nf, counts, transposed, *refs):
    n_prod, n_sides, n_fsdp = counts
    pairs, refs = refs[: 2 * n_prod], refs[2 * n_prod :]
    side_in, refs = refs[: 2 * n_sides], refs[2 * n_sides :]
    fsdp_in, refs = refs[:n_fsdp], refs[n_fsdp:]
    outs, side_out, fsdp_out = refs[:n_prod], refs[n_prod : n_prod + n_sides], refs[n_prod + n_sides : n_prod + n_sides + n_fsdp]
    scratch = refs[n_prod + n_sides + n_fsdp :]
    each = 17
    jobs = [
        Scatter(n, transposed[p], pairs[2 * p], pairs[2 * p + 1], outs[p], scratch[each * p : each * (p + 1)])
        for p in range(n_prod)
    ]
    fs = Fsdp(nf, fsdp_in, fsdp_out, [], [], scratch[each * n_prod :])
    a, lines = jobs[0].a, jobs[0].lines
    meet(jobs[0].near[:2], [("ctx", peer) for peer in jobs[0].peers] + [("fsdp", peer) for peer in fs.peers])

    order = []
    for k in range(lines):
        line = jnp.int32(0)
        for av in range(lines):
            line = jnp.where(a == av, sorted(range(lines), key=lambda j: (-abs(j - av), j))[k], line)
        order.append(line)

    for job in jobs:
        for line in order:
            job.compute(line)
    fs.start()
    steps = [(job, line) for job in jobs for line in order[:-1]]
    for step, (job, line) in enumerate(steps):
        job.pass_on(line)
        for j in range(step * n_sides // len(steps), (step + 1) * n_sides // len(steps)):
            side_out[j][...] = t_dot(side_in[2 * j][...], side_in[2 * j + 1][...]).astype(BF16)
        if step == len(order) - 2:
            fs.end()
    for job in jobs:
        job.own()
    for job in jobs:
        job.sent(order)
    fs.finish()


def product(call, n, nf, products, sides=(), fsdp=()):
    length = products[0][0].shape[0]
    if length > 1024 and (sides or len(products) > 1):
        sums = []
        for i, one in enumerate(products):
            total, *gathered = product(call if i == 0 else call + 10, n, nf, [one], fsdp=fsdp if i == 0 else ())
            sums.append(total)
            fsdp_out = gathered if i == 0 else fsdp_out
        return [*sums, *[t_dot(x, y).astype(BF16) for x, y in sides], *fsdp_out]
    rows = length // n
    shape = jax.ShapeDtypeStruct
    widths = [right.shape[0 if turned else 1] for _, right, turned in products]
    outs = [shape((rows, width), F32) for width in widths]
    outs += [shape((x.shape[1], y.shape[1]), BF16) for x, y in sides]
    outs += [shape((nf, *x.shape), x.dtype) for x in fsdp]
    inputs = [z for left, right, _ in products for z in (left, right)] + [z for side in sides for z in side]
    vmem_spec, any_spec = pl.BlockSpec(memory_space=pltpu.VMEM), pl.BlockSpec(memory_space=pl.ANY)
    return pl.pallas_call(
        functools.partial(
            product_body,
            n,
            nf,
            (len(products), len(sides), len(fsdp)),
            tuple(turned for _, _, turned in products),
        ),
        in_specs=[vmem_spec] * (len(inputs) + len(fsdp)),
        out_specs=[vmem_spec] * (len(outs) - len(fsdp)) + [any_spec] * len(fsdp),
        out_shape=outs,
        scratch_shapes=[s for width in widths for s in Scatter.scratch(n, rows, width)] + Fsdp.scratch(nf, fsdp, ()),
        name=f"product_{call}",
        compiler_params=pltpu.CompilerParams(collective_id=call, has_side_effects=True, vmem_limit_bytes=63 * 2**20),
    )(*inputs, *fsdp)


def row_moves(n, nf, heads):
    part, local = -(-heads // n) * HEAD_DIM // nf, heads * HEAD_DIM // nf
    moves = []
    for block, start, goal, size in head_moves(n, heads, 0, 0):
        done = 0
        while done < size:
            here, there = start + done, goal + done
            rows = min(size - done, part - here % part, local - there % local)
            moves.append((block, here % part, here // part, there // local, there % local, rows))
            done += rows
    return moves


def layout_body(moves, joint_ref, down_ref, out_ref, down_out, out_out, *outs):
    for ref, per_out in zip(outs, moves):
        for block, start, goal, size in per_out:
            ref[:, goal : goal + size] = joint_ref[block, :, start : start + size].astype(F32)
    down_out[...] = down_ref[...].astype(F32)
    out_out[...] = out_ref[...].astype(F32)


def lay_out(joint, down, out, widths, moves):
    n, rows, part = joint.shape
    step = next(s for s in (80, 16, rows) if rows % s == 0)
    grid = rows // step
    plain = [pl.BlockSpec((x.shape[0] // grid, x.shape[1]), lambda i: (i, 0)) for x in (down, out)]
    return pl.pallas_call(
        functools.partial(layout_body, tuple(tuple(m) for m in moves)),
        grid=(grid,),
        in_specs=[pl.BlockSpec((n, step, part), lambda i: (0, i, 0)), *plain],
        out_specs=plain + [pl.BlockSpec((step, width), lambda i: (i, 0)) for width in widths],
        out_shape=[jax.ShapeDtypeStruct(x.shape, F32) for x in (down, out)]
        + [jax.ShapeDtypeStruct((rows, width), F32) for width in widths],
        name="lay_out",
        cost_estimate=pl.CostEstimate(
            flops=0, bytes_accessed=6 * (rows * sum(widths) + down.size + out.size), transcendentals=0
        ),
        compiler_params=pltpu.CompilerParams(vmem_limit_bytes=60 * 2**20),
    )(joint, down, out)


def head_moves(n, heads, offset, goal):
    base, rest = divmod(heads, n)
    moves = [(c, offset, goal + c * base * HEAD_DIM, base * HEAD_DIM) for c in range(n) if base]
    moves += [
        (c, offset + base * HEAD_DIM, goal + (base * n + c) * HEAD_DIM, HEAD_DIM) for c in range(rest)
    ]
    return moves


def head_columns(value, width, c, n):
    heads = width // HEAD_DIM
    base, rest = divmod(heads, n)
    parts = []
    if base:
        parts.append(lax.dynamic_slice_in_dim(value, c * base * HEAD_DIM, base * HEAD_DIM, axis=-1))
    if rest:
        start = jnp.minimum(base * n + c, heads - 1) * HEAD_DIM
        extra = lax.dynamic_slice_in_dim(value, start, HEAD_DIM, axis=-1)
        parts.append(jnp.where(c < rest, extra, jnp.zeros_like(extra)))
    return jnp.concatenate(parts, axis=-1)


def place_heads(value, heads, c, n):
    base, rest = divmod(heads, n)
    out = jnp.zeros((heads * HEAD_DIM,), value.dtype)
    if rest:
        start = jnp.minimum(base * n + c, heads - 1) * HEAD_DIM
        extra = jnp.where(c < rest, value[base * HEAD_DIM :], 0.0)
        out = lax.dynamic_update_slice(out, extra, (start,))
    if base:
        out = lax.dynamic_update_slice(out, value[: base * HEAD_DIM], (c * base * HEAD_DIM,))
    return out


def head_rows(value, heads, c, f, n):
    base, rest = divmod(heads, n)
    local, width = value.shape
    pad = max(base, 1) * HEAD_DIM
    padded = jnp.pad(value, ((pad, pad), (0, 0)))
    parts = []
    if base:
        start = jnp.clip(c * base * HEAD_DIM - f * local + pad, 0, local + 2 * pad - base * HEAD_DIM)
        parts.append(lax.dynamic_slice_in_dim(padded, start, base * HEAD_DIM, axis=0))
    if rest:
        start = jnp.clip((base * n + c) * HEAD_DIM - f * local + pad, 0, local + 2 * pad - HEAD_DIM)
        extra = lax.dynamic_slice_in_dim(padded, start, HEAD_DIM, axis=0)
        parts.append(jnp.where(c < rest, extra, jnp.zeros_like(extra)))
    return jnp.concatenate(parts, axis=0)


def on_device(
    tokens,
    ln1_gain,
    ln1_shift,
    qkv_weight,
    qv_bias,
    out_weight,
    out_bias,
    ln2_gain,
    ln2_shift,
    up_weight,
    up_bias,
    down_weight,
    down_bias,
    block_table,
    cotangent,
):
    rows, width = tokens.shape[1:]
    heads = width // HEAD_DIM
    n = lax.axis_size("ctx")
    nf = lax.axis_size("fsdp")
    c = lax.axis_index("ctx")
    f = lax.axis_index("fsdp")
    slots = -(-heads // n)
    wide = slots * HEAD_DIM
    half = rows // 2
    local = width // nf
    ff = up_weight.shape[1]
    ff_local = ff // nf
    ff_part = ff_local // n

    within = jnp.arange(rows, dtype=jnp.int32)
    block_of = jnp.where(within[None, :] < half, block_table[:, None], 2 * n - 1 - block_table[:, None])
    place = (block_of * half + within[None, :] % half).reshape(-1)

    vectors = (ln1_gain, ln1_shift, qv_bias, out_bias, ln2_gain, ln2_shift, up_bias, down_bias)
    longest = max(v.shape[0] for v in vectors)
    flat = jnp.stack([jnp.pad(v, (0, longest - v.shape[0])) for v in vectors] * (-(-16 // len(vectors))))
    q_w = head_columns(qkv_weight[:, :width], width, c, n)
    k_w = head_columns(qkv_weight[:, width : 2 * width], width, c, n)
    v_w = head_columns(qkv_weight[:, 2 * width :], width, c, n)
    w_mine = jnp.concatenate([q_w, k_w, v_w], axis=1)
    out_mine = head_rows(out_weight, heads, c, f, n)
    x_all, packed, w_qkv, w_out = exchange(0, n, nf, ctx=[tokens[0]], fsdp=[flat, w_mine, out_mine])
    up_weight, down_weight, packed = lax.optimization_barrier((up_weight, down_weight, packed))
    w_out = jnp.sum(w_out.astype(F32), axis=0).astype(BF16)
    x_all = x_all.reshape(n * rows, width)
    w_qkv = w_qkv.reshape(width, 3 * wide)
    full = [packed[:, i, : v.shape[0]].reshape(-1).astype(F32) for i, v in enumerate(vectors)]
    gain1, shift1, b_qv, b_out, gain2, shift2, b_up, b_down = full

    b_up_mine = lax.dynamic_slice_in_dim(b_up.reshape(nf, n, ff_part), c, 1, axis=1).reshape(-1)
    bq = head_columns(b_qv[:width], width, c, n)
    bv = head_columns(b_qv[width:], width, c, n)

    n1_all, _ = ln_stats(x_all.astype(F32))
    act1 = (n1_all * gain1 + shift1).astype(BF16)
    proj = dot(act1, w_qkv)
    q = (proj[:, :wide] + bq).astype(BF16)
    k = proj[:, wide : 2 * wide].astype(BF16)
    v = (proj[:, 2 * wide :] + bv).astype(BF16)
    attn, o, total = attention_fwd(place, q, k, v, slots)
    up_mine = [lax.dynamic_slice_in_dim(up_weight, i * ff_local + c * ff_part, ff_part, axis=1) for i in range(nf)]
    mixed, w_up = product(1, n, nf, [(attn, w_out, False)], fsdp=[jnp.concatenate(up_mine, axis=1)])
    w_up = w_up.reshape(width, nf * ff_part)
    x = tokens[0].astype(F32)
    mid = x + mixed + b_out

    n2, rstd2 = ln_stats(mid)
    act2, g2_all, w_down = exchange(
        2,
        n,
        nf,
        ctx=[(n2 * gain2 + shift2).astype(BF16), cotangent[0]],
        fsdp=[lax.dynamic_slice_in_dim(down_weight, c * ff_part, ff_part, axis=0)],
    )
    act2 = act2.reshape(n * rows, width)
    g2_all = g2_all.reshape(n * rows, width)
    w_down = w_down.reshape(nf * ff_part, width)
    u = dot(act2, w_up) + b_up_mine
    activated, gelu_back = jax.vjp(lambda t: jax.nn.gelu(t, approximate=True), u)
    hidden = activated.astype(BF16)
    dh = dot_t(g2_all, w_down)
    du = gelu_back(dh)[0].astype(BF16)
    da2, fed, d_up, d_down = product(
        3, n, nf, [(du, w_up, True), (hidden, w_down, False)], sides=[(act2, du), (hidden, g2_all)]
    )
    result = mid + fed + b_down
    d_up = d_up.reshape(nf, local, nf * ff_part)
    d_down = d_down.reshape(nf, ff_part, width)
    d_up_bias = jnp.sum(du.astype(F32), axis=0)
    grad_out = cotangent[0].astype(F32)
    d_down_bias = jnp.sum(grad_out, axis=0)

    d_gain2 = jnp.sum(da2 * n2, axis=0)
    d_shift2 = jnp.sum(da2, axis=0)
    d_mid = grad_out + ln_back(da2, n2, rstd2, gain2)
    g1 = d_mid.astype(BF16)
    d_out_bias = jnp.sum(g1.astype(F32), axis=0)
    g1_all, d_up, d_down = exchange(4, n, nf, ctx=[g1], own=[d_up, d_down])
    g1_all = g1_all.reshape(n * rows, width)
    d_attn = dot_t(g1_all, w_out)
    gq, gk, gv = attention_bwd(place, q, k, v, d_attn, o, total, slots)
    g_qkv = jnp.concatenate([gq, gk, gv], axis=1)
    da1, d_qkv, d_out = product(5, n, nf, [(g_qkv, w_qkv, True)], sides=[(act1, g_qkv), (attn, g1_all)])
    d_qkv = d_qkv.reshape(nf, local, 3 * wide)
    d_out = d_out.reshape(nf, wide // nf, width)

    n1, rstd1 = ln_stats(x)
    d_gain1 = jnp.sum(da1 * n1, axis=0)
    d_shift1 = jnp.sum(da1, axis=0)
    input_grad = d_mid + ln_back(da1, n1, rstd1, gain1)

    dq_bias = place_heads(jnp.sum(gq.astype(F32), axis=0), heads, c, n)
    dv_bias = place_heads(jnp.sum(gv.astype(F32), axis=0), heads, c, n)
    up_placed = lax.dynamic_update_slice(
        jnp.zeros((nf, n, ff_part), F32), d_up_bias.reshape(nf, 1, ff_part), (0, c, 0)
    )
    smalls = (
        d_gain1,
        d_shift1,
        jnp.concatenate([dq_bias, dv_bias]),
        d_out_bias,
        d_gain2,
        d_shift2,
        up_placed.reshape(-1),
        d_down_bias,
    )
    packed = jnp.concatenate([s.reshape(nf, -1) for s in smalls], axis=1)
    packed = jnp.pad(packed, ((0, 0), (0, -packed.shape[1] % 1024))).reshape(nf, -1, 128)
    at_up = 3 * wide
    d_down, joint, _, packed, d_out = exchange(
        6,
        n,
        nf,
        ctx=[d_down],
        red=[d_qkv, d_out, packed],
        pack=[d_up],
        firsts=(0, at_up),
        moves=row_moves(n, nf, heads),
        kept=local,
    )
    mine = jnp.sum(packed, axis=0).reshape(-1)
    up_moves = [(i, at_up + j * ff_part, j * ff_local + i * ff_part, ff_part) for i in range(n) for j in range(nf)]
    qkv_moves = [m for i in range(3) for m in head_moves(n, heads, i * wide, i * width)]
    d_down_full, d_out_full, d_up_full, d_qkv_full = lay_out(
        joint, d_down.reshape(ff_local, width), d_out, (ff, 3 * width), (up_moves, qkv_moves)
    )
    out, at = [], 0
    for s in smalls:
        size = s.size // nf
        out.append(mine[at : at + size])
        at += size
    return (
        result[None],
        input_grad[None],
        out[0],
        out[1],
        d_qkv_full,
        out[2],
        d_out_full,
        out[3],
        out[4],
        out[5],
        d_up_full,
        out[6],
        d_down_full,
        out[7],
    )


def solution(mesh):
    rows, one, two = P("fsdp", "ctx", None), P("fsdp"), P("fsdp", None)
    return jax.shard_map(
        on_device,
        mesh=mesh,
        in_specs=(rows, one, one, two, one, two, one, one, one, two, one, two, one, P(), rows),
        out_specs=(rows, rows, one, one, two, one, two, one, one, one, two, one, two, one),
        check_vma=False,
    )
```

```python
import functools

import jax
import jax.numpy as jnp
from jax import lax
from jax.experimental import pallas as pl
from jax.experimental.pallas import tpu as pltpu
from jax.sharding import PartitionSpec as P

HEAD_DIM = 64
EPS = 1e-05
SCALE = 0.125
F32 = jnp.float32
BF16 = jnp.bfloat16
MESH = pl.DeviceIdType.MESH


def dot(left, right):
    return jnp.dot(left, right, preferred_element_type=F32)


def dot_t(left, right):
    return lax.dot_general(left, right, (((1,), (1,)), ((), ())), preferred_element_type=F32)


def t_dot(left, right):
    return lax.dot_general(left, right, (((0,), (0,)), ((), ())), preferred_element_type=F32)


def ln_stats(value):
    centre = value - jnp.mean(value, axis=-1, keepdims=True)
    spread = jnp.mean(centre * centre, axis=-1, keepdims=True)
    rstd = lax.rsqrt(spread + EPS)
    return centre * rstd, rstd


def ln_back(grad, normed, rstd, gain):
    dn = grad * gain
    first = jnp.mean(dn, axis=-1, keepdims=True)
    second = jnp.mean(dn * normed, axis=-1, keepdims=True)
    return (dn - first - normed * second) * rstd


def query_rows(rows):
    return 256


def forward_step(slots, step, ins, outs, scratch):
    qp_ref, kp_ref, q_ref, k_ref, v_ref = ins
    attn_ref, o_ref, l_ref = outs
    size = query_rows(q_ref.shape[0])
    rows = slice(step * size, (step + 1) * size)
    allowed = kp_ref[...] <= qp_ref[rows, :]
    for h in range(slots):
        cols = slice(h * HEAD_DIM, (h + 1) * HEAD_DIM)
        raw = dot_t(q_ref[rows, cols], k_ref[:, cols])
        e = jnp.where(allowed, jnp.exp(raw * SCALE), 0.0)
        total = jnp.sum(e, axis=1, keepdims=True)
        numer = dot(e.astype(BF16), v_ref[:, cols])
        o = numer / total
        o_ref[rows, cols] = o
        attn_ref[rows, cols] = o.astype(BF16)
        l_ref[rows, h : h + 1] = total


def backward_step(slots, step, ins, outs, scratch):
    qp_ref, kp_ref, q_ref, k_ref, v_ref, do_ref, o_ref, l_ref = ins
    dq_ref, dk_ref, dv_ref = outs
    dk_acc, dv_acc = scratch
    size = query_rows(q_ref.shape[0])
    steps = q_ref.shape[0] // size
    rows = slice(step * size, (step + 1) * size)
    allowed = kp_ref[...] <= qp_ref[rows, :]
    for h in range(slots):
        cols = slice(h * HEAD_DIM, (h + 1) * HEAD_DIM)
        q, k, v, do = q_ref[rows, cols], k_ref[:, cols], v_ref[:, cols], do_ref[rows, cols]
        total = l_ref[rows, h : h + 1]
        w = (do / total).astype(BF16)
        corr = jnp.sum(do * o_ref[rows, cols], axis=1, keepdims=True) / total
        e = jnp.where(allowed, jnp.exp(dot_t(q, k) * SCALE), 0.0)
        de = dot_t(w, v)
        ds = (e * (de - corr)).astype(BF16)
        dq_ref[rows, cols] = (dot(ds, k) * SCALE).astype(BF16)
        dk, dv = t_dot(ds, q), t_dot(e.astype(BF16), w)
        if step:
            dk, dv = dk + dk_acc[:, cols], dv + dv_acc[:, cols]
        if step < steps - 1:
            dk_acc[:, cols] = dk
            dv_acc[:, cols] = dv
        else:
            dk_ref[:, cols] = (dk * SCALE).astype(BF16)
            dv_ref[:, cols] = dv.astype(BF16)


def forward_work(place, q, k, v, slots):
    rows, wide = q.shape
    shape = jax.ShapeDtypeStruct
    outs = (shape((rows, wide), BF16), shape((rows, wide), F32), shape((rows, slots), F32))
    steps = rows // query_rows(rows)
    ins = (place.reshape(rows, 1), place.reshape(1, rows), q, k, v)
    return steps, functools.partial(forward_step, slots), ins, outs, ()


def backward_work(place, q, k, v, do, o, total, slots):
    rows, wide = q.shape
    outs = (jax.ShapeDtypeStruct((rows, wide), BF16),) * 3
    steps = rows // query_rows(rows)
    ins = (place.reshape(rows, 1), place.reshape(1, rows), q, k, v, do, o, total)
    return steps, functools.partial(backward_step, slots), ins, outs, (pltpu.VMEM((rows, wide), F32),) * 2


def split_axis(n):
    across = 2 if n <= 8 else 4
    return n // across, across


def place_of(me, lines, across):
    a, b = lax.div(me, across), lax.rem(me, across)
    near = [(a < lines - 1, me + across), (a > 0, me - across), (b < across - 1, me + 1), (b > 0, me - 1)]
    return a, b, near


def turned_rows(rows, dtype, across):
    tile = 16 if dtype == BF16 else 8
    share = 4 if rows <= 128 else 5
    return rows // share // tile * tile if across == 2 else 0


def meet(near, peers):
    barrier = pltpu.get_barrier_semaphore()
    for exists, target in near:

        @pl.when(exists)
        def _(target=target):
            pl.semaphore_signal(barrier, inc=1, device_id={"ctx": target}, device_id_type=MESH)

    for axis, peer in peers:
        pl.semaphore_signal(barrier, inc=1, device_id={axis: peer}, device_id_type=MESH)
    pl.semaphore_wait(barrier, len(peers) + sum(exists.astype(jnp.int32) for exists, _ in near))


class Fsdp:
    def __init__(self, nf, gather_in, gather_out, red_in, red_out, scratch):
        self.gather_in, self.gather_out, self.red_in, self.red_out = gather_in, gather_out, red_in, red_out
        n_gather, n_red = len(gather_in), len(red_in)
        self.near_in, self.stage, self.far_in = scratch[:n_red], scratch[n_red : 2 * n_red], scratch[2 * n_red : 3 * n_red]
        self.keep_sem, self.g_send, self.g_recv, self.r_send, self.r_recv = scratch[3 * n_red : 3 * n_red + 5]
        self.f = lax.axis_index("fsdp")
        self.core = lax.rem(self.f, 2)
        self.mate = self.f + 1 - 2 * self.core
        self.pairs = nf // 2
        self.pair = lax.div(self.f, 2)
        self.other = [lax.rem(self.pair + k, self.pairs) for k in range(1, self.pairs)]
        self.peers = [self.mate] + [2 * y + self.core for y in self.other] if n_gather + n_red else []

    @staticmethod
    def scratch(nf, gather, red):
        pairs = nf // 2
        dma = pltpu.SemaphoreType.DMA
        out = []
        for _ in range(3):
            out += [pltpu.VMEM((pairs, *x.shape[1:]), x.dtype) for x in red]
        g, r = max(len(gather), 1), max(len(red), 1)
        return out + [dma((g,)), dma((g, 2, nf)), dma((g, nf)), dma((r, 2, pairs)), dma((r, 2, pairs))]

    def copy(self, src, dst, send, recv, target):
        return pltpu.make_async_remote_copy(
            src_ref=src, dst_ref=dst, send_sem=send, recv_sem=recv, device_id={"fsdp": target}, device_id_type=MESH
        )

    def spread(self, i, source, target, own):
        out = self.gather_out[i].at[source]
        send = self.g_send.at[i, 0, target] if own else self.g_send.at[i, 1, source]
        return self.copy(self.gather_in[i] if own else out, out, send, self.g_recv.at[i, source], target)

    def keep(self, i):
        return pltpu.make_async_copy(self.gather_in[i], self.gather_out[i].at[self.f], self.keep_sem.at[i])

    def to_mate(self, j, y):
        src = self.red_in[j].at[2 * y + 1 - self.core]
        return self.copy(src, self.near_in[j].at[y], self.r_send.at[j, 0, y], self.r_recv.at[j, 0, y], self.mate)

    def to_far(self, j, y, source):
        send, recv = self.r_send.at[j, 1, y], self.r_recv.at[j, 1, source]
        return self.copy(self.stage[j].at[y], self.far_in[j].at[source], send, recv, 2 * y + self.core)

    def write(self, j, value):
        out, first = self.red_out[j]
        out[:, first : first + value.shape[1]] = value.astype(out.dtype)

    def start(self):
        for j in range(len(self.red_in)):
            for y in range(self.pairs):
                self.to_mate(j, y).start()
        for i in range(len(self.gather_in)):
            for target in self.peers[1:] + self.peers[:1]:
                self.spread(i, self.f, target, True).start()
            self.keep(i).start()

    def middle(self):
        for j in range(len(self.red_in)):
            for y in range(self.pairs):
                self.to_mate(j, y).wait_recv()
            for y in self.other:
                value = self.red_in[j][2 * y + self.core].astype(F32) + self.near_in[j][y].astype(F32)
                self.stage[j][y] = value.astype(self.stage[j].dtype)
                self.to_far(j, y, self.pair).start()

    def end(self):
        for j in range(len(self.red_in)):
            value = self.red_in[j][self.f].astype(F32) + self.near_in[j][self.pair].astype(F32)
            for y in self.other:
                self.to_far(j, y, y).wait_recv()
                value = value + self.far_in[j][y].astype(F32)
            self.write(j, value)
        for i in range(len(self.gather_in)):
            for y in self.other:
                source = 2 * y + self.core
                self.spread(i, source, self.mate, False).wait_recv()
                self.spread(i, source, self.mate, False).start()

    def finish(self):
        for i in range(len(self.gather_in)):
            self.spread(i, self.mate, self.mate, False).wait_recv()
            for y in self.other:
                self.spread(i, 2 * y + 1 - self.core, self.mate, False).wait_recv()
            self.keep(i).wait()
            for target in self.peers:
                self.spread(i, self.f, target, True).wait_send()
            for y in self.other:
                self.spread(i, 2 * y + self.core, self.mate, False).wait_send()
        for j in range(len(self.red_in)):
            for y in range(self.pairs):
                self.to_mate(j, y).wait_send()
            for y in self.other:
                self.to_far(j, y, self.pair).wait_send()


def exchange_body(n, nf, counts, firsts, moves, work, *refs):
    n_ctx, n_fsdp, n_own, n_red, n_pack, n_work_in, n_work_out, n_work_scratch = counts
    bounds = [0]
    for size in counts[:6]:
        bounds.append(bounds[-1] + size)
    ctx_in, fsdp_in, own_in, red_in, pack_in, work_in = (refs[i:j] for i, j in zip(bounds, bounds[1:]))
    refs = refs[bounds[-1] :]
    n_joint = len(firsts) - n_pack
    n_sums = n_red - n_joint + (1 if n_pack else 0)
    ctx_out, fsdp_out, own_out = refs[:n_ctx], refs[n_ctx : n_ctx + n_fsdp], refs[n_ctx + n_fsdp : n_ctx + n_fsdp + n_own]
    refs = refs[n_ctx + n_fsdp + n_own :]
    red_out, refs = refs[:n_sums], refs[n_sums:]
    if moves:
        placed, refs = refs[0], refs[1:]
    work_out, refs = refs[:n_work_out], refs[n_work_out:]
    work_scratch, refs = refs[:n_work_scratch], refs[n_work_scratch:]
    sums, scratch = refs[:n_sums], refs[n_sums:]
    copy_sem, send_sem, recv_sem, place_send, place_recv = scratch[:5]
    goals = [(out, 0) for out in own_out]
    goals += [(sums[0], firsts[j]) for j in range(n_joint)]
    goals += [(out, 0) for out in sums[1 if n_pack else 0 :]]
    fs = Fsdp(nf, fsdp_in, fsdp_out, own_in + red_in, goals, scratch[5:])

    lines, across = split_axis(n)
    me = lax.axis_index("ctx")
    a, b, near = place_of(me, lines, across)
    pieces = [(src, out, first, rows) for src, out in zip(ctx_in, ctx_out) for first, rows in cut(out.shape[1])]
    late = len(pieces)
    for src, out in reversed(list(zip(sums, red_out))):
        pieces += [(src, out, first, rows) for first, rows in cut(out.shape[1])]
    peers = [lax.rem(fs.f + k, nf) for k in range(1, nf)] if moves else fs.peers
    meet(near if pieces else [], [("fsdp", peer) for peer in peers])
    fs.start()

    def turned_part(i):
        return turned_rows(pieces[i][3], pieces[i][1].dtype, across)

    def hop(i, block, way, turned=False, own=False):
        source, out, first, size = pieces[i]
        last = turned_part(i)
        rows = pl.ds(first + size - last, last) if turned else pl.ds(first, size - last)
        return pltpu.make_async_remote_copy(
            src_ref=source.at[rows] if own else out.at[block, rows],
            dst_ref=out.at[block, rows],
            send_sem=send_sem.at[i, way, block, int(turned)],
            recv_sem=recv_sem.at[i, way, block, int(turned)],
            device_id={"ctx": me + (across, -across, 1, -1)[way]},
            device_id_type=MESH,
        )

    def keep(i):
        source, out, first, size = pieces[i]
        rows = pl.ds(first, size)
        return pltpu.make_async_copy(source.at[rows], out.at[me, rows], copy_sem.at[i])

    def each_own(i, act):
        for turned in (True, False) if turned_part(i) else (False,):
            for way in (2, 3, 0, 1):
                pl.when(near[way][0])(lambda way=way: act(hop(i, me, way, turned, True)))

    def each_twin(i, wait, act):
        if turned_part(i):
            twin = me + 1 - 2 * b
            for way in (2, 3):

                @pl.when(near[5 - way][0])
                def _(way=way):
                    if wait:
                        hop(i, twin, way, True).wait_recv()
                    for on in (0, 1):
                        pl.when(near[on][0])(lambda on=on: act(hop(i, twin, on, True)))

    def each_relay(i, d, wait, act):
        for way, there, shift in ((0, a >= d, -d * across), (1, a + d < lines, d * across)):

            @pl.when(there)
            def _(way=way, shift=shift):
                for turned, block in [(False, me + shift)] + (
                    [(True, me + shift), (True, me + 1 - 2 * b + shift)] if turned_part(i) else []
                ):
                    if wait:
                        hop(i, block, way, turned).wait_recv()
                    for on in (way,) if turned else (2, 3, way):
                        pl.when(near[on][0])(lambda on=on: act(hop(i, block, on, turned)))

    def start(copy):
        copy.start()

    def wait_send(copy):
        copy.wait_send()

    def begin(these):
        for i in these:
            each_own(i, start)
            keep(i).start()

    work_steps, work_fn = work
    points = 1 + (lines - 1) * len(pieces)
    passed = [0]

    def do_work():
        at = passed[0]
        passed[0] += 1
        for step in range(at * work_steps // points, (at + 1) * work_steps // points):
            work_fn(step, work_in, work_out, work_scratch)

    begin(range(late))
    fs.middle()
    do_work()
    for j in range(n_pack):
        first = firsts[n_joint + j]
        sums[0][:, first : first + pack_in[j].shape[1]] = pack_in[j][...]
    if n_sums:
        if late:
            each_twin(0, True, start)
            each_relay(0, 1, True, start)
            do_work()
        fs.end()
        begin(range(late, len(pieces)))
    for d in range(1, lines):
        for i in range(len(pieces)):
            if d == 1:
                if i == 0 and late and n_sums:
                    continue
                each_twin(i, True, start)
            each_relay(i, d, True, start)
            do_work()
    if not n_sums:
        fs.end()

    def crossed(i):
        for d in range(1, across):
            for step in range(lines):
                for sign in (1, -1) if step else (1,):
                    for way, there, shift in ((2, b >= d, -d), (3, b + d < across, d)):
                        other = a + sign * step

                        @pl.when(there & (other >= 0) & (other < lines))
                        def _(source=other * across + b + shift, way=way):
                            hop(i, source, way).wait_recv()
                            if d < across - 1:
                                pl.when(near[way][0])(lambda: hop(i, source, way).start())

    def place(k, act_local, act_send):
        block, row, src, dst, goal, size = moves[k]
        source, goal = red_out[1].at[block, pl.ds(row, size)], placed.at[pl.ds(goal, size)]
        if src == dst:
            pl.when(fs.f == src)(lambda: act_local(pltpu.make_async_copy(source, goal, place_send.at[k])))
            return
        remote = pltpu.make_async_remote_copy(
            src_ref=source,
            dst_ref=goal,
            send_sem=place_send.at[k],
            recv_sem=place_recv.at[k],
            device_id={"fsdp": jnp.int32(dst)},
            device_id_type=MESH,
        )
        pl.when(fs.f == src)(lambda: act_send(remote))
        if act_local is wait_copy:
            pl.when(fs.f == dst)(remote.wait_recv)

    def wait_copy(copy):
        copy.wait()

    if moves:
        ready = [i for i in range(len(pieces)) if pieces[i][1] is red_out[1]]
        for i in ready:
            crossed(i)
            keep(i).wait()
        for k in range(len(moves)):
            place(k, start, start)
    else:
        ready = []
    for i in range(len(pieces)):
        if i not in ready:
            crossed(i)
            keep(i).wait()
    for k in range(len(moves)):
        place(k, wait_copy, wait_send)

    for i in range(len(pieces)):
        each_own(i, wait_send)
        each_twin(i, False, wait_send)
        for d in range(1, lines):
            each_relay(i, d, False, wait_send)
        for d in range(1, across - 1):
            for line in range(lines):
                for way, there, shift in ((2, b >= d, -d), (3, b + d < across, d)):

                    @pl.when(there & near[way][0])
                    def _(i=i, source=line * across + b + shift, way=way):
                        hop(i, source, way).wait_send()

    fs.finish()


def cut(rows):
    if rows < 200:
        return [(0, rows)]
    half = rows // 32 * 16
    return [(0, rows - half), (rows - half, half)]


def exchange(call, n, nf, ctx=(), fsdp=(), own=(), red=(), pack=(), firsts=(), moves=(), kept=0, work=None):
    shape = jax.ShapeDtypeStruct
    sums = [shape(x.shape[1:], x.dtype) for x in red]
    if pack:
        joint = len(firsts) - len(pack)
        width = sum(x.shape[1] for x in [*sums[:joint], *pack])
        sums = [shape((pack[0].shape[0], width), pack[0].dtype)] + sums[joint:]
    outs = [shape((n, *x.shape), x.dtype) for x in ctx]
    outs += [shape((nf, *x.shape), x.dtype) for x in fsdp]
    outs += [shape(x.shape[1:], x.dtype) for x in own]
    outs += [shape((n, *x.shape), x.dtype) for x in sums]
    outs += [shape((kept, sums[1].shape[1]), sums[1].dtype)] if moves else []
    steps, work_fn, work_in, work_out, work_scratch = work or (0, None, (), (), ())
    gathered = max(sum(len(cut(x.shape[0])) for x in [*ctx, *sums]), 1)
    any_spec, vmem_spec = pl.BlockSpec(memory_space=pl.ANY), pl.BlockSpec(memory_space=pltpu.VMEM)
    inputs = (*ctx, *fsdp, *own, *red, *pack, *work_in)
    counts = [len(x) for x in (ctx, fsdp, own, red, pack, work_in, work_out, work_scratch)]
    dma = pltpu.SemaphoreType.DMA
    return pl.pallas_call(
        functools.partial(exchange_body, n, nf, tuple(counts), tuple(firsts), tuple(moves), (steps, work_fn)),
        in_specs=[vmem_spec] * len(inputs),
        out_specs=[any_spec] * (len(ctx) + len(fsdp))
        + [vmem_spec] * len(own)
        + [any_spec] * (len(sums) + (1 if moves else 0))
        + [vmem_spec] * len(work_out),
        out_shape=[*outs, *work_out],
        scratch_shapes=list(work_scratch)
        + [pltpu.VMEM(x.shape, x.dtype) for x in sums]
        + [dma((gathered,)), dma((gathered, 4, n, 2)), dma((gathered, 4, n, 2))]
        + [dma((max(len(moves), 1),))] * 2
        + Fsdp.scratch(nf, fsdp, [*own, *red]),
        name=f"exchange_{call}",
        compiler_params=pltpu.CompilerParams(collective_id=call, has_side_effects=True, vmem_limit_bytes=60 * 2**20),
    )(*inputs)


class Scatter:
    def __init__(self, n, transposed, left, right, out, scratch):
        self.left, self.right, self.out, self.transposed = left, right, out, transposed
        self.part, self.acc, self.acc_t, self.over_in, self.sums, self.sums_t = scratch[:6]
        self.line_in, self.line_in_t, self.twin_in = scratch[6:9]
        self.o_send, self.o_recv, self.l_send, self.l_recv, self.t_send, self.t_recv = scratch[9:15]
        self.w_send, self.w_recv = scratch[15:17]
        self.lines, self.across = split_axis(n)
        self.me = lax.axis_index("ctx")
        self.a, self.b, self.near = place_of(self.me, self.lines, self.across)
        self.rows = out.shape[0]
        self.last = turned_rows(self.rows, BF16, self.across)
        self.head, self.tail = pl.ds(0, self.rows - self.last), pl.ds(self.rows - self.last, self.last)
        self.peers = [self.me - self.b + lax.rem(self.b + k, self.across) for k in range(1, self.across)]

    @staticmethod
    def scratch(n, rows, width):
        lines, across = split_axis(n)
        last = turned_rows(rows, BF16, across)
        some = max(last, 16)
        vmem, dma = pltpu.VMEM, pltpu.SemaphoreType.DMA
        return [
            vmem((lines, across, rows, width), BF16),
            vmem((rows - last, width), F32),
            vmem((across, some, width), F32),
            vmem((across - 1, lines, rows - last, width), BF16),
            vmem((lines, rows - last, width), BF16),
            vmem((lines, across, some, width), BF16),
            vmem((2, lines, rows - last, width), BF16),
            vmem((2, lines, across, some, width), BF16),
            vmem((some, width), BF16),
            dma((across - 1, lines)),
            dma((across - 1, lines)),
            dma((2, lines)),
            dma((2, lines)),
            dma((2, lines)),
            dma((2, lines)),
            dma,
            dma,
        ]

    def copy(self, src, dst, send, recv, target):
        return pltpu.make_async_remote_copy(
            src_ref=src, dst_ref=dst, send_sem=send, recv_sem=recv, device_id={"ctx": target}, device_id_type=MESH
        )

    def over(self, line, k):
        src = self.part.at[line, lax.rem(self.b + k, self.across), self.head]
        send, recv = self.o_send.at[k - 1, line], self.o_recv.at[k - 1, line]
        return self.copy(src, self.over_in.at[k - 1, line], send, recv, self.peers[k - 1])

    def along(self, line, way):
        target = self.me + (self.across, -self.across)[way]
        send, recv = self.l_send.at[way, line], self.l_recv.at[way, line]
        return self.copy(self.sums.at[line], self.line_in.at[way, line], send, recv, target)

    def along_t(self, line, way):
        target = self.me + (self.across, -self.across)[way]
        send, recv = self.t_send.at[way, line], self.t_recv.at[way, line]
        return self.copy(self.sums_t.at[line], self.line_in_t.at[way, line], send, recv, target)

    def twin(self):
        return self.copy(self.sums_t.at[self.a, 1 - self.b], self.twin_in, self.w_send, self.w_recv, self.peers[0])

    def compute(self, line):
        size = self.across * self.rows
        lhs = self.left[pl.ds(pl.multiple_of(line * size, size), size), :]
        value = dot_t(lhs, self.right[...]) if self.transposed else dot(lhs, self.right[...])
        self.part[line] = value.astype(BF16).reshape(self.across, self.rows, value.shape[1])
        for k in range(1, self.across):
            self.over(line, k).start()

    def collect(self, line, acc, landed, hop, ways):
        for way, there in ways:

            @pl.when(there)
            def _(way=way):
                hop(line, way).wait_recv()
                acc[...] += landed[way, line].astype(F32)

    def across_sum(self, line):
        value = self.part[line, self.b, self.head].astype(F32)
        for k in range(1, self.across):
            self.over(line, k).wait_recv()
            value = value + self.over_in[k - 1, line].astype(F32)
        self.acc[...] = value

    def pass_on(self, line):
        up, down = line > self.a, line < self.a
        ways = ((0, up & (self.a > 0)), (1, down & (self.a < self.lines - 1)))
        if self.last:
            self.acc_t[...] = self.part[line, :, self.tail].astype(F32)
            self.collect(line, self.acc_t, self.line_in_t, self.along_t, ways)
            self.sums_t[line] = self.acc_t[...].astype(BF16)
            pl.when(up)(lambda: self.along_t(line, 0).start())
            pl.when(down)(lambda: self.along_t(line, 1).start())
        self.across_sum(line)
        self.collect(line, self.acc, self.line_in, self.along, ways)
        self.sums[line] = self.acc[...].astype(BF16)
        pl.when(up)(lambda: self.along(line, 0).start())
        pl.when(down)(lambda: self.along(line, 1).start())

    def own(self):
        ways = ((0, self.near[1][0]), (1, self.near[0][0]))
        if self.last:
            self.acc_t[...] = self.part[self.a, :, self.tail].astype(F32)
            self.collect(self.a, self.acc_t, self.line_in_t, self.along_t, ways)
            self.sums_t[self.a] = self.acc_t[...].astype(BF16)
            self.twin().start()
        self.across_sum(self.a)
        self.collect(self.a, self.acc, self.line_in, self.along, ways)
        self.out[self.head, :] = self.acc[...]
        if self.last:
            self.twin().wait_recv()
            self.out[self.tail, :] = self.acc_t[self.b] + self.twin_in[...].astype(F32)

    def sent(self, order):
        for line in order:
            for k in range(1, self.across):
                self.over(line, k).wait_send()
        for line in order[:-1]:
            for way, there in ((0, line > self.a), (1, line < self.a)):

                @pl.when(there)
                def _(way=way, line=line):
                    self.along(line, way).wait_send()
                    if self.last:
                        self.along_t(line, way).wait_send()

        if self.last:
            self.twin().wait_send()


def product_body(n, nf, counts, transposed, *refs):
    n_prod, n_sides, n_fsdp = counts
    pairs, refs = refs[: 2 * n_prod], refs[2 * n_prod :]
    side_in, refs = refs[: 2 * n_sides], refs[2 * n_sides :]
    fsdp_in, refs = refs[:n_fsdp], refs[n_fsdp:]
    outs, side_out, fsdp_out = refs[:n_prod], refs[n_prod : n_prod + n_sides], refs[n_prod + n_sides : n_prod + n_sides + n_fsdp]
    scratch = refs[n_prod + n_sides + n_fsdp :]
    each = 17
    jobs = [
        Scatter(n, transposed[p], pairs[2 * p], pairs[2 * p + 1], outs[p], scratch[each * p : each * (p + 1)])
        for p in range(n_prod)
    ]
    fs = Fsdp(nf, fsdp_in, fsdp_out, [], [], scratch[each * n_prod :])
    a, lines = jobs[0].a, jobs[0].lines
    meet(jobs[0].near[:2], [("ctx", peer) for peer in jobs[0].peers] + [("fsdp", peer) for peer in fs.peers])

    order = []
    for k in range(lines):
        line = jnp.int32(0)
        for av in range(lines):
            line = jnp.where(a == av, sorted(range(lines), key=lambda j: (-abs(j - av), j))[k], line)
        order.append(line)

    for job in jobs:
        for line in order:
            job.compute(line)
    fs.start()
    steps = [(job, line) for job in jobs for line in order[:-1]]
    bits = []
    for j in range(n_sides):
        size = side_in[2 * j].shape[1]
        width = -(-size // 3 // 128) * 128
        bits += [(j, first, min(width, size - first)) for first in range(0, size, width)]
    for step, (job, line) in enumerate(steps):
        job.pass_on(line)
        for j, first, size in bits[step * len(bits) // len(steps) : (step + 1) * len(bits) // len(steps)]:
            part = side_in[2 * j][:, first : first + size]
            side_out[j][first : first + size, :] = t_dot(part, side_in[2 * j + 1][...]).astype(BF16)
        if step == len(order) - 2:
            fs.end()
    for job in jobs:
        job.own()
    for job in jobs:
        job.sent(order)
    fs.finish()


def product(call, n, nf, products, sides=(), fsdp=()):
    length = products[0][0].shape[0]
    if length > 1024 and (sides or len(products) > 1):
        sums = []
        for i, one in enumerate(products):
            total, *gathered = product(call if i == 0 else call + 10, n, nf, [one], fsdp=fsdp if i == 0 else ())
            sums.append(total)
            fsdp_out = gathered if i == 0 else fsdp_out
        return [*sums, *[t_dot(x, y).astype(BF16) for x, y in sides], *fsdp_out]
    rows = length // n
    shape = jax.ShapeDtypeStruct
    widths = [right.shape[0 if turned else 1] for _, right, turned in products]
    outs = [shape((rows, width), F32) for width in widths]
    outs += [shape((x.shape[1], y.shape[1]), BF16) for x, y in sides]
    outs += [shape((nf, *x.shape), x.dtype) for x in fsdp]
    inputs = [z for left, right, _ in products for z in (left, right)] + [z for side in sides for z in side]
    vmem_spec, any_spec = pl.BlockSpec(memory_space=pltpu.VMEM), pl.BlockSpec(memory_space=pl.ANY)
    return pl.pallas_call(
        functools.partial(
            product_body,
            n,
            nf,
            (len(products), len(sides), len(fsdp)),
            tuple(turned for _, _, turned in products),
        ),
        in_specs=[vmem_spec] * (len(inputs) + len(fsdp)),
        out_specs=[vmem_spec] * (len(outs) - len(fsdp)) + [any_spec] * len(fsdp),
        out_shape=outs,
        scratch_shapes=[s for width in widths for s in Scatter.scratch(n, rows, width)] + Fsdp.scratch(nf, fsdp, ()),
        name=f"product_{call}",
        compiler_params=pltpu.CompilerParams(collective_id=call, has_side_effects=True, vmem_limit_bytes=63 * 2**20),
    )(*inputs, *fsdp)


def row_moves(n, nf, heads):
    part, local = -(-heads // n) * HEAD_DIM // nf, heads * HEAD_DIM // nf
    moves = []
    for block, start, goal, size in head_moves(n, heads, 0, 0):
        done = 0
        while done < size:
            here, there = start + done, goal + done
            rows = min(size - done, part - here % part, local - there % local)
            moves.append((block, here % part, here // part, there // local, there % local, rows))
            done += rows
    return moves


def layout_body(moves, joint_ref, down_ref, out_ref, down_out, out_out, *outs):
    for ref, per_out in zip(outs, moves):
        for block, start, goal, size in per_out:
            ref[:, goal : goal + size] = joint_ref[block, :, start : start + size].astype(F32)
    down_out[...] = down_ref[...].astype(F32)
    out_out[...] = out_ref[...].astype(F32)


def lay_out(joint, down, out, widths, moves):
    n, rows, part = joint.shape
    step = next(s for s in (80, 16, rows) if rows % s == 0)
    grid = rows // step
    plain = [pl.BlockSpec((x.shape[0] // grid, x.shape[1]), lambda i: (i, 0)) for x in (down, out)]
    return pl.pallas_call(
        functools.partial(layout_body, tuple(tuple(m) for m in moves)),
        grid=(grid,),
        in_specs=[pl.BlockSpec((n, step, part), lambda i: (0, i, 0)), *plain],
        out_specs=plain + [pl.BlockSpec((step, width), lambda i: (i, 0)) for width in widths],
        out_shape=[jax.ShapeDtypeStruct(x.shape, F32) for x in (down, out)]
        + [jax.ShapeDtypeStruct((rows, width), F32) for width in widths],
        name="lay_out",
        cost_estimate=pl.CostEstimate(
            flops=0, bytes_accessed=6 * (rows * sum(widths) + down.size + out.size), transcendentals=0
        ),
        compiler_params=pltpu.CompilerParams(vmem_limit_bytes=60 * 2**20),
    )(joint, down, out)


def head_moves(n, heads, offset, goal):
    base, rest = divmod(heads, n)
    moves = [(c, offset, goal + c * base * HEAD_DIM, base * HEAD_DIM) for c in range(n) if base]
    moves += [
        (c, offset + base * HEAD_DIM, goal + (base * n + c) * HEAD_DIM, HEAD_DIM) for c in range(rest)
    ]
    return moves


def head_columns(value, width, c, n):
    heads = width // HEAD_DIM
    base, rest = divmod(heads, n)
    parts = []
    if base:
        parts.append(lax.dynamic_slice_in_dim(value, c * base * HEAD_DIM, base * HEAD_DIM, axis=-1))
    if rest:
        start = jnp.minimum(base * n + c, heads - 1) * HEAD_DIM
        extra = lax.dynamic_slice_in_dim(value, start, HEAD_DIM, axis=-1)
        parts.append(jnp.where(c < rest, extra, jnp.zeros_like(extra)))
    return jnp.concatenate(parts, axis=-1)


def place_heads(value, heads, c, n):
    base, rest = divmod(heads, n)
    out = jnp.zeros((heads * HEAD_DIM,), value.dtype)
    if rest:
        start = jnp.minimum(base * n + c, heads - 1) * HEAD_DIM
        extra = jnp.where(c < rest, value[base * HEAD_DIM :], 0.0)
        out = lax.dynamic_update_slice(out, extra, (start,))
    if base:
        out = lax.dynamic_update_slice(out, value[: base * HEAD_DIM], (c * base * HEAD_DIM,))
    return out


def head_rows(value, heads, c, f, n):
    base, rest = divmod(heads, n)
    local, width = value.shape
    pad = max(base, 1) * HEAD_DIM
    padded = jnp.pad(value, ((pad, pad), (0, 0)))
    parts = []
    if base:
        start = jnp.clip(c * base * HEAD_DIM - f * local + pad, 0, local + 2 * pad - base * HEAD_DIM)
        parts.append(lax.dynamic_slice_in_dim(padded, start, base * HEAD_DIM, axis=0))
    if rest:
        start = jnp.clip((base * n + c) * HEAD_DIM - f * local + pad, 0, local + 2 * pad - HEAD_DIM)
        extra = lax.dynamic_slice_in_dim(padded, start, HEAD_DIM, axis=0)
        parts.append(jnp.where(c < rest, extra, jnp.zeros_like(extra)))
    return jnp.concatenate(parts, axis=0)


def on_device(
    tokens,
    ln1_gain,
    ln1_shift,
    qkv_weight,
    qv_bias,
    out_weight,
    out_bias,
    ln2_gain,
    ln2_shift,
    up_weight,
    up_bias,
    down_weight,
    down_bias,
    block_table,
    cotangent,
):
    rows, width = tokens.shape[1:]
    heads = width // HEAD_DIM
    n = lax.axis_size("ctx")
    nf = lax.axis_size("fsdp")
    c = lax.axis_index("ctx")
    f = lax.axis_index("fsdp")
    slots = -(-heads // n)
    wide = slots * HEAD_DIM
    half = rows // 2
    local = width // nf
    ff = up_weight.shape[1]
    ff_local = ff // nf
    ff_part = ff_local // n

    within = jnp.arange(rows, dtype=jnp.int32)
    block_of = jnp.where(within[None, :] < half, block_table[:, None], 2 * n - 1 - block_table[:, None])
    place = (block_of * half + within[None, :] % half).reshape(-1)

    vectors = (ln1_gain, ln1_shift, qv_bias, out_bias, ln2_gain, ln2_shift, up_bias, down_bias)
    longest = max(v.shape[0] for v in vectors)
    flat = jnp.stack([jnp.pad(v, (0, longest - v.shape[0])) for v in vectors] * (-(-16 // len(vectors))))
    q_w = head_columns(qkv_weight[:, :width], width, c, n)
    k_w = head_columns(qkv_weight[:, width : 2 * width], width, c, n)
    v_w = head_columns(qkv_weight[:, 2 * width :], width, c, n)
    w_mine = jnp.concatenate([q_w, k_w, v_w], axis=1)
    x_all, packed, w_qkv = exchange(0, n, nf, ctx=[tokens[0]], fsdp=[flat, w_mine])
    out_weight, up_weight, down_weight, packed = lax.optimization_barrier(
        (out_weight, up_weight, down_weight, packed)
    )
    x_all = x_all.reshape(n * rows, width)
    w_qkv = w_qkv.reshape(width, 3 * wide)
    full = [packed[:, i, : v.shape[0]].reshape(-1).astype(F32) for i, v in enumerate(vectors)]
    gain1, shift1, b_qv, b_out, gain2, shift2, b_up, b_down = full

    b_up_mine = lax.dynamic_slice_in_dim(b_up.reshape(nf, n, ff_part), c, 1, axis=1).reshape(-1)
    bq = head_columns(b_qv[:width], width, c, n)
    bv = head_columns(b_qv[width:], width, c, n)

    n1_all, _ = ln_stats(x_all.astype(F32))
    act1 = (n1_all * gain1 + shift1).astype(BF16)
    proj = dot(act1, w_qkv)
    q = (proj[:, :wide] + bq).astype(BF16)
    k = proj[:, wide : 2 * wide].astype(BF16)
    v = (proj[:, 2 * wide :] + bv).astype(BF16)
    g2_all, w_out, attn, o, total = exchange(
        1,
        n,
        nf,
        ctx=[cotangent[0]],
        fsdp=[head_rows(out_weight, heads, c, f, n)],
        work=forward_work(place, q, k, v, slots),
    )
    w_out = jnp.sum(w_out.astype(F32), axis=0).astype(BF16)
    up_mine = [lax.dynamic_slice_in_dim(up_weight, i * ff_local + c * ff_part, ff_part, axis=1) for i in range(nf)]
    mixed, w_up = product(7, n, nf, [(attn, w_out, False)], fsdp=[jnp.concatenate(up_mine, axis=1)])
    w_up = w_up.reshape(width, nf * ff_part)
    x = tokens[0].astype(F32)
    mid = x + mixed + b_out

    n2, rstd2 = ln_stats(mid)
    act2, w_down = exchange(
        2,
        n,
        nf,
        ctx=[(n2 * gain2 + shift2).astype(BF16)],
        fsdp=[lax.dynamic_slice_in_dim(down_weight, c * ff_part, ff_part, axis=0)],
    )
    act2 = act2.reshape(n * rows, width)
    g2_all = g2_all.reshape(n * rows, width)
    w_down = w_down.reshape(nf * ff_part, width)
    u = dot(act2, w_up) + b_up_mine
    activated, gelu_back = jax.vjp(lambda t: jax.nn.gelu(t, approximate=True), u)
    hidden = activated.astype(BF16)
    dh = dot_t(g2_all, w_down)
    du = gelu_back(dh)[0].astype(BF16)
    da2, fed, d_up, d_down = product(
        3, n, nf, [(du, w_up, True), (hidden, w_down, False)], sides=[(act2, du), (hidden, g2_all)]
    )
    result = mid + fed + b_down
    d_up = d_up.reshape(nf, local, nf * ff_part)
    d_down = d_down.reshape(nf, ff_part, width)
    d_up_bias = jnp.sum(du.astype(F32), axis=0)
    grad_out = cotangent[0].astype(F32)
    d_down_bias = jnp.sum(grad_out, axis=0)

    d_gain2 = jnp.sum(da2 * n2, axis=0)
    d_shift2 = jnp.sum(da2, axis=0)
    d_mid = grad_out + ln_back(da2, n2, rstd2, gain2)
    g1 = d_mid.astype(BF16)
    d_out_bias = jnp.sum(g1.astype(F32), axis=0)
    g1_all, d_up, d_down = exchange(4, n, nf, ctx=[g1], own=[d_up, d_down])
    g1_all = g1_all.reshape(n * rows, width)
    d_attn = dot_t(g1_all, w_out)
    d_down, gq, gk, gv = exchange(
        8, n, nf, ctx=[d_down], work=backward_work(place, q, k, v, d_attn, o, total, slots)
    )
    g_qkv = jnp.concatenate([gq, gk, gv], axis=1)
    da1, d_qkv, d_out = product(5, n, nf, [(g_qkv, w_qkv, True)], sides=[(act1, g_qkv), (attn, g1_all)])
    d_qkv = d_qkv.reshape(nf, local, 3 * wide)
    d_out = d_out.reshape(nf, wide // nf, width)

    n1, rstd1 = ln_stats(x)
    d_gain1 = jnp.sum(da1 * n1, axis=0)
    d_shift1 = jnp.sum(da1, axis=0)
    input_grad = d_mid + ln_back(da1, n1, rstd1, gain1)

    dq_bias = place_heads(jnp.sum(gq.astype(F32), axis=0), heads, c, n)
    dv_bias = place_heads(jnp.sum(gv.astype(F32), axis=0), heads, c, n)
    up_placed = lax.dynamic_update_slice(
        jnp.zeros((nf, n, ff_part), F32), d_up_bias.reshape(nf, 1, ff_part), (0, c, 0)
    )
    smalls = (
        d_gain1,
        d_shift1,
        jnp.concatenate([dq_bias, dv_bias]),
        d_out_bias,
        d_gain2,
        d_shift2,
        up_placed.reshape(-1),
        d_down_bias,
    )
    packed = jnp.concatenate([s.reshape(nf, -1) for s in smalls], axis=1)
    packed = jnp.pad(packed, ((0, 0), (0, -packed.shape[1] % 1024))).reshape(nf, -1, 128)
    at_up = 3 * wide
    joint, _, packed, d_out = exchange(
        6,
        n,
        nf,
        red=[d_qkv, d_out, packed],
        pack=[d_up],
        firsts=(0, at_up),
        moves=row_moves(n, nf, heads),
        kept=local,
    )
    mine = jnp.sum(packed, axis=0).reshape(-1)
    up_moves = [(i, at_up + j * ff_part, j * ff_local + i * ff_part, ff_part) for i in range(n) for j in range(nf)]
    qkv_moves = [m for i in range(3) for m in head_moves(n, heads, i * wide, i * width)]
    d_down_full, d_out_full, d_up_full, d_qkv_full = lay_out(
        joint, d_down.reshape(ff_local, width), d_out, (ff, 3 * width), (up_moves, qkv_moves)
    )
    out, at = [], 0
    for s in smalls:
        size = s.size // nf
        out.append(mine[at : at + size])
        at += size
    return (
        result[None],
        input_grad[None],
        out[0],
        out[1],
        d_qkv_full,
        out[2],
        d_out_full,
        out[3],
        out[4],
        out[5],
        d_up_full,
        out[6],
        d_down_full,
        out[7],
    )


def solution(mesh):
    rows, one, two = P("fsdp", "ctx", None), P("fsdp"), P("fsdp", None)
    return jax.shard_map(
        on_device,
        mesh=mesh,
        in_specs=(rows, one, one, two, one, two, one, one, one, two, one, two, one, P(), rows),
        out_specs=(rows, rows, one, one, two, one, two, one, one, one, two, one, two, one),
        check_vma=False,
    )
```

```python
import functools

import jax
import jax.numpy as jnp
from jax import lax
from jax.experimental import pallas as pl
from jax.experimental.pallas import tpu as pltpu
from jax.sharding import PartitionSpec as P

HEAD_DIM = 64
EPS = 1e-05
SCALE = 0.125
F32 = jnp.float32
BF16 = jnp.bfloat16
MESH = pl.DeviceIdType.MESH


def dot(left, right):
    return jnp.dot(left, right, preferred_element_type=F32)


def dot_t(left, right):
    return lax.dot_general(left, right, (((1,), (1,)), ((), ())), preferred_element_type=F32)


def t_dot(left, right):
    return lax.dot_general(left, right, (((0,), (0,)), ((), ())), preferred_element_type=F32)


def ln_stats(value):
    centre = value - jnp.mean(value, axis=-1, keepdims=True)
    spread = jnp.mean(centre * centre, axis=-1, keepdims=True)
    rstd = lax.rsqrt(spread + EPS)
    return centre * rstd, rstd


def ln_back(grad, normed, rstd, gain):
    dn = grad * gain
    first = jnp.mean(dn, axis=-1, keepdims=True)
    second = jnp.mean(dn * normed, axis=-1, keepdims=True)
    return (dn - first - normed * second) * rstd


def query_rows(rows):
    return 256


def forward_step(slots, step, ins, outs, scratch):
    qp_ref, kp_ref, q_ref, k_ref, v_ref = ins
    attn_ref, o_ref, l_ref = outs
    size = query_rows(q_ref.shape[0])
    rows = slice(step * size, (step + 1) * size)
    allowed = kp_ref[...] <= qp_ref[rows, :]
    for h in range(slots):
        cols = slice(h * HEAD_DIM, (h + 1) * HEAD_DIM)
        raw = dot_t(q_ref[rows, cols], k_ref[:, cols])
        e = jnp.where(allowed, jnp.exp(raw * SCALE), 0.0)
        total = jnp.sum(e, axis=1, keepdims=True)
        numer = dot(e.astype(BF16), v_ref[:, cols])
        o = numer / total
        o_ref[rows, cols] = o
        attn_ref[rows, cols] = o.astype(BF16)
        l_ref[rows, h : h + 1] = total


def backward_step(slots, step, ins, outs, scratch):
    qp_ref, kp_ref, q_ref, k_ref, v_ref, do_ref, o_ref, l_ref = ins
    dq_ref, dk_ref, dv_ref = outs
    dk_acc, dv_acc = scratch
    size = query_rows(q_ref.shape[0])
    steps = q_ref.shape[0] // size
    rows = slice(step * size, (step + 1) * size)
    allowed = kp_ref[...] <= qp_ref[rows, :]
    for h in range(slots):
        cols = slice(h * HEAD_DIM, (h + 1) * HEAD_DIM)
        q, k, v, do = q_ref[rows, cols], k_ref[:, cols], v_ref[:, cols], do_ref[rows, cols]
        total = l_ref[rows, h : h + 1]
        w = (do / total).astype(BF16)
        corr = jnp.sum(do * o_ref[rows, cols], axis=1, keepdims=True) / total
        e = jnp.where(allowed, jnp.exp(dot_t(q, k) * SCALE), 0.0)
        de = dot_t(w, v)
        ds = (e * (de - corr)).astype(BF16)
        dq_ref[rows, cols] = (dot(ds, k) * SCALE).astype(BF16)
        dk, dv = t_dot(ds, q), t_dot(e.astype(BF16), w)
        if step:
            dk, dv = dk + dk_acc[:, cols], dv + dv_acc[:, cols]
        if step < steps - 1:
            dk_acc[:, cols] = dk
            dv_acc[:, cols] = dv
        else:
            dk_ref[:, cols] = (dk * SCALE).astype(BF16)
            dv_ref[:, cols] = dv.astype(BF16)


def forward_work(place, q, k, v, slots):
    rows, wide = q.shape
    shape = jax.ShapeDtypeStruct
    outs = (shape((rows, wide), BF16), shape((rows, wide), F32), shape((rows, slots), F32))
    steps = rows // query_rows(rows)
    ins = (place.reshape(rows, 1), place.reshape(1, rows), q, k, v)
    return steps, functools.partial(forward_step, slots), ins, outs, ()


def backward_work(place, q, k, v, do, o, total, slots):
    rows, wide = q.shape
    outs = (jax.ShapeDtypeStruct((rows, wide), BF16),) * 3
    steps = rows // query_rows(rows)
    ins = (place.reshape(rows, 1), place.reshape(1, rows), q, k, v, do, o, total)
    return steps, functools.partial(backward_step, slots), ins, outs, (pltpu.VMEM((rows, wide), F32),) * 2


def split_axis(n):
    across = 2 if n <= 8 else 4
    return n // across, across


def place_of(me, lines, across):
    a, b = lax.div(me, across), lax.rem(me, across)
    near = [(a < lines - 1, me + across), (a > 0, me - across), (b < across - 1, me + 1), (b > 0, me - 1)]
    return a, b, near


def turned_rows(rows, dtype, across, many=False):
    tile = 16 if dtype == BF16 else 8
    share = 4 if rows <= 128 and not many else 5
    return rows // share // tile * tile if across == 2 else 0


def meet(near, peers):
    barrier = pltpu.get_barrier_semaphore()
    for exists, target in near:

        @pl.when(exists)
        def _(target=target):
            pl.semaphore_signal(barrier, inc=1, device_id={"ctx": target}, device_id_type=MESH)

    for axis, peer in peers:
        pl.semaphore_signal(barrier, inc=1, device_id={axis: peer}, device_id_type=MESH)
    pl.semaphore_wait(barrier, len(peers) + sum(exists.astype(jnp.int32) for exists, _ in near))


class Fsdp:
    def __init__(self, nf, gather_in, gather_out, red_in, red_out, scratch):
        self.gather_in, self.gather_out, self.red_in, self.red_out = gather_in, gather_out, red_in, red_out
        n_gather, n_red = len(gather_in), len(red_in)
        self.near_in, self.stage, self.far_in = scratch[:n_red], scratch[n_red : 2 * n_red], scratch[2 * n_red : 3 * n_red]
        self.keep_sem, self.g_send, self.g_recv, self.r_send, self.r_recv = scratch[3 * n_red : 3 * n_red + 5]
        self.f = lax.axis_index("fsdp")
        self.core = lax.rem(self.f, 2)
        self.mate = self.f + 1 - 2 * self.core
        self.pairs = nf // 2
        self.pair = lax.div(self.f, 2)
        self.other = [lax.rem(self.pair + k, self.pairs) for k in range(1, self.pairs)]
        self.peers = [self.mate] + [2 * y + self.core for y in self.other] if n_gather + n_red else []

    @staticmethod
    def scratch(nf, gather, red):
        pairs = nf // 2
        dma = pltpu.SemaphoreType.DMA
        out = []
        for _ in range(3):
            out += [pltpu.VMEM((pairs, *x.shape[1:]), x.dtype) for x in red]
        g, r = max(len(gather), 1), max(len(red), 1)
        return out + [dma((g,)), dma((g, 2, nf)), dma((g, nf)), dma((r, 2, pairs)), dma((r, 2, pairs))]

    def copy(self, src, dst, send, recv, target):
        return pltpu.make_async_remote_copy(
            src_ref=src, dst_ref=dst, send_sem=send, recv_sem=recv, device_id={"fsdp": target}, device_id_type=MESH
        )

    def spread(self, i, source, target, own):
        out = self.gather_out[i].at[source]
        send = self.g_send.at[i, 0, target] if own else self.g_send.at[i, 1, source]
        return self.copy(self.gather_in[i] if own else out, out, send, self.g_recv.at[i, source], target)

    def keep(self, i):
        return pltpu.make_async_copy(self.gather_in[i], self.gather_out[i].at[self.f], self.keep_sem.at[i])

    def to_mate(self, j, y):
        src = self.red_in[j].at[2 * y + 1 - self.core]
        return self.copy(src, self.near_in[j].at[y], self.r_send.at[j, 0, y], self.r_recv.at[j, 0, y], self.mate)

    def to_far(self, j, y, source):
        send, recv = self.r_send.at[j, 1, y], self.r_recv.at[j, 1, source]
        return self.copy(self.stage[j].at[y], self.far_in[j].at[source], send, recv, 2 * y + self.core)

    def write(self, j, value):
        out, first = self.red_out[j]
        out[:, first : first + value.shape[1]] = value.astype(out.dtype)

    def start(self):
        for j in range(len(self.red_in)):
            for y in range(self.pairs):
                self.to_mate(j, y).start()
        for i in range(len(self.gather_in)):
            for target in self.peers[1:] + self.peers[:1]:
                self.spread(i, self.f, target, True).start()
            self.keep(i).start()

    def middle(self):
        for j in range(len(self.red_in)):
            for y in range(self.pairs):
                self.to_mate(j, y).wait_recv()
            for y in self.other:
                value = self.red_in[j][2 * y + self.core].astype(F32) + self.near_in[j][y].astype(F32)
                self.stage[j][y] = value.astype(self.stage[j].dtype)
                self.to_far(j, y, self.pair).start()

    def end(self):
        for j in range(len(self.red_in)):
            value = self.red_in[j][self.f].astype(F32) + self.near_in[j][self.pair].astype(F32)
            for y in self.other:
                self.to_far(j, y, y).wait_recv()
                value = value + self.far_in[j][y].astype(F32)
            self.write(j, value)
        for i in range(len(self.gather_in)):
            for y in self.other:
                source = 2 * y + self.core
                self.spread(i, source, self.mate, False).wait_recv()
                self.spread(i, source, self.mate, False).start()

    def finish(self):
        for i in range(len(self.gather_in)):
            self.spread(i, self.mate, self.mate, False).wait_recv()
            for y in self.other:
                self.spread(i, 2 * y + 1 - self.core, self.mate, False).wait_recv()
            self.keep(i).wait()
            for target in self.peers:
                self.spread(i, self.f, target, True).wait_send()
            for y in self.other:
                self.spread(i, 2 * y + self.core, self.mate, False).wait_send()
        for j in range(len(self.red_in)):
            for y in range(self.pairs):
                self.to_mate(j, y).wait_send()
            for y in self.other:
                self.to_far(j, y, self.pair).wait_send()


def exchange_body(n, nf, counts, firsts, moves, work, *refs):
    n_ctx, n_fsdp, n_own, n_red, n_pack, n_work_in, n_work_out, n_work_scratch = counts
    bounds = [0]
    for size in counts[:6]:
        bounds.append(bounds[-1] + size)
    ctx_in, fsdp_in, own_in, red_in, pack_in, work_in = (refs[i:j] for i, j in zip(bounds, bounds[1:]))
    refs = refs[bounds[-1] :]
    n_joint = len(firsts) - n_pack
    n_sums = n_red - n_joint + (1 if n_pack else 0)
    ctx_out, fsdp_out, own_out = refs[:n_ctx], refs[n_ctx : n_ctx + n_fsdp], refs[n_ctx + n_fsdp : n_ctx + n_fsdp + n_own]
    refs = refs[n_ctx + n_fsdp + n_own :]
    red_out, refs = refs[:n_sums], refs[n_sums:]
    if moves:
        placed, refs = refs[0], refs[1:]
    work_out, refs = refs[:n_work_out], refs[n_work_out:]
    work_scratch, refs = refs[:n_work_scratch], refs[n_work_scratch:]
    sums, scratch = refs[:n_sums], refs[n_sums:]
    copy_sem, send_sem, recv_sem, place_send, place_recv = scratch[:5]
    goals = [(out, 0) for out in own_out]
    goals += [(sums[0], firsts[j]) for j in range(n_joint)]
    goals += [(out, 0) for out in sums[1 if n_pack else 0 :]]
    fs = Fsdp(nf, fsdp_in, fsdp_out, own_in + red_in, goals, scratch[5:])

    lines, across = split_axis(n)
    me = lax.axis_index("ctx")
    a, b, near = place_of(me, lines, across)
    pieces = [(src, out, first, rows) for src, out in zip(ctx_in, ctx_out) for first, rows in cut(out.shape[1])]
    late = len(pieces)
    for src, out in reversed(list(zip(sums, red_out))):
        pieces += [(src, out, first, rows) for first, rows in cut(out.shape[1])]
    peers = [lax.rem(fs.f + k, nf) for k in range(1, nf)] if moves else fs.peers
    meet(near if pieces else [], [("fsdp", peer) for peer in peers])
    fs.start()

    def turned_part(i):
        return turned_rows(pieces[i][3], pieces[i][1].dtype, across, len(pieces) > 1)

    def hop(i, block, way, turned=False, own=False):
        source, out, first, size = pieces[i]
        last = turned_part(i)
        rows = pl.ds(first + size - last, last) if turned else pl.ds(first, size - last)
        return pltpu.make_async_remote_copy(
            src_ref=source.at[rows] if own else out.at[block, rows],
            dst_ref=out.at[block, rows],
            send_sem=send_sem.at[i, way, block, int(turned)],
            recv_sem=recv_sem.at[i, way, block, int(turned)],
            device_id={"ctx": me + (across, -across, 1, -1)[way]},
            device_id_type=MESH,
        )

    def keep(i):
        source, out, first, size = pieces[i]
        rows = pl.ds(first, size)
        return pltpu.make_async_copy(source.at[rows], out.at[me, rows], copy_sem.at[i])

    def each_own(i, act):
        for turned in (True, False) if turned_part(i) else (False,):
            for way in (2, 3, 0, 1):
                pl.when(near[way][0])(lambda way=way: act(hop(i, me, way, turned, True)))

    def each_twin(i, wait, act):
        if turned_part(i):
            twin = me + 1 - 2 * b
            for way in (2, 3):

                @pl.when(near[5 - way][0])
                def _(way=way):
                    if wait:
                        hop(i, twin, way, True).wait_recv()
                    for on in (0, 1):
                        pl.when(near[on][0])(lambda on=on: act(hop(i, twin, on, True)))

    def each_relay(i, d, wait, act):
        for way, there, shift in ((0, a >= d, -d * across), (1, a + d < lines, d * across)):

            @pl.when(there)
            def _(way=way, shift=shift):
                for turned, block in [(False, me + shift)] + (
                    [(True, me + shift), (True, me + 1 - 2 * b + shift)] if turned_part(i) else []
                ):
                    if wait:
                        hop(i, block, way, turned).wait_recv()
                    for on in (way,) if turned else (2, 3, way):
                        pl.when(near[on][0])(lambda on=on: act(hop(i, block, on, turned)))

    def start(copy):
        copy.start()

    def wait_send(copy):
        copy.wait_send()

    def begin(these):
        for i in these:
            each_own(i, start)
            keep(i).start()

    work_steps, work_fn = work
    points = 1 + (lines - 1) * len(pieces)
    passed = [0]

    def do_work():
        at = passed[0]
        passed[0] += 1
        for step in range(at * work_steps // points, (at + 1) * work_steps // points):
            work_fn(step, work_in, work_out, work_scratch)

    begin(range(late))
    fs.middle()
    do_work()
    for j in range(n_pack):
        first = firsts[n_joint + j]
        sums[0][:, first : first + pack_in[j].shape[1]] = pack_in[j][...]
    if n_sums:
        if late:
            each_twin(0, True, start)
            each_relay(0, 1, True, start)
            do_work()
        fs.end()
        begin(range(late, len(pieces)))
    for d in range(1, lines):
        for i in range(len(pieces)):
            if d == 1:
                if i == 0 and late and n_sums:
                    continue
                each_twin(i, True, start)
            each_relay(i, d, True, start)
            do_work()
    if not n_sums:
        fs.end()

    def crossed(i):
        for d in range(1, across):
            for step in range(lines):
                for sign in (1, -1) if step else (1,):
                    for way, there, shift in ((2, b >= d, -d), (3, b + d < across, d)):
                        other = a + sign * step

                        @pl.when(there & (other >= 0) & (other < lines))
                        def _(source=other * across + b + shift, way=way):
                            hop(i, source, way).wait_recv()
                            if d < across - 1:
                                pl.when(near[way][0])(lambda: hop(i, source, way).start())

    def place(k, act_local, act_send):
        block, row, src, dst, goal, size = moves[k]
        source, goal = red_out[1].at[block, pl.ds(row, size)], placed.at[pl.ds(goal, size)]
        if src == dst:
            pl.when(fs.f == src)(lambda: act_local(pltpu.make_async_copy(source, goal, place_send.at[k])))
            return
        remote = pltpu.make_async_remote_copy(
            src_ref=source,
            dst_ref=goal,
            send_sem=place_send.at[k],
            recv_sem=place_recv.at[k],
            device_id={"fsdp": jnp.int32(dst)},
            device_id_type=MESH,
        )
        pl.when(fs.f == src)(lambda: act_send(remote))
        if act_local is wait_copy:
            pl.when(fs.f == dst)(remote.wait_recv)

    def wait_copy(copy):
        copy.wait()

    if moves:
        ready = [i for i in range(len(pieces)) if pieces[i][1] is red_out[1]]
        for i in ready:
            crossed(i)
            keep(i).wait()
        for k in range(len(moves)):
            place(k, start, start)
    else:
        ready = []
    for i in range(len(pieces)):
        if i not in ready:
            crossed(i)
            keep(i).wait()
    for k in range(len(moves)):
        place(k, wait_copy, wait_send)

    for i in range(len(pieces)):
        each_own(i, wait_send)
        each_twin(i, False, wait_send)
        for d in range(1, lines):
            each_relay(i, d, False, wait_send)
        for d in range(1, across - 1):
            for line in range(lines):
                for way, there, shift in ((2, b >= d, -d), (3, b + d < across, d)):

                    @pl.when(there & near[way][0])
                    def _(i=i, source=line * across + b + shift, way=way):
                        hop(i, source, way).wait_send()

    fs.finish()


def cut(rows):
    if rows < 200:
        return [(0, rows)]
    half = rows // 32 * 16
    return [(0, rows - half), (rows - half, half)]


def exchange(call, n, nf, ctx=(), fsdp=(), own=(), red=(), pack=(), firsts=(), moves=(), kept=0, work=None):
    shape = jax.ShapeDtypeStruct
    sums = [shape(x.shape[1:], x.dtype) for x in red]
    if pack:
        joint = len(firsts) - len(pack)
        width = sum(x.shape[1] for x in [*sums[:joint], *pack])
        sums = [shape((pack[0].shape[0], width), pack[0].dtype)] + sums[joint:]
    outs = [shape((n, *x.shape), x.dtype) for x in ctx]
    outs += [shape((nf, *x.shape), x.dtype) for x in fsdp]
    outs += [shape(x.shape[1:], x.dtype) for x in own]
    outs += [shape((n, *x.shape), x.dtype) for x in sums]
    outs += [shape((kept, sums[1].shape[1]), sums[1].dtype)] if moves else []
    steps, work_fn, work_in, work_out, work_scratch = work or (0, None, (), (), ())
    gathered = max(sum(len(cut(x.shape[0])) for x in [*ctx, *sums]), 1)
    any_spec, vmem_spec = pl.BlockSpec(memory_space=pl.ANY), pl.BlockSpec(memory_space=pltpu.VMEM)
    inputs = (*ctx, *fsdp, *own, *red, *pack, *work_in)
    counts = [len(x) for x in (ctx, fsdp, own, red, pack, work_in, work_out, work_scratch)]
    dma = pltpu.SemaphoreType.DMA
    return pl.pallas_call(
        functools.partial(exchange_body, n, nf, tuple(counts), tuple(firsts), tuple(moves), (steps, work_fn)),
        in_specs=[any_spec] * (len(ctx) + len(fsdp)) + [vmem_spec] * (len(inputs) - len(ctx) - len(fsdp)),
        out_specs=[any_spec] * (len(ctx) + len(fsdp))
        + [vmem_spec] * len(own)
        + [any_spec] * (len(sums) + (1 if moves else 0))
        + [vmem_spec] * len(work_out),
        out_shape=[*outs, *work_out],
        scratch_shapes=list(work_scratch)
        + [pltpu.VMEM(x.shape, x.dtype) for x in sums]
        + [dma((gathered,)), dma((gathered, 4, n, 2)), dma((gathered, 4, n, 2))]
        + [dma((max(len(moves), 1),))] * 2
        + Fsdp.scratch(nf, fsdp, [*own, *red]),
        name=f"exchange_{call}",
        compiler_params=pltpu.CompilerParams(collective_id=call, has_side_effects=True, vmem_limit_bytes=60 * 2**20),
    )(*inputs)


class Scatter:
    def __init__(self, n, many, transposed, left, right, out, scratch):
        self.left, self.right, self.out, self.transposed = left, right, out, transposed
        self.part, self.acc, self.acc_t, self.over_in, self.sums, self.sums_t = scratch[:6]
        self.line_in, self.line_in_t, self.twin_in = scratch[6:9]
        self.o_send, self.o_recv, self.l_send, self.l_recv, self.t_send, self.t_recv = scratch[9:15]
        self.w_send, self.w_recv = scratch[15:17]
        self.lines, self.across = split_axis(n)
        self.me = lax.axis_index("ctx")
        self.a, self.b, self.near = place_of(self.me, self.lines, self.across)
        self.rows = out.shape[0]
        self.last = turned_rows(self.rows, BF16, self.across, many)
        self.head, self.tail = pl.ds(0, self.rows - self.last), pl.ds(self.rows - self.last, self.last)
        self.peers = [self.me - self.b + lax.rem(self.b + k, self.across) for k in range(1, self.across)]

    @staticmethod
    def scratch(n, many, rows, width):
        lines, across = split_axis(n)
        last = turned_rows(rows, BF16, across, many)
        some = max(last, 16)
        vmem, dma = pltpu.VMEM, pltpu.SemaphoreType.DMA
        return [
            vmem((lines, across, rows, width), BF16),
            vmem((rows - last, width), F32),
            vmem((across, some, width), F32),
            vmem((across - 1, lines, rows - last, width), BF16),
            vmem((lines, rows - last, width), BF16),
            vmem((lines, across, some, width), BF16),
            vmem((2, lines, rows - last, width), BF16),
            vmem((2, lines, across, some, width), BF16),
            vmem((some, width), BF16),
            dma((across - 1, lines)),
            dma((across - 1, lines)),
            dma((2, lines)),
            dma((2, lines)),
            dma((2, lines)),
            dma((2, lines)),
            dma,
            dma,
        ]

    def copy(self, src, dst, send, recv, target):
        return pltpu.make_async_remote_copy(
            src_ref=src, dst_ref=dst, send_sem=send, recv_sem=recv, device_id={"ctx": target}, device_id_type=MESH
        )

    def over(self, line, k):
        src = self.part.at[line, lax.rem(self.b + k, self.across), self.head]
        send, recv = self.o_send.at[k - 1, line], self.o_recv.at[k - 1, line]
        return self.copy(src, self.over_in.at[k - 1, line], send, recv, self.peers[k - 1])

    def along(self, line, way):
        target = self.me + (self.across, -self.across)[way]
        send, recv = self.l_send.at[way, line], self.l_recv.at[way, line]
        return self.copy(self.sums.at[line], self.line_in.at[way, line], send, recv, target)

    def along_t(self, line, way):
        target = self.me + (self.across, -self.across)[way]
        send, recv = self.t_send.at[way, line], self.t_recv.at[way, line]
        return self.copy(self.sums_t.at[line], self.line_in_t.at[way, line], send, recv, target)

    def twin(self):
        return self.copy(self.sums_t.at[self.a, 1 - self.b], self.twin_in, self.w_send, self.w_recv, self.peers[0])

    def compute(self, line):
        size = self.across * self.rows
        lhs = self.left[pl.ds(pl.multiple_of(line * size, size), size), :]
        value = dot_t(lhs, self.right[...]) if self.transposed else dot(lhs, self.right[...])
        self.part[line] = value.astype(BF16).reshape(self.across, self.rows, value.shape[1])
        for k in range(1, self.across):
            self.over(line, k).start()

    def collect(self, line, acc, landed, hop, ways):
        for way, there in ways:

            @pl.when(there)
            def _(way=way):
                hop(line, way).wait_recv()
                acc[...] += landed[way, line].astype(F32)

    def across_sum(self, line):
        value = self.part[line, self.b, self.head].astype(F32)
        for k in range(1, self.across):
            self.over(line, k).wait_recv()
            value = value + self.over_in[k - 1, line].astype(F32)
        self.acc[...] = value

    def pass_on(self, line):
        up, down = line > self.a, line < self.a
        ways = ((0, up & (self.a > 0)), (1, down & (self.a < self.lines - 1)))
        if self.last:
            self.acc_t[...] = self.part[line, :, self.tail].astype(F32)
            self.collect(line, self.acc_t, self.line_in_t, self.along_t, ways)
            self.sums_t[line] = self.acc_t[...].astype(BF16)
            pl.when(up)(lambda: self.along_t(line, 0).start())
            pl.when(down)(lambda: self.along_t(line, 1).start())
        self.across_sum(line)
        self.collect(line, self.acc, self.line_in, self.along, ways)
        self.sums[line] = self.acc[...].astype(BF16)
        pl.when(up)(lambda: self.along(line, 0).start())
        pl.when(down)(lambda: self.along(line, 1).start())

    def own(self):
        ways = ((0, self.near[1][0]), (1, self.near[0][0]))
        if self.last:
            self.acc_t[...] = self.part[self.a, :, self.tail].astype(F32)
            self.collect(self.a, self.acc_t, self.line_in_t, self.along_t, ways)
            self.sums_t[self.a] = self.acc_t[...].astype(BF16)
            self.twin().start()
        self.across_sum(self.a)
        self.collect(self.a, self.acc, self.line_in, self.along, ways)
        self.out[self.head, :] = self.acc[...]
        if self.last:
            self.twin().wait_recv()
            self.out[self.tail, :] = self.acc_t[self.b] + self.twin_in[...].astype(F32)

    def sent(self, order):
        for line in order:
            for k in range(1, self.across):
                self.over(line, k).wait_send()
        for line in order[:-1]:
            for way, there in ((0, line > self.a), (1, line < self.a)):

                @pl.when(there)
                def _(way=way, line=line):
                    self.along(line, way).wait_send()
                    if self.last:
                        self.along_t(line, way).wait_send()

        if self.last:
            self.twin().wait_send()


def product_body(n, nf, counts, transposed, *refs):
    n_prod, n_sides, n_fsdp = counts
    pairs, refs = refs[: 2 * n_prod], refs[2 * n_prod :]
    side_in, refs = refs[: 2 * n_sides], refs[2 * n_sides :]
    fsdp_in, refs = refs[:n_fsdp], refs[n_fsdp:]
    outs, side_out, fsdp_out = refs[:n_prod], refs[n_prod : n_prod + n_sides], refs[n_prod + n_sides : n_prod + n_sides + n_fsdp]
    scratch = refs[n_prod + n_sides + n_fsdp :]
    each = 17
    jobs = [
        Scatter(n, n_prod > 1, transposed[p], pairs[2 * p], pairs[2 * p + 1], outs[p], scratch[each * p : each * (p + 1)])
        for p in range(n_prod)
    ]
    fs = Fsdp(nf, fsdp_in, fsdp_out, [], [], scratch[each * n_prod :])
    a, lines = jobs[0].a, jobs[0].lines
    meet(jobs[0].near[:2], [("ctx", peer) for peer in jobs[0].peers] + [("fsdp", peer) for peer in fs.peers])

    order = []
    for k in range(lines):
        line = jnp.int32(0)
        for av in range(lines):
            line = jnp.where(a == av, sorted(range(lines), key=lambda j: (-abs(j - av), j))[k], line)
        order.append(line)

    for job in jobs:
        for line in order:
            job.compute(line)
    fs.start()
    steps = [(job, line) for job in jobs for line in order[:-1]]
    bits = []
    for j in range(n_sides):
        size = side_in[2 * j].shape[1]
        width = -(-size // 3 // 128) * 128
        bits += [(j, first, min(width, size - first)) for first in range(0, size, width)]
    for step, (job, line) in enumerate(steps):
        job.pass_on(line)
        for j, first, size in bits[step * len(bits) // len(steps) : (step + 1) * len(bits) // len(steps)]:
            part = side_in[2 * j][:, first : first + size]
            side_out[j][first : first + size, :] = t_dot(part, side_in[2 * j + 1][...]).astype(BF16)
        if step == len(order) - 2:
            fs.end()
    for job in jobs:
        job.own()
    for job in jobs:
        job.sent(order)
    fs.finish()


def product(call, n, nf, products, sides=(), fsdp=()):
    length = products[0][0].shape[0]
    if length > 1024 and (sides or len(products) > 1):
        sums = []
        for i, one in enumerate(products):
            total, *gathered = product(call if i == 0 else call + 10, n, nf, [one], fsdp=fsdp if i == 0 else ())
            sums.append(total)
            fsdp_out = gathered if i == 0 else fsdp_out
        return [*sums, *[t_dot(x, y).astype(BF16) for x, y in sides], *fsdp_out]
    rows = length // n
    shape = jax.ShapeDtypeStruct
    widths = [right.shape[0 if turned else 1] for _, right, turned in products]
    outs = [shape((rows, width), F32) for width in widths]
    outs += [shape((x.shape[1], y.shape[1]), BF16) for x, y in sides]
    outs += [shape((nf, *x.shape), x.dtype) for x in fsdp]
    inputs = [z for left, right, _ in products for z in (left, right)] + [z for side in sides for z in side]
    vmem_spec, any_spec = pl.BlockSpec(memory_space=pltpu.VMEM), pl.BlockSpec(memory_space=pl.ANY)
    return pl.pallas_call(
        functools.partial(
            product_body,
            n,
            nf,
            (len(products), len(sides), len(fsdp)),
            tuple(turned for _, _, turned in products),
        ),
        in_specs=[vmem_spec] * (len(inputs) + len(fsdp)),
        out_specs=[vmem_spec] * (len(outs) - len(fsdp)) + [any_spec] * len(fsdp),
        out_shape=outs,
        scratch_shapes=[s for width in widths for s in Scatter.scratch(n, len(widths) > 1, rows, width)] + Fsdp.scratch(nf, fsdp, ()),
        name=f"product_{call}",
        compiler_params=pltpu.CompilerParams(collective_id=call, has_side_effects=True, vmem_limit_bytes=63 * 2**20),
    )(*inputs, *fsdp)


def row_moves(n, nf, heads):
    part, local = -(-heads // n) * HEAD_DIM // nf, heads * HEAD_DIM // nf
    moves = []
    for block, start, goal, size in head_moves(n, heads, 0, 0):
        done = 0
        while done < size:
            here, there = start + done, goal + done
            rows = min(size - done, part - here % part, local - there % local)
            moves.append((block, here % part, here // part, there // local, there % local, rows))
            done += rows
    return moves


def layout_body(moves, *refs):
    ins, outs = refs[: len(refs) // 2], refs[len(refs) // 2 :]
    for in_ref, out_ref, per_out in zip(ins, outs, moves):
        if per_out is None:
            out_ref[...] = in_ref[...].astype(F32)
            continue
        for block, start, goal, size in per_out:
            out_ref[:, goal : goal + size] = in_ref[block, :, start : start + size].astype(F32)


def lay_out(arrays, widths, moves):
    rows = next(x.shape[1] for x in arrays if x.ndim == 3)
    step = next(s for s in (80, 16, rows) if rows % s == 0)
    grid = rows // step
    in_specs, out_specs, outs = [], [], []
    for x, width in zip(arrays, widths):
        flat = pl.BlockSpec((x.shape[-2] // grid, width), lambda i: (i, 0))
        in_specs.append(pl.BlockSpec((x.shape[0], step, x.shape[2]), lambda i: (0, i, 0)) if x.ndim == 3 else flat)
        out_specs.append(flat)
        outs.append(jax.ShapeDtypeStruct((x.shape[-2], width), F32))
    return pl.pallas_call(
        functools.partial(layout_body, tuple(m and tuple(m) for m in moves)),
        grid=(grid,),
        in_specs=in_specs,
        out_specs=out_specs,
        out_shape=outs,
        name="lay_out",
        cost_estimate=pl.CostEstimate(
            flops=0, bytes_accessed=6 * sum(x.shape[0] * x.shape[1] for x in outs), transcendentals=0
        ),
        compiler_params=pltpu.CompilerParams(vmem_limit_bytes=60 * 2**20),
    )(*arrays)


def head_moves(n, heads, offset, goal):
    base, rest = divmod(heads, n)
    moves = [(c, offset, goal + c * base * HEAD_DIM, base * HEAD_DIM) for c in range(n) if base]
    moves += [
        (c, offset + base * HEAD_DIM, goal + (base * n + c) * HEAD_DIM, HEAD_DIM) for c in range(rest)
    ]
    return moves


def head_columns(value, width, c, n):
    heads = width // HEAD_DIM
    base, rest = divmod(heads, n)
    parts = []
    if base:
        parts.append(lax.dynamic_slice_in_dim(value, c * base * HEAD_DIM, base * HEAD_DIM, axis=-1))
    if rest:
        start = jnp.minimum(base * n + c, heads - 1) * HEAD_DIM
        extra = lax.dynamic_slice_in_dim(value, start, HEAD_DIM, axis=-1)
        parts.append(jnp.where(c < rest, extra, jnp.zeros_like(extra)))
    return jnp.concatenate(parts, axis=-1)


def place_heads(value, heads, c, n):
    base, rest = divmod(heads, n)
    out = jnp.zeros((heads * HEAD_DIM,), value.dtype)
    if rest:
        start = jnp.minimum(base * n + c, heads - 1) * HEAD_DIM
        extra = jnp.where(c < rest, value[base * HEAD_DIM :], 0.0)
        out = lax.dynamic_update_slice(out, extra, (start,))
    if base:
        out = lax.dynamic_update_slice(out, value[: base * HEAD_DIM], (c * base * HEAD_DIM,))
    return out


def head_rows(value, heads, c, f, n):
    base, rest = divmod(heads, n)
    local, width = value.shape
    pad = max(base, 1) * HEAD_DIM
    padded = jnp.pad(value, ((pad, pad), (0, 0)))
    parts = []
    if base:
        start = jnp.clip(c * base * HEAD_DIM - f * local + pad, 0, local + 2 * pad - base * HEAD_DIM)
        parts.append(lax.dynamic_slice_in_dim(padded, start, base * HEAD_DIM, axis=0))
    if rest:
        start = jnp.clip((base * n + c) * HEAD_DIM - f * local + pad, 0, local + 2 * pad - HEAD_DIM)
        extra = lax.dynamic_slice_in_dim(padded, start, HEAD_DIM, axis=0)
        parts.append(jnp.where(c < rest, extra, jnp.zeros_like(extra)))
    return jnp.concatenate(parts, axis=0)


def on_device(
    tokens,
    ln1_gain,
    ln1_shift,
    qkv_weight,
    qv_bias,
    out_weight,
    out_bias,
    ln2_gain,
    ln2_shift,
    up_weight,
    up_bias,
    down_weight,
    down_bias,
    block_table,
    cotangent,
):
    rows, width = tokens.shape[1:]
    heads = width // HEAD_DIM
    n = lax.axis_size("ctx")
    nf = lax.axis_size("fsdp")
    c = lax.axis_index("ctx")
    f = lax.axis_index("fsdp")
    slots = -(-heads // n)
    wide = slots * HEAD_DIM
    half = rows // 2
    local = width // nf
    ff = up_weight.shape[1]
    ff_local = ff // nf
    ff_part = ff_local // n

    within = jnp.arange(rows, dtype=jnp.int32)
    block_of = jnp.where(within[None, :] < half, block_table[:, None], 2 * n - 1 - block_table[:, None])
    place = (block_of * half + within[None, :] % half).reshape(-1)

    vectors = (ln1_gain, ln1_shift, qv_bias, out_bias, ln2_gain, ln2_shift, up_bias, down_bias)
    longest = max(v.shape[0] for v in vectors)
    flat = sum(
        jnp.pad(v.astype(F32)[None, :], ((i, 15 - i), (0, longest - v.shape[0]))) for i, v in enumerate(vectors)
    ).astype(BF16)
    q_w = head_columns(qkv_weight[:, :width], width, c, n)
    k_w = head_columns(qkv_weight[:, width : 2 * width], width, c, n)
    v_w = head_columns(qkv_weight[:, 2 * width :], width, c, n)
    w_mine = jnp.concatenate([q_w, k_w, v_w], axis=1)
    x_all, packed, w_qkv = exchange(0, n, nf, ctx=[tokens[0]], fsdp=[flat, w_mine])
    out_weight, up_weight, down_weight, packed = lax.optimization_barrier(
        (out_weight, up_weight, down_weight, packed)
    )
    x_all = x_all.reshape(n * rows, width)
    w_qkv = w_qkv.reshape(width, 3 * wide)
    full = [packed[:, i, : v.shape[0]].reshape(-1).astype(F32) for i, v in enumerate(vectors)]
    gain1, shift1, b_qv, b_out, gain2, shift2, b_up, b_down = full

    b_up_mine = lax.dynamic_slice_in_dim(b_up.reshape(nf, n, ff_part), c, 1, axis=1).reshape(-1)
    bq = head_columns(b_qv[:width], width, c, n)
    bv = head_columns(b_qv[width:], width, c, n)

    n1_all, _ = ln_stats(x_all.astype(F32))
    act1 = (n1_all * gain1 + shift1).astype(BF16)
    proj = dot(act1, w_qkv)
    q = (proj[:, :wide] + bq).astype(BF16)
    k = proj[:, wide : 2 * wide].astype(BF16)
    v = (proj[:, 2 * wide :] + bv).astype(BF16)
    g2_all, w_out, attn, o, total = exchange(
        1,
        n,
        nf,
        ctx=[cotangent[0]],
        fsdp=[head_rows(out_weight, heads, c, f, n)],
        work=forward_work(place, q, k, v, slots),
    )
    w_out = jnp.sum(w_out.astype(F32), axis=0).astype(BF16)
    up_mine = [lax.dynamic_slice_in_dim(up_weight, i * ff_local + c * ff_part, ff_part, axis=1) for i in range(nf)]
    mixed, w_up = product(7, n, nf, [(attn, w_out, False)], fsdp=[jnp.concatenate(up_mine, axis=1)])
    w_up = w_up.reshape(width, nf * ff_part)
    x = tokens[0].astype(F32)
    mid = x + mixed + b_out

    n2, rstd2 = ln_stats(mid)
    act2, w_down = exchange(
        2,
        n,
        nf,
        ctx=[(n2 * gain2 + shift2).astype(BF16)],
        fsdp=[lax.dynamic_slice_in_dim(down_weight, c * ff_part, ff_part, axis=0)],
    )
    act2 = act2.reshape(n * rows, width)
    g2_all = g2_all.reshape(n * rows, width)
    w_down = w_down.reshape(nf * ff_part, width)
    u = dot(act2, w_up) + b_up_mine
    activated, gelu_back = jax.vjp(lambda t: jax.nn.gelu(t, approximate=True), u)
    hidden = activated.astype(BF16)
    dh = dot_t(g2_all, w_down)
    du = gelu_back(dh)[0].astype(BF16)
    da2, fed, d_up, d_down = product(
        3, n, nf, [(du, w_up, True), (hidden, w_down, False)], sides=[(act2, du), (hidden, g2_all)]
    )
    result = mid + fed + b_down
    d_up = d_up.reshape(nf, local, nf * ff_part)
    d_down = d_down.reshape(nf, ff_part, width)
    d_up_bias = jnp.sum(du.astype(F32), axis=0)
    grad_out = cotangent[0].astype(F32)
    d_down_bias = jnp.sum(grad_out, axis=0)

    d_gain2 = jnp.sum(da2 * n2, axis=0)
    d_shift2 = jnp.sum(da2, axis=0)
    d_mid = grad_out + ln_back(da2, n2, rstd2, gain2)
    g1 = d_mid.astype(BF16)
    d_out_bias = jnp.sum(g1.astype(F32), axis=0)
    g1_all, d_up, d_down = exchange(4, n, nf, ctx=[g1], own=[d_up, d_down])
    g1_all = g1_all.reshape(n * rows, width)
    d_attn = dot_t(g1_all, w_out)
    d_up, gq, gk, gv = exchange(
        8, n, nf, ctx=[d_up], work=backward_work(place, q, k, v, d_attn, o, total, slots)
    )
    g_qkv = jnp.concatenate([gq, gk, gv], axis=1)
    da1, d_qkv, d_out = product(5, n, nf, [(g_qkv, w_qkv, True)], sides=[(act1, g_qkv), (attn, g1_all)])
    d_qkv = d_qkv.reshape(nf, local, 3 * wide)
    d_out = d_out.reshape(nf, wide // nf, width)

    n1, rstd1 = ln_stats(x)
    d_gain1 = jnp.sum(da1 * n1, axis=0)
    d_shift1 = jnp.sum(da1, axis=0)
    input_grad = d_mid + ln_back(da1, n1, rstd1, gain1)

    dq_bias = place_heads(jnp.sum(gq.astype(F32), axis=0), heads, c, n)
    dv_bias = place_heads(jnp.sum(gv.astype(F32), axis=0), heads, c, n)
    up_placed = lax.dynamic_update_slice(
        jnp.zeros((nf, n, ff_part), F32), d_up_bias.reshape(nf, 1, ff_part), (0, c, 0)
    )
    smalls = (
        d_gain1,
        d_shift1,
        jnp.concatenate([dq_bias, dv_bias]),
        d_out_bias,
        d_gain2,
        d_shift2,
        up_placed.reshape(-1),
        d_down_bias,
    )
    packed = jnp.concatenate([s.reshape(nf, -1) for s in smalls], axis=1)
    packed = jnp.pad(packed, ((0, 0), (0, -packed.shape[1] % 1024))).reshape(nf, -1, 128)
    d_down, d_qkv, _, packed, d_out = exchange(
        6, n, nf, ctx=[d_down], red=[d_qkv, d_out, packed], moves=row_moves(n, nf, heads), kept=local
    )
    mine = jnp.sum(packed, axis=0).reshape(-1)
    up_moves = [(i, j * ff_part, j * ff_local + i * ff_part, ff_part) for i in range(n) for j in range(nf)]
    qkv_moves = [m for i in range(3) for m in head_moves(n, heads, i * wide, i * width)]
    d_down_full, d_out_full, d_up_full, d_qkv_full = lay_out(
        (d_down.reshape(ff_local, width), d_out, d_up, d_qkv),
        (width, width, ff, 3 * width),
        (None, None, up_moves, qkv_moves),
    )
    out, at = [], 0
    for s in smalls:
        size = s.size // nf
        out.append(mine[at : at + size])
        at += size
    return (
        result[None],
        input_grad[None],
        out[0],
        out[1],
        d_qkv_full,
        out[2],
        d_out_full,
        out[3],
        out[4],
        out[5],
        d_up_full,
        out[6],
        d_down_full,
        out[7],
    )


def solution(mesh):
    rows, one, two = P("fsdp", "ctx", None), P("fsdp"), P("fsdp", None)
    return jax.shard_map(
        on_device,
        mesh=mesh,
        in_specs=(rows, one, one, two, one, two, one, one, one, two, one, two, one, P(), rows),
        out_specs=(rows, rows, one, one, two, one, two, one, one, one, two, one, two, one),
        check_vma=False,
    )
```

```python
import functools

import jax
import jax.numpy as jnp
from jax import lax
from jax.experimental import pallas as pl
from jax.experimental.pallas import tpu as pltpu
from jax.sharding import PartitionSpec as P

HEAD_DIM = 64
EPS = 1e-05
SCALE = 0.125
F32 = jnp.float32
BF16 = jnp.bfloat16
MESH = pl.DeviceIdType.MESH


def dot(left, right):
    return jnp.dot(left, right, preferred_element_type=F32)


def dot_t(left, right):
    return lax.dot_general(left, right, (((1,), (1,)), ((), ())), preferred_element_type=F32)


def t_dot(left, right):
    return lax.dot_general(left, right, (((0,), (0,)), ((), ())), preferred_element_type=F32)


def ln_stats(value):
    centre = value - jnp.mean(value, axis=-1, keepdims=True)
    spread = jnp.mean(centre * centre, axis=-1, keepdims=True)
    rstd = lax.rsqrt(spread + EPS)
    return centre * rstd, rstd


def ln_back(grad, normed, rstd, gain):
    dn = grad * gain
    first = jnp.mean(dn, axis=-1, keepdims=True)
    second = jnp.mean(dn * normed, axis=-1, keepdims=True)
    return (dn - first - normed * second) * rstd


def query_rows(rows):
    return 256


def forward_step(slots, step, ins, outs, scratch, gathered):
    qp_ref, kp_ref, q_ref, k_ref, v_ref = ins
    attn_ref, o_ref, l_ref = outs
    size = query_rows(q_ref.shape[0])
    rows = slice(step * size, (step + 1) * size)
    allowed = kp_ref[...] <= qp_ref[rows, :]
    for h in range(slots):
        cols = slice(h * HEAD_DIM, (h + 1) * HEAD_DIM)
        raw = dot_t(q_ref[rows, cols], k_ref[:, cols])
        e = jnp.where(allowed, jnp.exp(raw * SCALE), 0.0)
        total = jnp.sum(e, axis=1, keepdims=True)
        numer = dot(e.astype(BF16), v_ref[:, cols])
        o = numer / total
        o_ref[rows, cols] = o
        attn_ref[rows, cols] = o.astype(BF16)
        l_ref[rows, h : h + 1] = total


def backward_step(slots, step, ins, outs, scratch, gathered):
    qp_ref, kp_ref, q_ref, k_ref, v_ref, w_ref, o_ref, l_ref = ins
    dq_ref, dk_ref, dv_ref = outs
    dk_acc, dv_acc, do_ref, g_ref, sem = scratch
    if step == 0:
        copy = pltpu.make_async_copy(gathered[0], g_ref, sem)
        copy.start()
        copy.wait()
        each = g_ref.shape[1]
        for j in range(g_ref.shape[0]):
            do_ref[j * each : (j + 1) * each, :] = dot_t(g_ref[j], w_ref[...])
    size = query_rows(q_ref.shape[0])
    steps = q_ref.shape[0] // size
    rows = slice(step * size, (step + 1) * size)
    allowed = kp_ref[...] <= qp_ref[rows, :]
    for h in range(slots):
        cols = slice(h * HEAD_DIM, (h + 1) * HEAD_DIM)
        q, k, v, do = q_ref[rows, cols], k_ref[:, cols], v_ref[:, cols], do_ref[rows, cols]
        total = l_ref[rows, h : h + 1]
        w = (do / total).astype(BF16)
        corr = jnp.sum(do * o_ref[rows, cols], axis=1, keepdims=True) / total
        e = jnp.where(allowed, jnp.exp(dot_t(q, k) * SCALE), 0.0)
        de = dot_t(w, v)
        ds = (e * (de - corr)).astype(BF16)
        dq_ref[rows, cols] = (dot(ds, k) * SCALE).astype(BF16)
        dk, dv = t_dot(ds, q), t_dot(e.astype(BF16), w)
        if step:
            dk, dv = dk + dk_acc[:, cols], dv + dv_acc[:, cols]
        if step < steps - 1:
            dk_acc[:, cols] = dk
            dv_acc[:, cols] = dv
        else:
            dk_ref[:, cols] = (dk * SCALE).astype(BF16)
            dv_ref[:, cols] = dv.astype(BF16)


def forward_work(place, q, k, v, slots):
    rows, wide = q.shape
    shape = jax.ShapeDtypeStruct
    outs = (shape((rows, wide), BF16), shape((rows, wide), F32), shape((rows, slots), F32))
    steps = rows // query_rows(rows)
    ins = (place.reshape(rows, 1), place.reshape(1, rows), q, k, v)
    return steps, functools.partial(forward_step, slots), False, ins, outs, ()


def backward_work(place, q, k, v, weight, o, total, slots, g):
    rows, wide = q.shape
    outs = (jax.ShapeDtypeStruct((rows, wide), BF16),) * 3
    steps = rows // query_rows(rows)
    ins = (place.reshape(rows, 1), place.reshape(1, rows), q, k, v, weight, o, total)
    scratch = (pltpu.VMEM((rows, wide), F32),) * 3
    scratch += (pltpu.VMEM((rows // g.shape[0], *g.shape), g.dtype), pltpu.SemaphoreType.DMA)
    return steps, functools.partial(backward_step, slots), True, ins, outs, scratch


def stack_body(*refs):
    out = refs[-1]
    out[...] = jnp.zeros_like(out)
    for i, ref in enumerate(refs[:-1]):
        out[i : i + 1, : ref.shape[0]] = ref[...].reshape(1, ref.shape[0])


def stack_rows(vectors, longest):
    return pl.pallas_call(
        stack_body,
        in_specs=[pl.BlockSpec(memory_space=pltpu.VMEM)] * len(vectors),
        out_specs=pl.BlockSpec(memory_space=pltpu.VMEM),
        out_shape=jax.ShapeDtypeStruct((16, longest), vectors[0].dtype),
        name="stack_rows",
    )(*vectors)


def split_axis(n):
    across = 2 if n <= 8 else 4
    return n // across, across


def place_of(me, lines, across):
    a, b = lax.div(me, across), lax.rem(me, across)
    near = [(a < lines - 1, me + across), (a > 0, me - across), (b < across - 1, me + 1), (b > 0, me - 1)]
    return a, b, near


def turned_rows(rows, dtype, across, many=False):
    tile = 16 if dtype == BF16 else 8
    share = 4 if rows <= 128 and not many else 5
    return rows // share // tile * tile if across == 2 else 0


def meet(near, peers):
    barrier = pltpu.get_barrier_semaphore()
    for exists, target in near:

        @pl.when(exists)
        def _(target=target):
            pl.semaphore_signal(barrier, inc=1, device_id={"ctx": target}, device_id_type=MESH)

    for axis, peer in peers:
        pl.semaphore_signal(barrier, inc=1, device_id={axis: peer}, device_id_type=MESH)
    pl.semaphore_wait(barrier, len(peers) + sum(exists.astype(jnp.int32) for exists, _ in near))


class Fsdp:
    def __init__(self, nf, gather_in, gather_out, red_in, red_out, scratch):
        self.gather_in, self.gather_out, self.red_in, self.red_out = gather_in, gather_out, red_in, red_out
        n_gather, n_red = len(gather_in), len(red_in)
        self.near_in, self.stage, self.far_in = scratch[:n_red], scratch[n_red : 2 * n_red], scratch[2 * n_red : 3 * n_red]
        self.keep_sem, self.g_send, self.g_recv, self.r_send, self.r_recv = scratch[3 * n_red : 3 * n_red + 5]
        self.f = lax.axis_index("fsdp")
        self.core = lax.rem(self.f, 2)
        self.mate = self.f + 1 - 2 * self.core
        self.pairs = nf // 2
        self.pair = lax.div(self.f, 2)
        self.other = [lax.rem(self.pair + k, self.pairs) for k in range(1, self.pairs)]
        self.peers = [self.mate] + [2 * y + self.core for y in self.other] if n_gather + n_red else []

    @staticmethod
    def scratch(nf, gather, red):
        pairs = nf // 2
        dma = pltpu.SemaphoreType.DMA
        out = []
        for _ in range(3):
            out += [pltpu.VMEM((pairs, *x.shape[1:]), x.dtype) for x in red]
        g, r = max(len(gather), 1), max(len(red), 1)
        return out + [dma((g,)), dma((g, 2, nf)), dma((g, nf)), dma((r, 2, pairs)), dma((r, 2, pairs))]

    def copy(self, src, dst, send, recv, target):
        return pltpu.make_async_remote_copy(
            src_ref=src, dst_ref=dst, send_sem=send, recv_sem=recv, device_id={"fsdp": target}, device_id_type=MESH
        )

    def spread(self, i, source, target, own):
        out = self.gather_out[i].at[source]
        send = self.g_send.at[i, 0, target] if own else self.g_send.at[i, 1, source]
        return self.copy(self.gather_in[i] if own else out, out, send, self.g_recv.at[i, source], target)

    def keep(self, i):
        return pltpu.make_async_copy(self.gather_in[i], self.gather_out[i].at[self.f], self.keep_sem.at[i])

    def to_mate(self, j, y):
        src = self.red_in[j].at[2 * y + 1 - self.core]
        return self.copy(src, self.near_in[j].at[y], self.r_send.at[j, 0, y], self.r_recv.at[j, 0, y], self.mate)

    def to_far(self, j, y, source):
        send, recv = self.r_send.at[j, 1, y], self.r_recv.at[j, 1, source]
        return self.copy(self.stage[j].at[y], self.far_in[j].at[source], send, recv, 2 * y + self.core)

    def write(self, j, value):
        out, first = self.red_out[j]
        out[:, first : first + value.shape[1]] = value.astype(out.dtype)

    def start(self):
        for j in range(len(self.red_in)):
            for y in range(self.pairs):
                self.to_mate(j, y).start()
        for i in range(len(self.gather_in)):
            for target in self.peers[1:] + self.peers[:1]:
                self.spread(i, self.f, target, True).start()
            self.keep(i).start()

    def middle(self):
        for j in range(len(self.red_in)):
            for y in range(self.pairs):
                self.to_mate(j, y).wait_recv()
            for y in self.other:
                value = self.red_in[j][2 * y + self.core].astype(F32) + self.near_in[j][y].astype(F32)
                self.stage[j][y] = value.astype(self.stage[j].dtype)
                self.to_far(j, y, self.pair).start()

    def end(self, first, last):
        for j in range(first, last):
            value = self.red_in[j][self.f].astype(F32) + self.near_in[j][self.pair].astype(F32)
            for y in self.other:
                self.to_far(j, y, y).wait_recv()
                value = value + self.far_in[j][y].astype(F32)
            self.write(j, value)

    def forward(self):
        for i in range(len(self.gather_in)):
            for y in self.other:
                source = 2 * y + self.core
                self.spread(i, source, self.mate, False).wait_recv()
                self.spread(i, source, self.mate, False).start()

    def finish(self):
        for i in range(len(self.gather_in)):
            self.spread(i, self.mate, self.mate, False).wait_recv()
            for y in self.other:
                self.spread(i, 2 * y + 1 - self.core, self.mate, False).wait_recv()
            self.keep(i).wait()
            for target in self.peers:
                self.spread(i, self.f, target, True).wait_send()
            for y in self.other:
                self.spread(i, 2 * y + self.core, self.mate, False).wait_send()
        for j in range(len(self.red_in)):
            for y in range(self.pairs):
                self.to_mate(j, y).wait_send()
            for y in self.other:
                self.to_far(j, y, self.pair).wait_send()


def exchange_body(n, nf, counts, firsts, moves, work, *refs):
    n_ctx, n_fsdp, n_own, n_red, n_pack, n_work_in, n_work_out, n_work_scratch = counts
    bounds = [0]
    for size in counts[:6]:
        bounds.append(bounds[-1] + size)
    ctx_in, fsdp_in, own_in, red_in, pack_in, work_in = (refs[i:j] for i, j in zip(bounds, bounds[1:]))
    refs = refs[bounds[-1] :]
    n_joint = len(firsts) - n_pack
    n_sums = n_red - n_joint + (1 if n_pack else 0)
    ctx_out, fsdp_out, own_out = refs[:n_ctx], refs[n_ctx : n_ctx + n_fsdp], refs[n_ctx + n_fsdp : n_ctx + n_fsdp + n_own]
    refs = refs[n_ctx + n_fsdp + n_own :]
    red_out, refs = refs[:n_sums], refs[n_sums:]
    if moves:
        placed, refs = refs[0], refs[1:]
    work_out, refs = refs[:n_work_out], refs[n_work_out:]
    work_scratch, refs = refs[:n_work_scratch], refs[n_work_scratch:]
    sums, scratch = refs[:n_sums], refs[n_sums:]
    copy_sem, send_sem, recv_sem, place_send, place_recv = scratch[:5]
    goals = [(sums[0], firsts[j]) for j in range(n_joint)]
    goals += [(out, 0) for out in sums[1 if n_pack else 0 :]]
    goals += [(out, 0) for out in own_out]
    fs = Fsdp(nf, fsdp_in, fsdp_out, red_in + own_in, goals, scratch[5:])

    lines, across = split_axis(n)
    me = lax.axis_index("ctx")
    a, b, near = place_of(me, lines, across)
    pieces = [(src, out, first, rows) for src, out in zip(ctx_in, ctx_out) for first, rows in cut(out.shape[1])]
    late = len(pieces)
    for src, out in reversed(list(zip(sums, red_out))):
        pieces += [(src, out, first, rows) for first, rows in cut(out.shape[1])]
    peers = [lax.rem(fs.f + k, nf) for k in range(1, nf)] if moves else fs.peers
    meet(near if pieces else [], [("fsdp", peer) for peer in peers])
    fs.start()

    def turned_part(i):
        return turned_rows(pieces[i][3], pieces[i][1].dtype, across, len(pieces) > 1)

    def hop(i, block, way, turned=False, own=False):
        source, out, first, size = pieces[i]
        last = turned_part(i)
        rows = pl.ds(first + size - last, last) if turned else pl.ds(first, size - last)
        return pltpu.make_async_remote_copy(
            src_ref=source.at[rows] if own else out.at[block, rows],
            dst_ref=out.at[block, rows],
            send_sem=send_sem.at[i, way, block, int(turned)],
            recv_sem=recv_sem.at[i, way, block, int(turned)],
            device_id={"ctx": me + (across, -across, 1, -1)[way]},
            device_id_type=MESH,
        )

    def keep(i):
        source, out, first, size = pieces[i]
        rows = pl.ds(first, size)
        return pltpu.make_async_copy(source.at[rows], out.at[me, rows], copy_sem.at[i])

    def each_own(i, act):
        for turned in (True, False) if turned_part(i) else (False,):
            for way in (2, 3, 0, 1):
                pl.when(near[way][0])(lambda way=way: act(hop(i, me, way, turned, True)))

    def each_twin(i, wait, act):
        if turned_part(i):
            twin = me + 1 - 2 * b
            for way in (2, 3):

                @pl.when(near[5 - way][0])
                def _(way=way):
                    if wait:
                        hop(i, twin, way, True).wait_recv()
                    for on in (0, 1):
                        pl.when(near[on][0])(lambda on=on: act(hop(i, twin, on, True)))

    def each_relay(i, d, wait, act):
        for way, there, shift in ((0, a >= d, -d * across), (1, a + d < lines, d * across)):

            @pl.when(there)
            def _(way=way, shift=shift):
                for turned, block in [(False, me + shift)] + (
                    [(True, me + shift), (True, me + 1 - 2 * b + shift)] if turned_part(i) else []
                ):
                    if wait:
                        hop(i, block, way, turned).wait_recv()
                    for on in (way,) if turned else (2, 3, way):
                        pl.when(near[on][0])(lambda on=on: act(hop(i, block, on, turned)))

    def start(copy):
        copy.start()

    def wait_send(copy):
        copy.wait_send()

    def begin(these):
        for i in these:
            each_own(i, start)
            keep(i).start()

    def crossed(i):
        for d in range(1, across):
            for step in range(lines):
                for sign in (1, -1) if step else (1,):
                    for way, there, shift in ((2, b >= d, -d), (3, b + d < across, d)):
                        other = a + sign * step

                        @pl.when(there & (other >= 0) & (other < lines))
                        def _(source=other * across + b + shift, way=way):
                            hop(i, source, way).wait_recv()
                            if d < across - 1:
                                pl.when(near[way][0])(lambda: hop(i, source, way).start())

    work_steps, work_fn, gated = work
    plan = []

    def add(act, *args, then_work=True):
        plan.append((functools.partial(act, *args), then_work))

    def hops(i, d):
        if d == 1:
            each_twin(i, True, start)
        each_relay(i, d, True, start)

    def complete(i):
        crossed(i)
        keep(i).wait()

    begin(range(late))
    fs.middle()
    for j in range(n_pack):
        first = firsts[n_joint + j]
        sums[0][:, first : first + pack_in[j].shape[1]] = pack_in[j][...]
    early = set()
    if n_sums:
        early = {(i, 1) for i in range(late)} | ({(i, 2) for i in range(late)} if gated else set())
        for d in (1, 2):
            for i in range(late):
                if (i, d) in early:
                    add(hops, i, d, then_work=not gated)
        add(fs.end, 0, n_red, then_work=False)
        add(begin, range(late, len(pieces)), then_work=False)
    if gated:
        for i in range(late):
            for d in range(3, lines):
                add(hops, i, d, then_work=False)
                early.add((i, d))
        for i in range(late):
            add(complete, i, then_work=i == late - 1)
        add(fs.end, n_red, n_red + n_own)
    for d in range(1, lines):
        for i in range(len(pieces)):
            if (i, d) not in early:
                add(hops, i, d)
    if not gated:
        add(fs.end, n_red, n_red + n_own)
    add(fs.forward, then_work=False)
    points = sum(then_work for _, then_work in plan)
    at = 0
    for act, then_work in plan:
        act()
        if then_work:
            for step in range(at * work_steps // points, (at + 1) * work_steps // points):
                work_fn(step, work_in, work_out, work_scratch, ctx_out)
            at += 1

    def place(k, act_local, act_send):
        block, row, src, dst, goal, size = moves[k]
        source, goal = red_out[1].at[block, pl.ds(row, size)], placed.at[pl.ds(goal, size)]
        if src == dst:
            pl.when(fs.f == src)(lambda: act_local(pltpu.make_async_copy(source, goal, place_send.at[k])))
            return
        remote = pltpu.make_async_remote_copy(
            src_ref=source,
            dst_ref=goal,
            send_sem=place_send.at[k],
            recv_sem=place_recv.at[k],
            device_id={"fsdp": jnp.int32(dst)},
            device_id_type=MESH,
        )
        pl.when(fs.f == src)(lambda: act_send(remote))
        if act_local is wait_copy:
            pl.when(fs.f == dst)(remote.wait_recv)

    def wait_copy(copy):
        copy.wait()

    if moves:
        ready = [i for i in range(len(pieces)) if pieces[i][1] is red_out[1]]
        assert not gated
        for i in ready:
            crossed(i)
            keep(i).wait()
        for k in range(len(moves)):
            place(k, start, start)
    else:
        ready = range(late) if gated else []
    for i in range(len(pieces)):
        if i not in ready:
            complete(i)
    for k in range(len(moves)):
        place(k, wait_copy, wait_send)

    for i in range(len(pieces)):
        each_own(i, wait_send)
        each_twin(i, False, wait_send)
        for d in range(1, lines):
            each_relay(i, d, False, wait_send)
        for d in range(1, across - 1):
            for line in range(lines):
                for way, there, shift in ((2, b >= d, -d), (3, b + d < across, d)):

                    @pl.when(there & near[way][0])
                    def _(i=i, source=line * across + b + shift, way=way):
                        hop(i, source, way).wait_send()

    fs.finish()


def cut(rows):
    if rows < 200:
        return [(0, rows)]
    half = rows // 32 * 16
    return [(0, rows - half), (rows - half, half)]


def exchange(call, n, nf, ctx=(), fsdp=(), own=(), red=(), pack=(), firsts=(), moves=(), kept=0, work=None):
    shape = jax.ShapeDtypeStruct
    sums = [shape(x.shape[1:], x.dtype) for x in red]
    if pack:
        joint = len(firsts) - len(pack)
        width = sum(x.shape[1] for x in [*sums[:joint], *pack])
        sums = [shape((pack[0].shape[0], width), pack[0].dtype)] + sums[joint:]
    outs = [shape((n, *x.shape), x.dtype) for x in ctx]
    outs += [shape((nf, *x.shape), x.dtype) for x in fsdp]
    outs += [shape(x.shape[1:], x.dtype) for x in own]
    outs += [shape((n, *x.shape), x.dtype) for x in sums]
    outs += [shape((kept, sums[1].shape[1]), sums[1].dtype)] if moves else []
    steps, work_fn, gated, work_in, work_out, work_scratch = work or (0, None, False, (), (), ())
    gathered = max(sum(len(cut(x.shape[0])) for x in [*ctx, *sums]), 1)
    any_spec, vmem_spec = pl.BlockSpec(memory_space=pl.ANY), pl.BlockSpec(memory_space=pltpu.VMEM)
    inputs = (*ctx, *fsdp, *own, *red, *pack, *work_in)
    counts = [len(x) for x in (ctx, fsdp, own, red, pack, work_in, work_out, work_scratch)]
    dma = pltpu.SemaphoreType.DMA
    return pl.pallas_call(
        functools.partial(exchange_body, n, nf, tuple(counts), tuple(firsts), tuple(moves), (steps, work_fn, gated)),
        in_specs=[any_spec] * (len(ctx) + len(fsdp)) + [vmem_spec] * (len(inputs) - len(ctx) - len(fsdp)),
        out_specs=[any_spec] * (len(ctx) + len(fsdp))
        + [vmem_spec] * len(own)
        + [any_spec] * (len(sums) + (1 if moves else 0))
        + [vmem_spec] * len(work_out),
        out_shape=[*outs, *work_out],
        scratch_shapes=list(work_scratch)
        + [pltpu.VMEM(x.shape, x.dtype) for x in sums]
        + [dma((gathered,)), dma((gathered, 4, n, 2)), dma((gathered, 4, n, 2))]
        + [dma((max(len(moves), 1),))] * 2
        + Fsdp.scratch(nf, fsdp, [*red, *own]),
        name=f"exchange_{call}",
        compiler_params=pltpu.CompilerParams(collective_id=call, has_side_effects=True, vmem_limit_bytes=60 * 2**20),
    )(*inputs)


class Scatter:
    def __init__(self, n, many, transposed, left, right, out, scratch):
        self.left, self.right, self.out, self.transposed = left, right, out, transposed
        self.part, self.acc, self.acc_t, self.over_in, self.sums, self.sums_t = scratch[:6]
        self.line_in, self.line_in_t, self.twin_in = scratch[6:9]
        self.o_send, self.o_recv, self.l_send, self.l_recv, self.t_send, self.t_recv = scratch[9:15]
        self.w_send, self.w_recv = scratch[15:17]
        self.lines, self.across = split_axis(n)
        self.me = lax.axis_index("ctx")
        self.a, self.b, self.near = place_of(self.me, self.lines, self.across)
        self.rows = out.shape[0]
        self.last = turned_rows(self.rows, BF16, self.across, many)
        self.head, self.tail = pl.ds(0, self.rows - self.last), pl.ds(self.rows - self.last, self.last)
        self.peers = [self.me - self.b + lax.rem(self.b + k, self.across) for k in range(1, self.across)]

    @staticmethod
    def scratch(n, many, rows, width):
        lines, across = split_axis(n)
        last = turned_rows(rows, BF16, across, many)
        some = max(last, 16)
        vmem, dma = pltpu.VMEM, pltpu.SemaphoreType.DMA
        return [
            vmem((lines, across, rows, width), BF16),
            vmem((rows - last, width), F32),
            vmem((across, some, width), F32),
            vmem((across - 1, lines, rows - last, width), BF16),
            vmem((lines, rows - last, width), BF16),
            vmem((lines, across, some, width), BF16),
            vmem((2, lines, rows - last, width), BF16),
            vmem((2, lines, across, some, width), BF16),
            vmem((some, width), BF16),
            dma((across - 1, lines)),
            dma((across - 1, lines)),
            dma((2, lines)),
            dma((2, lines)),
            dma((2, lines)),
            dma((2, lines)),
            dma,
            dma,
        ]

    def copy(self, src, dst, send, recv, target):
        return pltpu.make_async_remote_copy(
            src_ref=src, dst_ref=dst, send_sem=send, recv_sem=recv, device_id={"ctx": target}, device_id_type=MESH
        )

    def over(self, line, k):
        src = self.part.at[line, lax.rem(self.b + k, self.across), self.head]
        send, recv = self.o_send.at[k - 1, line], self.o_recv.at[k - 1, line]
        return self.copy(src, self.over_in.at[k - 1, line], send, recv, self.peers[k - 1])

    def along(self, line, way):
        target = self.me + (self.across, -self.across)[way]
        send, recv = self.l_send.at[way, line], self.l_recv.at[way, line]
        return self.copy(self.sums.at[line], self.line_in.at[way, line], send, recv, target)

    def along_t(self, line, way):
        target = self.me + (self.across, -self.across)[way]
        send, recv = self.t_send.at[way, line], self.t_recv.at[way, line]
        return self.copy(self.sums_t.at[line], self.line_in_t.at[way, line], send, recv, target)

    def twin(self):
        return self.copy(self.sums_t.at[self.a, 1 - self.b], self.twin_in, self.w_send, self.w_recv, self.peers[0])

    def compute(self, line):
        size = self.across * self.rows
        lhs = self.left[pl.ds(pl.multiple_of(line * size, size), size), :]
        value = dot_t(lhs, self.right[...]) if self.transposed else dot(lhs, self.right[...])
        self.part[line] = value.astype(BF16).reshape(self.across, self.rows, value.shape[1])
        for k in range(1, self.across):
            self.over(line, k).start()

    def collect(self, line, acc, landed, hop, ways):
        for way, there in ways:

            @pl.when(there)
            def _(way=way):
                hop(line, way).wait_recv()
                acc[...] += landed[way, line].astype(F32)

    def across_sum(self, line):
        value = self.part[line, self.b, self.head].astype(F32)
        for k in range(1, self.across):
            self.over(line, k).wait_recv()
            value = value + self.over_in[k - 1, line].astype(F32)
        self.acc[...] = value

    def pass_on(self, line):
        up, down = line > self.a, line < self.a
        ways = ((0, up & (self.a > 0)), (1, down & (self.a < self.lines - 1)))
        if self.last:
            self.acc_t[...] = self.part[line, :, self.tail].astype(F32)
            self.collect(line, self.acc_t, self.line_in_t, self.along_t, ways)
            self.sums_t[line] = self.acc_t[...].astype(BF16)
            pl.when(up)(lambda: self.along_t(line, 0).start())
            pl.when(down)(lambda: self.along_t(line, 1).start())
        self.across_sum(line)
        self.collect(line, self.acc, self.line_in, self.along, ways)
        self.sums[line] = self.acc[...].astype(BF16)
        pl.when(up)(lambda: self.along(line, 0).start())
        pl.when(down)(lambda: self.along(line, 1).start())

    def own(self):
        ways = ((0, self.near[1][0]), (1, self.near[0][0]))
        if self.last:
            self.acc_t[...] = self.part[self.a, :, self.tail].astype(F32)
            self.collect(self.a, self.acc_t, self.line_in_t, self.along_t, ways)
            self.sums_t[self.a] = self.acc_t[...].astype(BF16)
            self.twin().start()
        self.across_sum(self.a)
        self.collect(self.a, self.acc, self.line_in, self.along, ways)
        self.out[self.head, :] = self.acc[...]
        if self.last:
            self.twin().wait_recv()
            self.out[self.tail, :] = self.acc_t[self.b] + self.twin_in[...].astype(F32)

    def sent(self, order):
        for line in order:
            for k in range(1, self.across):
                self.over(line, k).wait_send()
        for line in order[:-1]:
            for way, there in ((0, line > self.a), (1, line < self.a)):

                @pl.when(there)
                def _(way=way, line=line):
                    self.along(line, way).wait_send()
                    if self.last:
                        self.along_t(line, way).wait_send()

        if self.last:
            self.twin().wait_send()


def product_body(n, nf, counts, transposed, *refs):
    n_prod, n_sides, n_fsdp = counts
    pairs, refs = refs[: 2 * n_prod], refs[2 * n_prod :]
    side_in, refs = refs[: 2 * n_sides], refs[2 * n_sides :]
    fsdp_in, refs = refs[:n_fsdp], refs[n_fsdp:]
    outs, side_out, fsdp_out = refs[:n_prod], refs[n_prod : n_prod + n_sides], refs[n_prod + n_sides : n_prod + n_sides + n_fsdp]
    scratch = refs[n_prod + n_sides + n_fsdp :]
    side_at, side_sem, scratch = scratch[: 2 * n_sides], scratch[2 * n_sides], scratch[2 * n_sides + 1 :]
    fetches = [pltpu.make_async_copy(side_in[j], side_at[j], side_sem.at[j]) for j in range(2 * n_sides)]
    each = 17
    jobs = [
        Scatter(n, n_prod > 1, transposed[p], pairs[2 * p], pairs[2 * p + 1], outs[p], scratch[each * p : each * (p + 1)])
        for p in range(n_prod)
    ]
    fs = Fsdp(nf, fsdp_in, fsdp_out, [], [], scratch[each * n_prod :])
    a, lines = jobs[0].a, jobs[0].lines
    meet(jobs[0].near[:2], [("ctx", peer) for peer in jobs[0].peers] + [("fsdp", peer) for peer in fs.peers])

    order = []
    for k in range(lines):
        line = jnp.int32(0)
        for av in range(lines):
            line = jnp.where(a == av, sorted(range(lines), key=lambda j: (-abs(j - av), j))[k], line)
        order.append(line)

    for fetch in fetches:
        fetch.start()
    for job in jobs:
        for line in order:
            job.compute(line)
    fs.start()
    steps = [(job, line) for job in jobs for line in order[:-1]]
    bits = []
    for j in range(n_sides):
        size = side_in[2 * j].shape[1]
        width = -(-size // 3 // 128) * 128
        bits += [(j, first, min(width, size - first)) for first in range(0, size, width)]
    for step, (job, line) in enumerate(steps):
        job.pass_on(line)
        for j, first, size in bits[step * len(bits) // len(steps) : (step + 1) * len(bits) // len(steps)]:
            if first == 0:
                fetches[2 * j].wait()
                fetches[2 * j + 1].wait()
            part = side_at[2 * j][:, first : first + size]
            side_out[j][first : first + size, :] = t_dot(part, side_at[2 * j + 1][...]).astype(BF16)
        if step == len(order) - 2:
            fs.forward()
    for job in jobs:
        job.own()
    for job in jobs:
        job.sent(order)
    fs.finish()


def product(call, n, nf, products, sides=(), fsdp=()):
    length = products[0][0].shape[0]
    if length > 1024 and (sides or len(products) > 1):
        sums = []
        for i, one in enumerate(products):
            total, *gathered = product(call if i == 0 else call + 10, n, nf, [one], fsdp=fsdp if i == 0 else ())
            sums.append(total)
            fsdp_out = gathered if i == 0 else fsdp_out
        return [*sums, *[t_dot(x, y).astype(BF16) for x, y in sides], *fsdp_out]
    rows = length // n
    shape = jax.ShapeDtypeStruct
    widths = [right.shape[0 if turned else 1] for _, right, turned in products]
    outs = [shape((rows, width), F32) for width in widths]
    outs += [shape((x.shape[1], y.shape[1]), BF16) for x, y in sides]
    outs += [shape((nf, *x.shape), x.dtype) for x in fsdp]
    inputs = [z for left, right, _ in products for z in (left, right)] + [z for side in sides for z in side]
    vmem_spec, any_spec = pl.BlockSpec(memory_space=pltpu.VMEM), pl.BlockSpec(memory_space=pl.ANY)
    return pl.pallas_call(
        functools.partial(
            product_body,
            n,
            nf,
            (len(products), len(sides), len(fsdp)),
            tuple(turned for _, _, turned in products),
        ),
        in_specs=[vmem_spec] * (2 * len(products)) + [any_spec] * (2 * len(sides) + len(fsdp)),
        out_specs=[vmem_spec] * (len(outs) - len(fsdp)) + [any_spec] * len(fsdp),
        out_shape=outs,
        scratch_shapes=[pltpu.VMEM(z.shape, z.dtype) for side in sides for z in side]
        + [pltpu.SemaphoreType.DMA((max(2 * len(sides), 1),))]
        + [s for width in widths for s in Scatter.scratch(n, len(widths) > 1, rows, width)] + Fsdp.scratch(nf, fsdp, ()),
        name=f"product_{call}",
        compiler_params=pltpu.CompilerParams(collective_id=call, has_side_effects=True, vmem_limit_bytes=63 * 2**20),
    )(*inputs, *fsdp)


def row_moves(n, nf, heads):
    part, local = -(-heads // n) * HEAD_DIM // nf, heads * HEAD_DIM // nf
    moves = []
    for block, start, goal, size in head_moves(n, heads, 0, 0):
        done = 0
        while done < size:
            here, there = start + done, goal + done
            rows = min(size - done, part - here % part, local - there % local)
            moves.append((block, here % part, here // part, there // local, there % local, rows))
            done += rows
    return moves


def layout_body(moves, *refs):
    ins, outs = refs[: len(refs) // 2], refs[len(refs) // 2 :]
    for in_ref, out_ref, per_out in zip(ins, outs, moves):
        if per_out is None:
            out_ref[...] = in_ref[...].astype(F32)
            continue
        for block, start, goal, size in per_out:
            out_ref[:, goal : goal + size] = in_ref[block, :, start : start + size].astype(F32)


def lay_out(arrays, widths, moves):
    rows = next(x.shape[1] for x in arrays if x.ndim == 3)
    step = next(s for s in (80, 16, rows) if rows % s == 0)
    grid = rows // step
    in_specs, out_specs, outs = [], [], []
    for x, width in zip(arrays, widths):
        flat = pl.BlockSpec((x.shape[-2] // grid, width), lambda i: (i, 0))
        in_specs.append(pl.BlockSpec((x.shape[0], step, x.shape[2]), lambda i: (0, i, 0)) if x.ndim == 3 else flat)
        out_specs.append(flat)
        outs.append(jax.ShapeDtypeStruct((x.shape[-2], width), F32))
    return pl.pallas_call(
        functools.partial(layout_body, tuple(m and tuple(m) for m in moves)),
        grid=(grid,),
        in_specs=in_specs,
        out_specs=out_specs,
        out_shape=outs,
        name="lay_out",
        cost_estimate=pl.CostEstimate(
            flops=0, bytes_accessed=6 * sum(x.shape[0] * x.shape[1] for x in outs), transcendentals=0
        ),
        compiler_params=pltpu.CompilerParams(vmem_limit_bytes=60 * 2**20),
    )(*arrays)


def head_moves(n, heads, offset, goal):
    base, rest = divmod(heads, n)
    moves = [(c, offset, goal + c * base * HEAD_DIM, base * HEAD_DIM) for c in range(n) if base]
    moves += [
        (c, offset + base * HEAD_DIM, goal + (base * n + c) * HEAD_DIM, HEAD_DIM) for c in range(rest)
    ]
    return moves


def head_columns(value, width, c, n):
    heads = width // HEAD_DIM
    base, rest = divmod(heads, n)
    parts = []
    if base:
        parts.append(lax.dynamic_slice_in_dim(value, c * base * HEAD_DIM, base * HEAD_DIM, axis=-1))
    if rest:
        start = jnp.minimum(base * n + c, heads - 1) * HEAD_DIM
        extra = lax.dynamic_slice_in_dim(value, start, HEAD_DIM, axis=-1)
        parts.append(jnp.where(c < rest, extra, jnp.zeros_like(extra)))
    return jnp.concatenate(parts, axis=-1)


def place_heads(value, heads, c, n):
    base, rest = divmod(heads, n)
    out = jnp.zeros((heads * HEAD_DIM,), value.dtype)
    if rest:
        start = jnp.minimum(base * n + c, heads - 1) * HEAD_DIM
        extra = jnp.where(c < rest, value[base * HEAD_DIM :], 0.0)
        out = lax.dynamic_update_slice(out, extra, (start,))
    if base:
        out = lax.dynamic_update_slice(out, value[: base * HEAD_DIM], (c * base * HEAD_DIM,))
    return out


def head_rows(value, heads, c, f, n):
    base, rest = divmod(heads, n)
    local, width = value.shape
    pad = max(base, 1) * HEAD_DIM
    padded = jnp.pad(value, ((pad, pad), (0, 0)))
    parts = []
    if base:
        start = jnp.clip(c * base * HEAD_DIM - f * local + pad, 0, local + 2 * pad - base * HEAD_DIM)
        parts.append(lax.dynamic_slice_in_dim(padded, start, base * HEAD_DIM, axis=0))
    if rest:
        start = jnp.clip((base * n + c) * HEAD_DIM - f * local + pad, 0, local + 2 * pad - HEAD_DIM)
        extra = lax.dynamic_slice_in_dim(padded, start, HEAD_DIM, axis=0)
        parts.append(jnp.where(c < rest, extra, jnp.zeros_like(extra)))
    return jnp.concatenate(parts, axis=0)


def on_device(
    tokens,
    ln1_gain,
    ln1_shift,
    qkv_weight,
    qv_bias,
    out_weight,
    out_bias,
    ln2_gain,
    ln2_shift,
    up_weight,
    up_bias,
    down_weight,
    down_bias,
    block_table,
    cotangent,
):
    rows, width = tokens.shape[1:]
    heads = width // HEAD_DIM
    n = lax.axis_size("ctx")
    nf = lax.axis_size("fsdp")
    c = lax.axis_index("ctx")
    f = lax.axis_index("fsdp")
    slots = -(-heads // n)
    wide = slots * HEAD_DIM
    half = rows // 2
    local = width // nf
    ff = up_weight.shape[1]
    ff_local = ff // nf
    ff_part = ff_local // n

    within = jnp.arange(rows, dtype=jnp.int32)
    block_of = jnp.where(within[None, :] < half, block_table[:, None], 2 * n - 1 - block_table[:, None])
    place = (block_of * half + within[None, :] % half).reshape(-1)

    vectors = (ln1_gain, ln1_shift, qv_bias, out_bias, ln2_gain, ln2_shift, up_bias, down_bias)
    longest = max(v.shape[0] for v in vectors)
    flat = stack_rows(vectors, longest)
    q_w = head_columns(qkv_weight[:, :width], width, c, n)
    k_w = head_columns(qkv_weight[:, width : 2 * width], width, c, n)
    v_w = head_columns(qkv_weight[:, 2 * width :], width, c, n)
    w_mine = jnp.concatenate([q_w, k_w, v_w], axis=1)
    x_all, packed, w_qkv = exchange(0, n, nf, ctx=[tokens[0]], fsdp=[flat, w_mine])
    out_weight, up_weight, down_weight, packed = lax.optimization_barrier(
        (out_weight, up_weight, down_weight, packed)
    )
    x_all = x_all.reshape(n * rows, width)
    w_qkv = w_qkv.reshape(width, 3 * wide)
    full = [packed[:, i, : v.shape[0]].reshape(-1).astype(F32) for i, v in enumerate(vectors)]
    gain1, shift1, b_qv, b_out, gain2, shift2, b_up, b_down = full

    b_up_mine = lax.dynamic_slice_in_dim(b_up.reshape(nf, n, ff_part), c, 1, axis=1).reshape(-1)
    bq = head_columns(b_qv[:width], width, c, n)
    bv = head_columns(b_qv[width:], width, c, n)

    n1_all, _ = ln_stats(x_all.astype(F32))
    act1 = (n1_all * gain1 + shift1).astype(BF16)
    proj = dot(act1, w_qkv)
    q = (proj[:, :wide] + bq).astype(BF16)
    k = proj[:, wide : 2 * wide].astype(BF16)
    v = (proj[:, 2 * wide :] + bv).astype(BF16)
    g2_all, w_out, attn, o, total = exchange(
        1,
        n,
        nf,
        ctx=[cotangent[0]],
        fsdp=[head_rows(out_weight, heads, c, f, n)],
        work=forward_work(place, q, k, v, slots),
    )
    up_mine = [lax.dynamic_slice_in_dim(up_weight, i * ff_local + c * ff_part, ff_part, axis=1) for i in range(nf)]
    w_out = functools.reduce(jnp.add, [w_out[i] for i in range(nf)])
    mixed, w_up = product(7, n, nf, [(attn, w_out, False)], fsdp=[jnp.concatenate(up_mine, axis=1)])
    w_up = w_up.reshape(width, nf * ff_part)
    x = tokens[0].astype(F32)
    mid = x + mixed + b_out

    n2, rstd2 = ln_stats(mid)
    act2, w_down = exchange(
        2,
        n,
        nf,
        ctx=[(n2 * gain2 + shift2).astype(BF16)],
        fsdp=[lax.dynamic_slice_in_dim(down_weight, c * ff_part, ff_part, axis=0)],
    )
    act2 = act2.reshape(n * rows, width)
    g2_all = g2_all.reshape(n * rows, width)
    w_down = w_down.reshape(nf * ff_part, width)
    u = dot(act2, w_up) + b_up_mine
    activated, gelu_back = jax.vjp(lambda t: jax.nn.gelu(t, approximate=True), u)
    hidden = activated.astype(BF16)
    dh = dot_t(g2_all, w_down)
    du = gelu_back(dh)[0].astype(BF16)
    da2, fed, d_up, d_down = product(
        3, n, nf, [(du, w_up, True), (hidden, w_down, False)], sides=[(act2, du), (hidden, g2_all)]
    )
    result = mid + fed + b_down
    d_up = d_up.reshape(nf, local, nf * ff_part)
    d_down = d_down.reshape(nf, ff_part, width)
    d_up_bias = jnp.sum(du.astype(F32), axis=0)
    grad_out = cotangent[0].astype(F32)
    d_down_bias = jnp.sum(grad_out, axis=0)

    d_gain2 = jnp.sum(da2 * n2, axis=0)
    d_shift2 = jnp.sum(da2, axis=0)
    d_mid = grad_out + ln_back(da2, n2, rstd2, gain2)
    g1 = d_mid.astype(BF16)
    d_out_bias = jnp.sum(g1.astype(F32), axis=0)
    g1_all, d_down, d_up, gq, gk, gv = exchange(
        4, n, nf, ctx=[g1], own=[d_down], red=[d_up], work=backward_work(place, q, k, v, w_out, o, total, slots, g1)
    )
    g1_all = g1_all.reshape(n * rows, width)
    g_qkv = jnp.concatenate([gq, gk, gv], axis=1)
    da1, d_qkv, d_out = product(5, n, nf, [(g_qkv, w_qkv, True)], sides=[(act1, g_qkv), (attn, g1_all)])
    d_qkv = d_qkv.reshape(nf, local, 3 * wide)
    d_out = d_out.reshape(nf, wide // nf, width)

    n1, rstd1 = ln_stats(x)
    d_gain1 = jnp.sum(da1 * n1, axis=0)
    d_shift1 = jnp.sum(da1, axis=0)
    input_grad = d_mid + ln_back(da1, n1, rstd1, gain1)

    dq_bias = place_heads(jnp.sum(gq.astype(F32), axis=0), heads, c, n)
    dv_bias = place_heads(jnp.sum(gv.astype(F32), axis=0), heads, c, n)
    up_placed = lax.dynamic_update_slice(
        jnp.zeros((nf, n, ff_part), F32), d_up_bias.reshape(nf, 1, ff_part), (0, c, 0)
    )
    smalls = (
        d_gain1,
        d_shift1,
        jnp.concatenate([dq_bias, dv_bias]),
        d_out_bias,
        d_gain2,
        d_shift2,
        up_placed.reshape(-1),
        d_down_bias,
    )
    packed = jnp.concatenate([s.reshape(nf, -1) for s in smalls], axis=1)
    packed = jnp.pad(packed, ((0, 0), (0, -packed.shape[1] % 1024))).reshape(nf, -1, 128)
    d_down, d_qkv, _, packed, d_out = exchange(
        6, n, nf, ctx=[d_down], red=[d_qkv, d_out, packed], moves=row_moves(n, nf, heads), kept=local
    )
    mine = jnp.sum(packed, axis=0).reshape(-1)
    up_moves = [(i, j * ff_part, j * ff_local + i * ff_part, ff_part) for i in range(n) for j in range(nf)]
    qkv_moves = [m for i in range(3) for m in head_moves(n, heads, i * wide, i * width)]
    d_down_full, d_out_full, d_up_full, d_qkv_full = lay_out(
        (d_down.reshape(ff_local, width), d_out, d_up, d_qkv),
        (width, width, ff, 3 * width),
        (None, None, up_moves, qkv_moves),
    )
    out, at = [], 0
    for s in smalls:
        size = s.size // nf
        out.append(mine[at : at + size])
        at += size
    return (
        result[None],
        input_grad[None],
        out[0],
        out[1],
        d_qkv_full,
        out[2],
        d_out_full,
        out[3],
        out[4],
        out[5],
        d_up_full,
        out[6],
        d_down_full,
        out[7],
    )


def solution(mesh):
    rows, one, two = P("fsdp", "ctx", None), P("fsdp"), P("fsdp", None)
    return jax.shard_map(
        on_device,
        mesh=mesh,
        in_specs=(rows, one, one, two, one, two, one, one, one, two, one, two, one, P(), rows),
        out_specs=(rows, rows, one, one, two, one, two, one, one, one, two, one, two, one),
        check_vma=False,
    )
```

```python
import functools

import jax
import jax.numpy as jnp
from jax import lax
from jax.experimental import pallas as pl
from jax.experimental.pallas import tpu as pltpu
from jax.sharding import PartitionSpec as P

HEAD_DIM = 64
EPS = 1e-05
SCALE = 0.125
F32 = jnp.float32
BF16 = jnp.bfloat16
MESH = pl.DeviceIdType.MESH


def dot(left, right):
    return jnp.dot(left, right, preferred_element_type=F32)


def dot_t(left, right):
    return lax.dot_general(left, right, (((1,), (1,)), ((), ())), preferred_element_type=F32)


def t_dot(left, right):
    return lax.dot_general(left, right, (((0,), (0,)), ((), ())), preferred_element_type=F32)


def ln_stats(value):
    centre = value - jnp.mean(value, axis=-1, keepdims=True)
    spread = jnp.mean(centre * centre, axis=-1, keepdims=True)
    rstd = lax.rsqrt(spread + EPS)
    return centre * rstd, rstd


def ln_back(grad, normed, rstd, gain):
    dn = grad * gain
    first = jnp.mean(dn, axis=-1, keepdims=True)
    second = jnp.mean(dn * normed, axis=-1, keepdims=True)
    return (dn - first - normed * second) * rstd


def query_rows(rows):
    return 256


def head_groups(slots):
    return [range(h, min(h + 2, slots)) for h in range(0, slots, 2)]


def forward_step(slots, step, ins, outs, scratch, gathered):
    qp_ref, kp_ref, q_ref, k_ref, v_ref = ins
    attn_ref, o_ref, l_ref = outs
    size = query_rows(q_ref.shape[0])
    groups = head_groups(slots)
    block, group = divmod(step, len(groups))
    rows = slice(block * size, (block + 1) * size)
    allowed = kp_ref[...] <= qp_ref[rows, :]
    for h in groups[group]:
        cols = slice(h * HEAD_DIM, (h + 1) * HEAD_DIM)
        raw = dot_t(q_ref[rows, cols], k_ref[:, cols])
        e = jnp.where(allowed, jnp.exp(raw * SCALE), 0.0)
        total = jnp.sum(e, axis=1, keepdims=True)
        numer = dot(e.astype(BF16), v_ref[:, cols])
        o = numer / total
        o_ref[rows, cols] = o
        attn_ref[rows, cols] = o.astype(BF16)
        l_ref[rows, h : h + 1] = total


def backward_step(slots, step, ins, outs, scratch, gathered):
    qp_ref, kp_ref, q_ref, k_ref, v_ref, w_ref, o_ref, l_ref = ins
    dq_ref, dk_ref, dv_ref = outs
    dk_acc, dv_acc, do_ref, g_ref, sem = scratch
    if step == 0:
        copy = pltpu.make_async_copy(gathered[0], g_ref, sem)
        copy.start()
        copy.wait()
        each = g_ref.shape[1]
        for j in range(g_ref.shape[0]):
            do_ref[j * each : (j + 1) * each, :] = dot_t(g_ref[j], w_ref[...])
    size = query_rows(q_ref.shape[0])
    blocks = q_ref.shape[0] // size
    groups = head_groups(slots)
    block, group = divmod(step, len(groups))
    rows = slice(block * size, (block + 1) * size)
    allowed = kp_ref[...] <= qp_ref[rows, :]
    for h in groups[group]:
        cols = slice(h * HEAD_DIM, (h + 1) * HEAD_DIM)
        q, k, v, do = q_ref[rows, cols], k_ref[:, cols], v_ref[:, cols], do_ref[rows, cols]
        total = l_ref[rows, h : h + 1]
        w = (do / total).astype(BF16)
        corr = jnp.sum(do * o_ref[rows, cols], axis=1, keepdims=True) / total
        e = jnp.where(allowed, jnp.exp(dot_t(q, k) * SCALE), 0.0)
        de = dot_t(w, v)
        ds = (e * (de - corr)).astype(BF16)
        dq_ref[rows, cols] = (dot(ds, k) * SCALE).astype(BF16)
        dk, dv = t_dot(ds, q), t_dot(e.astype(BF16), w)
        if block:
            dk, dv = dk + dk_acc[:, cols], dv + dv_acc[:, cols]
        if block < blocks - 1:
            dk_acc[:, cols] = dk
            dv_acc[:, cols] = dv
        else:
            dk_ref[:, cols] = (dk * SCALE).astype(BF16)
            dv_ref[:, cols] = dv.astype(BF16)


def forward_work(place, q, k, v, slots):
    rows, wide = q.shape
    shape = jax.ShapeDtypeStruct
    outs = (shape((rows, wide), BF16), shape((rows, wide), F32), shape((rows, slots), F32))
    steps = rows // query_rows(rows) * len(head_groups(slots))
    ins = (place.reshape(rows, 1), place.reshape(1, rows), q, k, v)
    return steps, functools.partial(forward_step, slots), False, ins, outs, ()


def backward_work(place, q, k, v, weight, o, total, slots, g):
    rows, wide = q.shape
    outs = (jax.ShapeDtypeStruct((rows, wide), BF16),) * 3
    steps = rows // query_rows(rows) * len(head_groups(slots))
    ins = (place.reshape(rows, 1), place.reshape(1, rows), q, k, v, weight, o, total)
    scratch = (pltpu.VMEM((rows, wide), F32),) * 3
    scratch += (pltpu.VMEM((rows // g.shape[0], *g.shape), g.dtype), pltpu.SemaphoreType.DMA)
    return steps, functools.partial(backward_step, slots), True, ins, outs, scratch


def stack_body(*refs):
    out = refs[-1]
    out[...] = jnp.zeros_like(out)
    for i, ref in enumerate(refs[:-1]):
        out[i : i + 1, : ref.shape[0]] = ref[...].reshape(1, ref.shape[0])


def stack_rows(vectors, longest):
    return pl.pallas_call(
        stack_body,
        in_specs=[pl.BlockSpec(memory_space=pltpu.VMEM)] * len(vectors),
        out_specs=pl.BlockSpec(memory_space=pltpu.VMEM),
        out_shape=jax.ShapeDtypeStruct((16, longest), vectors[0].dtype),
        name="stack_rows",
    )(*vectors)


def split_axis(n):
    across = 2 if n <= 8 else 4
    return n // across, across


def place_of(me, lines, across):
    a, b = lax.div(me, across), lax.rem(me, across)
    near = [(a < lines - 1, me + across), (a > 0, me - across), (b < across - 1, me + 1), (b > 0, me - 1)]
    return a, b, near


def turned_rows(rows, dtype, across, many=False):
    tile = 16 if dtype == BF16 else 8
    share = 4 if rows <= 128 and not many else 5
    return rows // share // tile * tile if across == 2 else 0


def meet(near, peers):
    barrier = pltpu.get_barrier_semaphore()
    for exists, target in near:

        @pl.when(exists)
        def _(target=target):
            pl.semaphore_signal(barrier, inc=1, device_id={"ctx": target}, device_id_type=MESH)

    for axis, peer in peers:
        pl.semaphore_signal(barrier, inc=1, device_id={axis: peer}, device_id_type=MESH)
    pl.semaphore_wait(barrier, len(peers) + sum(exists.astype(jnp.int32) for exists, _ in near))


class Fsdp:
    def __init__(self, nf, gather_in, gather_out, red_in, red_out, scratch):
        self.gather_in, self.gather_out, self.red_in, self.red_out = gather_in, gather_out, red_in, red_out
        n_gather, n_red = len(gather_in), len(red_in)
        self.near_in, self.stage, self.far_in = scratch[:n_red], scratch[n_red : 2 * n_red], scratch[2 * n_red : 3 * n_red]
        self.keep_sem, self.g_send, self.g_recv, self.r_send, self.r_recv = scratch[3 * n_red : 3 * n_red + 5]
        self.f = lax.axis_index("fsdp")
        self.core = lax.rem(self.f, 2)
        self.mate = self.f + 1 - 2 * self.core
        self.pairs = nf // 2
        self.pair = lax.div(self.f, 2)
        self.other = [lax.rem(self.pair + k, self.pairs) for k in range(1, self.pairs)]
        self.peers = [self.mate] + [2 * y + self.core for y in self.other] if n_gather + n_red else []

    @staticmethod
    def scratch(nf, gather, red):
        pairs = nf // 2
        dma = pltpu.SemaphoreType.DMA
        out = []
        for _ in range(3):
            out += [pltpu.VMEM((pairs, *x.shape[1:]), x.dtype) for x in red]
        g, r = max(len(gather), 1), max(len(red), 1)
        return out + [dma((g,)), dma((g, 2, nf)), dma((g, nf)), dma((r, 2, pairs)), dma((r, 2, pairs))]

    def copy(self, src, dst, send, recv, target):
        return pltpu.make_async_remote_copy(
            src_ref=src, dst_ref=dst, send_sem=send, recv_sem=recv, device_id={"fsdp": target}, device_id_type=MESH
        )

    def spread(self, i, source, target, own):
        out = self.gather_out[i].at[source]
        send = self.g_send.at[i, 0, target] if own else self.g_send.at[i, 1, source]
        return self.copy(self.gather_in[i] if own else out, out, send, self.g_recv.at[i, source], target)

    def keep(self, i):
        return pltpu.make_async_copy(self.gather_in[i], self.gather_out[i].at[self.f], self.keep_sem.at[i])

    def to_mate(self, j, y):
        src = self.red_in[j].at[2 * y + 1 - self.core]
        return self.copy(src, self.near_in[j].at[y], self.r_send.at[j, 0, y], self.r_recv.at[j, 0, y], self.mate)

    def to_far(self, j, y, source):
        send, recv = self.r_send.at[j, 1, y], self.r_recv.at[j, 1, source]
        return self.copy(self.stage[j].at[y], self.far_in[j].at[source], send, recv, 2 * y + self.core)

    def start(self):
        for j in range(len(self.red_in)):
            for y in range(self.pairs):
                self.to_mate(j, y).start()
        for i in range(len(self.gather_in)):
            for target in self.peers[1:] + self.peers[:1]:
                self.spread(i, self.f, target, True).start()
            self.keep(i).start()

    def middle(self):
        for j in range(len(self.red_in)):
            for y in range(self.pairs):
                self.to_mate(j, y).wait_recv()
            for y in self.other:
                value = self.red_in[j][2 * y + self.core].astype(F32) + self.near_in[j][y].astype(F32)
                self.stage[j][y] = value.astype(self.stage[j].dtype)
                self.to_far(j, y, self.pair).start()

    def end(self, first, last):
        for j in range(first, last):
            value = self.red_in[j][self.f].astype(F32) + self.near_in[j][self.pair].astype(F32)
            for y in self.other:
                self.to_far(j, y, y).wait_recv()
                value = value + self.far_in[j][y].astype(F32)
            self.red_out[j][...] = value.astype(self.red_out[j].dtype)

    def forward(self):
        for i in range(len(self.gather_in)):
            for y in self.other:
                source = 2 * y + self.core
                self.spread(i, source, self.mate, False).wait_recv()
                self.spread(i, source, self.mate, False).start()

    def finish(self):
        for i in range(len(self.gather_in)):
            self.spread(i, self.mate, self.mate, False).wait_recv()
            for y in self.other:
                self.spread(i, 2 * y + 1 - self.core, self.mate, False).wait_recv()
            self.keep(i).wait()
            for target in self.peers:
                self.spread(i, self.f, target, True).wait_send()
            for y in self.other:
                self.spread(i, 2 * y + self.core, self.mate, False).wait_send()
        for j in range(len(self.red_in)):
            for y in range(self.pairs):
                self.to_mate(j, y).wait_send()
            for y in self.other:
                self.to_far(j, y, self.pair).wait_send()


def exchange_body(n, nf, counts, moves, work, *refs):
    n_ctx, n_fsdp, n_own, n_red, n_work_in, n_work_out, n_work_scratch = counts
    bounds = [0]
    for size in counts[:5]:
        bounds.append(bounds[-1] + size)
    ctx_in, fsdp_in, own_in, red_in, work_in = (refs[i:j] for i, j in zip(bounds, bounds[1:]))
    refs = refs[bounds[-1] :]
    ctx_out, fsdp_out, own_out = refs[:n_ctx], refs[n_ctx : n_ctx + n_fsdp], refs[n_ctx + n_fsdp : n_ctx + n_fsdp + n_own]
    refs = refs[n_ctx + n_fsdp + n_own :]
    red_out, refs = refs[:n_red], refs[n_red:]
    if moves:
        placed, refs = refs[0], refs[1:]
    work_out, refs = refs[:n_work_out], refs[n_work_out:]
    work_scratch, refs = refs[:n_work_scratch], refs[n_work_scratch:]
    sums, scratch = refs[:n_red], refs[n_red:]
    copy_sem, send_sem, recv_sem, place_send, place_recv = scratch[:5]
    fs = Fsdp(nf, fsdp_in, fsdp_out, red_in + own_in, sums + own_out, scratch[5:])

    lines, across = split_axis(n)
    me = lax.axis_index("ctx")
    a, b, near = place_of(me, lines, across)
    pieces = [(src, out, first, rows) for src, out in zip(ctx_in, ctx_out) for first, rows in cut(out.shape[1])]
    late = len(pieces)
    second = late
    for src, out in zip(sums, red_out):
        second = len(pieces)
        pieces += [(src, out, first, rows) for first, rows in cut(out.shape[1])]
    peers = [lax.rem(fs.f + k, nf) for k in range(1, nf)] if moves else fs.peers
    meet(near if pieces else [], [("fsdp", peer) for peer in peers])

    def turned_part(i):
        return turned_rows(pieces[i][3], pieces[i][1].dtype, across, len(pieces) > 1)

    def hop(i, block, way, turned=False, own=False):
        source, out, first, size = pieces[i]
        last = turned_part(i)
        rows = pl.ds(first + size - last, last) if turned else pl.ds(first, size - last)
        return pltpu.make_async_remote_copy(
            src_ref=source.at[rows] if own else out.at[block, rows],
            dst_ref=out.at[block, rows],
            send_sem=send_sem.at[i, way, block, int(turned)],
            recv_sem=recv_sem.at[i, way, block, int(turned)],
            device_id={"ctx": me + (across, -across, 1, -1)[way]},
            device_id_type=MESH,
        )

    def keep(i):
        source, out, first, size = pieces[i]
        rows = pl.ds(first, size)
        return pltpu.make_async_copy(source.at[rows], out.at[me, rows], copy_sem.at[i])

    def each_own(i, act):
        for turned in (True, False) if turned_part(i) else (False,):
            for way in (2, 3, 0, 1):
                pl.when(near[way][0])(lambda way=way: act(hop(i, me, way, turned, True)))

    def each_twin(i, wait, act):
        if turned_part(i):
            twin = me + 1 - 2 * b
            for way in (2, 3):

                @pl.when(near[5 - way][0])
                def _(way=way):
                    if wait:
                        hop(i, twin, way, True).wait_recv()
                    for on in (0, 1):
                        pl.when(near[on][0])(lambda on=on: act(hop(i, twin, on, True)))

    def each_relay(i, d, wait, act):
        for way, there, shift in ((0, a >= d, -d * across), (1, a + d < lines, d * across)):

            @pl.when(there)
            def _(way=way, shift=shift):
                for turned, block in [(False, me + shift)] + (
                    [(True, me + shift), (True, me + 1 - 2 * b + shift)] if turned_part(i) else []
                ):
                    if wait:
                        hop(i, block, way, turned).wait_recv()
                    for on in (way,) if turned else (2, 3, way):
                        pl.when(near[on][0])(lambda on=on: act(hop(i, block, on, turned)))

    def start(copy):
        copy.start()

    def wait_send(copy):
        copy.wait_send()

    def begin(these):
        for i in these:
            each_own(i, start)
            keep(i).start()

    def crossed(i):
        for d in range(1, across):
            for step in range(lines):
                for sign in (1, -1) if step else (1,):
                    for way, there, shift in ((2, b >= d, -d), (3, b + d < across, d)):
                        other = a + sign * step

                        @pl.when(there & (other >= 0) & (other < lines))
                        def _(source=other * across + b + shift, way=way):
                            hop(i, source, way).wait_recv()
                            if d < across - 1:
                                pl.when(near[way][0])(lambda: hop(i, source, way).start())

    def place(k, act_local, act_send):
        block, row, src, dst, goal, size = moves[k]
        source, goal = red_out[0].at[block, pl.ds(row, size)], placed.at[pl.ds(goal, size)]
        if src == dst:
            pl.when(fs.f == src)(lambda: act_local(pltpu.make_async_copy(source, goal, place_send.at[k])))
            return
        remote = pltpu.make_async_remote_copy(
            src_ref=source,
            dst_ref=goal,
            send_sem=place_send.at[k],
            recv_sem=place_recv.at[k],
            device_id={"fsdp": jnp.int32(dst)},
            device_id_type=MESH,
        )
        pl.when(fs.f == src)(lambda: act_send(remote))
        if act_local is wait_copy:
            pl.when(fs.f == dst)(remote.wait_recv)

    def wait_copy(copy):
        copy.wait()

    work_steps, work_fn, gated = work
    plan = []

    def add(act, *args, then_work=True):
        plan.append((functools.partial(act, *args), then_work))

    def hops(i, d):
        if d == 1:
            each_twin(i, True, start)
        each_relay(i, d, True, start)

    def complete(i):
        crossed(i)
        keep(i).wait()

    begin(range(late))
    fs.start()
    fs.middle()
    if not gated:
        add(lambda: None)
    before, after = range(second), range(second, len(pieces))
    ready = []
    if gated:
        for d in range(1, lines):
            for i in range(late):
                add(hops, i, d, then_work=False)
            if d == 2:
                add(fs.end, 0, n_red, then_work=False)
                add(begin, range(late, len(pieces)), then_work=False)
        ready = range(late)
        for i in ready:
            add(complete, i, then_work=i == late - 1)
        add(fs.end, n_red, n_red + n_own)
        for d in range(1, lines):
            for i in range(late, len(pieces)):
                add(hops, i, d)
    elif n_red:
        add(fs.end, 0, n_red - 1)
        add(begin, range(late, second))
        for i in before:
            add(hops, i, 1)
        add(fs.end, n_red - 1, n_red)
        add(begin, after)
        for d in range(2, lines):
            for i in before:
                add(hops, i, d)
            for i in after if d == 2 else ():
                add(hops, i, 1)
        if moves:
            ready = [i for i in before if pieces[i][1] is red_out[0]]
            for i in ready:
                add(complete, i)
            for k in range(len(moves)):
                add(place, k, start, start)
        for d in range(2, lines):
            for i in after:
                add(hops, i, d)
    else:
        for d in range(1, lines):
            for i in range(len(pieces)):
                add(hops, i, d)
            if d == lines - 2:
                add(fs.forward, then_work=False)
        add(fs.end, 0, n_own)
    points = sum(then_work for _, then_work in plan)
    at = 0
    for act, then_work in plan:
        act()
        if then_work:
            for step in range(at * work_steps // points, (at + 1) * work_steps // points):
                work_fn(step, work_in, work_out, work_scratch, ctx_out)
            at += 1

    for i in range(len(pieces)):
        if i not in ready:
            complete(i)
    for k in range(len(moves)):
        place(k, wait_copy, wait_send)

    for i in range(len(pieces)):
        each_own(i, wait_send)
        each_twin(i, False, wait_send)
        for d in range(1, lines):
            each_relay(i, d, False, wait_send)
        for d in range(1, across - 1):
            for line in range(lines):
                for way, there, shift in ((2, b >= d, -d), (3, b + d < across, d)):

                    @pl.when(there & near[way][0])
                    def _(i=i, source=line * across + b + shift, way=way):
                        hop(i, source, way).wait_send()

    fs.finish()


def cut(rows):
    if rows < 200:
        return [(0, rows)]
    half = rows // 32 * 16
    return [(0, rows - half), (rows - half, half)]


def exchange(call, n, nf, ctx=(), fsdp=(), own=(), red=(), moves=(), kept=0, work=None):
    shape = jax.ShapeDtypeStruct
    sums = [shape(x.shape[1:], x.dtype) for x in red]
    outs = [shape((n, *x.shape), x.dtype) for x in ctx]
    outs += [shape((nf, *x.shape), x.dtype) for x in fsdp]
    outs += [shape(x.shape[1:], x.dtype) for x in own]
    outs += [shape((n, *x.shape), x.dtype) for x in sums]
    outs += [shape((kept, sums[0].shape[1]), sums[0].dtype)] if moves else []
    steps, work_fn, gated, work_in, work_out, work_scratch = work or (0, None, False, (), (), ())
    gathered = max(sum(len(cut(x.shape[0])) for x in [*ctx, *sums]), 1)
    any_spec, vmem_spec = pl.BlockSpec(memory_space=pl.ANY), pl.BlockSpec(memory_space=pltpu.VMEM)
    inputs = (*ctx, *fsdp, *own, *red, *work_in)
    counts = [len(x) for x in (ctx, fsdp, own, red, work_in, work_out, work_scratch)]
    dma = pltpu.SemaphoreType.DMA
    return pl.pallas_call(
        functools.partial(exchange_body, n, nf, tuple(counts), tuple(moves), (steps, work_fn, gated)),
        in_specs=[any_spec] * (len(ctx) + len(fsdp)) + [vmem_spec] * (len(inputs) - len(ctx) - len(fsdp)),
        out_specs=[any_spec] * (len(ctx) + len(fsdp))
        + [vmem_spec] * len(own)
        + [any_spec] * (len(sums) + (1 if moves else 0))
        + [vmem_spec] * len(work_out),
        out_shape=[*outs, *work_out],
        scratch_shapes=list(work_scratch)
        + [pltpu.VMEM(x.shape, x.dtype) for x in sums]
        + [dma((gathered,)), dma((gathered, 4, n, 2)), dma((gathered, 4, n, 2))]
        + [dma((max(len(moves), 1),))] * 2
        + Fsdp.scratch(nf, fsdp, [*red, *own]),
        name=f"exchange_{call}",
        compiler_params=pltpu.CompilerParams(collective_id=call, has_side_effects=True, vmem_limit_bytes=60 * 2**20),
    )(*inputs)


class Scatter:
    def __init__(self, n, many, transposed, left, right, out, scratch):
        self.left, self.right, self.out, self.transposed = left, right, out, transposed
        self.part, self.acc, self.acc_t, self.over_in, self.sums, self.sums_t = scratch[:6]
        self.line_in, self.line_in_t, self.twin_in = scratch[6:9]
        self.o_send, self.o_recv, self.l_send, self.l_recv, self.t_send, self.t_recv = scratch[9:15]
        self.w_send, self.w_recv = scratch[15:17]
        self.lines, self.across = split_axis(n)
        self.me = lax.axis_index("ctx")
        self.a, self.b, self.near = place_of(self.me, self.lines, self.across)
        self.rows = out.shape[0]
        self.last = turned_rows(self.rows, BF16, self.across, many)
        self.head, self.tail = pl.ds(0, self.rows - self.last), pl.ds(self.rows - self.last, self.last)
        self.peers = [self.me - self.b + lax.rem(self.b + k, self.across) for k in range(1, self.across)]

    @staticmethod
    def scratch(n, many, rows, width):
        lines, across = split_axis(n)
        last = turned_rows(rows, BF16, across, many)
        some = max(last, 16)
        vmem, dma = pltpu.VMEM, pltpu.SemaphoreType.DMA
        return [
            vmem((lines, across, rows, width), BF16),
            vmem((rows - last, width), F32),
            vmem((across, some, width), F32),
            vmem((across - 1, lines, rows - last, width), BF16),
            vmem((lines, rows - last, width), BF16),
            vmem((lines, across, some, width), BF16),
            vmem((2, lines, rows - last, width), BF16),
            vmem((2, lines, across, some, width), BF16),
            vmem((some, width), BF16),
            dma((across - 1, lines)),
            dma((across - 1, lines)),
            dma((2, lines)),
            dma((2, lines)),
            dma((2, lines)),
            dma((2, lines)),
            dma,
            dma,
        ]

    def copy(self, src, dst, send, recv, target):
        return pltpu.make_async_remote_copy(
            src_ref=src, dst_ref=dst, send_sem=send, recv_sem=recv, device_id={"ctx": target}, device_id_type=MESH
        )

    def over(self, line, k):
        src = self.part.at[line, lax.rem(self.b + k, self.across), self.head]
        send, recv = self.o_send.at[k - 1, line], self.o_recv.at[k - 1, line]
        return self.copy(src, self.over_in.at[k - 1, line], send, recv, self.peers[k - 1])

    def along(self, line, way):
        target = self.me + (self.across, -self.across)[way]
        send, recv = self.l_send.at[way, line], self.l_recv.at[way, line]
        return self.copy(self.sums.at[line], self.line_in.at[way, line], send, recv, target)

    def along_t(self, line, way):
        target = self.me + (self.across, -self.across)[way]
        send, recv = self.t_send.at[way, line], self.t_recv.at[way, line]
        return self.copy(self.sums_t.at[line], self.line_in_t.at[way, line], send, recv, target)

    def twin(self):
        return self.copy(self.sums_t.at[self.a, 1 - self.b], self.twin_in, self.w_send, self.w_recv, self.peers[0])

    def compute(self, line):
        size = self.across * self.rows
        lhs = self.left[pl.ds(pl.multiple_of(line * size, size), size), :]
        value = dot_t(lhs, self.right[...]) if self.transposed else dot(lhs, self.right[...])
        self.part[line] = value.astype(BF16).reshape(self.across, self.rows, value.shape[1])
        for k in range(1, self.across):
            self.over(line, k).start()

    def collect(self, line, acc, landed, hop, ways):
        for way, there in ways:

            @pl.when(there)
            def _(way=way):
                hop(line, way).wait_recv()
                acc[...] += landed[way, line].astype(F32)

    def across_sum(self, line):
        value = self.part[line, self.b, self.head].astype(F32)
        for k in range(1, self.across):
            self.over(line, k).wait_recv()
            value = value + self.over_in[k - 1, line].astype(F32)
        self.acc[...] = value

    def pass_on(self, line):
        up, down = line > self.a, line < self.a
        ways = ((0, up & (self.a > 0)), (1, down & (self.a < self.lines - 1)))
        if self.last:
            self.acc_t[...] = self.part[line, :, self.tail].astype(F32)
            self.collect(line, self.acc_t, self.line_in_t, self.along_t, ways)
            self.sums_t[line] = self.acc_t[...].astype(BF16)
            pl.when(up)(lambda: self.along_t(line, 0).start())
            pl.when(down)(lambda: self.along_t(line, 1).start())
        self.across_sum(line)
        self.collect(line, self.acc, self.line_in, self.along, ways)
        self.sums[line] = self.acc[...].astype(BF16)
        pl.when(up)(lambda: self.along(line, 0).start())
        pl.when(down)(lambda: self.along(line, 1).start())

    def own(self):
        ways = ((0, self.near[1][0]), (1, self.near[0][0]))
        if self.last:
            self.acc_t[...] = self.part[self.a, :, self.tail].astype(F32)
            self.collect(self.a, self.acc_t, self.line_in_t, self.along_t, ways)
            self.sums_t[self.a] = self.acc_t[...].astype(BF16)
            self.twin().start()
        self.across_sum(self.a)
        self.collect(self.a, self.acc, self.line_in, self.along, ways)
        self.out[self.head, :] = self.acc[...]
        if self.last:
            self.twin().wait_recv()
            self.out[self.tail, :] = self.acc_t[self.b] + self.twin_in[...].astype(F32)

    def sent(self, order):
        for line in order:
            for k in range(1, self.across):
                self.over(line, k).wait_send()
        for line in order[:-1]:
            for way, there in ((0, line > self.a), (1, line < self.a)):

                @pl.when(there)
                def _(way=way, line=line):
                    self.along(line, way).wait_send()
                    if self.last:
                        self.along_t(line, way).wait_send()

        if self.last:
            self.twin().wait_send()


def product_body(n, nf, counts, transposed, *refs):
    n_prod, n_sides, n_fsdp = counts
    pairs, refs = refs[: 2 * n_prod], refs[2 * n_prod :]
    side_in, refs = refs[: 2 * n_sides], refs[2 * n_sides :]
    fsdp_in, refs = refs[:n_fsdp], refs[n_fsdp:]
    outs, side_out, fsdp_out = refs[:n_prod], refs[n_prod : n_prod + n_sides], refs[n_prod + n_sides : n_prod + n_sides + n_fsdp]
    scratch = refs[n_prod + n_sides + n_fsdp :]
    side_at, side_sem, scratch = scratch[: 2 * n_sides], scratch[2 * n_sides], scratch[2 * n_sides + 1 :]
    fetches = [pltpu.make_async_copy(side_in[j], side_at[j], side_sem.at[j]) for j in range(2 * n_sides)]
    each = 17
    jobs = [
        Scatter(n, n_prod > 1, transposed[p], pairs[2 * p], pairs[2 * p + 1], outs[p], scratch[each * p : each * (p + 1)])
        for p in range(n_prod)
    ]
    fs = Fsdp(nf, fsdp_in, fsdp_out, [], [], scratch[each * n_prod :])
    a, lines = jobs[0].a, jobs[0].lines
    meet(jobs[0].near[:2], [("ctx", peer) for peer in jobs[0].peers] + [("fsdp", peer) for peer in fs.peers])

    order = []
    for k in range(lines):
        line = jnp.int32(0)
        for av in range(lines):
            line = jnp.where(a == av, sorted(range(lines), key=lambda j: (-abs(j - av), j))[k], line)
        order.append(line)

    for fetch in fetches:
        fetch.start()
    for job in jobs:
        for line in order:
            job.compute(line)
    fs.start()
    steps = [(job, line) for job in jobs for line in order[:-1]]
    bits = []
    for j in range(n_sides):
        size = side_in[2 * j].shape[1]
        width = -(-size // 3 // 128) * 128
        bits += [(j, first, min(width, size - first)) for first in range(0, size, width)]
    for step, (job, line) in enumerate(steps):
        job.pass_on(line)
        for j, first, size in bits[step * len(bits) // len(steps) : (step + 1) * len(bits) // len(steps)]:
            if first == 0:
                fetches[2 * j].wait()
                fetches[2 * j + 1].wait()
            part = side_at[2 * j][:, first : first + size]
            side_out[j][first : first + size, :] = t_dot(part, side_at[2 * j + 1][...]).astype(BF16)
        if step == len(order) - 3:
            fs.forward()
    for job in jobs:
        job.own()
    for job in jobs:
        job.sent(order)
    fs.finish()


def product(call, n, nf, products, sides=(), fsdp=()):
    length = products[0][0].shape[0]
    if length > 1024 and (sides or len(products) > 1):
        sums = []
        for i, one in enumerate(products):
            total, *gathered = product(call if i == 0 else call + 10, n, nf, [one], fsdp=fsdp if i == 0 else ())
            sums.append(total)
            fsdp_out = gathered if i == 0 else fsdp_out
        return [*sums, *[t_dot(x, y).astype(BF16) for x, y in sides], *fsdp_out]
    rows = length // n
    shape = jax.ShapeDtypeStruct
    widths = [right.shape[0 if turned else 1] for _, right, turned in products]
    outs = [shape((rows, width), F32) for width in widths]
    outs += [shape((x.shape[1], y.shape[1]), BF16) for x, y in sides]
    outs += [shape((nf, *x.shape), x.dtype) for x in fsdp]
    inputs = [z for left, right, _ in products for z in (left, right)] + [z for side in sides for z in side]
    vmem_spec, any_spec = pl.BlockSpec(memory_space=pltpu.VMEM), pl.BlockSpec(memory_space=pl.ANY)
    return pl.pallas_call(
        functools.partial(
            product_body,
            n,
            nf,
            (len(products), len(sides), len(fsdp)),
            tuple(turned for _, _, turned in products),
        ),
        in_specs=[vmem_spec] * (2 * len(products)) + [any_spec] * (2 * len(sides) + len(fsdp)),
        out_specs=[vmem_spec] * (len(outs) - len(fsdp)) + [any_spec] * len(fsdp),
        out_shape=outs,
        scratch_shapes=[pltpu.VMEM(z.shape, z.dtype) for side in sides for z in side]
        + [pltpu.SemaphoreType.DMA((max(2 * len(sides), 1),))]
        + [s for width in widths for s in Scatter.scratch(n, len(widths) > 1, rows, width)] + Fsdp.scratch(nf, fsdp, ()),
        name=f"product_{call}",
        compiler_params=pltpu.CompilerParams(collective_id=call, has_side_effects=True, vmem_limit_bytes=63 * 2**20),
    )(*inputs, *fsdp)


def row_moves(n, nf, heads):
    part, local = -(-heads // n) * HEAD_DIM // nf, heads * HEAD_DIM // nf
    moves = []
    for block, start, goal, size in head_moves(n, heads, 0, 0):
        done = 0
        while done < size:
            here, there = start + done, goal + done
            rows = min(size - done, part - here % part, local - there % local)
            moves.append((block, here % part, here // part, there // local, there % local, rows))
            done += rows
    return moves


def layout_body(moves, *refs):
    ins, outs = refs[: len(refs) // 2], refs[len(refs) // 2 :]
    for in_ref, out_ref, per_out in zip(ins, outs, moves):
        if per_out is None:
            out_ref[...] = in_ref[...].astype(F32)
            continue
        for block, start, goal, size in per_out:
            out_ref[:, goal : goal + size] = in_ref[block, :, start : start + size].astype(F32)


def lay_out(arrays, widths, moves):
    rows = next(x.shape[1] for x in arrays if x.ndim == 3)
    step = next(s for s in (80, 16, rows) if rows % s == 0)
    grid = rows // step
    in_specs, out_specs, outs = [], [], []
    for x, width in zip(arrays, widths):
        flat = pl.BlockSpec((x.shape[-2] // grid, width), lambda i: (i, 0))
        in_specs.append(pl.BlockSpec((x.shape[0], step, x.shape[2]), lambda i: (0, i, 0)) if x.ndim == 3 else flat)
        out_specs.append(flat)
        outs.append(jax.ShapeDtypeStruct((x.shape[-2], width), F32))
    return pl.pallas_call(
        functools.partial(layout_body, tuple(m and tuple(m) for m in moves)),
        grid=(grid,),
        in_specs=in_specs,
        out_specs=out_specs,
        out_shape=outs,
        name="lay_out",
        cost_estimate=pl.CostEstimate(
            flops=0, bytes_accessed=6 * sum(x.shape[0] * x.shape[1] for x in outs), transcendentals=0
        ),
        compiler_params=pltpu.CompilerParams(vmem_limit_bytes=60 * 2**20),
    )(*arrays)


def head_moves(n, heads, offset, goal):
    base, rest = divmod(heads, n)
    moves = [(c, offset, goal + c * base * HEAD_DIM, base * HEAD_DIM) for c in range(n) if base]
    moves += [
        (c, offset + base * HEAD_DIM, goal + (base * n + c) * HEAD_DIM, HEAD_DIM) for c in range(rest)
    ]
    return moves


def head_columns(value, width, c, n):
    heads = width // HEAD_DIM
    base, rest = divmod(heads, n)
    parts = []
    if base:
        parts.append(lax.dynamic_slice_in_dim(value, c * base * HEAD_DIM, base * HEAD_DIM, axis=-1))
    if rest:
        start = jnp.minimum(base * n + c, heads - 1) * HEAD_DIM
        extra = lax.dynamic_slice_in_dim(value, start, HEAD_DIM, axis=-1)
        parts.append(jnp.where(c < rest, extra, jnp.zeros_like(extra)))
    return jnp.concatenate(parts, axis=-1)


def place_heads(value, heads, c, n):
    base, rest = divmod(heads, n)
    out = jnp.zeros((heads * HEAD_DIM,), value.dtype)
    if rest:
        start = jnp.minimum(base * n + c, heads - 1) * HEAD_DIM
        extra = jnp.where(c < rest, value[base * HEAD_DIM :], 0.0)
        out = lax.dynamic_update_slice(out, extra, (start,))
    if base:
        out = lax.dynamic_update_slice(out, value[: base * HEAD_DIM], (c * base * HEAD_DIM,))
    return out


def head_rows(value, heads, c, f, n):
    base, rest = divmod(heads, n)
    local, width = value.shape
    pad = max(base, 1) * HEAD_DIM
    padded = jnp.pad(value, ((pad, pad), (0, 0)))
    parts = []
    if base:
        start = jnp.clip(c * base * HEAD_DIM - f * local + pad, 0, local + 2 * pad - base * HEAD_DIM)
        parts.append(lax.dynamic_slice_in_dim(padded, start, base * HEAD_DIM, axis=0))
    if rest:
        start = jnp.clip((base * n + c) * HEAD_DIM - f * local + pad, 0, local + 2 * pad - HEAD_DIM)
        extra = lax.dynamic_slice_in_dim(padded, start, HEAD_DIM, axis=0)
        parts.append(jnp.where(c < rest, extra, jnp.zeros_like(extra)))
    return jnp.concatenate(parts, axis=0)


def on_device(
    tokens,
    ln1_gain,
    ln1_shift,
    qkv_weight,
    qv_bias,
    out_weight,
    out_bias,
    ln2_gain,
    ln2_shift,
    up_weight,
    up_bias,
    down_weight,
    down_bias,
    block_table,
    cotangent,
):
    rows, width = tokens.shape[1:]
    heads = width // HEAD_DIM
    n = lax.axis_size("ctx")
    nf = lax.axis_size("fsdp")
    c = lax.axis_index("ctx")
    f = lax.axis_index("fsdp")
    slots = -(-heads // n)
    wide = slots * HEAD_DIM
    half = rows // 2
    local = width // nf
    ff = up_weight.shape[1]
    ff_local = ff // nf
    ff_part = ff_local // n

    within = jnp.arange(rows, dtype=jnp.int32)
    block_of = jnp.where(within[None, :] < half, block_table[:, None], 2 * n - 1 - block_table[:, None])
    place = (block_of * half + within[None, :] % half).reshape(-1)

    vectors = (ln1_gain, ln1_shift, qv_bias, out_bias, ln2_gain, ln2_shift, up_bias, down_bias)
    longest = max(v.shape[0] for v in vectors)
    flat = stack_rows(vectors, longest)
    q_w = head_columns(qkv_weight[:, :width], width, c, n)
    k_w = head_columns(qkv_weight[:, width : 2 * width], width, c, n)
    v_w = head_columns(qkv_weight[:, 2 * width :], width, c, n)
    w_mine = jnp.concatenate([q_w, k_w, v_w], axis=1)
    x_all, packed, w_qkv = exchange(0, n, nf, ctx=[tokens[0]], fsdp=[flat, w_mine])
    out_weight, up_weight, down_weight, packed = lax.optimization_barrier(
        (out_weight, up_weight, down_weight, packed)
    )
    x_all = x_all.reshape(n * rows, width)
    w_qkv = w_qkv.reshape(width, 3 * wide)
    full = [packed[:, i, : v.shape[0]].reshape(-1).astype(F32) for i, v in enumerate(vectors)]
    gain1, shift1, b_qv, b_out, gain2, shift2, b_up, b_down = full

    b_up_mine = lax.dynamic_slice_in_dim(b_up.reshape(nf, n, ff_part), c, 1, axis=1).reshape(-1)
    bq = head_columns(b_qv[:width], width, c, n)
    bv = head_columns(b_qv[width:], width, c, n)

    n1_all, _ = ln_stats(x_all.astype(F32))
    act1 = (n1_all * gain1 + shift1).astype(BF16)
    proj = dot(act1, w_qkv)
    q = (proj[:, :wide] + bq).astype(BF16)
    k = proj[:, wide : 2 * wide].astype(BF16)
    v = (proj[:, 2 * wide :] + bv).astype(BF16)
    g2_all, w_out, attn, o, total = exchange(
        1,
        n,
        nf,
        ctx=[cotangent[0]],
        fsdp=[head_rows(out_weight, heads, c, f, n)],
        work=forward_work(place, q, k, v, slots),
    )
    up_mine = [lax.dynamic_slice_in_dim(up_weight, i * ff_local + c * ff_part, ff_part, axis=1) for i in range(nf)]
    w_out = functools.reduce(jnp.add, [w_out[i] for i in range(nf)])
    mixed, w_up = product(7, n, nf, [(attn, w_out, False)], fsdp=[jnp.concatenate(up_mine, axis=1)])
    w_up = w_up.reshape(width, nf * ff_part)
    x = tokens[0].astype(F32)
    mid = x + mixed + b_out

    n2, rstd2 = ln_stats(mid)
    act2, w_down = exchange(
        2,
        n,
        nf,
        ctx=[(n2 * gain2 + shift2).astype(BF16)],
        fsdp=[lax.dynamic_slice_in_dim(down_weight, c * ff_part, ff_part, axis=0)],
    )
    act2 = act2.reshape(n * rows, width)
    g2_all = g2_all.reshape(n * rows, width)
    w_down = w_down.reshape(nf * ff_part, width)
    u = dot(act2, w_up) + b_up_mine
    activated, gelu_back = jax.vjp(lambda t: jax.nn.gelu(t, approximate=True), u)
    hidden = activated.astype(BF16)
    dh = dot_t(g2_all, w_down)
    du = gelu_back(dh)[0].astype(BF16)
    da2, fed, d_up, d_down = product(
        3, n, nf, [(du, w_up, True), (hidden, w_down, False)], sides=[(act2, du), (hidden, g2_all)]
    )
    result = mid + fed + b_down
    d_up = d_up.reshape(nf, local, nf * ff_part)
    d_down = d_down.reshape(nf, ff_part, width)
    d_up_bias = jnp.sum(du.astype(F32), axis=0)
    grad_out = cotangent[0].astype(F32)
    d_down_bias = jnp.sum(grad_out, axis=0)

    d_gain2 = jnp.sum(da2 * n2, axis=0)
    d_shift2 = jnp.sum(da2, axis=0)
    d_mid = grad_out + ln_back(da2, n2, rstd2, gain2)
    g1 = d_mid.astype(BF16)
    d_out_bias = jnp.sum(g1.astype(F32), axis=0)
    g1_all, d_down, d_up, gq, gk, gv = exchange(
        4, n, nf, ctx=[g1], own=[d_down], red=[d_up], work=backward_work(place, q, k, v, w_out, o, total, slots, g1)
    )
    g1_all = g1_all.reshape(n * rows, width)
    g_qkv = jnp.concatenate([gq, gk, gv], axis=1)
    da1, d_qkv, d_out = product(5, n, nf, [(g_qkv, w_qkv, True)], sides=[(act1, g_qkv), (attn, g1_all)])
    d_qkv = d_qkv.reshape(nf, local, 3 * wide)
    d_out = d_out.reshape(nf, wide // nf, width)

    n1, rstd1 = ln_stats(x)
    d_gain1 = jnp.sum(da1 * n1, axis=0)
    d_shift1 = jnp.sum(da1, axis=0)
    input_grad = d_mid + ln_back(da1, n1, rstd1, gain1)

    dq_bias = place_heads(jnp.sum(gq.astype(F32), axis=0), heads, c, n)
    dv_bias = place_heads(jnp.sum(gv.astype(F32), axis=0), heads, c, n)
    up_placed = lax.dynamic_update_slice(
        jnp.zeros((nf, n, ff_part), F32), d_up_bias.reshape(nf, 1, ff_part), (0, c, 0)
    )
    smalls = (
        d_gain1,
        d_shift1,
        jnp.concatenate([dq_bias, dv_bias]),
        d_out_bias,
        d_gain2,
        d_shift2,
        up_placed.reshape(-1),
        d_down_bias,
    )
    packed = jnp.concatenate([s.reshape(nf, -1) for s in smalls], axis=1)
    packed = jnp.pad(packed, ((0, 0), (0, -packed.shape[1] % 1024))).reshape(nf, -1, 128)
    d_down, _, packed, d_qkv, d_out = exchange(
        6, n, nf, ctx=[d_down], red=[d_out, packed, d_qkv], moves=row_moves(n, nf, heads), kept=local
    )
    mine = jnp.sum(packed, axis=0).reshape(-1)
    up_moves = [(i, j * ff_part, j * ff_local + i * ff_part, ff_part) for i in range(n) for j in range(nf)]
    qkv_moves = [m for i in range(3) for m in head_moves(n, heads, i * wide, i * width)]
    d_down_full, d_out_full, d_up_full, d_qkv_full = lay_out(
        (d_down.reshape(ff_local, width), d_out, d_up, d_qkv),
        (width, width, ff, 3 * width),
        (None, None, up_moves, qkv_moves),
    )
    out, at = [], 0
    for s in smalls:
        size = s.size // nf
        out.append(mine[at : at + size])
        at += size
    return (
        result[None],
        input_grad[None],
        out[0],
        out[1],
        d_qkv_full,
        out[2],
        d_out_full,
        out[3],
        out[4],
        out[5],
        d_up_full,
        out[6],
        d_down_full,
        out[7],
    )


def solution(mesh):
    rows, one, two = P("fsdp", "ctx", None), P("fsdp"), P("fsdp", None)
    return jax.shard_map(
        on_device,
        mesh=mesh,
        in_specs=(rows, one, one, two, one, two, one, one, one, two, one, two, one, P(), rows),
        out_specs=(rows, rows, one, one, two, one, two, one, one, one, two, one, two, one),
        check_vma=False,
    )
```

```python
import functools

import jax
import jax.numpy as jnp
from jax import lax
from jax.experimental import pallas as pl
from jax.experimental.pallas import tpu as pltpu
from jax.sharding import PartitionSpec as P

HEAD_DIM = 64
EPS = 1e-05
SCALE = 0.125
F32 = jnp.float32
BF16 = jnp.bfloat16
MESH = pl.DeviceIdType.MESH


def dot(left, right):
    return jnp.dot(left, right, preferred_element_type=F32)


def dot_t(left, right):
    return lax.dot_general(left, right, (((1,), (1,)), ((), ())), preferred_element_type=F32)


def t_dot(left, right):
    return lax.dot_general(left, right, (((0,), (0,)), ((), ())), preferred_element_type=F32)


def ln_stats(value):
    centre = value - jnp.mean(value, axis=-1, keepdims=True)
    spread = jnp.mean(centre * centre, axis=-1, keepdims=True)
    rstd = lax.rsqrt(spread + EPS)
    return centre * rstd, rstd


def ln_back(grad, normed, rstd, gain):
    dn = grad * gain
    first = jnp.mean(dn, axis=-1, keepdims=True)
    second = jnp.mean(dn * normed, axis=-1, keepdims=True)
    return (dn - first - normed * second) * rstd


def query_rows(rows):
    return 256


def head_groups(slots):
    return [range(h, min(h + 2, slots)) for h in range(0, slots, 2)]


def forward_step(slots, step, ins, outs, scratch, gathered):
    qp_ref, kp_ref, q_ref, k_ref, v_ref = ins
    attn_ref, o_ref, l_ref = outs
    size = query_rows(q_ref.shape[0])
    groups = head_groups(slots)
    block, group = divmod(step, len(groups))
    rows = slice(block * size, (block + 1) * size)
    allowed = kp_ref[...] <= qp_ref[rows, :]
    for h in groups[group]:
        cols = slice(h * HEAD_DIM, (h + 1) * HEAD_DIM)
        raw = dot_t(q_ref[rows, cols], k_ref[:, cols])
        e = jnp.where(allowed, jnp.exp(raw * SCALE), 0.0)
        total = jnp.sum(e, axis=1, keepdims=True)
        numer = dot(e.astype(BF16), v_ref[:, cols])
        o = numer / total
        o_ref[rows, cols] = o
        attn_ref[rows, cols] = o.astype(BF16)
        l_ref[rows, h : h + 1] = total


def backward_step(slots, step, ins, outs, scratch, gathered):
    qp_ref, kp_ref, q_ref, k_ref, v_ref, w_ref, o_ref, l_ref = ins
    dq_ref, dk_ref, dv_ref = outs
    dk_acc, dv_acc, do_ref, g_ref, sem = scratch
    if step == 0:
        copy = pltpu.make_async_copy(gathered[0], g_ref, sem)
        copy.start()
        copy.wait()
        each = g_ref.shape[1]
        for j in range(g_ref.shape[0]):
            do_ref[j * each : (j + 1) * each, :] = dot_t(g_ref[j], w_ref[...])
    size = query_rows(q_ref.shape[0])
    blocks = q_ref.shape[0] // size
    groups = head_groups(slots)
    block, group = divmod(step, len(groups))
    rows = slice(block * size, (block + 1) * size)
    allowed = kp_ref[...] <= qp_ref[rows, :]
    for h in groups[group]:
        cols = slice(h * HEAD_DIM, (h + 1) * HEAD_DIM)
        q, k, v, do = q_ref[rows, cols], k_ref[:, cols], v_ref[:, cols], do_ref[rows, cols]
        total = l_ref[rows, h : h + 1]
        w = (do / total).astype(BF16)
        corr = jnp.sum(do * o_ref[rows, cols], axis=1, keepdims=True) / total
        e = jnp.where(allowed, jnp.exp(dot_t(q, k) * SCALE), 0.0)
        de = dot_t(w, v)
        ds = (e * (de - corr)).astype(BF16)
        dq_ref[rows, cols] = (dot(ds, k) * SCALE).astype(BF16)
        dk, dv = t_dot(ds, q), t_dot(e.astype(BF16), w)
        if block:
            dk, dv = dk + dk_acc[:, cols], dv + dv_acc[:, cols]
        if block < blocks - 1:
            dk_acc[:, cols] = dk
            dv_acc[:, cols] = dv
        else:
            dk_ref[:, cols] = (dk * SCALE).astype(BF16)
            dv_ref[:, cols] = dv.astype(BF16)


def forward_work(place, q, k, v, slots):
    rows, wide = q.shape
    shape = jax.ShapeDtypeStruct
    outs = (shape((rows, wide), BF16), shape((rows, wide), F32), shape((rows, slots), F32))
    steps = rows // query_rows(rows) * len(head_groups(slots))
    ins = (place.reshape(rows, 1), place.reshape(1, rows), q, k, v)
    return steps, functools.partial(forward_step, slots), False, ins, outs, ()


def backward_work(place, q, k, v, weight, o, total, slots, g):
    rows, wide = q.shape
    outs = (jax.ShapeDtypeStruct((rows, wide), BF16),) * 3
    steps = rows // query_rows(rows) * len(head_groups(slots))
    ins = (place.reshape(rows, 1), place.reshape(1, rows), q, k, v, weight, o, total)
    scratch = (pltpu.VMEM((rows, wide), F32),) * 3
    scratch += (pltpu.VMEM((rows // g.shape[0], *g.shape), g.dtype), pltpu.SemaphoreType.DMA)
    return steps, functools.partial(backward_step, slots), True, ins, outs, scratch


def stack_body(*refs):
    out = refs[-1]
    out[...] = jnp.zeros_like(out)
    for i, ref in enumerate(refs[:-1]):
        out[i : i + 1, : ref.shape[0]] = ref[...].reshape(1, ref.shape[0])


def stack_rows(vectors, longest):
    return pl.pallas_call(
        stack_body,
        in_specs=[pl.BlockSpec(memory_space=pltpu.VMEM)] * len(vectors),
        out_specs=pl.BlockSpec(memory_space=pltpu.VMEM),
        out_shape=jax.ShapeDtypeStruct((16, longest), vectors[0].dtype),
        name="stack_rows",
    )(*vectors)


def split_axis(n):
    across = 2 if n <= 8 else 4
    return n // across, across


def place_of(me, lines, across):
    a, b = lax.div(me, across), lax.rem(me, across)
    near = [(a < lines - 1, me + across), (a > 0, me - across), (b < across - 1, me + 1), (b > 0, me - 1)]
    return a, b, near


def turned_rows(rows, dtype, across, many=False):
    tile = 16 if dtype == BF16 else 8
    share = 4 if rows <= 128 and not many else 5
    return rows // share // tile * tile if across == 2 else 0


def meet(near, peers):
    barrier = pltpu.get_barrier_semaphore()
    for exists, target in near:

        @pl.when(exists)
        def _(target=target):
            pl.semaphore_signal(barrier, inc=1, device_id={"ctx": target}, device_id_type=MESH)

    for axis, peer in peers:
        pl.semaphore_signal(barrier, inc=1, device_id={axis: peer}, device_id_type=MESH)
    pl.semaphore_wait(barrier, len(peers) + sum(exists.astype(jnp.int32) for exists, _ in near))


class Fsdp:
    def __init__(self, nf, gather_in, gather_out, red_in, red_out, scratch):
        self.gather_in, self.gather_out, self.red_in, self.red_out = gather_in, gather_out, red_in, red_out
        n_gather, n_red = len(gather_in), len(red_in)
        self.near_in, self.stage, self.far_in = scratch[:n_red], scratch[n_red : 2 * n_red], scratch[2 * n_red : 3 * n_red]
        self.keep_sem, self.g_send, self.g_recv, self.r_send, self.r_recv = scratch[3 * n_red : 3 * n_red + 5]
        self.f = lax.axis_index("fsdp")
        self.core = lax.rem(self.f, 2)
        self.mate = self.f + 1 - 2 * self.core
        self.pairs = nf // 2
        self.pair = lax.div(self.f, 2)
        self.other = [lax.rem(self.pair + k, self.pairs) for k in range(1, self.pairs)]
        self.peers = [self.mate] + [2 * y + self.core for y in self.other] if n_gather + n_red else []

    @staticmethod
    def scratch(nf, gather, red):
        pairs = nf // 2
        dma = pltpu.SemaphoreType.DMA
        out = []
        for _ in range(3):
            out += [pltpu.VMEM((pairs, *x.shape[1:]), x.dtype) for x in red]
        g, r = max(len(gather), 1), max(len(red), 1)
        return out + [dma((g,)), dma((g, 2, nf)), dma((g, nf)), dma((r, 2, pairs)), dma((r, 2, pairs))]

    def copy(self, src, dst, send, recv, target):
        return pltpu.make_async_remote_copy(
            src_ref=src, dst_ref=dst, send_sem=send, recv_sem=recv, device_id={"fsdp": target}, device_id_type=MESH
        )

    def spread(self, i, source, target, own):
        out = self.gather_out[i].at[source]
        send = self.g_send.at[i, 0, target] if own else self.g_send.at[i, 1, source]
        return self.copy(self.gather_in[i] if own else out, out, send, self.g_recv.at[i, source], target)

    def keep(self, i):
        return pltpu.make_async_copy(self.gather_in[i], self.gather_out[i].at[self.f], self.keep_sem.at[i])

    def to_mate(self, j, y):
        src = self.red_in[j].at[2 * y + 1 - self.core]
        return self.copy(src, self.near_in[j].at[y], self.r_send.at[j, 0, y], self.r_recv.at[j, 0, y], self.mate)

    def to_far(self, j, y, source):
        send, recv = self.r_send.at[j, 1, y], self.r_recv.at[j, 1, source]
        return self.copy(self.stage[j].at[y], self.far_in[j].at[source], send, recv, 2 * y + self.core)

    def start(self):
        for j in range(len(self.red_in)):
            for y in range(self.pairs):
                self.to_mate(j, y).start()
        for i in range(len(self.gather_in)):
            for target in self.peers[1:] + self.peers[:1]:
                self.spread(i, self.f, target, True).start()
            self.keep(i).start()

    def middle(self):
        for j in range(len(self.red_in)):
            for y in range(self.pairs):
                self.to_mate(j, y).wait_recv()
            for y in self.other:
                value = self.red_in[j][2 * y + self.core].astype(F32) + self.near_in[j][y].astype(F32)
                self.stage[j][y] = value.astype(self.stage[j].dtype)
                self.to_far(j, y, self.pair).start()

    def end(self, first, last):
        for j in range(first, last):
            value = self.red_in[j][self.f].astype(F32) + self.near_in[j][self.pair].astype(F32)
            for y in self.other:
                self.to_far(j, y, y).wait_recv()
                value = value + self.far_in[j][y].astype(F32)
            self.red_out[j][...] = value.astype(self.red_out[j].dtype)

    def forward(self):
        for i in range(len(self.gather_in)):
            for y in self.other:
                source = 2 * y + self.core
                self.spread(i, source, self.mate, False).wait_recv()
                self.spread(i, source, self.mate, False).start()

    def finish(self):
        for i in range(len(self.gather_in)):
            self.spread(i, self.mate, self.mate, False).wait_recv()
            for y in self.other:
                self.spread(i, 2 * y + 1 - self.core, self.mate, False).wait_recv()
            self.keep(i).wait()
            for target in self.peers:
                self.spread(i, self.f, target, True).wait_send()
            for y in self.other:
                self.spread(i, 2 * y + self.core, self.mate, False).wait_send()
        for j in range(len(self.red_in)):
            for y in range(self.pairs):
                self.to_mate(j, y).wait_send()
            for y in self.other:
                self.to_far(j, y, self.pair).wait_send()


def exchange_body(n, nf, counts, moves, work, *refs):
    n_ctx, n_fsdp, n_own, n_red, n_work_in, n_work_out, n_work_scratch = counts
    bounds = [0]
    for size in counts[:5]:
        bounds.append(bounds[-1] + size)
    ctx_in, fsdp_in, own_in, red_in, work_in = (refs[i:j] for i, j in zip(bounds, bounds[1:]))
    refs = refs[bounds[-1] :]
    ctx_out, fsdp_out, own_out = refs[:n_ctx], refs[n_ctx : n_ctx + n_fsdp], refs[n_ctx + n_fsdp : n_ctx + n_fsdp + n_own]
    refs = refs[n_ctx + n_fsdp + n_own :]
    red_out, refs = refs[:n_red], refs[n_red:]
    if moves:
        placed, refs = refs[0], refs[1:]
    work_out, refs = refs[:n_work_out], refs[n_work_out:]
    work_scratch, refs = refs[:n_work_scratch], refs[n_work_scratch:]
    sums, scratch = refs[:n_red], refs[n_red:]
    copy_sem, send_sem, recv_sem, place_send, place_recv = scratch[:5]
    fs = Fsdp(nf, fsdp_in, fsdp_out, red_in + own_in, sums + own_out, scratch[5:])

    lines, across = split_axis(n)
    me = lax.axis_index("ctx")
    a, b, near = place_of(me, lines, across)
    pieces = [(src, out, first, rows) for src, out in zip(ctx_in, ctx_out) for first, rows in cut(out.shape[1])]
    late = len(pieces)
    second = late
    for src, out in zip(sums, red_out):
        second = len(pieces)
        pieces += [(src, out, first, rows) for first, rows in cut(out.shape[1])]
    peers = [lax.rem(fs.f + k, nf) for k in range(1, nf)] if moves else fs.peers
    meet(near if pieces else [], [("fsdp", peer) for peer in peers])

    def turned_part(i):
        return turned_rows(pieces[i][3], pieces[i][1].dtype, across, len(pieces) > 1)

    def hop(i, block, way, turned=False, own=False):
        source, out, first, size = pieces[i]
        last = turned_part(i)
        rows = pl.ds(first + size - last, last) if turned else pl.ds(first, size - last)
        return pltpu.make_async_remote_copy(
            src_ref=source.at[rows] if own else out.at[block, rows],
            dst_ref=out.at[block, rows],
            send_sem=send_sem.at[i, way, block, int(turned)],
            recv_sem=recv_sem.at[i, way, block, int(turned)],
            device_id={"ctx": me + (across, -across, 1, -1)[way]},
            device_id_type=MESH,
        )

    def keep(i):
        source, out, first, size = pieces[i]
        rows = pl.ds(first, size)
        return pltpu.make_async_copy(source.at[rows], out.at[me, rows], copy_sem.at[i])

    def each_own(i, act):
        for turned in (True, False) if turned_part(i) else (False,):
            for way in (2, 3, 0, 1):
                pl.when(near[way][0])(lambda way=way: act(hop(i, me, way, turned, True)))

    def each_twin(i, wait, act):
        if turned_part(i):
            twin = me + 1 - 2 * b
            for way in (2, 3):

                @pl.when(near[5 - way][0])
                def _(way=way):
                    if wait:
                        hop(i, twin, way, True).wait_recv()
                    for on in (0, 1):
                        pl.when(near[on][0])(lambda on=on: act(hop(i, twin, on, True)))

    def each_relay(i, d, wait, act):
        for way, there, shift in ((0, a >= d, -d * across), (1, a + d < lines, d * across)):

            @pl.when(there)
            def _(way=way, shift=shift):
                for turned, block in [(False, me + shift)] + (
                    [(True, me + shift), (True, me + 1 - 2 * b + shift)] if turned_part(i) else []
                ):
                    if wait:
                        hop(i, block, way, turned).wait_recv()
                    for on in (way,) if turned else (2, 3, way):
                        pl.when(near[on][0])(lambda on=on: act(hop(i, block, on, turned)))

    def start(copy):
        copy.start()

    def wait_send(copy):
        copy.wait_send()

    def begin(these):
        for i in these:
            each_own(i, start)
            keep(i).start()

    def crossed(i):
        for d in range(1, across):
            for step in range(lines):
                for sign in (1, -1) if step else (1,):
                    for way, there, shift in ((2, b >= d, -d), (3, b + d < across, d)):
                        other = a + sign * step

                        @pl.when(there & (other >= 0) & (other < lines))
                        def _(source=other * across + b + shift, way=way):
                            hop(i, source, way).wait_recv()
                            if d < across - 1:
                                pl.when(near[way][0])(lambda: hop(i, source, way).start())

    def place(k, act_local, act_send):
        block, row, src, dst, goal, size = moves[k]
        source, goal = red_out[0].at[block, pl.ds(row, size)], placed.at[pl.ds(goal, size)]
        if src == dst:
            pl.when(fs.f == src)(lambda: act_local(pltpu.make_async_copy(source, goal, place_send.at[k])))
            return
        remote = pltpu.make_async_remote_copy(
            src_ref=source,
            dst_ref=goal,
            send_sem=place_send.at[k],
            recv_sem=place_recv.at[k],
            device_id={"fsdp": jnp.int32(dst)},
            device_id_type=MESH,
        )
        pl.when(fs.f == src)(lambda: act_send(remote))
        if act_local is wait_copy:
            pl.when(fs.f == dst)(remote.wait_recv)

    def wait_copy(copy):
        copy.wait()

    work_steps, work_fn, gated = work
    plan = []

    def add(act, *args, then_work=True):
        plan.append((functools.partial(act, *args), then_work))

    def hops(i, d):
        if d == 1:
            each_twin(i, True, start)
        each_relay(i, d, True, start)

    def complete(i):
        crossed(i)
        keep(i).wait()

    begin(range(late))
    fs.start()
    fs.middle()
    if not gated:
        add(lambda: None)
    before, after = range(second), range(second, len(pieces))
    ready = []
    if gated:
        for d in range(1, lines):
            for i in range(late):
                add(hops, i, d, then_work=False)
            if d == 2:
                add(fs.end, 0, n_red, then_work=False)
                add(begin, range(late, len(pieces)), then_work=False)
        ready = range(late)
        for i in ready:
            add(complete, i, then_work=i == late - 1)
        add(fs.end, n_red, n_red + n_own)
        for d in range(1, lines):
            for i in range(late, len(pieces)):
                add(hops, i, d)
    elif n_red:
        add(fs.end, 0, n_red - 1)
        add(begin, range(late, second))
        for i in before:
            add(hops, i, 1)
        add(fs.end, n_red - 1, n_red)
        add(begin, after)
        for d in range(2, lines):
            for i in before:
                add(hops, i, d)
            for i in after if d == 2 else ():
                add(hops, i, 1)
        if moves:
            ready = [i for i in before if pieces[i][1] is red_out[0]]
            for i in ready:
                add(complete, i)
            for k in range(len(moves)):
                add(place, k, start, start)
        for d in range(2, lines):
            for i in after:
                add(hops, i, d)
    else:
        for d in range(1, lines):
            for i in range(len(pieces)):
                add(hops, i, d)
            if d == lines - 2:
                add(fs.forward, then_work=False)
        add(fs.end, 0, n_own)
    points = sum(then_work for _, then_work in plan)
    at = 0
    for act, then_work in plan:
        act()
        if then_work:
            for step in range(at * work_steps // points, (at + 1) * work_steps // points):
                work_fn(step, work_in, work_out, work_scratch, ctx_out)
            at += 1

    for i in range(len(pieces)):
        if i not in ready:
            complete(i)
    for k in range(len(moves)):
        place(k, wait_copy, wait_send)

    for i in range(len(pieces)):
        each_own(i, wait_send)
        each_twin(i, False, wait_send)
        for d in range(1, lines):
            each_relay(i, d, False, wait_send)
        for d in range(1, across - 1):
            for line in range(lines):
                for way, there, shift in ((2, b >= d, -d), (3, b + d < across, d)):

                    @pl.when(there & near[way][0])
                    def _(i=i, source=line * across + b + shift, way=way):
                        hop(i, source, way).wait_send()

    fs.finish()


def cut(rows):
    if rows < 200:
        return [(0, rows)]
    half = rows // 32 * 16
    return [(0, rows - half), (rows - half, half)]


def exchange(call, n, nf, ctx=(), fsdp=(), own=(), red=(), moves=(), kept=0, work=None):
    shape = jax.ShapeDtypeStruct
    sums = [shape(x.shape[1:], x.dtype) for x in red]
    outs = [shape((n, *x.shape), x.dtype) for x in ctx]
    outs += [shape((nf, *x.shape), x.dtype) for x in fsdp]
    outs += [shape(x.shape[1:], x.dtype) for x in own]
    outs += [shape((n, *x.shape), x.dtype) for x in sums]
    outs += [shape((kept, sums[0].shape[1]), sums[0].dtype)] if moves else []
    steps, work_fn, gated, work_in, work_out, work_scratch = work or (0, None, False, (), (), ())
    gathered = max(sum(len(cut(x.shape[0])) for x in [*ctx, *sums]), 1)
    any_spec, vmem_spec = pl.BlockSpec(memory_space=pl.ANY), pl.BlockSpec(memory_space=pltpu.VMEM)
    inputs = (*ctx, *fsdp, *own, *red, *work_in)
    counts = [len(x) for x in (ctx, fsdp, own, red, work_in, work_out, work_scratch)]
    dma = pltpu.SemaphoreType.DMA
    return pl.pallas_call(
        functools.partial(exchange_body, n, nf, tuple(counts), tuple(moves), (steps, work_fn, gated)),
        in_specs=[any_spec] * (len(ctx) + len(fsdp)) + [vmem_spec] * (len(inputs) - len(ctx) - len(fsdp)),
        out_specs=[any_spec] * (len(ctx) + len(fsdp))
        + [vmem_spec] * len(own)
        + [any_spec] * (len(sums) + (1 if moves else 0))
        + [vmem_spec] * len(work_out),
        out_shape=[*outs, *work_out],
        scratch_shapes=list(work_scratch)
        + [pltpu.VMEM(x.shape, x.dtype) for x in sums]
        + [dma((gathered,)), dma((gathered, 4, n, 2)), dma((gathered, 4, n, 2))]
        + [dma((max(len(moves), 1),))] * 2
        + Fsdp.scratch(nf, fsdp, [*red, *own]),
        name=f"exchange_{call}",
        compiler_params=pltpu.CompilerParams(collective_id=call, has_side_effects=True, vmem_limit_bytes=60 * 2**20),
    )(*inputs)


class Scatter:
    def __init__(self, n, many, transposed, left, right, out, scratch):
        self.left, self.right, self.out, self.transposed = left, right, out, transposed
        self.part, self.acc, self.acc_t, self.over_in, self.sums, self.sums_t = scratch[:6]
        self.line_in, self.line_in_t, self.twin_in = scratch[6:9]
        self.o_send, self.o_recv, self.l_send, self.l_recv, self.t_send, self.t_recv = scratch[9:15]
        self.w_send, self.w_recv = scratch[15:17]
        self.lines, self.across = split_axis(n)
        self.me = lax.axis_index("ctx")
        self.a, self.b, self.near = place_of(self.me, self.lines, self.across)
        self.rows = out.shape[0]
        self.last = turned_rows(self.rows, BF16, self.across, many)
        self.head, self.tail = pl.ds(0, self.rows - self.last), pl.ds(self.rows - self.last, self.last)
        self.peers = [self.me - self.b + lax.rem(self.b + k, self.across) for k in range(1, self.across)]

    @staticmethod
    def scratch(n, many, rows, width):
        lines, across = split_axis(n)
        last = turned_rows(rows, BF16, across, many)
        some = max(last, 16)
        vmem, dma = pltpu.VMEM, pltpu.SemaphoreType.DMA
        return [
            vmem((lines, across, rows, width), BF16),
            vmem((rows - last, width), F32),
            vmem((across, some, width), F32),
            vmem((across - 1, lines, rows - last, width), BF16),
            vmem((lines, rows - last, width), BF16),
            vmem((lines, across, some, width), BF16),
            vmem((2, lines, rows - last, width), BF16),
            vmem((2, lines, across, some, width), BF16),
            vmem((some, width), BF16),
            dma((across - 1, lines)),
            dma((across - 1, lines)),
            dma((2, lines)),
            dma((2, lines)),
            dma((2, lines)),
            dma((2, lines)),
            dma,
            dma,
        ]

    def copy(self, src, dst, send, recv, target):
        return pltpu.make_async_remote_copy(
            src_ref=src, dst_ref=dst, send_sem=send, recv_sem=recv, device_id={"ctx": target}, device_id_type=MESH
        )

    def over(self, line, k):
        src = self.part.at[line, lax.rem(self.b + k, self.across), self.head]
        send, recv = self.o_send.at[k - 1, line], self.o_recv.at[k - 1, line]
        return self.copy(src, self.over_in.at[k - 1, line], send, recv, self.peers[k - 1])

    def along(self, line, way):
        target = self.me + (self.across, -self.across)[way]
        send, recv = self.l_send.at[way, line], self.l_recv.at[way, line]
        return self.copy(self.sums.at[line], self.line_in.at[way, line], send, recv, target)

    def along_t(self, line, way):
        target = self.me + (self.across, -self.across)[way]
        send, recv = self.t_send.at[way, line], self.t_recv.at[way, line]
        return self.copy(self.sums_t.at[line], self.line_in_t.at[way, line], send, recv, target)

    def twin(self):
        return self.copy(self.sums_t.at[self.a, 1 - self.b], self.twin_in, self.w_send, self.w_recv, self.peers[0])

    def compute(self, line):
        size = self.across * self.rows
        lhs = self.left[pl.ds(pl.multiple_of(line * size, size), size), :]
        value = dot_t(lhs, self.right[...]) if self.transposed else dot(lhs, self.right[...])
        self.part[line] = value.astype(BF16).reshape(self.across, self.rows, value.shape[1])
        for k in range(1, self.across):
            self.over(line, k).start()

    def collect(self, line, acc, landed, hop, ways):
        for way, there in ways:

            @pl.when(there)
            def _(way=way):
                hop(line, way).wait_recv()
                acc[...] += landed[way, line].astype(F32)

    def across_sum(self, line):
        value = self.part[line, self.b, self.head].astype(F32)
        for k in range(1, self.across):
            self.over(line, k).wait_recv()
            value = value + self.over_in[k - 1, line].astype(F32)
        self.acc[...] = value

    def pass_on(self, line):
        up, down = line > self.a, line < self.a
        ways = ((0, up & (self.a > 0)), (1, down & (self.a < self.lines - 1)))
        if self.last:
            self.acc_t[...] = self.part[line, :, self.tail].astype(F32)
            self.collect(line, self.acc_t, self.line_in_t, self.along_t, ways)
            self.sums_t[line] = self.acc_t[...].astype(BF16)
            pl.when(up)(lambda: self.along_t(line, 0).start())
            pl.when(down)(lambda: self.along_t(line, 1).start())
        self.across_sum(line)
        self.collect(line, self.acc, self.line_in, self.along, ways)
        self.sums[line] = self.acc[...].astype(BF16)
        pl.when(up)(lambda: self.along(line, 0).start())
        pl.when(down)(lambda: self.along(line, 1).start())

    def own(self):
        ways = ((0, self.near[1][0]), (1, self.near[0][0]))
        if self.last:
            self.acc_t[...] = self.part[self.a, :, self.tail].astype(F32)
            self.collect(self.a, self.acc_t, self.line_in_t, self.along_t, ways)
            self.sums_t[self.a] = self.acc_t[...].astype(BF16)
            self.twin().start()
        self.across_sum(self.a)
        self.collect(self.a, self.acc, self.line_in, self.along, ways)
        self.out[self.head, :] = self.acc[...]
        if self.last:
            self.twin().wait_recv()
            self.out[self.tail, :] = self.acc_t[self.b] + self.twin_in[...].astype(F32)

    def sent(self, order):
        for line in order:
            for k in range(1, self.across):
                self.over(line, k).wait_send()
        for line in order[:-1]:
            for way, there in ((0, line > self.a), (1, line < self.a)):

                @pl.when(there)
                def _(way=way, line=line):
                    self.along(line, way).wait_send()
                    if self.last:
                        self.along_t(line, way).wait_send()

        if self.last:
            self.twin().wait_send()


def product_body(n, nf, counts, transposed, *refs):
    n_prod, n_sides, n_fsdp = counts
    pairs, refs = refs[: 2 * n_prod], refs[2 * n_prod :]
    side_in, refs = refs[: 2 * n_sides], refs[2 * n_sides :]
    fsdp_in, refs = refs[:n_fsdp], refs[n_fsdp:]
    outs, side_out, fsdp_out = refs[:n_prod], refs[n_prod : n_prod + n_sides], refs[n_prod + n_sides : n_prod + n_sides + n_fsdp]
    scratch = refs[n_prod + n_sides + n_fsdp :]
    side_at, side_sem, scratch = scratch[: 2 * n_sides], scratch[2 * n_sides], scratch[2 * n_sides + 1 :]
    fetches = [pltpu.make_async_copy(side_in[j], side_at[j], side_sem.at[j]) for j in range(2 * n_sides)]
    each = 17
    jobs = [
        Scatter(n, n_prod > 1, transposed[p], pairs[2 * p], pairs[2 * p + 1], outs[p], scratch[each * p : each * (p + 1)])
        for p in range(n_prod)
    ]
    fs = Fsdp(nf, fsdp_in, fsdp_out, [], [], scratch[each * n_prod :])
    a, lines = jobs[0].a, jobs[0].lines
    meet(jobs[0].near[:2], [("ctx", peer) for peer in jobs[0].peers] + [("fsdp", peer) for peer in fs.peers])

    order = []
    for k in range(lines):
        line = jnp.int32(0)
        for av in range(lines):
            line = jnp.where(a == av, sorted(range(lines), key=lambda j: (-abs(j - av), j))[k], line)
        order.append(line)

    for fetch in fetches:
        fetch.start()
    for job in jobs:
        for line in order:
            job.compute(line)
    fs.start()
    steps = [(job, line) for job in jobs for line in order[:-1]]
    bits = []
    for j in range(n_sides):
        size = side_in[2 * j].shape[1]
        width = -(-size // 3 // 128) * 128
        bits += [(j, first, min(width, size - first)) for first in range(0, size, width)]
    for step, (job, line) in enumerate(steps):
        job.pass_on(line)
        for j, first, size in bits[step * len(bits) // len(steps) : (step + 1) * len(bits) // len(steps)]:
            if first == 0:
                fetches[2 * j].wait()
                fetches[2 * j + 1].wait()
            part = side_at[2 * j][:, first : first + size]
            side_out[j][first : first + size, :] = t_dot(part, side_at[2 * j + 1][...]).astype(BF16)
        if step == len(order) - 3:
            fs.forward()
    for job in jobs:
        job.own()
    for job in jobs:
        job.sent(order)
    fs.finish()


def product(call, n, nf, products, sides=(), fsdp=()):
    length = products[0][0].shape[0]
    if length > 1024 and (sides or len(products) > 1):
        sums = []
        for i, one in enumerate(products):
            total, *gathered = product(call if i == 0 else call + 10, n, nf, [one], fsdp=fsdp if i == 0 else ())
            sums.append(total)
            fsdp_out = gathered if i == 0 else fsdp_out
        return [*sums, *[t_dot(x, y).astype(BF16) for x, y in sides], *fsdp_out]
    rows = length // n
    shape = jax.ShapeDtypeStruct
    widths = [right.shape[0 if turned else 1] for _, right, turned in products]
    outs = [shape((rows, width), F32) for width in widths]
    outs += [shape((x.shape[1], y.shape[1]), BF16) for x, y in sides]
    outs += [shape((nf, *x.shape), x.dtype) for x in fsdp]
    inputs = [z for left, right, _ in products for z in (left, right)] + [z for side in sides for z in side]
    vmem_spec, any_spec = pl.BlockSpec(memory_space=pltpu.VMEM), pl.BlockSpec(memory_space=pl.ANY)
    return pl.pallas_call(
        functools.partial(
            product_body,
            n,
            nf,
            (len(products), len(sides), len(fsdp)),
            tuple(turned for _, _, turned in products),
        ),
        in_specs=[vmem_spec] * (2 * len(products)) + [any_spec] * (2 * len(sides) + len(fsdp)),
        out_specs=[vmem_spec] * (len(outs) - len(fsdp)) + [any_spec] * len(fsdp),
        out_shape=outs,
        scratch_shapes=[pltpu.VMEM(z.shape, z.dtype) for side in sides for z in side]
        + [pltpu.SemaphoreType.DMA((max(2 * len(sides), 1),))]
        + [s for width in widths for s in Scatter.scratch(n, len(widths) > 1, rows, width)] + Fsdp.scratch(nf, fsdp, ()),
        name=f"product_{call}",
        compiler_params=pltpu.CompilerParams(collective_id=call, has_side_effects=True, vmem_limit_bytes=63 * 2**20),
    )(*inputs, *fsdp)


def row_moves(n, nf, heads):
    part, local = -(-heads // n) * HEAD_DIM // nf, heads * HEAD_DIM // nf
    moves = []
    for block, start, goal, size in head_moves(n, heads, 0, 0):
        done = 0
        while done < size:
            here, there = start + done, goal + done
            rows = min(size - done, part - here % part, local - there % local)
            moves.append((block, here % part, here // part, there // local, there % local, rows))
            done += rows
    return moves


def layout_body(moves, *refs):
    ins, outs = refs[: len(refs) // 2], refs[len(refs) // 2 :]
    for in_ref, out_ref, per_out in zip(ins, outs, moves):
        if per_out is None:
            out_ref[...] = in_ref[...].astype(F32)
            continue
        for block, start, goal, size in per_out:
            out_ref[:, goal : goal + size] = in_ref[block, :, start : start + size].astype(F32)


def lay_out(arrays, widths, moves):
    rows = next(x.shape[1] for x in arrays if x.ndim == 3)
    step = next(s for s in (80, 16, rows) if rows % s == 0)
    grid = rows // step
    in_specs, out_specs, outs = [], [], []
    for x, width in zip(arrays, widths):
        flat = pl.BlockSpec((x.shape[-2] // grid, width), lambda i: (i, 0))
        in_specs.append(pl.BlockSpec((x.shape[0], step, x.shape[2]), lambda i: (0, i, 0)) if x.ndim == 3 else flat)
        out_specs.append(flat)
        outs.append(jax.ShapeDtypeStruct((x.shape[-2], width), F32))
    return pl.pallas_call(
        functools.partial(layout_body, tuple(m and tuple(m) for m in moves)),
        grid=(grid,),
        in_specs=in_specs,
        out_specs=out_specs,
        out_shape=outs,
        name="lay_out",
        cost_estimate=pl.CostEstimate(
            flops=0, bytes_accessed=6 * sum(x.shape[0] * x.shape[1] for x in outs), transcendentals=0
        ),
        compiler_params=pltpu.CompilerParams(vmem_limit_bytes=60 * 2**20),
    )(*arrays)


def head_moves(n, heads, offset, goal):
    base, rest = divmod(heads, n)
    moves = [(c, offset, goal + c * base * HEAD_DIM, base * HEAD_DIM) for c in range(n) if base]
    moves += [
        (c, offset + base * HEAD_DIM, goal + (base * n + c) * HEAD_DIM, HEAD_DIM) for c in range(rest)
    ]
    return moves


def head_columns(value, width, c, n):
    heads = width // HEAD_DIM
    base, rest = divmod(heads, n)
    parts = []
    if base:
        parts.append(lax.dynamic_slice_in_dim(value, c * base * HEAD_DIM, base * HEAD_DIM, axis=-1))
    if rest:
        start = jnp.minimum(base * n + c, heads - 1) * HEAD_DIM
        extra = lax.dynamic_slice_in_dim(value, start, HEAD_DIM, axis=-1)
        parts.append(jnp.where(c < rest, extra, jnp.zeros_like(extra)))
    return jnp.concatenate(parts, axis=-1)


def place_heads(value, heads, c, n):
    base, rest = divmod(heads, n)
    out = jnp.zeros((heads * HEAD_DIM,), value.dtype)
    if rest:
        start = jnp.minimum(base * n + c, heads - 1) * HEAD_DIM
        extra = jnp.where(c < rest, value[base * HEAD_DIM :], 0.0)
        out = lax.dynamic_update_slice(out, extra, (start,))
    if base:
        out = lax.dynamic_update_slice(out, value[: base * HEAD_DIM], (c * base * HEAD_DIM,))
    return out


def head_rows(value, heads, c, f, n):
    base, rest = divmod(heads, n)
    local, width = value.shape
    pad = max(base, 1) * HEAD_DIM
    padded = jnp.pad(value, ((pad, pad), (0, 0)))
    parts = []
    if base:
        start = jnp.clip(c * base * HEAD_DIM - f * local + pad, 0, local + 2 * pad - base * HEAD_DIM)
        parts.append(lax.dynamic_slice_in_dim(padded, start, base * HEAD_DIM, axis=0))
    if rest:
        start = jnp.clip((base * n + c) * HEAD_DIM - f * local + pad, 0, local + 2 * pad - HEAD_DIM)
        extra = lax.dynamic_slice_in_dim(padded, start, HEAD_DIM, axis=0)
        parts.append(jnp.where(c < rest, extra, jnp.zeros_like(extra)))
    return jnp.concatenate(parts, axis=0)


def on_device(
    tokens,
    ln1_gain,
    ln1_shift,
    qkv_weight,
    qv_bias,
    out_weight,
    out_bias,
    ln2_gain,
    ln2_shift,
    up_weight,
    up_bias,
    down_weight,
    down_bias,
    block_table,
    cotangent,
):
    rows, width = tokens.shape[1:]
    heads = width // HEAD_DIM
    n = lax.axis_size("ctx")
    nf = lax.axis_size("fsdp")
    c = lax.axis_index("ctx")
    f = lax.axis_index("fsdp")
    slots = -(-heads // n)
    wide = slots * HEAD_DIM
    half = rows // 2
    local = width // nf
    ff = up_weight.shape[1]
    ff_local = ff // nf
    ff_part = ff_local // n

    within = jnp.arange(rows, dtype=jnp.int32)
    block_of = jnp.where(within[None, :] < half, block_table[:, None], 2 * n - 1 - block_table[:, None])
    place = (block_of * half + within[None, :] % half).reshape(-1)

    vectors = (ln1_gain, ln1_shift, qv_bias, out_bias, ln2_gain, ln2_shift, up_bias, down_bias)
    longest = max(v.shape[0] for v in vectors)
    flat = stack_rows(vectors, longest)
    q_w = head_columns(qkv_weight[:, :width], width, c, n)
    k_w = head_columns(qkv_weight[:, width : 2 * width], width, c, n)
    v_w = head_columns(qkv_weight[:, 2 * width :], width, c, n)
    w_mine = jnp.concatenate([q_w, k_w, v_w], axis=1)
    x = tokens[0].astype(F32)
    n1, rstd1 = ln_stats(x)
    n1_all, packed, w_qkv = exchange(0, n, nf, ctx=[n1.astype(BF16)], fsdp=[flat, w_mine])
    out_weight, up_weight, down_weight, packed = lax.optimization_barrier(
        (out_weight, up_weight, down_weight, packed)
    )
    n1_all = n1_all.reshape(n * rows, width)
    w_qkv = w_qkv.reshape(width, 3 * wide)
    full = [packed[:, i, : v.shape[0]].reshape(-1).astype(F32) for i, v in enumerate(vectors)]
    gain1, shift1, b_qv, b_out, gain2, shift2, b_up, b_down = full

    b_up_mine = lax.dynamic_slice_in_dim(b_up.reshape(nf, n, ff_part), c, 1, axis=1).reshape(-1)
    bq = head_columns(b_qv[:width], width, c, n)
    bv = head_columns(b_qv[width:], width, c, n)

    act1 = (n1_all.astype(F32) * gain1 + shift1).astype(BF16)
    proj = dot(act1, w_qkv)
    q = (proj[:, :wide] + bq).astype(BF16)
    k = proj[:, wide : 2 * wide].astype(BF16)
    v = (proj[:, 2 * wide :] + bv).astype(BF16)
    g2_all, w_out, attn, o, total = exchange(
        1,
        n,
        nf,
        ctx=[cotangent[0]],
        fsdp=[head_rows(out_weight, heads, c, f, n)],
        work=forward_work(place, q, k, v, slots),
    )
    up_mine = [lax.dynamic_slice_in_dim(up_weight, i * ff_local + c * ff_part, ff_part, axis=1) for i in range(nf)]
    w_out = functools.reduce(jnp.add, [w_out[i] for i in range(nf)])
    mixed, w_up = product(7, n, nf, [(attn, w_out, False)], fsdp=[jnp.concatenate(up_mine, axis=1)])
    w_up = w_up.reshape(width, nf * ff_part)
    mid = x + mixed + b_out

    n2, rstd2 = ln_stats(mid)
    act2, w_down = exchange(
        2,
        n,
        nf,
        ctx=[(n2 * gain2 + shift2).astype(BF16)],
        fsdp=[lax.dynamic_slice_in_dim(down_weight, c * ff_part, ff_part, axis=0)],
    )
    act2 = act2.reshape(n * rows, width)
    g2_all = g2_all.reshape(n * rows, width)
    w_down = w_down.reshape(nf * ff_part, width)
    u = dot(act2, w_up) + b_up_mine
    activated, gelu_back = jax.vjp(lambda t: jax.nn.gelu(t, approximate=True), u)
    hidden = activated.astype(BF16)
    dh = dot_t(g2_all, w_down)
    du = gelu_back(dh)[0].astype(BF16)
    da2, fed, d_up, d_down = product(
        3, n, nf, [(du, w_up, True), (hidden, w_down, False)], sides=[(act2, du), (hidden, g2_all)]
    )
    result = mid + fed + b_down
    d_up = d_up.reshape(nf, local, nf * ff_part)
    d_down = d_down.reshape(nf, ff_part, width)
    d_up_bias = jnp.sum(du.astype(F32), axis=0)
    grad_out = cotangent[0].astype(F32)
    d_down_bias = jnp.sum(grad_out, axis=0)

    d_gain2 = jnp.sum(da2 * n2, axis=0)
    d_shift2 = jnp.sum(da2, axis=0)
    d_mid = grad_out + ln_back(da2, n2, rstd2, gain2)
    g1 = d_mid.astype(BF16)
    d_out_bias = jnp.sum(g1.astype(F32), axis=0)
    g1_all, d_down, d_up, gq, gk, gv = exchange(
        4, n, nf, ctx=[g1], own=[d_down], red=[d_up], work=backward_work(place, q, k, v, w_out, o, total, slots, g1)
    )
    g1_all = g1_all.reshape(n * rows, width)
    g_qkv = jnp.concatenate([gq, gk, gv], axis=1)
    da1, d_qkv, d_out = product(5, n, nf, [(g_qkv, w_qkv, True)], sides=[(act1, g_qkv), (attn, g1_all)])
    d_qkv = d_qkv.reshape(nf, local, 3 * wide)
    d_out = d_out.reshape(nf, wide // nf, width)

    d_gain1 = jnp.sum(da1 * n1, axis=0)
    d_shift1 = jnp.sum(da1, axis=0)
    input_grad = d_mid + ln_back(da1, n1, rstd1, gain1)

    dq_bias = place_heads(jnp.sum(gq.astype(F32), axis=0), heads, c, n)
    dv_bias = place_heads(jnp.sum(gv.astype(F32), axis=0), heads, c, n)
    up_placed = lax.dynamic_update_slice(
        jnp.zeros((nf, n, ff_part), F32), d_up_bias.reshape(nf, 1, ff_part), (0, c, 0)
    )
    smalls = (
        d_gain1,
        d_shift1,
        jnp.concatenate([dq_bias, dv_bias]),
        d_out_bias,
        d_gain2,
        d_shift2,
        up_placed.reshape(-1),
        d_down_bias,
    )
    packed = jnp.concatenate([s.reshape(nf, -1) for s in smalls], axis=1)
    packed = jnp.pad(packed, ((0, 0), (0, -packed.shape[1] % 1024))).reshape(nf, -1, 128)
    d_down, _, packed, d_qkv, d_out = exchange(
        6, n, nf, ctx=[d_down], red=[d_out, packed, d_qkv], moves=row_moves(n, nf, heads), kept=local
    )
    mine = jnp.sum(packed, axis=0).reshape(-1)
    up_moves = [(i, j * ff_part, j * ff_local + i * ff_part, ff_part) for i in range(n) for j in range(nf)]
    qkv_moves = [m for i in range(3) for m in head_moves(n, heads, i * wide, i * width)]
    d_down_full, d_out_full, d_up_full, d_qkv_full = lay_out(
        (d_down.reshape(ff_local, width), d_out, d_up, d_qkv),
        (width, width, ff, 3 * width),
        (None, None, up_moves, qkv_moves),
    )
    out, at = [], 0
    for s in smalls:
        size = s.size // nf
        out.append(mine[at : at + size])
        at += size
    return (
        result[None],
        input_grad[None],
        out[0],
        out[1],
        d_qkv_full,
        out[2],
        d_out_full,
        out[3],
        out[4],
        out[5],
        d_up_full,
        out[6],
        d_down_full,
        out[7],
    )


def solution(mesh):
    rows, one, two = P("fsdp", "ctx", None), P("fsdp"), P("fsdp", None)
    return jax.shard_map(
        on_device,
        mesh=mesh,
        in_specs=(rows, one, one, two, one, two, one, one, one, two, one, two, one, P(), rows),
        out_specs=(rows, rows, one, one, two, one, two, one, one, one, two, one, two, one),
        check_vma=False,
    )
```
